32 devices in a mesh: batch: 8 (over y, x, core), heads: 4 (over z).
Axes of the slice: x: 2, y: 2, z: 4, core: 2. Of those that a mesh axis runs over, the one named last changes fastest.
Arguments:
- tokens: bfloat16 [24576, 768], P('batch'), may hold values from -5 to 5
- qkv_weight: bfloat16 [768, 3, 768], P(None, None, 'heads'), may hold values from -0.21875 to 0.21875
- qv_bias: float32 [2, 768], replicated, may hold values from -3 to 3
- conv_weight: float32 [12, 33], replicated, may hold values from -0.875 to 0.875
- out_weight: bfloat16 [768, 768], P('heads'), may hold values from -0.21875 to 0.21875
- out_bias: float32 [768], replicated, may hold values from -1.75 to 1.75
- norm1_gain: float32 [768], replicated, may hold values from 0.5 to 1.5
- norm1_bias: float32 [768], replicated, may hold values from -1.75 to 1.75
- ffn_in_weight: bfloat16 [768, 3072], P(None, ('batch', 'heads')), may hold values from -0.21875 to 0.21875
- ffn_in_bias: bfloat16 [3072], P(('batch', 'heads')), may hold values from -3 to 3
- ffn_out_weight: bfloat16 [3072, 768], P(('batch', 'heads')), may hold values from -0.109375 to 0.109375
- ffn_out_bias: float32 [768], replicated, may hold values from -1.75 to 1.75
- norm2_gain: float32 [768], replicated, may hold values from 0.5 to 1.5
- norm2_bias: float32 [768], replicated, may hold values from -1.75 to 1.75
- cotangent: bfloat16 [24576, 768], P(('batch', 'heads')), may hold values from -12 to 12
- seq_lengths: int32 [24], P('batch'), may hold values from 0 to 3072, as said below
- segment_ids: int32 [24576], P('batch'), may hold values from 0 to 3, as said below
- landmark_bounds: int32 [24, 64], P('batch'), may hold values from 0 to 3024, as said below
Outputs:
- out: bfloat16 [24576, 768], P(('batch', 'heads'))
- input_grad: float32 [24576, 768], P(('batch', 'heads'))
- qkv_weight_grad: float32 [768, 3, 768], P('batch', None, 'heads')
- qv_bias_grad: float32 [2, 768], P(None, 'heads')
- conv_grad: float32 [12, 33], P('heads')
- out_weight_grad: float32 [768, 768], P('heads', 'batch')
- ffn_in_grad: float32 [768, 3072], P(None, ('batch', 'heads'))
- ffn_in_bias_grad: float32 [3072], P(('batch', 'heads'))
- ffn_out_grad: float32 [3072, 768], P(('batch', 'heads'))
- vector_grads: float32 [6, 768], P(None, ('batch', 'heads'))
- condition: float32 [], replicated
The draws below stay inside these ranges and needn't reach their ends.
Inputs may be any that keep to these rules, and one draw needn't show every extreme that they name: `seq_lengths`: each index of batch holds 3 slots: sequences of 1024 to 3072 tokens first, then empty slots of length 0; the lengths of one index sum to at most 3072; at least one index holds a single sequence of 3072 tokens. `segment_ids`: the live tokens of an index of batch lie in order of slot from its first token slot on, each slot's tokens contiguous; the remaining token slots carry 3. landmark_bounds[s, j] = (j times the length of slot s) // 64.
All inputs are finite; a program needn't handle non-finite values.
Results may differ from the reference program's by a relative error of at most 0.013.
Values may be sent and summed in bfloat16 or wider, within the bound.
A program may use at most 448 MiB of HBM per device.

```python
import math
import jax
import jax.numpy as jnp
from jax import lax

D = 768
H = 12
HEAD_DIM = 64
FF = 3072
LANDMARKS = 64
KERNEL = 33
PINV_ITERS = 6
MINLEN = 1024
MAXLEN = 3072
TOK_DEV = 3072
SEQ_DEV = 3
TOKENS = 24576
N_BATCH = 8


def pack_lengths(key):
    pack_count = TOKENS // TOK_DEV
    base_key = jax.random.fold_in(key, 911)
    key_len, key_whole, key_force = jax.random.split(base_key, 3)
    raw_lengths = jax.random.randint(key_len, (pack_count, SEQ_DEV), MINLEN, MAXLEN // 2 + 1)
    seq_ends = jnp.cumsum(raw_lengths, axis=1)
    lengths = jnp.where(seq_ends <= TOK_DEV, raw_lengths, 0)
    whole_pack = jax.random.randint(key_whole, (pack_count,), 0, 8) == 0
    forced = jax.random.randint(key_force, (), 0, pack_count)
    whole_pack = jnp.logical_or(whole_pack, jnp.arange(pack_count) == forced)
    single = jnp.where(jnp.arange(SEQ_DEV) == 0, MAXLEN, 0)
    lengths = jnp.where(whole_pack[:, None], single[None, :], lengths)
    return lengths.astype(jnp.int32)


def draw_seq_lengths(key, part):
    return pack_lengths(key).reshape(-1)


def draw_segment_ids(key, part):
    lengths = pack_lengths(key)
    seq_ends = jnp.cumsum(lengths, axis=1).astype(jnp.int32)
    places = jnp.arange(TOK_DEV, dtype=jnp.int32)
    slot_ids = jnp.sum((seq_ends[:, None, :] <= places[None, :, None]).astype(jnp.int32), axis=2)
    return slot_ids.reshape(-1).astype(jnp.int32)


def draw_landmark_bounds(key, part):
    lengths = pack_lengths(key)
    marks_at = jnp.arange(LANDMARKS, dtype=jnp.int32)
    bounds = marks_at[None, None, :] * lengths[:, :, None] // LANDMARKS
    return bounds.reshape(-1, LANDMARKS).astype(jnp.int32)


def draw_tokens(key, part):
    key_noise, key_freq, key_phase, key_amp = jax.random.split(jax.random.fold_in(key, 17), 4)
    places = (jnp.arange(TOKENS, dtype=jnp.int32) % TOK_DEV).astype(jnp.float32)[:, None]
    frequency = jnp.exp(jax.random.uniform(key_freq, (D,), minval=math.log(2.0 * math.pi / MAXLEN), maxval=math.log(2.0 * math.pi / 16.0)))
    phase_shift = jax.random.uniform(key_phase, (D,), minval=0.0, maxval=2.0 * math.pi)
    noise_part = 0.8 * jnp.clip(jax.random.normal(key_noise, (TOKENS, D)), -4.0, 4.0)
    amplitude = jax.random.uniform(key_amp, (D,), minval=0.6, maxval=1.2)
    return (noise_part + amplitude[None, :] * jnp.sin(places * frequency[None, :] + phase_shift[None, :])).astype(jnp.bfloat16)


def raised(values, stream_key, source, target, blocks, factor):
    def block_of(axis_at):
        return (jnp.arange(values.shape[axis_at]) // (values.shape[axis_at] // blocks)).reshape((-1,) + (1,) * (values.ndim - 1 - axis_at))

    one_side = jax.random.permutation(stream_key, blocks)[block_of(target)]
    other_side = (block_of(target) + blocks // 2) % blocks
    return jnp.where((block_of(source) == one_side) | (block_of(source) == other_side), factor * values, values)


def level_of(key, shape, cuts, low, largest):
    level, own = 1.0, jax.random.fold_in(key, 6)
    for dim, parts in cuts:
        steps = jnp.exp(jax.random.uniform(jax.random.fold_in(own, dim), (parts,), jnp.float32, low / len(cuts), largest / len(cuts)))
        level = level * jnp.repeat(steps, shape[dim] // parts).reshape([-1 if axis == dim else 1 for axis in range(len(shape))])
    return level


def centred(key, dims, deviation, bound, cuts=(), kind=jnp.bfloat16):
    gain = level_of(key, dims, cuts, -0.22, 0.18) if cuts else 1.0
    entries = jax.random.normal(key, dims, jnp.float32) * deviation * gain
    return jnp.minimum(jnp.maximum(entries, -bound), bound).astype(kind)


def gaussian_with(stream_key, extent, scale, reach, cuts, heavy, held_as=jnp.bfloat16):
    drawn = scale * jax.random.normal(stream_key, extent, jnp.float32)
    if cuts:
        drawn = drawn * level_of(stream_key, extent, cuts, -0.22, 0.18)
    return jnp.clip(raised(drawn, jax.random.fold_in(stream_key, 3), *heavy), -reach, reach).astype(held_as)


def setup_inputs(seed: int = 0) -> dict:
    keys = jax.random.split(jax.random.key(seed), 19)
    tokens = draw_tokens(jax.random.fold_in(keys[18], 71), 0)
    qkv_weight = centred(keys[1], (D, 3, H * HEAD_DIM), D ** -0.5, 0.21875, ((2, 4),))
    qv_bias = centred(keys[2], (2, H * HEAD_DIM), 0.5, 3.0, (), jnp.float32)
    conv_weight = centred(keys[3], (H, KERNEL), 0.15, 0.875, (), jnp.float32)
    out_weight = centred(keys[4], (H * HEAD_DIM, D), (H * HEAD_DIM) ** -0.5, 0.21875, ((0, 4),))
    out_bias = centred(keys[5], (D,), 0.3, 1.75, (), jnp.float32)
    norm1_gain = jnp.clip(1.0 + 0.1 * jax.random.normal(keys[6], (D,), jnp.float32), 0.5, 1.5)
    norm1_bias = centred(keys[7], (D,), 0.3, 1.75, (), jnp.float32)
    ffn_in_weight = centred(keys[8], (D, FF), D ** -0.5, 0.21875, ((1, 32),))
    ffn_in_bias = centred(keys[9], (FF,), 0.5, 3.0, ((0, 32),))
    ffn_out_weight = centred(keys[10], (FF, D), FF ** -0.5, 0.109375, ((0, 32),))
    ffn_out_bias = centred(keys[11], (D,), 0.3, 1.75, (), jnp.float32)
    norm2_gain = jnp.clip(1.0 + 0.1 * jax.random.normal(keys[12], (D,), jnp.float32), 0.5, 1.5)
    norm2_bias = centred(keys[13], (D,), 0.3, 1.75, (), jnp.float32)
    cotangent = gaussian_with(keys[14], (TOKENS, D), 1.0, 12.0, ((0, 32),), (0, 1, 32, 2.75))
    seq_lengths = draw_seq_lengths(jax.random.fold_in(keys[18], 71), 0)
    segment_ids = draw_segment_ids(jax.random.fold_in(keys[18], 71), 0)
    landmark_bounds = draw_landmark_bounds(jax.random.fold_in(keys[18], 71), 0)
    return dict(tokens=tokens, qkv_weight=qkv_weight, qv_bias=qv_bias, conv_weight=conv_weight, out_weight=out_weight, out_bias=out_bias, norm1_gain=norm1_gain, norm1_bias=norm1_bias, ffn_in_weight=ffn_in_weight, ffn_in_bias=ffn_in_bias, ffn_out_weight=ffn_out_weight, ffn_out_bias=ffn_out_bias, norm2_gain=norm2_gain, norm2_bias=norm2_bias, cotangent=cotangent, seq_lengths=seq_lengths, segment_ids=segment_ids, landmark_bounds=landmark_bounds)


best_precision = lax.Precision.HIGHEST
mask_fill = -1000000000.0
norm_eps = 1e-05

@jax.custom_vjp
def low(v):
    return lax.optimization_barrier(v.astype(jnp.bfloat16)).astype(jnp.float32)

@jax.custom_vjp
def low_back(v):
    return v

def low_keep(v):
    return (low(v), None)

def low_pass(kept, grad):
    return (grad,)

def back_keep(v):
    return (v, None)

def back_low(kept, grad):
    return (low(grad),)
low.defvjp(low_keep, low_pass)
low_back.defvjp(back_keep, back_low)

def layer_norm(row_data, gain_vec, shift_vec):
    centre = row_data - lax.optimization_barrier(jnp.mean(row_data, axis=1, keepdims=True))
    spread = lax.optimization_barrier(jnp.mean(centre * centre, axis=1, keepdims=True))
    return centre * lax.rsqrt(spread + norm_eps) * gain_vec[None, :] + shift_vec[None, :]

def gelu_exact(values):
    return jax.nn.gelu(values, approximate=False)

def pack_layout(lengths, slot_ids, bounds):
    slot_count = lengths.shape[0]
    tok_count = slot_ids.shape[0]
    mark_count = bounds.shape[1]
    starts = (jnp.cumsum(lengths) - lengths).astype(jnp.int32)
    slot_hit = slot_ids[:, None] == jnp.arange(slot_count, dtype=jnp.int32)[None, :]
    tok_start = lax.optimization_barrier(jnp.sum(jnp.where(slot_hit, starts[None, :], 0), axis=1)).astype(jnp.int32)
    position = jnp.arange(tok_count, dtype=jnp.int32) - tok_start
    tok_bounds = lax.optimization_barrier(jnp.sum(jnp.where(slot_hit[:, :, None], bounds[None, :, :], 0), axis=1)).astype(jnp.int32)
    mark_index = lax.optimization_barrier(jnp.sum((tok_bounds <= position[:, None]).astype(jnp.int32), axis=1)).astype(jnp.int32) - 1
    mark_id = slot_ids * mark_count + mark_index
    all_marks = slot_count * mark_count
    member = (jnp.arange(all_marks, dtype=jnp.int32)[:, None] == mark_id[None, :]).astype(jnp.float32)
    inv_count = 1.0 / jnp.maximum(lax.optimization_barrier(jnp.sum(member, axis=1)), 1.0)
    same_slot = slot_ids[:, None] == (jnp.arange(all_marks, dtype=jnp.int32) // mark_count)[None, :]
    live_tok = (slot_ids < slot_count).astype(jnp.float32)
    live_slot = (lengths > 0).astype(jnp.float32)
    return (member, inv_count, same_slot, slot_ids, live_tok, live_slot)

def batch_mul(left, right):
    return jnp.einsum('sij,sjk->sik', left, right, precision=best_precision)

def head_mix(q_rows, k_rows, v_rows, conv_taps, layout):
    member, inv_count, same_slot, token_slot, live_tok, live_slot = layout
    slot_count = live_slot.shape[0]
    tok_count, head_dim = q_rows.shape
    mark_count = member.shape[0] // slot_count
    root_scale = head_dim ** (-0.25)
    q_scaled = q_rows * root_scale
    k_scaled = k_rows * root_scale
    q_marks = jnp.dot(member, q_scaled, precision=best_precision) * inv_count[:, None]
    k_marks = jnp.dot(member, k_scaled, precision=best_precision) * inv_count[:, None]
    first_scores = jnp.where(same_slot, jnp.dot(q_scaled, k_marks.T, precision=best_precision), mask_fill)
    first_kernel = jax.nn.softmax(first_scores, axis=1)
    q_blocks = q_marks.reshape(slot_count, mark_count, head_dim)
    k_blocks = k_marks.reshape(slot_count, mark_count, head_dim)
    middle_kernel = jax.nn.softmax(jnp.einsum('sid,sjd->sij', q_blocks, k_blocks, precision=best_precision), axis=2)
    column_sums = lax.optimization_barrier(jnp.sum(middle_kernel, axis=1))
    col_bound = lax.optimization_barrier(jnp.max(column_sums, axis=1))
    inverse = jnp.swapaxes(middle_kernel, 1, 2) / col_bound[:, None, None]
    identity_mat = jnp.eye(mark_count, dtype=jnp.float32)[None, :, :]
    for sweep_index in range(PINV_ITERS):
        product = batch_mul(middle_kernel, inverse)
        inner_poly = 7.0 * identity_mat - product
        inner_poly = 15.0 * identity_mat - batch_mul(product, inner_poly)
        inner_poly = 13.0 * identity_mat - batch_mul(product, inner_poly)
        inverse = 0.25 * batch_mul(inverse, inner_poly)
    last_scores = jnp.where(same_slot.T, jnp.dot(q_marks, k_scaled.T, precision=best_precision), mask_fill)
    last_kernel = jax.nn.softmax(last_scores, axis=1)
    mark_values = jnp.dot(last_kernel, v_rows, precision=best_precision)
    mixed_marks = jnp.einsum('sij,sjd->sid', inverse, mark_values.reshape(slot_count, mark_count, head_dim), precision=best_precision).reshape(slot_count * mark_count, head_dim)
    attended = jnp.dot(first_kernel, mixed_marks, precision=best_precision)
    half_width = conv_taps.shape[0] // 2
    padded_v = jnp.pad(v_rows, ((half_width, half_width), (0, 0)))
    padded_slot = jnp.pad(token_slot, (half_width, half_width), constant_values=-1)
    convolved = jnp.zeros_like(v_rows)
    for tap_index in range(conv_taps.shape[0]):
        same_seq = (padded_slot[tap_index:tap_index + tok_count] == token_slot).astype(jnp.float32)
        convolved = convolved + conv_taps[tap_index] * padded_v[tap_index:tap_index + tok_count] * same_seq[:, None]
    mixed_rows = (attended + convolved) * live_tok[:, None]
    return (mixed_rows, jnp.sum(col_bound * live_slot))

def heads_mix(layout, q_all, k_all, v_all, conv_all):
    tok_count = q_all.shape[0]
    head_count = conv_all.shape[0]
    head_dim = q_all.shape[1] // head_count

    def split_heads(row_data):
        return jnp.transpose(row_data.reshape(tok_count, head_count, head_dim), (1, 0, 2))

    def one_head(operands):
        return head_mix(operands[0], operands[1], operands[2], operands[3], layout)
    mixed_rows, bound_sums = lax.map(jax.checkpoint(one_head), (split_heads(q_all), split_heads(k_all), split_heads(v_all), conv_all))
    merged = jnp.transpose(mixed_rows, (1, 0, 2)).reshape(tok_count, head_count * head_dim)
    return (merged, jnp.sum(bound_sums))

def reference(tokens, qkv_weight, qv_bias, conv_weight, out_weight, out_bias, norm1_gain, norm1_bias, ffn_in_weight, ffn_in_bias, ffn_out_weight, ffn_out_bias, norm2_gain, norm2_bias, cotangent, seq_lengths, segment_ids, landmark_bounds):
    tok_packs = tokens.astype(jnp.float32).reshape(N_BATCH, TOK_DEV, D)
    length_packs = seq_lengths.reshape(N_BATCH, SEQ_DEV)
    slot_packs = segment_ids.reshape(N_BATCH, TOK_DEV)
    bound_packs = landmark_bounds.reshape(N_BATCH, SEQ_DEV, LANDMARKS)
    params = (qkv_weight.astype(jnp.float32), qv_bias.astype(jnp.float32), conv_weight.astype(jnp.float32), out_weight.astype(jnp.float32), out_bias.astype(jnp.float32), norm1_gain.astype(jnp.float32), norm1_bias.astype(jnp.float32), ffn_in_weight.astype(jnp.float32), ffn_in_bias.astype(jnp.float32), ffn_out_weight.astype(jnp.float32), ffn_out_bias.astype(jnp.float32), norm2_gain.astype(jnp.float32), norm2_bias.astype(jnp.float32))

    def forward(tok_all, qkv_w, qv_b, conv_w, out_w, out_b, gain_one, shift_one, in_w, in_b, down_w, down_b, gain_two, shift_two):

        def pack_step(totals, pack_item):
            tok_rows, lengths, slot_ids, bounds = pack_item
            layout = pack_layout(lengths, slot_ids, bounds)
            projected = jnp.dot(tok_rows, qkv_w.reshape(D, 3 * H * HEAD_DIM), precision=best_precision).reshape(TOK_DEV, 3, H * HEAD_DIM)
            bias_rows = jnp.stack([qv_b[0], jnp.zeros_like(qv_b[0]), qv_b[1]])
            qkv_low = low(low_back(projected + bias_rows[None, :, :]))
            mixed_rows, bound_sum = heads_mix(layout, qkv_low[:, 0], qkv_low[:, 1], qkv_low[:, 2], conv_w)
            mixed_low = low(low_back(mixed_rows))
            attn_rows = low_back(jnp.dot(mixed_low, out_w, precision=best_precision) + out_b[None, :])
            norm1_out = layer_norm(tok_rows + attn_rows, gain_one, shift_one)
            pre_act = low_back(jnp.dot(low(norm1_out), in_w, precision=best_precision) + in_b[None, :])
            hidden_low = low(gelu_exact(pre_act))
            ffn_result = low_back(jnp.dot(hidden_low, down_w, precision=best_precision) + down_b[None, :])
            final_out = layer_norm(norm1_out + ffn_result, gain_two, shift_two)
            return (totals + bound_sum, final_out)
        bound_total, outs_packed = lax.scan(jax.checkpoint(pack_step), jnp.zeros((), jnp.float32), (tok_all, length_packs, slot_packs, bound_packs))
        return (outs_packed.reshape(N_BATCH * TOK_DEV, D), bound_total)
    final_out, pullback, bound_total = jax.vjp(forward, tok_packs, *params, has_aux=True)
    gradients = pullback(cotangent.astype(jnp.float32))
    live_total = jnp.sum((seq_lengths > 0).astype(jnp.float32)) * H
    condition = bound_total / live_total
    vector_grads = jnp.stack([gradients[11], gradients[12], gradients[13], gradients[6], gradients[7], gradients[5]])
    return (final_out.astype(jnp.bfloat16), gradients[0].reshape(N_BATCH * TOK_DEV, D), gradients[1], gradients[2], gradients[3], gradients[4], gradients[8], gradients[9], gradients[10], vector_grads, condition)
```

```python
from functools import partial

import jax
import jax.numpy as jnp
from jax import lax
from jax.experimental import pallas as pl
from jax.experimental.pallas import tpu as pltpu
from jax.sharding import PartitionSpec as P

HEAD_DIM = 64
PINV_ITERS = 6
TILE = 512
SUB = 128

f32 = jnp.float32
low = jnp.bfloat16
mask_fill = -1000000000.0


def split(x):
    high = x.astype(low)
    return high, (x - high.astype(f32)).astype(low)


def mul(a, b):
    return lax.dot_general(a, b, (((1,), (0,)), ((), ())), preferred_element_type=f32)


def mul_t(a, b):
    return lax.dot_general(a, b, (((1,), (1,)), ((), ())), preferred_element_type=f32)


def wide(form, left, right):
    left_high, left_low = split(left)
    right_high, right_low = split(right)
    return form(left_high, right_high) + (
        form(left_high, right_low) + form(left_low, right_high)
    )


def block_grid(rows, cols):
    row_block = lax.broadcasted_iota(jnp.int32, (rows, cols), 0) // HEAD_DIM
    col_block = lax.broadcasted_iota(jnp.int32, (rows, cols), 1) // HEAD_DIM
    return row_block == col_block


def spread(x, blocks):
    count = blocks.shape[0] // x.shape[0]
    return jnp.where(blocks, jnp.concatenate([x] * count, axis=0), jnp.zeros_like(x[:1, :1]))


def fold(x, blocks):
    kept = jnp.where(blocks, x, jnp.zeros_like(x[:1, :1]))
    rows = HEAD_DIM
    out = kept[:rows]
    for n in range(1, x.shape[0] // rows):
        out = out + kept[n * rows : (n + 1) * rows]
    return out


def pack_mul(left, right, blocks):
    left_high, left_low = split(left)
    right_high, right_low = split(right)
    right_high, right_low = spread_low(right_high, blocks), spread_low(right_low, blocks)
    return mul(left_high, right_high) + (mul(left_high, right_low) + mul(left_low, right_high))


def pack_mul_t(left, right, blocks):
    left_high, left_low = split(left)
    right_high, right_low = split(right)
    right_high, right_low = spread_low(right_high, blocks), spread_low(right_low, blocks)
    return mul_t(left_high, right_high) + (mul_t(left_high, right_low) + mul_t(left_low, right_high))


def spread_low(x, blocks):
    return spread(x.astype(f32), blocks).astype(low)


def slot_bounds(len_ref, s, slots):
    start = jnp.int32(0)
    for n in range(slots):
        start = start + jnp.where(n < s, len_ref[n], 0)
    return start, start + len_ref[s]


def eye_pack(width):
    row = lax.broadcasted_iota(jnp.int32, (HEAD_DIM, width), 0)
    col = lax.broadcasted_iota(jnp.int32, (HEAD_DIM, width), 1) % HEAD_DIM
    return jnp.where(row == col, 1.0, 0.0).astype(f32)


def lane_mask(start, end, at, width):
    tok = at + lax.broadcasted_iota(jnp.int32, (1, width), 1)
    return (tok >= start) & (tok < end)


def band(taps_row, width):
    row = lax.broadcasted_iota(jnp.int32, (SUB, 3 * SUB), 0)
    col = lax.broadcasted_iota(jnp.int32, (SUB, 3 * SUB), 1)
    off = col - row - (SUB - width // 2)
    out = jnp.zeros((SUB, 3 * SUB), f32)
    for n in range(width):
        out = jnp.where(off == n, taps_row[:, n : n + 1], out)
    return out


def slot_marks(len_ref, at, slots, marks, width):
    rows = slots * marks
    row = lax.broadcasted_iota(jnp.int32, (rows, 1), 0)
    slot = row // marks
    mark = row % marks
    start = jnp.zeros((rows, 1), jnp.int32)
    length = jnp.zeros((rows, 1), jnp.int32)
    for n in range(slots):
        start = start + jnp.where(slot > n, len_ref[n], 0)
        length = jnp.where(slot == n, len_ref[n], length)
    lower = start + (mark * length) // marks
    upper = start + ((mark + 1) * length) // marks
    inv_count = 1.0 / jnp.maximum((upper - lower).astype(f32), 1.0)
    tok = at + lax.broadcasted_iota(jnp.int32, (rows, width), 1)
    member = jnp.where((tok >= lower) & (tok < upper), 1.0, 0.0)
    return member, inv_count


def mix_forward_kernel(
    slots, marks, taps,
    len_ref, tok_ref, weight_ref, bias_ref, conv_ref,
    qkv_ref, first_ref, last_ref, mixed_ref, mark_ref, value_ref, inner_ref,
    denom_ref, middle_ref, steps_ref, inverse_ref, bound_ref,
    vpad, scores, vsum,
):
    step = pl.program_id(0)
    width = first_ref.shape[0]
    heads = width // HEAD_DIM
    tok_count = qkv_ref.shape[1]
    tiles = tok_count // TILE
    packed = slots * marks
    at = pl.multiple_of(step * TILE, TILE)

    @pl.when(step == 0)
    def _():
        mark_ref[...] = jnp.zeros_like(mark_ref)
        vsum[...] = jnp.zeros_like(vsum)
        vpad[:, :SUB] = jnp.zeros((width, SUB), low)
        vpad[:, tok_count + SUB :] = jnp.zeros((width, SUB), low)

    rows = (mul_t(weight_ref[...], tok_ref[...]) + bias_ref[...]).astype(low)
    qkv_ref[:, pl.ds(at, TILE)] = rows
    vpad[:, pl.ds(pl.multiple_of(at + SUB, SUB), TILE)] = rows[2 * width :]
    member, inv_count = slot_marks(len_ref, at, slots, marks, TILE)
    mark_ref[...] += mul_t(member.astype(low), rows[: 2 * width])
    vsum[...] += mul_t(jnp.ones((8, TILE), low), rows[2 * width :])
    first_ref[:, pl.ds(at, TILE)] = jnp.zeros((width, TILE), low)
    last_ref[:, pl.ds(at, TILE)] = jnp.zeros((width, TILE), low)
    mixed_ref[:, pl.ds(at, TILE)] = jnp.zeros((width, TILE), low)

    @pl.when(step == tiles - 1)
    def _():
        mark_ref[...] = mark_ref[...] * inv_count
        head_blocks = block_grid(width, width)
        slot_blocks = block_grid(packed, packed)
        eye = eye_pack(packed)
        scale = HEAD_DIM ** -0.5

        middles, inverses_t, products = [], [], []
        bound_total = jnp.zeros((1, 1), f32)
        lane_slot = lax.broadcasted_iota(jnp.int32, (1, packed), 1) // marks
        for h in range(heads):
            q_marks = mark_ref[:, h * HEAD_DIM : (h + 1) * HEAD_DIM]
            k_marks = mark_ref[:, width + h * HEAD_DIM : width + (h + 1) * HEAD_DIM]
            sim = wide(mul_t, q_marks, k_marks) * scale
            sim = jnp.where(slot_blocks, sim, -1e30)
            sim = jnp.exp(sim - jnp.max(sim, axis=1, keepdims=True))
            sim = sim / jnp.sum(sim, axis=1, keepdims=True)
            middle = fold(sim, slot_blocks)
            col_sums = jnp.sum(middle, axis=0, keepdims=True)
            bound = jnp.zeros((1, packed), f32)
            for s in range(slots):
                top = jnp.max(jnp.where(lane_slot == s, col_sums, 0.0), axis=1, keepdims=True)
                bound = jnp.where(lane_slot == s, top, bound)
                bound_total += jnp.where(len_ref[s] > 0, top, 0.0)
            middle_ref[h] = middle
            middles.append(middle)
            inverses_t.append(middle / bound)
            products.append(pack_mul_t(middle, middle, slot_blocks) / bound)
        bound_ref[...] = jnp.broadcast_to(bound_total, bound_ref.shape)

        def newton(n, carry):
            out = []
            for h in range(heads):
                inverse_t, product = carry[h]
                square = pack_mul(product, product, slot_blocks)
                cube = pack_mul(product, square, slot_blocks)
                fourth = pack_mul(square, square, slot_blocks)
                second = 15.0 * eye - 7.0 * product + square
                third = 13.0 * eye - 15.0 * product + 7.0 * square - cube
                steps_ref[n, 0, h] = product
                steps_ref[n, 1, h] = second
                steps_ref[n, 2, h] = third
                steps_ref[n, 3, h] = inverse_t
                out.append(
                    (
                        0.25 * pack_mul(third, inverse_t, slot_blocks),
                        0.25 * (13.0 * product - 15.0 * square + 7.0 * cube - fourth),
                    )
                )
            return tuple(out)

        final = lax.fori_loop(0, PINV_ITERS, newton, tuple(zip(inverses_t, products)))
        for h in range(heads):
            inverse_ref[h] = final[h][0]

        def one_slot(s, _):
            start, end = slot_bounds(len_ref, s, slots)
            lo, hi = start // TILE, (end + TILE - 1) // TILE
            hi = jnp.where(end > start, hi, lo)
            own = mark_ref[pl.ds(pl.multiple_of(s * marks, marks), marks), :] * scale
            q_block = spread(own[:, :width], head_blocks).astype(low)
            k_block = spread(own[:, width:], head_blocks).astype(low)

            def score_tile(n, top):
                t = pl.multiple_of(n * TILE, TILE)
                mask = lane_mask(start, end, t, TILE)
                sim = mul(k_block, qkv_ref[:width, pl.ds(t, TILE)])
                sim = sim.reshape(heads, marks, TILE)
                sim = jnp.exp(sim - jnp.max(sim, axis=1, keepdims=True))
                sim = sim / jnp.sum(sim, axis=1, keepdims=True)
                sim = sim.reshape(width, TILE)
                old = first_ref[:, pl.ds(t, TILE)].astype(f32)
                first_ref[:, pl.ds(t, TILE)] = jnp.where(mask, sim, old).astype(low)
                sim = mul(q_block, qkv_ref[width : 2 * width, pl.ds(t, TILE)])
                sim = jnp.where(mask, sim, mask_fill)
                scores[:, pl.ds(t, TILE)] = sim
                for c in range(TILE // SUB):
                    top = jnp.maximum(top, sim[:, c * SUB : (c + 1) * SUB])
                return top

            top = lax.fori_loop(lo, hi, score_tile, jnp.full((width, SUB), mask_fill, f32))
            top = jnp.max(top, axis=1, keepdims=True)

            def value_tile(n, carry):
                denom, total = carry
                t = pl.multiple_of(n * TILE, TILE)
                mask = lane_mask(start, end, t, TILE)
                part = jnp.exp(scores[:, pl.ds(t, TILE)] - top)
                old = last_ref[:, pl.ds(t, TILE)].astype(f32)
                last_ref[:, pl.ds(t, TILE)] = jnp.where(mask, part, old).astype(low)
                total = total + mul_t(part.astype(low), qkv_ref[2 * width :, pl.ds(t, TILE)])
                for c in range(TILE // SUB):
                    denom = denom + part[:, c * SUB : (c + 1) * SUB]
                return denom, total

            denom, total = lax.fori_loop(
                lo, hi, value_tile,
                (jnp.zeros((width, SUB), f32), jnp.zeros((width, width), f32)),
            )
            denom = jnp.sum(denom, axis=1, keepdims=True)
            inv = 1.0 / jnp.where(denom > 0.0, denom, 1.0)
            denom_ref[s] = inv
            values = fold(total * inv, head_blocks)
            values = jnp.where(end > start, values, vsum[:1] / tok_count)
            value_ref[pl.ds(pl.multiple_of(s * marks, marks), marks), :] = values
            return 0

        lax.fori_loop(0, slots, one_slot, 0)

        lane_head = lax.broadcasted_iota(jnp.int32, (1, width), 1) // HEAD_DIM
        inner = jnp.zeros((packed, width), f32)
        for h in range(heads):
            inverse = pack_mul_t(eye, final[h][0], slot_blocks)
            own_values = jnp.where(lane_head == h, value_ref[...], 0.0)
            inner = inner + wide(mul, spread(inverse, slot_blocks), own_values)
        inner_ref[...] = inner

        bands = [band(conv_ref[h : h + 1, :], taps).astype(low) for h in range(heads)]

        def out_slot(s, _):
            start, end = slot_bounds(len_ref, s, slots)
            lo, hi = start // TILE, (end + TILE - 1) // TILE
            hi = jnp.where(end > start, hi, lo)
            own = inner_ref[pl.ds(pl.multiple_of(s * marks, marks), marks), :]
            a_block = jnp.transpose(spread(own, head_blocks)).astype(low)

            def out_tile(n, _):
                t = pl.multiple_of(n * TILE, TILE)
                mask = lane_mask(start, end, t, TILE)
                rows = mul(a_block, first_ref[:, pl.ds(t, TILE)])
                rows = rows + convolve(vpad, bands, start, end, t, heads)
                old = mixed_ref[:, pl.ds(t, TILE)].astype(f32)
                mixed_ref[:, pl.ds(t, TILE)] = jnp.where(mask, rows, old).astype(low)
                return 0

            return lax.fori_loop(lo, hi, out_tile, 0)

        lax.fori_loop(0, slots, out_slot, 0)


def windows(padded, start, end, t):
    full = padded[:, pl.ds(t, TILE + 2 * SUB)]
    keep = lane_mask(start, end, t - SUB, TILE + 2 * SUB)
    return jnp.where(keep, full.astype(f32), 0.0).astype(low)


def convolve(padded, bands, start, end, t, heads):
    full = windows(padded, start, end, t)
    out = []
    count = TILE // SUB
    for h in range(heads):
        own = full[h * HEAD_DIM : (h + 1) * HEAD_DIM]
        stack = jnp.concatenate(
            [own[:, c * SUB : (c + 3) * SUB] for c in range(count)], axis=0
        )
        res = mul_t(stack, bands[h])
        out.append(
            jnp.concatenate(
                [res[c * HEAD_DIM : (c + 1) * HEAD_DIM] for c in range(count)], axis=1
            )
        )
    return jnp.concatenate(out, axis=0)


def mix_backward_kernel(
    slots, marks, taps,
    len_ref, grad_ref, qkv_ref, first_ref, last_ref, mark_ref, value_ref, inner_ref,
    denom_ref, middle_ref, steps_ref, inverse_ref, conv_ref,
    out_ref, bias_ref, conv_out_ref,
    gpad, vpad, ds_first, ds_last, conv_grad, d_inner, d_k, d_q, d_value,
):
    width = first_ref.shape[0]
    heads = width // HEAD_DIM
    tok_count = qkv_ref.shape[1]
    packed = slots * marks
    scale = HEAD_DIM ** -0.5
    head_blocks = block_grid(width, width)
    slot_blocks = block_grid(packed, packed)
    eye = eye_pack(packed)
    count = TILE // SUB

    for padded, source in ((gpad, grad_ref[...]), (vpad, qkv_ref[2 * width :, :])):
        padded[:, :SUB] = jnp.zeros((width, SUB), low)
        padded[:, tok_count + SUB :] = jnp.zeros((width, SUB), low)
        padded[:, SUB : tok_count + SUB] = source
    out_ref[...] = jnp.zeros_like(out_ref)
    ds_first[...] = jnp.zeros_like(ds_first)
    ds_last[...] = jnp.zeros_like(ds_last)
    conv_grad[...] = jnp.zeros_like(conv_grad)

    def reach(s):
        start, end = slot_bounds(len_ref, s, slots)
        lo, hi = start // TILE, (end + TILE - 1) // TILE
        return start, end, lo, jnp.where(end > start, hi, lo)

    def own_rows(s):
        return pl.ds(pl.multiple_of(s * marks, marks), marks)

    def first_slot(s, _):
        start, end, lo, hi = reach(s)
        a_block = spread(inner_ref[own_rows(s), :], head_blocks).astype(low)

        def tile(n, carry):
            inner_total, key_total = carry
            t = pl.multiple_of(n * TILE, TILE)
            mask = lane_mask(start, end, t, TILE)
            own_grad = grad_ref[:, pl.ds(t, TILE)]
            kernel_rows = jnp.where(mask, first_ref[:, pl.ds(t, TILE)].astype(f32), 0.0)
            d_kernel = mul(a_block, own_grad)
            prod = (kernel_rows * d_kernel).reshape(heads, marks, TILE)
            row_sum = jnp.sum(prod, axis=1, keepdims=True)
            d_sim = prod - kernel_rows.reshape(heads, marks, TILE) * row_sum
            d_sim = d_sim.reshape(width, TILE)
            d_sim_low = d_sim.astype(low)
            old = ds_first[:, pl.ds(t, TILE)].astype(f32)
            ds_first[:, pl.ds(t, TILE)] = jnp.where(mask, d_sim, old).astype(low)
            inner_total = inner_total + mul_t(kernel_rows.astype(low), own_grad)
            key_total = key_total + mul_t(d_sim_low, qkv_ref[:width, pl.ds(t, TILE)])
            full = windows(vpad, start, end, t)
            grad_own = jnp.where(mask, own_grad.astype(f32), 0.0).astype(low)
            for h in range(heads):
                sel = slice(h * HEAD_DIM, (h + 1) * HEAD_DIM)
                left = jnp.concatenate(
                    [grad_own[sel, c * SUB : (c + 1) * SUB] for c in range(count)], axis=0
                )
                right = jnp.concatenate(
                    [full[sel, c * SUB : (c + 3) * SUB] for c in range(count)], axis=0
                )
                conv_grad[h] += lax.dot_general(
                    left, right, (((0,), (0,)), ((), ())), preferred_element_type=f32
                )
            return inner_total, key_total

        zero = jnp.zeros((width, width), f32)
        inner_total, key_total = lax.fori_loop(lo, hi, tile, (zero, zero))
        d_inner[own_rows(s), :] = fold(inner_total, head_blocks)
        d_k[own_rows(s), :] = fold(key_total, head_blocks) * scale
        return 0

    lax.fori_loop(0, slots, first_slot, 0)

    row = lax.broadcasted_iota(jnp.int32, (SUB, 3 * SUB), 0)
    col = lax.broadcasted_iota(jnp.int32, (SUB, 3 * SUB), 1)
    off = col - row - (SUB - taps // 2)
    tap_lane = lax.broadcasted_iota(jnp.int32, (1, SUB), 1)
    for h in range(heads):
        found = jnp.zeros((1, SUB), f32)
        square = conv_grad[h]
        for n in range(taps):
            part = jnp.sum(jnp.where(off == n, square, 0.0), axis=0, keepdims=True)
            part = jnp.sum(part, axis=1, keepdims=True)
            found = jnp.where(tap_lane == n, part, found)
        conv_out_ref[h : h + 1, :] = found

    lane_head = lax.broadcasted_iota(jnp.int32, (1, width), 1) // HEAD_DIM
    value_total = jnp.zeros((packed, width), f32)
    d_inverses = []
    for h in range(heads):
        own = jnp.where(lane_head == h, d_inner[...], 0.0)
        value_total = value_total + wide(mul, spread(inverse_ref[h], slot_blocks), own)
        d_inverses.append(fold(wide(mul_t, own, value_ref[...]), slot_blocks))
    d_value[...] = value_total

    middles_t = [pack_mul_t(eye, middle_ref[h], slot_blocks) for h in range(heads)]

    def newton(k, carry):
        n = PINV_ITERS - 1 - k
        out = []
        for h in range(heads):
            d_inverse, d_middle = carry[h]
            product = steps_ref[n, 0, h]
            second = steps_ref[n, 1, h]
            third = steps_ref[n, 2, h]
            inverse_t = steps_ref[n, 3, h]
            middle_t = middles_t[h]
            d_third = 0.25 * pack_mul(inverse_t, d_inverse, slot_blocks)
            d_second = -pack_mul(product, d_third, slot_blocks)
            d_first = -pack_mul(product, d_second, slot_blocks)
            d_product = (
                -pack_mul(d_third, second, slot_blocks)
                - pack_mul(d_second, 7.0 * eye - product, slot_blocks)
                - d_first
            )
            d_middle = d_middle + pack_mul(d_product, inverse_t, slot_blocks)
            d_inverse = 0.25 * pack_mul(d_inverse, third, slot_blocks) + pack_mul(
                middle_t, d_product, slot_blocks
            )
            out.append((d_inverse, d_middle))
        return tuple(out)

    zero = jnp.zeros((HEAD_DIM, packed), f32)
    final = lax.fori_loop(0, PINV_ITERS, newton, tuple((x, zero) for x in d_inverses))
    lane_slot = lax.broadcasted_iota(jnp.int32, (1, packed), 1) // marks
    dq_total = jnp.zeros((packed, width), f32)
    dk_total = jnp.zeros((packed, width), f32)
    for h in range(heads):
        d_inverse, d_middle = final[h]
        middle = middle_ref[h]
        first_t = steps_ref[0, 3, h]
        d_inverse_t = pack_mul_t(eye, d_inverse, slot_blocks)
        col_sums = jnp.sum(middle, axis=0, keepdims=True)
        share = jnp.sum(d_inverse_t * first_t, axis=0, keepdims=True)
        bound = jnp.zeros((1, packed), f32)
        d_bound = jnp.zeros((1, packed), f32)
        hits = jnp.zeros((1, packed), f32)
        for s in range(slots):
            mine = lane_slot == s
            top = jnp.max(jnp.where(mine, col_sums, 0.0), axis=1, keepdims=True)
            total = jnp.sum(jnp.where(mine, share, 0.0), axis=1, keepdims=True)
            number = jnp.sum(
                jnp.where(mine & (col_sums == top), 1.0, 0.0), axis=1, keepdims=True
            )
            bound = jnp.where(mine, top, bound)
            d_bound = jnp.where(mine, -total / top, d_bound)
            hits = jnp.where(mine, number, hits)
        d_middle = d_middle + d_inverse_t / bound
        d_middle = d_middle + jnp.where(col_sums == bound, d_bound / hits, 0.0)
        prod = spread(middle * d_middle, slot_blocks)
        d_sim = prod - spread(middle, slot_blocks) * jnp.sum(prod, axis=1, keepdims=True)
        d_sim = d_sim * scale
        own = lane_head == h
        q_marks = jnp.where(own, mark_ref[:, :width], 0.0)
        k_marks = jnp.where(own, mark_ref[:, width:], 0.0)
        dq_total = dq_total + wide(mul, d_sim, k_marks)
        dk_total = dk_total + wide(mul, jnp.transpose(d_sim), q_marks)
    d_q[...] = dq_total
    d_k[...] += dk_total

    flipped = []
    for h in range(heads):
        flipped.append(
            band(
                jnp.concatenate(
                    [conv_ref[h : h + 1, n : n + 1] for n in reversed(range(taps))], axis=1
                ),
                taps,
            ).astype(low)
        )

    def last_slot(s, _):
        start, end, lo, hi = reach(s)
        inv = denom_ref[s]
        own_d = d_value[own_rows(s), :]
        own_v = value_ref[own_rows(s), :]
        d_block = spread(own_d, head_blocks)
        row_sum = jnp.sum(
            d_block * jnp.concatenate([own_v] * heads, axis=0), axis=1, keepdims=True
        )
        row_sum = row_sum * inv
        d_block = d_block * inv
        d_block_t = jnp.transpose(d_block).astype(low)
        d_block = d_block.astype(low)

        def tile(n, query_total):
            t = pl.multiple_of(n * TILE, TILE)
            mask = lane_mask(start, end, t, TILE)
            kernel_rows = jnp.where(mask, last_ref[:, pl.ds(t, TILE)].astype(f32), 0.0)
            v_rows = qkv_ref[2 * width :, pl.ds(t, TILE)]
            d_sim = kernel_rows * (mul(d_block, v_rows) - row_sum)
            d_low = d_sim.astype(low)
            old = ds_last[:, pl.ds(t, TILE)].astype(f32)
            ds_last[:, pl.ds(t, TILE)] = jnp.where(mask, d_sim, old).astype(low)
            dv = mul(d_block_t, kernel_rows.astype(low))
            dv = dv + convolve(gpad, flipped, start, end, t, heads)
            old = out_ref[2 * width :, pl.ds(t, TILE)].astype(f32)
            out_ref[2 * width :, pl.ds(t, TILE)] = jnp.where(mask, dv, old).astype(low)
            return query_total + mul_t(d_low, qkv_ref[width : 2 * width, pl.ds(t, TILE)])

        query_total = lax.fori_loop(lo, hi, tile, jnp.zeros((width, width), f32))
        d_q[own_rows(s), :] += fold(query_total, head_blocks) * scale
        return 0

    lax.fori_loop(0, slots, last_slot, 0)

    inv_count = slot_marks(len_ref, 0, slots, marks, SUB)[1]
    d_q[...] = d_q[...] * inv_count
    d_k[...] = d_k[...] * inv_count

    def final_slot(s, _):
        start, end, lo, hi = reach(s)
        length = end - start
        own = mark_ref[own_rows(s), :] * scale

        def left(block, d_mark):
            wide_rows = jnp.concatenate([spread(block, head_blocks), d_mark], axis=0)
            return jnp.transpose(wide_rows).astype(low)

        q_left = left(own[:, width:], d_q[own_rows(s), :])
        k_left = left(own[:, :width], d_k[own_rows(s), :])
        mark = lax.broadcasted_iota(jnp.int32, (marks, 1), 0)
        lower = start + (mark * length) // marks
        upper = start + ((mark + 1) * length) // marks

        def tile(n, _):
            t = pl.multiple_of(n * TILE, TILE)
            mask = lane_mask(start, end, t, TILE)
            tok = t + lax.broadcasted_iota(jnp.int32, (marks, TILE), 1)
            member = jnp.where((tok >= lower) & (tok < upper), 1.0, 0.0).astype(low)
            for at, lhs, source in ((0, q_left, ds_first), (width, k_left, ds_last)):
                rhs = jnp.concatenate([source[:, pl.ds(t, TILE)], member], axis=0)
                rows = mul(lhs, rhs)
                old = out_ref[at : at + width, pl.ds(t, TILE)].astype(f32)
                out_ref[at : at + width, pl.ds(t, TILE)] = jnp.where(mask, rows, old).astype(low)
            return 0

        return lax.fori_loop(lo, hi, tile, 0)

    lax.fori_loop(0, slots, final_slot, 0)

    def bias_tile(n, carry):
        t = pl.multiple_of(n * TILE, TILE)
        q_sum, v_sum = carry
        q_rows = out_ref[:width, pl.ds(t, TILE)].astype(f32)
        v_rows = out_ref[2 * width :, pl.ds(t, TILE)].astype(f32)
        for c in range(count):
            q_sum = q_sum + q_rows[:, c * SUB : (c + 1) * SUB]
            v_sum = v_sum + v_rows[:, c * SUB : (c + 1) * SUB]
        return q_sum, v_sum

    zero = jnp.zeros((width, SUB), f32)
    q_sum, v_sum = lax.fori_loop(0, tok_count // TILE, bias_tile, (zero, zero))
    bias_ref[:, 0:1] = jnp.sum(q_sum, axis=1, keepdims=True)
    bias_ref[:, 1:2] = jnp.sum(v_sum, axis=1, keepdims=True)


def mix_forward(seq_lengths, tokens, weight_t, bias_col, conv_own, slots, marks):
    tok_count, model = tokens.shape
    width = weight_t.shape[0] // 3
    heads = width // HEAD_DIM
    packed = slots * marks
    taps = conv_own.shape[1]
    whole = lambda *shape: pl.BlockSpec(shape, lambda i, lens: (0,) * len(shape))
    shapes = [
        ((3 * width, tok_count), low),
        ((width, tok_count), low),
        ((width, tok_count), low),
        ((width, tok_count), low),
        ((packed, 2 * width), f32),
        ((packed, width), f32),
        ((packed, width), f32),
        ((slots, width, 1), f32),
        ((heads, HEAD_DIM, packed), f32),
        ((PINV_ITERS, 4, heads, HEAD_DIM, packed), f32),
        ((heads, HEAD_DIM, packed), f32),
        ((8, 128), f32),
    ]
    return pl.pallas_call(
        partial(mix_forward_kernel, slots, marks, taps),
        out_shape=[jax.ShapeDtypeStruct(s, t) for s, t in shapes],
        grid_spec=pltpu.PrefetchScalarGridSpec(
            num_scalar_prefetch=1,
            grid=(tok_count // TILE,),
            in_specs=[
                pl.BlockSpec((TILE, model), lambda i, lens: (i, 0)),
                whole(3 * width, model),
                whole(3 * width, 1),
                whole(heads, taps),
            ],
            out_specs=[whole(*s) for s, _ in shapes],
            scratch_shapes=[
                pltpu.VMEM((width, tok_count + 2 * SUB), low),
                pltpu.VMEM((width, tok_count), f32),
                pltpu.VMEM((8, width), f32),
            ],
        ),
        compiler_params=pltpu.CompilerParams(vmem_limit_bytes=56 * 1024 * 1024),
        name="mix_forward",
    )(seq_lengths, tokens, weight_t, bias_col, conv_own)


def mix_backward(seq_lengths, grad_t, saved, conv_own, slots, marks):
    qkv_t, first, last, mark, value, inner, denom, middle, steps, inverse = saved
    width, tok_count = grad_t.shape
    heads = width // HEAD_DIM
    packed = slots * marks
    taps = conv_own.shape[1]
    args = (grad_t, qkv_t, first, last, mark, value, inner, denom, middle, steps, inverse, conv_own)
    whole = lambda shape: pl.BlockSpec(
        shape, lambda i, lens: (0,) * len(shape), pipeline_mode=pl.Buffered(1)
    )
    shapes = [((3 * width, tok_count), low), ((width, 2), f32), ((heads, SUB), f32)]
    square = pltpu.VMEM((packed, width), f32)
    return pl.pallas_call(
        partial(mix_backward_kernel, slots, marks, taps),
        out_shape=[jax.ShapeDtypeStruct(s, t) for s, t in shapes],
        grid_spec=pltpu.PrefetchScalarGridSpec(
            num_scalar_prefetch=1,
            grid=(1,),
            in_specs=[whole(x.shape) for x in args],
            out_specs=[whole(s) for s, _ in shapes],
            scratch_shapes=[
                pltpu.VMEM((width, tok_count + 2 * SUB), low),
                pltpu.VMEM((width, tok_count + 2 * SUB), low),
                pltpu.VMEM((width, tok_count), low),
                pltpu.VMEM((width, tok_count), low),
                pltpu.VMEM((heads, SUB, 3 * SUB), f32),
                square, square, square, square,
            ],
        ),
        compiler_params=pltpu.CompilerParams(vmem_limit_bytes=56 * 1024 * 1024),
        name="mix_backward",
    )(seq_lengths, *args)


contract_rows = (((0,), (0,)), ((), ()))
contract_cols = (((1,), (1,)), ((), ()))
norm_eps = 1e-05


def split_up(x, dim, peers):
    before, after = (x.shape[:dim], x.shape[dim + 1 :])
    return jnp.moveaxis(x.reshape(*before, peers, -1, *after), dim, 0)


def sum_at_owner(x, axis, dim):
    peers = lax.axis_size(axis)
    tiles = lax.all_to_all(split_up(x, dim, peers), axis, 0, 0, tiled=True)
    return jnp.sum(tiles.astype(f32), axis=0)


def layer_norm(row_data, gain_vec, shift_vec):
    centre = row_data - jnp.mean(row_data, axis=1, keepdims=True)
    spread_row = jnp.mean(centre * centre, axis=1, keepdims=True)
    return centre * lax.rsqrt(spread_row + norm_eps) * gain_vec[None, :] + shift_vec[None, :]


def gelu_exact(values):
    return jax.nn.gelu(values, approximate=False)


def body(
    tokens,
    qkv_weight,
    qv_bias,
    conv_weight,
    out_weight,
    out_bias,
    norm1_gain,
    norm1_bias,
    ffn_in_weight,
    ffn_in_bias,
    ffn_out_weight,
    ffn_out_bias,
    norm2_gain,
    norm2_bias,
    cotangent,
    seq_lengths,
    segment_ids,
    landmark_bounds,
):
    tok_count, model_width = tokens.shape
    head_width = qkv_weight.shape[2]
    heads_here = head_width // HEAD_DIM
    head_total = conv_weight.shape[0]
    kernel_taps = conv_weight.shape[1]
    slots, marks = landmark_bounds.shape
    quarter = tok_count // lax.axis_size("heads")
    head_index = lax.axis_index("heads")
    own_start = head_index * quarter
    both = ("batch", "heads")
    own_rows_low = lax.dynamic_slice_in_dim(tokens, own_start, quarter, 0)
    own_tokens = own_rows_low.astype(f32)
    conv_own = lax.dynamic_slice_in_dim(conv_weight, head_index * heads_here, heads_here, 0)
    qv_own = lax.dynamic_slice_in_dim(qv_bias, head_index * head_width, head_width, 1)
    flat_qkv = qkv_weight.reshape(model_width, 3 * head_width)
    bias_col = jnp.concatenate([qv_own[0], jnp.zeros_like(qv_own[0]), qv_own[1]])[:, None]
    forward = mix_forward(
        seq_lengths, tokens, jnp.transpose(flat_qkv), bias_col, conv_own, slots, marks
    )
    qkv_t, first, last, mixed_t, mark, value, inner, denom, middle, steps, inverse, bound = forward
    bound_total = bound[0, 0]
    attn_part = lax.psum_scatter(
        lax.dot_general(mixed_t, out_weight, contract_rows, preferred_element_type=f32).astype(low),
        "heads",
        scatter_dimension=0,
        tiled=True,
    ).astype(f32)
    live_count = jnp.sum((seq_lengths > 0).astype(f32)) * heads_here
    first_res = own_tokens + attn_part + out_bias[None, :]
    norm1_out, norm1_pull = jax.vjp(layer_norm, first_res, norm1_gain, norm1_bias)
    norm1_low = norm1_out.astype(low)
    ff_own = ffn_out_weight.shape[0]
    bias_row = jnp.zeros((16, model_width), low).at[0, :ff_own].set(ffn_in_bias)
    whole_in = lax.all_gather(ffn_in_weight, both, axis=1, tiled=True)
    out_pack = lax.all_gather(jnp.concatenate([ffn_out_weight, bias_row], axis=0), both, axis=0)
    whole_out = out_pack[:, :ff_own].reshape(-1, model_width)
    whole_in_bias = out_pack[:, ff_own, :ff_own].reshape(-1)
    pre_act = (
        jnp.dot(norm1_low, whole_in, preferred_element_type=f32)
        + whole_in_bias.astype(f32)[None, :]
    )
    hidden_act, gelu_pull = jax.vjp(gelu_exact, pre_act)
    hidden_low = hidden_act.astype(low)
    ffn_result = jnp.dot(hidden_low, whole_out, preferred_element_type=f32) + ffn_out_bias[None, :]
    final_out, norm2_pull = jax.vjp(layer_norm, norm1_out + ffn_result, norm2_gain, norm2_bias)
    grad_second, grad_gain_two, grad_shift_two = norm2_pull(cotangent.astype(f32))
    grad_ffn_low = grad_second.astype(low)
    grad_ffn_bias = jnp.sum(grad_ffn_low.astype(f32), axis=0)
    down_term = lax.dot_general(
        hidden_low, grad_ffn_low, contract_rows, preferred_element_type=f32
    ).astype(low)
    grad_hidden = lax.dot_general(
        grad_ffn_low, whole_out, contract_cols, preferred_element_type=f32
    )
    grad_pre = gelu_pull(grad_hidden)[0].astype(low)
    grad_in_bias = jnp.sum(grad_pre.astype(f32), axis=0)
    up_term = lax.dot_general(
        norm1_low, grad_pre, contract_rows, preferred_element_type=f32
    ).astype(low)
    grad_norm1 = grad_second + lax.dot_general(
        grad_pre, whole_in, contract_cols, preferred_element_type=f32
    )
    grad_first, grad_gain_one, grad_shift_one = norm1_pull(grad_norm1)
    grad_attn_low = grad_first.astype(low)
    grad_out_bias = jnp.sum(grad_attn_low.astype(f32), axis=0)
    piece_rows = lax.all_gather(grad_attn_low, "heads", axis=0, tiled=True)
    grad_mix_t = lax.dot_general(
        out_weight, piece_rows, contract_cols, preferred_element_type=f32
    ).astype(low)
    grad_mix_t, down_term, up_term = lax.optimization_barrier((grad_mix_t, down_term, up_term))
    up_share = lax.psum_scatter(up_term, both, scatter_dimension=1, tiled=True).astype(f32)
    down_share = lax.psum_scatter(down_term, both, scatter_dimension=0, tiled=True).astype(f32)
    saved = (qkv_t, first, last, mark, value, inner, denom, middle, steps, inverse)
    grad_t, grad_bias, grad_conv = mix_backward(
        seq_lengths, grad_mix_t, saved, conv_own, slots, marks
    )
    out_part = lax.dot_general(
        mixed_t, piece_rows, (((1,), (0,)), ((), ())), preferred_element_type=f32
    )
    grad_qv_own = jnp.transpose(grad_bias)
    qkv_part = lax.dot_general(
        tokens, grad_t, (((0,), (1,)), ((), ())), preferred_element_type=f32
    ).reshape(model_width, 3, head_width)
    input_part = lax.psum_scatter(
        lax.dot_general(
            grad_t, flat_qkv, (((0,), (1,)), ((), ())), preferred_element_type=f32
        ).astype(low),
        "heads",
        scatter_dimension=0,
        tiled=True,
    ).astype(f32)
    input_grad = grad_first + input_part
    conv_full = lax.dynamic_update_slice_in_dim(
        jnp.zeros((head_total, kernel_taps), f32),
        grad_conv[:, :kernel_taps],
        head_index * heads_here,
        0,
    )
    bias_full = lax.dynamic_update_slice_in_dim(
        jnp.zeros((2, head_total * HEAD_DIM), f32), grad_qv_own, head_index * head_width, 1
    )
    qkv_share, out_share = (
        sum_at_owner(qkv_part.astype(low), "batch", 0),
        sum_at_owner(out_part.astype(low), "batch", 1),
    )
    vector_all = jnp.stack(
        [grad_ffn_bias, grad_gain_two, grad_shift_two, grad_gain_one, grad_shift_one, grad_out_bias]
    )
    in_bias_share, vector_share = (
        lax.psum_scatter(grad_in_bias, both, scatter_dimension=0, tiled=True),
        lax.psum_scatter(vector_all, both, scatter_dimension=1, tiled=True),
    )
    conv_sum, bias_sum, bound_all, count_all = lax.psum(
        (conv_full, bias_full, bound_total, live_count), both
    )
    conv_out = lax.dynamic_slice_in_dim(conv_sum, head_index * heads_here, heads_here, 0)
    bias_out = lax.dynamic_slice_in_dim(bias_sum, head_index * head_width, head_width, 1)
    condition = bound_all / count_all
    return (
        final_out.astype(low),
        input_grad,
        qkv_share,
        bias_out,
        conv_out,
        out_share,
        up_share,
        in_bias_share,
        down_share,
        vector_share,
        condition,
    )


def solution(mesh):
    in_specs = (
        P("batch", None),
        P(None, None, "heads"),
        P(),
        P(),
        P("heads", None),
        P(),
        P(),
        P(),
        P(None, ("batch", "heads")),
        P(("batch", "heads")),
        P(("batch", "heads"), None),
        P(),
        P(),
        P(),
        P(("batch", "heads"), None),
        P("batch"),
        P("batch"),
        P("batch", None),
    )
    out_specs = (
        P(("batch", "heads"), None),
        P(("batch", "heads"), None),
        P("batch", None, "heads"),
        P(None, "heads"),
        P("heads", None),
        P("heads", "batch"),
        P(None, ("batch", "heads")),
        P(("batch", "heads")),
        P(("batch", "heads"), None),
        P(None, ("batch", "heads")),
        P(),
    )
    return jax.shard_map(body, mesh=mesh, in_specs=in_specs, out_specs=out_specs, check_vma=False)
```

```python
from functools import partial

import jax
import jax.numpy as jnp
from jax import lax
from jax.experimental import pallas as pl
from jax.experimental.pallas import tpu as pltpu
from jax.sharding import PartitionSpec as P

HEAD_DIM = 64
PINV_ITERS = 6
TILE = 512
SUB = 128

f32 = jnp.float32
low = jnp.bfloat16
mask_fill = -1000000000.0


def split(x):
    high = x.astype(low)
    return high, (x - high.astype(f32)).astype(low)


def mul(a, b):
    return lax.dot_general(a, b, (((1,), (0,)), ((), ())), preferred_element_type=f32)


def mul_t(a, b):
    return lax.dot_general(a, b, (((1,), (1,)), ((), ())), preferred_element_type=f32)


def wide(form, left, right):
    left_high, left_low = split(left)
    right_high, right_low = split(right)
    return form(left_high, right_high) + (
        form(left_high, right_low) + form(left_low, right_high)
    )


def block_grid(rows, cols):
    row_block = lax.broadcasted_iota(jnp.int32, (rows, cols), 0) // HEAD_DIM
    col_block = lax.broadcasted_iota(jnp.int32, (rows, cols), 1) // HEAD_DIM
    return row_block == col_block


def spread(x, blocks):
    count = blocks.shape[0] // x.shape[0]
    return jnp.where(blocks, jnp.concatenate([x] * count, axis=0), jnp.zeros_like(x[:1, :1]))


def fold(x, blocks):
    kept = jnp.where(blocks, x, jnp.zeros_like(x[:1, :1]))
    rows = HEAD_DIM
    out = kept[:rows]
    for n in range(1, x.shape[0] // rows):
        out = out + kept[n * rows : (n + 1) * rows]
    return out


def pack_mul(left, right, blocks):
    left_high, left_low = split(left)
    right_high, right_low = split(right)
    right_high, right_low = spread_low(right_high, blocks), spread_low(right_low, blocks)
    return mul(left_high, right_high) + (mul(left_high, right_low) + mul(left_low, right_high))


def pack_mul_t(left, right, blocks):
    left_high, left_low = split(left)
    right_high, right_low = split(right)
    right_high, right_low = spread_low(right_high, blocks), spread_low(right_low, blocks)
    return mul_t(left_high, right_high) + (mul_t(left_high, right_low) + mul_t(left_low, right_high))


def spread_low(x, blocks):
    return spread(x.astype(f32), blocks).astype(low)


def slot_bounds(len_ref, s, slots):
    start = jnp.int32(0)
    for n in range(slots):
        start = start + jnp.where(n < s, len_ref[n], 0)
    return start, start + len_ref[s]


def eye_pack(width):
    row = lax.broadcasted_iota(jnp.int32, (HEAD_DIM, width), 0)
    col = lax.broadcasted_iota(jnp.int32, (HEAD_DIM, width), 1) % HEAD_DIM
    return jnp.where(row == col, 1.0, 0.0).astype(f32)


def lane_mask(start, end, at, width):
    tok = at + lax.broadcasted_iota(jnp.int32, (1, width), 1)
    return (tok >= start) & (tok < end)


def band(taps_row, width):
    row = lax.broadcasted_iota(jnp.int32, (SUB, 3 * SUB), 0)
    col = lax.broadcasted_iota(jnp.int32, (SUB, 3 * SUB), 1)
    off = col - row - (SUB - width // 2)
    out = jnp.zeros((SUB, 3 * SUB), f32)
    for n in range(width):
        out = jnp.where(off == n, taps_row[:, n : n + 1], out)
    return out


def slot_marks(len_ref, at, slots, marks, width):
    rows = slots * marks
    row = lax.broadcasted_iota(jnp.int32, (rows, 1), 0)
    slot = row // marks
    mark = row % marks
    start = jnp.zeros((rows, 1), jnp.int32)
    length = jnp.zeros((rows, 1), jnp.int32)
    for n in range(slots):
        start = start + jnp.where(slot > n, len_ref[n], 0)
        length = jnp.where(slot == n, len_ref[n], length)
    lower = start + (mark * length) // marks
    upper = start + ((mark + 1) * length) // marks
    inv_count = 1.0 / jnp.maximum((upper - lower).astype(f32), 1.0)
    tok = at + lax.broadcasted_iota(jnp.int32, (rows, width), 1)
    member = jnp.where((tok >= lower) & (tok < upper), 1.0, 0.0)
    return member, inv_count


def mix_forward_kernel(
    slots, marks, taps,
    len_ref, tok_ref, weight_ref, bias_ref, conv_ref,
    qkv_ref, first_ref, last_ref, mixed_ref, mark_ref, value_ref, inner_ref,
    denom_ref, middle_ref, steps_ref, inverse_ref, bound_ref,
    vpad, scores, vsum,
):
    step = pl.program_id(0)
    width = first_ref.shape[0]
    heads = width // HEAD_DIM
    tok_count = qkv_ref.shape[1]
    tiles = tok_count // TILE
    packed = slots * marks
    at = pl.multiple_of(step * TILE, TILE)

    @pl.when(step == 0)
    def _():
        mark_ref[...] = jnp.zeros_like(mark_ref)
        vsum[...] = jnp.zeros_like(vsum)
        vpad[:, :SUB] = jnp.zeros((width, SUB), low)
        vpad[:, tok_count + SUB :] = jnp.zeros((width, SUB), low)

    rows = (mul_t(weight_ref[...], tok_ref[...]) + bias_ref[...]).astype(low)
    qkv_ref[:, pl.ds(at, TILE)] = rows
    vpad[:, pl.ds(pl.multiple_of(at + SUB, SUB), TILE)] = rows[2 * width :]
    member, inv_count = slot_marks(len_ref, at, slots, marks, TILE)
    mark_ref[...] += mul_t(member.astype(low), rows[: 2 * width])
    vsum[...] += mul_t(jnp.ones((8, TILE), low), rows[2 * width :])
    first_ref[:, pl.ds(at, TILE)] = jnp.zeros((width, TILE), low)
    last_ref[:, pl.ds(at, TILE)] = jnp.zeros((width, TILE), low)
    mixed_ref[:, pl.ds(at, TILE)] = jnp.zeros((width, TILE), low)

    @pl.when(step == tiles - 1)
    def _():
        mark_ref[...] = mark_ref[...] * inv_count
        head_blocks = block_grid(width, width)
        slot_blocks = block_grid(packed, packed)
        eye = eye_pack(packed)
        scale = HEAD_DIM ** -0.5

        middles, inverses_t, products = [], [], []
        bound_total = jnp.zeros((1, 1), f32)
        lane_slot = lax.broadcasted_iota(jnp.int32, (1, packed), 1) // marks
        for h in range(heads):
            q_marks = mark_ref[:, h * HEAD_DIM : (h + 1) * HEAD_DIM]
            k_marks = mark_ref[:, width + h * HEAD_DIM : width + (h + 1) * HEAD_DIM]
            sim = wide(mul_t, q_marks, k_marks) * scale
            sim = jnp.where(slot_blocks, sim, -1e30)
            sim = jnp.exp(sim - jnp.max(sim, axis=1, keepdims=True))
            sim = sim / jnp.sum(sim, axis=1, keepdims=True)
            middle = fold(sim, slot_blocks)
            col_sums = jnp.sum(middle, axis=0, keepdims=True)
            bound = jnp.zeros((1, packed), f32)
            for s in range(slots):
                top = jnp.max(jnp.where(lane_slot == s, col_sums, 0.0), axis=1, keepdims=True)
                bound = jnp.where(lane_slot == s, top, bound)
                bound_total += jnp.where(len_ref[s] > 0, top, 0.0)
            middle_ref[h] = middle
            middles.append(middle)
            inverses_t.append(middle / bound)
            products.append(pack_mul_t(middle, middle, slot_blocks) / bound)
        bound_ref[...] = jnp.broadcast_to(bound_total, bound_ref.shape)

        def newton(n, carry):
            out = []
            for h in range(heads):
                inverse_t, product = carry[h]
                square = pack_mul(product, product, slot_blocks)
                cube = pack_mul(product, square, slot_blocks)
                fourth = pack_mul(square, square, slot_blocks)
                second = 15.0 * eye - 7.0 * product + square
                third = 13.0 * eye - 15.0 * product + 7.0 * square - cube
                steps_ref[n, 0, h] = product
                steps_ref[n, 1, h] = second
                steps_ref[n, 2, h] = third
                steps_ref[n, 3, h] = inverse_t
                out.append(
                    (
                        0.25 * pack_mul(third, inverse_t, slot_blocks),
                        0.25 * (13.0 * product - 15.0 * square + 7.0 * cube - fourth),
                    )
                )
            return tuple(out)

        final = lax.fori_loop(0, PINV_ITERS, newton, tuple(zip(inverses_t, products)))
        for h in range(heads):
            inverse_ref[h] = final[h][0]

        def one_slot(s, _):
            start, end = slot_bounds(len_ref, s, slots)
            lo, hi = start // TILE, (end + TILE - 1) // TILE
            hi = jnp.where(end > start, hi, lo)
            own = mark_ref[pl.ds(pl.multiple_of(s * marks, marks), marks), :] * scale
            q_block = spread(own[:, :width], head_blocks).astype(low)
            k_block = spread(own[:, width:], head_blocks).astype(low)

            def score_tile(n, top):
                t = pl.multiple_of(n * TILE, TILE)
                mask = lane_mask(start, end, t, TILE)
                sim = mul(k_block, qkv_ref[:width, pl.ds(t, TILE)])
                sim = sim.reshape(heads, marks, TILE)
                sim = jnp.exp(sim - jnp.max(sim, axis=1, keepdims=True))
                sim = sim / jnp.sum(sim, axis=1, keepdims=True)
                sim = sim.reshape(width, TILE)
                old = first_ref[:, pl.ds(t, TILE)].astype(f32)
                first_ref[:, pl.ds(t, TILE)] = jnp.where(mask, sim, old).astype(low)
                sim = mul(q_block, qkv_ref[width : 2 * width, pl.ds(t, TILE)])
                sim = jnp.where(mask, sim, mask_fill)
                scores[:, pl.ds(t, TILE)] = sim
                for c in range(TILE // SUB):
                    top = jnp.maximum(top, sim[:, c * SUB : (c + 1) * SUB])
                return top

            top = lax.fori_loop(lo, hi, score_tile, jnp.full((width, SUB), mask_fill, f32))
            top = jnp.max(top, axis=1, keepdims=True)

            def value_tile(n, carry):
                denom, total = carry
                t = pl.multiple_of(n * TILE, TILE)
                mask = lane_mask(start, end, t, TILE)
                part = jnp.exp(scores[:, pl.ds(t, TILE)] - top)
                old = last_ref[:, pl.ds(t, TILE)].astype(f32)
                last_ref[:, pl.ds(t, TILE)] = jnp.where(mask, part, old).astype(low)
                total = total + mul_t(part.astype(low), qkv_ref[2 * width :, pl.ds(t, TILE)])
                for c in range(TILE // SUB):
                    denom = denom + part[:, c * SUB : (c + 1) * SUB]
                return denom, total

            denom, total = lax.fori_loop(
                lo, hi, value_tile,
                (jnp.zeros((width, SUB), f32), jnp.zeros((width, width), f32)),
            )
            denom = jnp.sum(denom, axis=1, keepdims=True)
            inv = 1.0 / jnp.where(denom > 0.0, denom, 1.0)
            denom_ref[s] = inv
            values = fold(total * inv, head_blocks)
            values = jnp.where(end > start, values, vsum[:1] / tok_count)
            value_ref[pl.ds(pl.multiple_of(s * marks, marks), marks), :] = values
            return 0

        lax.fori_loop(0, slots, one_slot, 0)

        lane_head = lax.broadcasted_iota(jnp.int32, (1, width), 1) // HEAD_DIM
        inner = jnp.zeros((packed, width), f32)
        for h in range(heads):
            inverse = pack_mul_t(eye, final[h][0], slot_blocks)
            own_values = jnp.where(lane_head == h, value_ref[...], 0.0)
            inner = inner + wide(mul, spread(inverse, slot_blocks), own_values)
        inner_ref[...] = inner

        bands = [band(conv_ref[h : h + 1, :], taps).astype(low) for h in range(heads)]

        def out_slot(s, _):
            start, end = slot_bounds(len_ref, s, slots)
            lo, hi = start // TILE, (end + TILE - 1) // TILE
            hi = jnp.where(end > start, hi, lo)
            own = inner_ref[pl.ds(pl.multiple_of(s * marks, marks), marks), :]
            a_block = jnp.transpose(spread(own, head_blocks)).astype(low)

            def out_tile(n, _):
                t = pl.multiple_of(n * TILE, TILE)
                mask = lane_mask(start, end, t, TILE)
                rows = mul(a_block, first_ref[:, pl.ds(t, TILE)])
                rows = rows + convolve(vpad, bands, start, end, t, heads)
                old = mixed_ref[:, pl.ds(t, TILE)].astype(f32)
                mixed_ref[:, pl.ds(t, TILE)] = jnp.where(mask, rows, old).astype(low)
                return 0

            return lax.fori_loop(lo, hi, out_tile, 0)

        lax.fori_loop(0, slots, out_slot, 0)


def windows(padded, start, end, t):
    full = padded[:, pl.ds(t, TILE + 2 * SUB)]
    keep = lane_mask(start, end, t - SUB, TILE + 2 * SUB)
    return jnp.where(keep, full.astype(f32), 0.0).astype(low)


def convolve(padded, bands, start, end, t, heads):
    full = windows(padded, start, end, t)
    out = []
    count = TILE // SUB
    for h in range(heads):
        own = full[h * HEAD_DIM : (h + 1) * HEAD_DIM]
        stack = jnp.concatenate(
            [own[:, c * SUB : (c + 3) * SUB] for c in range(count)], axis=0
        )
        res = mul_t(stack, bands[h])
        out.append(
            jnp.concatenate(
                [res[c * HEAD_DIM : (c + 1) * HEAD_DIM] for c in range(count)], axis=1
            )
        )
    return jnp.concatenate(out, axis=0)


def mix_backward_kernel(
    slots, marks, taps,
    len_ref, grad_ref, qkv_ref, first_ref, last_ref, mark_ref, value_ref, inner_ref,
    denom_ref, middle_ref, steps_ref, inverse_ref, conv_ref,
    out_ref, bias_ref, conv_out_ref,
    gpad, vpad, ds_first, ds_last, conv_grad, d_inner, d_k, d_q, d_value,
):
    width = first_ref.shape[0]
    heads = width // HEAD_DIM
    tok_count = qkv_ref.shape[1]
    packed = slots * marks
    scale = HEAD_DIM ** -0.5
    head_blocks = block_grid(width, width)
    slot_blocks = block_grid(packed, packed)
    eye = eye_pack(packed)
    count = TILE // SUB

    for padded, source in ((gpad, grad_ref[...]), (vpad, qkv_ref[2 * width :, :])):
        padded[:, :SUB] = jnp.zeros((width, SUB), low)
        padded[:, tok_count + SUB :] = jnp.zeros((width, SUB), low)
        padded[:, SUB : tok_count + SUB] = source
    out_ref[...] = jnp.zeros_like(out_ref)
    ds_first[...] = jnp.zeros_like(ds_first)
    ds_last[...] = jnp.zeros_like(ds_last)
    conv_grad[...] = jnp.zeros_like(conv_grad)

    def reach(s):
        start, end = slot_bounds(len_ref, s, slots)
        lo, hi = start // TILE, (end + TILE - 1) // TILE
        return start, end, lo, jnp.where(end > start, hi, lo)

    def own_rows(s):
        return pl.ds(pl.multiple_of(s * marks, marks), marks)

    def first_slot(s, _):
        start, end, lo, hi = reach(s)
        a_block = spread(inner_ref[own_rows(s), :], head_blocks).astype(low)

        def tile(n, carry):
            inner_total, key_total = carry
            t = pl.multiple_of(n * TILE, TILE)
            mask = lane_mask(start, end, t, TILE)
            own_grad = grad_ref[:, pl.ds(t, TILE)]
            kernel_rows = jnp.where(mask, first_ref[:, pl.ds(t, TILE)].astype(f32), 0.0)
            d_kernel = mul(a_block, own_grad)
            prod = (kernel_rows * d_kernel).reshape(heads, marks, TILE)
            row_sum = jnp.sum(prod, axis=1, keepdims=True)
            d_sim = prod - kernel_rows.reshape(heads, marks, TILE) * row_sum
            d_sim = d_sim.reshape(width, TILE)
            d_sim_low = d_sim.astype(low)
            old = ds_first[:, pl.ds(t, TILE)].astype(f32)
            ds_first[:, pl.ds(t, TILE)] = jnp.where(mask, d_sim, old).astype(low)
            inner_total = inner_total + mul_t(kernel_rows.astype(low), own_grad)
            key_total = key_total + mul_t(d_sim_low, qkv_ref[:width, pl.ds(t, TILE)])
            full = windows(vpad, start, end, t)
            grad_own = jnp.where(mask, own_grad.astype(f32), 0.0).astype(low)
            for h in range(heads):
                sel = slice(h * HEAD_DIM, (h + 1) * HEAD_DIM)
                left = jnp.concatenate(
                    [grad_own[sel, c * SUB : (c + 1) * SUB] for c in range(count)], axis=0
                )
                right = jnp.concatenate(
                    [full[sel, c * SUB : (c + 3) * SUB] for c in range(count)], axis=0
                )
                conv_grad[h] += lax.dot_general(
                    left, right, (((0,), (0,)), ((), ())), preferred_element_type=f32
                )
            return inner_total, key_total

        zero = jnp.zeros((width, width), f32)
        inner_total, key_total = lax.fori_loop(lo, hi, tile, (zero, zero))
        d_inner[own_rows(s), :] = fold(inner_total, head_blocks)
        d_k[own_rows(s), :] = fold(key_total, head_blocks) * scale
        return 0

    lax.fori_loop(0, slots, first_slot, 0)

    row = lax.broadcasted_iota(jnp.int32, (SUB, 3 * SUB), 0)
    col = lax.broadcasted_iota(jnp.int32, (SUB, 3 * SUB), 1)
    off = col - row - (SUB - taps // 2)
    tap_lane = lax.broadcasted_iota(jnp.int32, (1, SUB), 1)
    for h in range(heads):
        found = jnp.zeros((1, SUB), f32)
        square = conv_grad[h]
        for n in range(taps):
            part = jnp.sum(jnp.where(off == n, square, 0.0), axis=0, keepdims=True)
            part = jnp.sum(part, axis=1, keepdims=True)
            found = jnp.where(tap_lane == n, part, found)
        conv_out_ref[h : h + 1, :] = found

    lane_head = lax.broadcasted_iota(jnp.int32, (1, width), 1) // HEAD_DIM
    value_total = jnp.zeros((packed, width), f32)
    d_inverses = []
    for h in range(heads):
        own = jnp.where(lane_head == h, d_inner[...], 0.0)
        value_total = value_total + wide(mul, spread(inverse_ref[h], slot_blocks), own)
        d_inverses.append(fold(wide(mul_t, own, value_ref[...]), slot_blocks))
    d_value[...] = value_total

    middles_t = [pack_mul_t(eye, middle_ref[h], slot_blocks) for h in range(heads)]

    def newton(k, carry):
        n = PINV_ITERS - 1 - k
        out = []
        for h in range(heads):
            d_inverse, d_middle = carry[h]
            product = steps_ref[n, 0, h]
            second = steps_ref[n, 1, h]
            third = steps_ref[n, 2, h]
            inverse_t = steps_ref[n, 3, h]
            middle_t = middles_t[h]
            d_third = 0.25 * pack_mul(inverse_t, d_inverse, slot_blocks)
            d_second = -pack_mul(product, d_third, slot_blocks)
            d_first = -pack_mul(product, d_second, slot_blocks)
            d_product = (
                -pack_mul(d_third, second, slot_blocks)
                - pack_mul(d_second, 7.0 * eye - product, slot_blocks)
                - d_first
            )
            d_middle = d_middle + pack_mul(d_product, inverse_t, slot_blocks)
            d_inverse = 0.25 * pack_mul(d_inverse, third, slot_blocks) + pack_mul(
                middle_t, d_product, slot_blocks
            )
            out.append((d_inverse, d_middle))
        return tuple(out)

    zero = jnp.zeros((HEAD_DIM, packed), f32)
    final = lax.fori_loop(0, PINV_ITERS, newton, tuple((x, zero) for x in d_inverses))
    lane_slot = lax.broadcasted_iota(jnp.int32, (1, packed), 1) // marks
    dq_total = jnp.zeros((packed, width), f32)
    dk_total = jnp.zeros((packed, width), f32)
    for h in range(heads):
        d_inverse, d_middle = final[h]
        middle = middle_ref[h]
        first_t = steps_ref[0, 3, h]
        d_inverse_t = pack_mul_t(eye, d_inverse, slot_blocks)
        col_sums = jnp.sum(middle, axis=0, keepdims=True)
        share = jnp.sum(d_inverse_t * first_t, axis=0, keepdims=True)
        bound = jnp.zeros((1, packed), f32)
        d_bound = jnp.zeros((1, packed), f32)
        hits = jnp.zeros((1, packed), f32)
        for s in range(slots):
            mine = lane_slot == s
            top = jnp.max(jnp.where(mine, col_sums, 0.0), axis=1, keepdims=True)
            total = jnp.sum(jnp.where(mine, share, 0.0), axis=1, keepdims=True)
            number = jnp.sum(
                jnp.where(mine & (col_sums == top), 1.0, 0.0), axis=1, keepdims=True
            )
            bound = jnp.where(mine, top, bound)
            d_bound = jnp.where(mine, -total / top, d_bound)
            hits = jnp.where(mine, number, hits)
        d_middle = d_middle + d_inverse_t / bound
        d_middle = d_middle + jnp.where(col_sums == bound, d_bound / hits, 0.0)
        prod = spread(middle * d_middle, slot_blocks)
        d_sim = prod - spread(middle, slot_blocks) * jnp.sum(prod, axis=1, keepdims=True)
        d_sim = d_sim * scale
        own = lane_head == h
        q_marks = jnp.where(own, mark_ref[:, :width], 0.0)
        k_marks = jnp.where(own, mark_ref[:, width:], 0.0)
        dq_total = dq_total + wide(mul, d_sim, k_marks)
        dk_total = dk_total + wide(mul, jnp.transpose(d_sim), q_marks)
    d_q[...] = dq_total
    d_k[...] += dk_total

    flipped = []
    for h in range(heads):
        flipped.append(
            band(
                jnp.concatenate(
                    [conv_ref[h : h + 1, n : n + 1] for n in reversed(range(taps))], axis=1
                ),
                taps,
            ).astype(low)
        )

    def last_slot(s, _):
        start, end, lo, hi = reach(s)
        inv = denom_ref[s]
        own_d = d_value[own_rows(s), :]
        own_v = value_ref[own_rows(s), :]
        d_block = spread(own_d, head_blocks)
        row_sum = jnp.sum(
            d_block * jnp.concatenate([own_v] * heads, axis=0), axis=1, keepdims=True
        )
        row_sum = row_sum * inv
        d_block = d_block * inv
        d_block_t = jnp.transpose(d_block).astype(low)
        d_block = d_block.astype(low)

        def tile(n, query_total):
            t = pl.multiple_of(n * TILE, TILE)
            mask = lane_mask(start, end, t, TILE)
            kernel_rows = jnp.where(mask, last_ref[:, pl.ds(t, TILE)].astype(f32), 0.0)
            v_rows = qkv_ref[2 * width :, pl.ds(t, TILE)]
            d_sim = kernel_rows * (mul(d_block, v_rows) - row_sum)
            d_low = d_sim.astype(low)
            old = ds_last[:, pl.ds(t, TILE)].astype(f32)
            ds_last[:, pl.ds(t, TILE)] = jnp.where(mask, d_sim, old).astype(low)
            dv = mul(d_block_t, kernel_rows.astype(low))
            dv = dv + convolve(gpad, flipped, start, end, t, heads)
            old = out_ref[2 * width :, pl.ds(t, TILE)].astype(f32)
            out_ref[2 * width :, pl.ds(t, TILE)] = jnp.where(mask, dv, old).astype(low)
            return query_total + mul_t(d_low, qkv_ref[width : 2 * width, pl.ds(t, TILE)])

        query_total = lax.fori_loop(lo, hi, tile, jnp.zeros((width, width), f32))
        d_q[own_rows(s), :] += fold(query_total, head_blocks) * scale
        return 0

    lax.fori_loop(0, slots, last_slot, 0)

    inv_count = slot_marks(len_ref, 0, slots, marks, SUB)[1]
    d_q[...] = d_q[...] * inv_count
    d_k[...] = d_k[...] * inv_count

    def final_slot(s, _):
        start, end, lo, hi = reach(s)
        length = end - start
        own = mark_ref[own_rows(s), :] * scale

        def left(block, d_mark):
            wide_rows = jnp.concatenate([spread(block, head_blocks), d_mark], axis=0)
            return jnp.transpose(wide_rows).astype(low)

        q_left = left(own[:, width:], d_q[own_rows(s), :])
        k_left = left(own[:, :width], d_k[own_rows(s), :])
        mark = lax.broadcasted_iota(jnp.int32, (marks, 1), 0)
        lower = start + (mark * length) // marks
        upper = start + ((mark + 1) * length) // marks

        def tile(n, _):
            t = pl.multiple_of(n * TILE, TILE)
            mask = lane_mask(start, end, t, TILE)
            tok = t + lax.broadcasted_iota(jnp.int32, (marks, TILE), 1)
            member = jnp.where((tok >= lower) & (tok < upper), 1.0, 0.0).astype(low)
            for at, lhs, source in ((0, q_left, ds_first), (width, k_left, ds_last)):
                rhs = jnp.concatenate([source[:, pl.ds(t, TILE)], member], axis=0)
                rows = mul(lhs, rhs)
                old = out_ref[at : at + width, pl.ds(t, TILE)].astype(f32)
                out_ref[at : at + width, pl.ds(t, TILE)] = jnp.where(mask, rows, old).astype(low)
            return 0

        return lax.fori_loop(lo, hi, tile, 0)

    lax.fori_loop(0, slots, final_slot, 0)

    def bias_tile(n, carry):
        t = pl.multiple_of(n * TILE, TILE)
        q_sum, v_sum = carry
        q_rows = out_ref[:width, pl.ds(t, TILE)].astype(f32)
        v_rows = out_ref[2 * width :, pl.ds(t, TILE)].astype(f32)
        for c in range(count):
            q_sum = q_sum + q_rows[:, c * SUB : (c + 1) * SUB]
            v_sum = v_sum + v_rows[:, c * SUB : (c + 1) * SUB]
        return q_sum, v_sum

    zero = jnp.zeros((width, SUB), f32)
    q_sum, v_sum = lax.fori_loop(0, tok_count // TILE, bias_tile, (zero, zero))
    bias_ref[:, 0:1] = jnp.sum(q_sum, axis=1, keepdims=True)
    bias_ref[:, 1:2] = jnp.sum(v_sum, axis=1, keepdims=True)


def mix_forward(seq_lengths, tokens, weight_t, bias_col, conv_own, slots, marks):
    tok_count, model = tokens.shape
    width = weight_t.shape[0] // 3
    heads = width // HEAD_DIM
    packed = slots * marks
    taps = conv_own.shape[1]
    whole = lambda *shape: pl.BlockSpec(shape, lambda i, lens: (0,) * len(shape))
    shapes = [
        ((3 * width, tok_count), low),
        ((width, tok_count), low),
        ((width, tok_count), low),
        ((width, tok_count), low),
        ((packed, 2 * width), f32),
        ((packed, width), f32),
        ((packed, width), f32),
        ((slots, width, 1), f32),
        ((heads, HEAD_DIM, packed), f32),
        ((PINV_ITERS, 4, heads, HEAD_DIM, packed), f32),
        ((heads, HEAD_DIM, packed), f32),
        ((8, 128), f32),
    ]
    return pl.pallas_call(
        partial(mix_forward_kernel, slots, marks, taps),
        out_shape=[jax.ShapeDtypeStruct(s, t) for s, t in shapes],
        grid_spec=pltpu.PrefetchScalarGridSpec(
            num_scalar_prefetch=1,
            grid=(tok_count // TILE,),
            in_specs=[
                pl.BlockSpec((TILE, model), lambda i, lens: (i, 0)),
                whole(3 * width, model),
                whole(3 * width, 1),
                whole(heads, taps),
            ],
            out_specs=[whole(*s) for s, _ in shapes],
            scratch_shapes=[
                pltpu.VMEM((width, tok_count + 2 * SUB), low),
                pltpu.VMEM((width, tok_count), f32),
                pltpu.VMEM((8, width), f32),
            ],
        ),
        compiler_params=pltpu.CompilerParams(vmem_limit_bytes=56 * 1024 * 1024),
        name="mix_forward",
    )(seq_lengths, tokens, weight_t, bias_col, conv_own)


def mix_backward(seq_lengths, grad_t, saved, conv_own, slots, marks):
    qkv_t, first, last, mark, value, inner, denom, middle, steps, inverse = saved
    width, tok_count = grad_t.shape
    heads = width // HEAD_DIM
    packed = slots * marks
    taps = conv_own.shape[1]
    args = (grad_t, qkv_t, first, last, mark, value, inner, denom, middle, steps, inverse, conv_own)
    whole = lambda shape: pl.BlockSpec(
        shape, lambda i, lens: (0,) * len(shape), pipeline_mode=pl.Buffered(1)
    )
    shapes = [((3 * width, tok_count), low), ((width, 2), f32), ((heads, SUB), f32)]
    square = pltpu.VMEM((packed, width), f32)
    return pl.pallas_call(
        partial(mix_backward_kernel, slots, marks, taps),
        out_shape=[jax.ShapeDtypeStruct(s, t) for s, t in shapes],
        grid_spec=pltpu.PrefetchScalarGridSpec(
            num_scalar_prefetch=1,
            grid=(1,),
            in_specs=[whole(x.shape) for x in args],
            out_specs=[whole(s) for s, _ in shapes],
            scratch_shapes=[
                pltpu.VMEM((width, tok_count + 2 * SUB), low),
                pltpu.VMEM((width, tok_count + 2 * SUB), low),
                pltpu.VMEM((width, tok_count), low),
                pltpu.VMEM((width, tok_count), low),
                pltpu.VMEM((heads, SUB, 3 * SUB), f32),
                square, square, square, square,
            ],
        ),
        compiler_params=pltpu.CompilerParams(vmem_limit_bytes=56 * 1024 * 1024),
        name="mix_backward",
    )(seq_lengths, *args)


contract_rows = (((0,), (0,)), ((), ()))
contract_cols = (((1,), (1,)), ((), ()))
norm_eps = 1e-05


def split_up(x, dim, peers):
    before, after = (x.shape[:dim], x.shape[dim + 1 :])
    return jnp.moveaxis(x.reshape(*before, peers, -1, *after), dim, 0)


def sum_at_owner(x, axis, dim):
    peers = lax.axis_size(axis)
    tiles = lax.all_to_all(split_up(x, dim, peers), axis, 0, 0, tiled=True)
    return jnp.sum(tiles.astype(f32), axis=0)


def layer_norm(row_data, gain_vec, shift_vec):
    centre = row_data - jnp.mean(row_data, axis=1, keepdims=True)
    spread_row = jnp.mean(centre * centre, axis=1, keepdims=True)
    return centre * lax.rsqrt(spread_row + norm_eps) * gain_vec[None, :] + shift_vec[None, :]


def gelu_exact(values):
    return jax.nn.gelu(values, approximate=False)


def body(
    tokens,
    qkv_weight,
    qv_bias,
    conv_weight,
    out_weight,
    out_bias,
    norm1_gain,
    norm1_bias,
    ffn_in_weight,
    ffn_in_bias,
    ffn_out_weight,
    ffn_out_bias,
    norm2_gain,
    norm2_bias,
    cotangent,
    seq_lengths,
    segment_ids,
    landmark_bounds,
):
    tok_count, model_width = tokens.shape
    head_width = qkv_weight.shape[2]
    heads_here = head_width // HEAD_DIM
    head_total = conv_weight.shape[0]
    kernel_taps = conv_weight.shape[1]
    slots, marks = landmark_bounds.shape
    quarter = tok_count // lax.axis_size("heads")
    head_index = lax.axis_index("heads")
    own_start = head_index * quarter
    both = ("batch", "heads")
    own_rows_low = lax.dynamic_slice_in_dim(tokens, own_start, quarter, 0)
    own_tokens = own_rows_low.astype(f32)
    conv_own = lax.dynamic_slice_in_dim(conv_weight, head_index * heads_here, heads_here, 0)
    qv_own = lax.dynamic_slice_in_dim(qv_bias, head_index * head_width, head_width, 1)
    flat_qkv = qkv_weight.reshape(model_width, 3 * head_width)
    bias_col = jnp.concatenate([qv_own[0], jnp.zeros_like(qv_own[0]), qv_own[1]])[:, None]
    forward = mix_forward(
        seq_lengths, tokens, jnp.transpose(flat_qkv), bias_col, conv_own, slots, marks
    )
    qkv_t, first, last, mixed_t, mark, value, inner, denom, middle, steps, inverse, bound = forward
    bound_total = bound[0, 0]
    attn_part = lax.psum_scatter(
        lax.dot_general(mixed_t, out_weight, contract_rows, preferred_element_type=f32).astype(low),
        "heads",
        scatter_dimension=0,
        tiled=True,
    ).astype(f32)
    live_count = jnp.sum((seq_lengths > 0).astype(f32)) * heads_here
    first_res = own_tokens + attn_part + out_bias[None, :]
    norm1_out, norm1_pull = jax.vjp(layer_norm, first_res, norm1_gain, norm1_bias)
    norm1_low = norm1_out.astype(low)
    ff_own = ffn_out_weight.shape[0]
    bias_row = jnp.zeros((16, model_width), low).at[0, :ff_own].set(ffn_in_bias)
    whole_in = lax.all_gather(ffn_in_weight, both, axis=1, tiled=True)
    out_pack = lax.all_gather(jnp.concatenate([ffn_out_weight, bias_row], axis=0), both, axis=0)
    whole_out = out_pack[:, :ff_own].reshape(-1, model_width)
    whole_in_bias = out_pack[:, ff_own, :ff_own].reshape(-1)
    pre_act = (
        jnp.dot(norm1_low, whole_in, preferred_element_type=f32)
        + whole_in_bias.astype(f32)[None, :]
    )
    hidden_act, gelu_pull = jax.vjp(gelu_exact, pre_act)
    hidden_low = hidden_act.astype(low)
    ffn_result = jnp.dot(hidden_low, whole_out, preferred_element_type=f32) + ffn_out_bias[None, :]
    final_out, norm2_pull = jax.vjp(layer_norm, norm1_out + ffn_result, norm2_gain, norm2_bias)
    grad_second, grad_gain_two, grad_shift_two = norm2_pull(cotangent.astype(f32))
    grad_ffn_low = grad_second.astype(low)
    grad_ffn_bias = jnp.sum(grad_ffn_low.astype(f32), axis=0)
    down_term = lax.dot_general(
        hidden_low, grad_ffn_low, contract_rows, preferred_element_type=f32
    ).astype(low)
    grad_hidden = lax.dot_general(
        grad_ffn_low, whole_out, contract_cols, preferred_element_type=f32
    )
    grad_pre = gelu_pull(grad_hidden)[0].astype(low)
    grad_in_bias = jnp.sum(grad_pre.astype(f32), axis=0)
    up_term = lax.dot_general(
        norm1_low, grad_pre, contract_rows, preferred_element_type=f32
    ).astype(low)
    grad_norm1 = grad_second + lax.dot_general(
        grad_pre, whole_in, contract_cols, preferred_element_type=f32
    )
    grad_first, grad_gain_one, grad_shift_one = norm1_pull(grad_norm1)
    grad_attn_low = grad_first.astype(low)
    grad_out_bias = jnp.sum(grad_attn_low.astype(f32), axis=0)
    piece_rows = lax.all_gather(grad_attn_low, "heads", axis=0, tiled=True)
    grad_mix_t = lax.dot_general(
        out_weight, piece_rows, contract_cols, preferred_element_type=f32
    ).astype(low)
    grad_mix_t, down_term, up_term = lax.optimization_barrier((grad_mix_t, down_term, up_term))
    up_share = lax.psum_scatter(up_term, both, scatter_dimension=1, tiled=True).astype(f32)
    down_share = lax.psum_scatter(down_term, both, scatter_dimension=0, tiled=True).astype(f32)
    saved = (qkv_t, first, last, mark, value, inner, denom, middle, steps, inverse)
    grad_t, grad_bias, grad_conv = mix_backward(
        seq_lengths, grad_mix_t, saved, conv_own, slots, marks
    )
    out_part = lax.dot_general(
        mixed_t, piece_rows, (((1,), (0,)), ((), ())), preferred_element_type=f32
    )
    grad_qv_own = jnp.transpose(grad_bias)
    qkv_part = lax.dot_general(
        tokens, grad_t, (((0,), (1,)), ((), ())), preferred_element_type=f32
    ).reshape(model_width, 3, head_width)
    input_part = lax.psum_scatter(
        lax.dot_general(
            grad_t, flat_qkv, (((0,), (1,)), ((), ())), preferred_element_type=f32
        ).astype(low),
        "heads",
        scatter_dimension=0,
        tiled=True,
    ).astype(f32)
    input_grad = grad_first + input_part
    conv_full = lax.dynamic_update_slice_in_dim(
        jnp.zeros((head_total, kernel_taps), f32),
        grad_conv[:, :kernel_taps],
        head_index * heads_here,
        0,
    )
    bias_full = lax.dynamic_update_slice_in_dim(
        jnp.zeros((2, head_total * HEAD_DIM), f32), grad_qv_own, head_index * head_width, 1
    )
    qkv_share, out_share = (
        sum_at_owner(qkv_part.astype(low), "batch", 0),
        sum_at_owner(out_part.astype(low), "batch", 1),
    )
    vector_all = jnp.stack(
        [grad_ffn_bias, grad_gain_two, grad_shift_two, grad_gain_one, grad_shift_one, grad_out_bias]
    )
    in_bias_share, vector_share = (
        lax.psum_scatter(grad_in_bias, both, scatter_dimension=0, tiled=True),
        lax.psum_scatter(vector_all, both, scatter_dimension=1, tiled=True),
    )
    conv_sum, bias_sum, bound_all, count_all = lax.psum(
        (conv_full, bias_full, bound_total, live_count), both
    )
    conv_out = lax.dynamic_slice_in_dim(conv_sum, head_index * heads_here, heads_here, 0)
    bias_out = lax.dynamic_slice_in_dim(bias_sum, head_index * head_width, head_width, 1)
    condition = bound_all / count_all
    return (
        final_out.astype(low),
        input_grad,
        qkv_share,
        bias_out,
        conv_out,
        out_share,
        up_share,
        in_bias_share,
        down_share,
        vector_share,
        condition,
    )


def place():
    b, z = lax.axis_index("batch"), lax.axis_index("heads")
    core, x, y = b % 2, (b // 2) % 2, b // 4
    return b, z, b + 1 - 2 * core, b + 2 - 4 * x, b + 4 - 8 * y


def remote(src, dst, send, recv, device):
    return pltpu.make_async_remote_copy(
        src_ref=src,
        dst_ref=dst,
        send_sem=send,
        recv_sem=recv,
        device_id=device,
        device_id_type=pl.DeviceIdType.MESH,
    )


def greet(devices):
    barrier = pltpu.get_barrier_semaphore()
    for device in devices:
        pl.semaphore_signal(
            barrier, inc=1, device_id=device, device_id_type=pl.DeviceIdType.MESH
        )
    pl.semaphore_wait(barrier, len(devices))


def exchange_kernel(
    pieces,
    mixed_ref, in_ref, down_ref, misc_ref,
    all_ref, in_all, down_all, misc_all,
    a_send, a_recv, l_send, l_recv, p_send, p_recv, own_sem,
):
    b, z, bc, bx, by = place()
    peers = [(b, lax.rem(z + i, 4)) for i in (1, 2, 3)]
    greet(peers + [(bc, z), (bx, z), (by, z)])
    quarter = all_ref.shape[2]
    owns = (in_ref, down_ref, misc_ref)
    alls = (in_all, down_all, misc_all)

    local = [
        pltpu.make_async_copy(own, everything.at[b, z], own_sem.at[n])
        for n, (own, everything) in enumerate(zip(owns, alls))
    ]

    def columns(n):
        return pl.ds(pl.multiple_of(n * quarter, quarter), quarter)

    local.append(
        pltpu.make_async_copy(mixed_ref.at[:, columns(z)], all_ref.at[z], own_sem.at[3])
    )
    for copy in local:
        copy.start()

    def line(up, hop, n):
        array, start, count, _ = pieces[n]
        rows = pl.ds(start, count)
        origin = z - hop + 1 if up else z + hop - 1
        dst = alls[array].at[b, origin, rows]
        src = owns[array].at[rows] if hop == 1 else dst
        side = 0 if up else 1
        return remote(
            src, dst, l_send.at[side, hop - 1, n], l_recv.at[side, hop - 1, n],
            (b, z + 1 if up else z - 1),
        )

    def line_in(up, hop, n):
        array, start, count, _ = pieces[n]
        origin = z - hop if up else z + hop
        dst = alls[array].at[b, origin, pl.ds(start, count)]
        side = 0 if up else 1
        return remote(
            dst, dst, l_send.at[side, hop - 1, n], l_recv.at[side, hop - 1, n],
            (b, z - 1 if up else z + 1),
        )

    def has(up, hop):
        return z >= hop if up else z <= 3 - hop

    def sends(up, hop):
        return ((z < 3) & (z >= hop - 1)) if up else ((z > 0) & (z <= 4 - hop))

    count = len(pieces)
    for n in range(count):
        for up in (True, False):

            @pl.when(sends(up, 1))
            def _():
                line(up, 1, n).start()

    def block(n, who):
        array, start, rows, _ = pieces[n]
        return alls[array].at[who, :, pl.ds(start, rows)]

    def pair(n, slot, who, device):
        ref = block(n, who)
        return remote(ref, ref, p_send.at[n, slot], p_recv.at[n, slot], (device, z))

    both = bx + by - b
    issued = []

    def first(n):
        p = by if pieces[n][3] else bx
        copy = pair(n, 0, b, p)
        copy.start()
        issued.append(copy)

    def second(n):
        p, q = (by, bx) if pieces[n][3] else (bx, by)
        pair(n, 0, p, p).wait_recv()
        for slot, who in ((1, b), (2, p)):
            copy = pair(n, slot, who, q)
            copy.start()
            issued.append(copy)

    def third(n):
        p, q = (by, bx) if pieces[n][3] else (bx, by)
        pair(n, 1, q, q).wait_recv()
        pair(n, 2, both, q).wait_recv()
        for slot, who in enumerate((b, bx, by, both)):
            copy = pair(n, 3 + slot, who, bc)
            copy.start()
            issued.append(copy)

    def fourth(n):
        flip = bc - b
        for slot, who in enumerate((b, bx, by, both)):
            pair(n, 3 + slot, who + flip, bc).wait_recv()

    for copy in local:
        copy.wait()
    for n in range(count + 3):
        if n < count:
            for hop in (1, 2, 3):
                for up in (True, False):

                    @pl.when(has(up, hop))
                    def _():
                        line_in(up, hop, n).wait_recv()

                    if hop < 3:

                        @pl.when(sends(up, hop + 1))
                        def _():
                            line(up, hop + 1, n).start()

            first(n)
        if n == count - 1:
            for i, (_, to) in enumerate(peers):
                copy = remote(
                    mixed_ref.at[:, columns(to)], all_ref.at[z],
                    a_send.at[i], a_recv.at[i], (b, to),
                )
                copy.start()
                issued.append(copy)
        if 0 <= n - 1 < count:
            second(n - 1)
        if 0 <= n - 2 < count:
            third(n - 2)
        if 0 <= n - 3 < count:
            fourth(n - 3)
    for i in (1, 2, 3):
        source = lax.rem(z + 4 - i, 4)
        ref = all_ref.at[source]
        remote(ref, ref, a_send.at[i - 1], a_recv.at[i - 1], (b, source)).wait_recv()
    for n in range(count):
        for hop in (1, 2, 3):
            for up in (True, False):

                @pl.when(sends(up, hop))
                def _():
                    line(up, hop, n).wait_send()

    for copy in issued:
        copy.wait_send()


def exchange(mixed_t, in_own, down_own, misc_own):
    width, tok_count = mixed_t.shape
    ff, model = in_own.shape
    misc = misc_own.shape[0]
    half = ff // 2
    pieces = (
        (2, 0, misc, 0),
        (0, 0, half, 0), (1, 0, half, 1), (0, half, half, 0), (1, half, half, 1),
    )
    shape = lambda *s: jax.ShapeDtypeStruct(s, low)
    vmem = pl.BlockSpec(memory_space=pltpu.VMEM)
    hbm = pl.BlockSpec(memory_space=pl.ANY)
    dma = pltpu.SemaphoreType.DMA
    n = len(pieces)
    return pl.pallas_call(
        partial(exchange_kernel, pieces),
        out_shape=[
            shape(4, width, tok_count // 4),
            shape(8, 4, ff, model), shape(8, 4, ff, model), shape(8, 4, misc, model),
        ],
        in_specs=[vmem] * 4,
        out_specs=[hbm] * 4,
        scratch_shapes=[
            dma((3,)), dma((3,)), dma((2, 3, n)), dma((2, 3, n)), dma((n, 7)), dma((n, 7)),
            dma((4,)),
        ],
        compiler_params=pltpu.CompilerParams(collective_id=1, has_side_effects=True),
        name="exchange",
    )(mixed_t, in_own, down_own, misc_own)


def turn_kernel(grad_ref, out_ref, send, recv, own_sem):
    b, z, _, _, _ = place()
    peers = [(b, lax.rem(z + i, 4)) for i in (1, 2, 3)]
    greet(peers)
    width, quarter = out_ref.shape[0], grad_ref.shape[1]

    def rows(n):
        return pl.ds(pl.multiple_of(n * width, width), width)

    def columns(n):
        return pl.ds(pl.multiple_of(n * quarter, quarter), quarter)

    copies = []
    for i, (_, to) in enumerate(peers):
        copy = remote(
            grad_ref.at[rows(to)], out_ref.at[:, columns(z)], send.at[i], recv.at[i], (b, to)
        )
        copy.start()
        copies.append(copy)
    own = pltpu.make_async_copy(grad_ref.at[rows(z)], out_ref.at[:, columns(z)], own_sem.at[0])
    own.start()
    for i in (1, 2, 3):
        source = lax.rem(z + 4 - i, 4)
        ref = out_ref.at[:, columns(source)]
        remote(ref, ref, send.at[i - 1], recv.at[i - 1], (b, source)).wait_recv()
    for copy in copies:
        copy.wait_send()
    own.wait()


def turn(grad_all, width):
    quarter = grad_all.shape[1]
    dma = pltpu.SemaphoreType.DMA
    return pl.pallas_call(
        turn_kernel,
        out_shape=jax.ShapeDtypeStruct((width, 4 * quarter), low),
        in_specs=[pl.BlockSpec(memory_space=pltpu.VMEM)],
        out_specs=pl.BlockSpec(memory_space=pl.ANY),
        scratch_shapes=[dma((3,)), dma((3,)), dma((1,))],
        compiler_params=pltpu.CompilerParams(collective_id=2, has_side_effects=True),
        name="turn",
    )(grad_all)


def tail_kernel(
    part_ref, first_ref, down_ref, up_ref, outw_ref, qkvw_ref, small_ref,
    input_ref, down_own, up_own, outw_own, qkvw_own, small_out,
    up_in, down_in, core_down, core_up, core_outw, core_qkvw,
    one_down, one_up, one_outw, one_qkvw, two_down, two_up, two_outw, two_qkvw,
    z_down, z_up, z_outw, small_in,
    z_send, z_recv, c_send, c_recv, x_send, x_recv, e_send, e_recv, s_send, s_recv,
):
    b, z, bc, bx, by = place()
    both = bx + by - b
    flip = bc - b
    peers = [(b, lax.rem(z + i, 4)) for i in (1, 2, 3)]
    greet(peers + [(bc, z), (bx, z), (by, z)])
    chunks = up_in.shape[1]
    size = up_in.shape[2]
    issued = []

    fulls = (down_ref, up_ref, outw_ref, qkvw_ref)
    cores = (core_down, core_up, core_outw, core_qkvw)
    ones = (one_down, one_up, one_outw, one_qkvw)
    twos = (two_down, two_up, two_outw, two_qkvw)
    kinds = len(fulls)
    groups = (b, bx, by, both)

    def at(n, who):
        return fulls[n].at[:, who] if n == 2 else fulls[n].at[who]

    for slot, who in enumerate(groups):
        for n in range(kinds):
            copy = remote(
                at(n, who + flip), cores[n].at[slot], c_send.at[n, slot], c_recv.at[n, slot],
                (bc, z),
            )
            copy.start()
            issued.append(copy)

    def flow(up, owner, c):
        buf = up_in if up else down_in
        side = 0 if up else 1
        return remote(
            buf.at[owner, c], buf.at[owner, c], z_send.at[side, owner, c],
            z_recv.at[side, owner, c], (b, z + 1 if up else z - 1),
        )

    def flow_first(up, owner, c):
        buf = up_in if up else down_in
        side = 0 if up else 1
        return remote(
            part_ref.at[owner, c], buf.at[owner, c], z_send.at[side, owner, c],
            z_recv.at[side, owner, c], (b, z + 1 if up else z - 1),
        )

    def z_event(k, c):
        for up in (True, False):
            owner = 3 - k if up else k
            buf = up_in if up else down_in
            at_end = (z == 0) if up else (z == 3)
            inner = ((z > 0) & (z < owner)) if up else ((z < 3) & (z > owner))

            @pl.when(at_end)
            def _():
                flow_first(up, owner, c).start()

            @pl.when(inner)
            def _():
                flow(up, owner, c).wait_recv()
                buf[owner, c] = (
                    buf[owner, c].astype(f32) + part_ref[owner, c].astype(f32)
                ).astype(low)
                flow(up, owner, c).start()

    def core_event(n):
        for slot, who in enumerate(groups):
            ref = cores[n].at[slot]
            remote(ref, ref, c_send.at[n, slot], c_recv.at[n, slot], (bc, z)).wait_recv()
            mine = fulls[n][:, who] if n == 2 else fulls[n][who]
            cores[n][slot] = (cores[n][slot].astype(f32) + mine.astype(f32)).astype(low)
        first, second = (2, 1) if n % 2 == 0 else (1, 2)
        partner = by if n % 2 == 0 else bx
        for i, (src, dst) in enumerate(((first, 0), (3, 1))):
            copy = remote(
                cores[n].at[src], ones[n].at[dst], x_send.at[n, i], x_recv.at[n, i], (partner, z)
            )
            copy.start()
            issued.append(copy)

    def one_event(n):
        first, second = (2, 1) if n % 2 == 0 else (1, 2)
        partner, other = (by, bx) if n % 2 == 0 else (bx, by)
        for i, slot in ((0, 0), (1, second)):
            ref = ones[n].at[i]
            remote(ref, ref, x_send.at[n, i], x_recv.at[n, i], (partner, z)).wait_recv()
            ones[n][i] = (ones[n][i].astype(f32) + cores[n][slot].astype(f32)).astype(low)
        copy = remote(
            ones[n].at[1], twos[n], x_send.at[n, 2], x_recv.at[n, 2], (other, z)
        )
        copy.start()
        issued.append(copy)

    z_bufs = (z_down, z_up, z_outw)

    def two_event(n):
        other = bx if n % 2 == 0 else by
        ref = twos[n]
        remote(ref, ref, x_send.at[n, 2], x_recv.at[n, 2], (other, z)).wait_recv()
        if n == 3:
            qkvw_own[...] = twos[n][...].astype(f32) + ones[n][0].astype(f32)
            return
        twos[n][...] = (twos[n][...].astype(f32) + ones[n][0].astype(f32)).astype(low)
        for i, (_, to) in enumerate(peers):
            copy = remote(
                twos[n].at[to], z_bufs[n].at[i], e_send.at[n, i], e_recv.at[n, i], (b, to)
            )
            copy.start()
            issued.append(copy)

    def end_event(n):
        total = twos[n][z].astype(f32)
        for i in range(3):
            source = lax.rem(z + 3 - i, 4)
            ref = z_bufs[n].at[i]
            remote(ref, ref, e_send.at[n, i], e_recv.at[n, i], (b, source)).wait_recv()
            total = total + z_bufs[n][i].astype(f32)
        (down_own, up_own, outw_own)[n][...] = total

    zf = z + 1 - 2 * (z % 2)
    zg = z + 2 - 4 * (z // 2)
    partners = ((bc, z), (bx, z), (by, z), (b, zf), (b, zg))

    def small_start(k):
        copy = remote(
            small_out.at[k], small_in.at[k], s_send.at[k], s_recv.at[k], partners[k]
        )
        copy.start()
        issued.append(copy)

    def small_event(k):
        ref = small_in.at[k]
        remote(ref, ref, s_send.at[k], s_recv.at[k], partners[k]).wait_recv()
        small_out[k + 1] = small_out[k] + small_in[k]
        if k < 4:
            small_start(k + 1)

    small_out[0] = small_ref[...]
    small_start(0)

    z_list = [(k, c) for k in range(3) for c in range(chunks)]
    other = (
        [partial(core_event, n) for n in (0, 1, 2, 3)]
        + [partial(small_event, 0), partial(small_event, 1)]
        + [partial(one_event, n) for n in (0, 1, 2, 3)]
        + [partial(small_event, 2), partial(small_event, 3)]
        + [partial(two_event, n) for n in (0, 1, 2, 3)]
        + [partial(small_event, 4)]
    )
    lead = 2
    for k, c in z_list[:lead]:
        z_event(k, c)
    rest = z_list[lead:]
    for n in range(max(len(rest), len(other))):
        if n < len(other):
            other[n]()
        if n < len(rest):
            z_event(*rest[n])
    for n in (0, 1, 2):
        end_event(n)

    for c in range(chunks):
        rows = pl.ds(c * size, size)
        input_ref[rows] = first_ref[rows] + part_ref[z, c].astype(f32)

    for c in range(chunks):
        rows = pl.ds(c * size, size)
        for up in (True, False):
            buf = up_in if up else down_in

            @pl.when((z > 0) if up else (z < 3))
            def _():
                side = 0 if up else 1
                ref = buf.at[z, c]
                remote(
                    ref, ref, z_send.at[side, z, c], z_recv.at[side, z, c],
                    (b, z - 1 if up else z + 1),
                ).wait_recv()
                input_ref[rows] += buf[z, c].astype(f32)

    for k, c in z_list:
        for up in (True, False):
            owner = 3 - k if up else k

            @pl.when((z < owner) if up else (z > owner))
            def _():
                flow(up, owner, c).wait_send()

    for copy in issued:
        copy.wait_send()


def tail(part, first, down, up, outw, qkvw, small):
    quarter, model = first.shape
    chunks = 4
    size = quarter // chunks
    ff = down.shape[2]
    on, oh = outw.shape[2:]
    qn, qh = qkvw.shape[1:]
    blocks = ((4, ff, model), (4, ff, model), (4, on, oh), (qn, qh))
    own = lambda *s: jax.ShapeDtypeStruct(s, f32)
    vm = lambda *s: pltpu.VMEM(s, low)
    dma = pltpu.SemaphoreType.DMA
    return pl.pallas_call(
        tail_kernel,
        out_shape=[
            own(quarter, model), own(ff, model), own(ff, model), own(on, oh), own(qn, qh),
            own(6, *small.shape),
        ],
        in_specs=[pl.BlockSpec(memory_space=pltpu.VMEM)] * 7,
        out_specs=[pl.BlockSpec(memory_space=pltpu.VMEM)] * 6,
        scratch_shapes=[
            vm(4, chunks, size, model), vm(4, chunks, size, model),
            *[vm(4, *s) for s in blocks],
            *[vm(2, *s) for s in blocks],
            *[vm(*s) for s in blocks],
            *[vm(3, *s[1:]) for s in blocks[:3]],
            pltpu.VMEM((5, *small.shape), f32),
            dma((2, 4, chunks)), dma((2, 4, chunks)), dma((4, 4)), dma((4, 4)),
            dma((4, 3)), dma((4, 3)), dma((3, 3)), dma((3, 3)), dma((5,)), dma((5,)),
        ],
        compiler_params=pltpu.CompilerParams(
            collective_id=3, has_side_effects=True, vmem_limit_bytes=62 * 1024 * 1024
        ),
        name="tail",
    )(part.reshape(4, chunks, size, model), first, down, up, outw, qkvw, small)


def slice_body(
    tokens,
    qkv_weight,
    qv_bias,
    conv_weight,
    out_weight,
    out_bias,
    norm1_gain,
    norm1_bias,
    ffn_in_weight,
    ffn_in_bias,
    ffn_out_weight,
    ffn_out_bias,
    norm2_gain,
    norm2_bias,
    cotangent,
    seq_lengths,
    segment_ids,
    landmark_bounds,
):
    tok_count, model = tokens.shape
    width = qkv_weight.shape[2]
    heads_here = width // HEAD_DIM
    kernel_taps = conv_weight.shape[1]
    slots, marks = landmark_bounds.shape
    quarter = tok_count // 4
    z = lax.axis_index("heads")
    b = lax.axis_index("batch")
    own_tokens = lax.dynamic_slice_in_dim(tokens, z * quarter, quarter, 0).astype(f32)
    conv_own = lax.dynamic_slice_in_dim(conv_weight, z * heads_here, heads_here, 0)
    qv_own = lax.dynamic_slice_in_dim(qv_bias, z * width, width, 1)
    flat_qkv = qkv_weight.reshape(model, 3 * width)
    bias_col = jnp.concatenate([qv_own[0], jnp.zeros_like(qv_own[0]), qv_own[1]])[:, None]
    forward = mix_forward(
        seq_lengths, tokens, jnp.transpose(flat_qkv), bias_col, conv_own, slots, marks
    )
    qkv_t, first, last, mixed_t, mark, value, inner, denom, middle, steps, inverse, bound = forward
    ff_own = ffn_out_weight.shape[0]
    share = width // 8
    misc_rows = 32
    misc_own = jnp.concatenate(
        [
            lax.dynamic_slice_in_dim(out_weight, b * share, share, 0),
            jnp.zeros((misc_rows - share, model), low).at[0, :ff_own].set(ffn_in_bias),
        ],
        axis=0,
    )
    mixed_all, in_all, down_all, misc_all = exchange(
        mixed_t, jnp.transpose(ffn_in_weight), ffn_out_weight, misc_own
    )
    mixed_all = mixed_all.reshape(4 * width, quarter)
    whole_in = in_all.reshape(-1, model)
    whole_down = down_all.reshape(-1, model)
    whole_out = jnp.swapaxes(misc_all[:, :, :share], 0, 1).reshape(4 * width, model)
    whole_bias = misc_all[:, :, share, :ff_own].reshape(-1).astype(f32)

    attn = lax.dot_general(mixed_all, whole_out, contract_rows, preferred_element_type=f32)
    first_res = own_tokens + attn + out_bias[None, :]
    norm1_out, norm1_pull = jax.vjp(layer_norm, first_res, norm1_gain, norm1_bias)
    norm1_low = norm1_out.astype(low)
    pre_act = (
        lax.dot_general(norm1_low, whole_in, contract_cols, preferred_element_type=f32)
        + whole_bias[None, :]
    )
    hidden_act, gelu_pull = jax.vjp(gelu_exact, pre_act)
    hidden_low = hidden_act.astype(low)
    ffn_result = jnp.dot(hidden_low, whole_down, preferred_element_type=f32) + ffn_out_bias[None, :]
    final_out, norm2_pull = jax.vjp(layer_norm, norm1_out + ffn_result, norm2_gain, norm2_bias)
    grad_second, grad_gain_two, grad_shift_two = norm2_pull(cotangent.astype(f32))
    grad_ffn_low = grad_second.astype(low)
    grad_ffn_bias = jnp.sum(grad_ffn_low.astype(f32), axis=0)
    grad_hidden = lax.dot_general(
        grad_ffn_low, whole_down, contract_cols, preferred_element_type=f32
    )
    grad_pre = gelu_pull(grad_hidden)[0].astype(low)
    grad_in_bias = jnp.sum(grad_pre.astype(f32), axis=0)
    grad_norm1 = grad_second + jnp.dot(grad_pre, whole_in, preferred_element_type=f32)
    grad_first, grad_gain_one, grad_shift_one = norm1_pull(grad_norm1)
    grad_attn_low = grad_first.astype(low)
    grad_out_bias = jnp.sum(grad_attn_low.astype(f32), axis=0)
    grad_mix_all = lax.dot_general(
        whole_out, grad_attn_low, contract_cols, preferred_element_type=f32
    ).astype(low)
    grad_mix_t = turn(grad_mix_all, width)
    saved = (qkv_t, first, last, mark, value, inner, denom, middle, steps, inverse)
    grad_t, grad_bias, grad_conv = mix_backward(
        seq_lengths, grad_mix_t, saved, conv_own, slots, marks
    )
    part = lax.dot_general(
        grad_t, flat_qkv, (((0,), (1,)), ((), ())), preferred_element_type=f32
    ).astype(low)
    down_term = lax.dot_general(
        hidden_low, grad_ffn_low, contract_rows, preferred_element_type=f32
    ).astype(low)
    up_term = lax.dot_general(
        grad_pre, norm1_low, contract_rows, preferred_element_type=f32
    ).astype(low)
    out_term = lax.dot_general(
        grad_attn_low,
        mixed_all.reshape(4, width, quarter),
        (((0,), (2,)), ((), ())),
        preferred_element_type=f32,
    ).astype(low)
    out_term = jnp.swapaxes(out_term, 0, 1).reshape(4, 8, model // 8, width)
    qkv_term = lax.dot_general(
        tokens, grad_t, (((0,), (1,)), ((), ())), preferred_element_type=f32
    ).astype(low)

    flat = jnp.concatenate(
        [
            grad_in_bias,
            grad_ffn_bias, grad_gain_two, grad_shift_two,
            grad_gain_one, grad_shift_one, grad_out_bias,
        ]
    )
    head_total = conv_weight.shape[0]
    conv_full = lax.dynamic_update_slice_in_dim(
        jnp.zeros((head_total, kernel_taps), f32), grad_conv[:, :kernel_taps], z * heads_here, 0
    )
    bias_full = lax.dynamic_update_slice_in_dim(
        jnp.zeros((2, 4 * width), f32), jnp.transpose(grad_bias), z * width, 1
    )
    live_count = jnp.sum((seq_lengths > 0).astype(f32)) * heads_here
    scalars = jnp.stack([bound[0, 0], live_count])
    small = jnp.concatenate([flat, bias_full.reshape(-1), conv_full.reshape(-1), scalars])
    lanes = 768
    rows = -(-small.shape[0] // (8 * lanes)) * 8
    small = jnp.pad(small, (0, rows * lanes - small.shape[0])).reshape(rows, lanes)
    ff = ff_own * 32
    input_grad, down_share, up_share, out_share, qkv_share, sums = tail(
        part,
        grad_first,
        down_term.reshape(8, 4, ff_own, model),
        up_term.reshape(8, 4, ff_own, model),
        out_term,
        qkv_term.reshape(8, model // 8, 3 * width),
        small,
    )
    sums = sums[5].reshape(-1)
    index = b * 4 + z
    in_bias_share = lax.dynamic_slice_in_dim(sums, index * ff_own, ff_own, 0)
    vectors = sums[ff : ff + 6 * model].reshape(6, model)
    vector_share = lax.dynamic_slice_in_dim(vectors, index * (model // 32), model // 32, 1)
    at = ff + 6 * model
    bias_sum = sums[at : at + 8 * width].reshape(2, 4 * width)
    bias_out = lax.dynamic_slice_in_dim(bias_sum, z * width, width, 1)
    at = at + 8 * width
    conv_sum = sums[at : at + head_total * kernel_taps].reshape(head_total, kernel_taps)
    conv_out = lax.dynamic_slice_in_dim(conv_sum, z * heads_here, heads_here, 0)
    at = at + head_total * kernel_taps
    condition = sums[at] / sums[at + 1]
    return (
        final_out.astype(low),
        input_grad,
        qkv_share.reshape(model // 8, 3, width),
        bias_out,
        conv_out,
        jnp.transpose(out_share),
        jnp.transpose(up_share),
        in_bias_share,
        down_share,
        vector_share,
        condition,
    )


def solution(mesh):
    chosen = slice_body if dict(mesh.shape) == {"batch": 8, "heads": 4} else body
    in_specs = (
        P("batch", None),
        P(None, None, "heads"),
        P(),
        P(),
        P("heads", None),
        P(),
        P(),
        P(),
        P(None, ("batch", "heads")),
        P(("batch", "heads")),
        P(("batch", "heads"), None),
        P(),
        P(),
        P(),
        P(("batch", "heads"), None),
        P("batch"),
        P("batch"),
        P("batch", None),
    )
    out_specs = (
        P(("batch", "heads"), None),
        P(("batch", "heads"), None),
        P("batch", None, "heads"),
        P(None, "heads"),
        P("heads", None),
        P("heads", "batch"),
        P(None, ("batch", "heads")),
        P(("batch", "heads")),
        P(("batch", "heads"), None),
        P(None, ("batch", "heads")),
        P(),
    )
    return jax.shard_map(chosen, mesh=mesh, in_specs=in_specs, out_specs=out_specs, check_vma=False)
```

```python
from functools import partial

import jax
import jax.numpy as jnp
from jax import lax
from jax.experimental import pallas as pl
from jax.experimental.pallas import tpu as pltpu
from jax.sharding import PartitionSpec as P

HEAD_DIM = 64
PINV_ITERS = 6
TILE = 512
SUB = 128

f32 = jnp.float32
low = jnp.bfloat16
mask_fill = -1000000000.0


def split(x):
    high = x.astype(low)
    return high, (x - high.astype(f32)).astype(low)


def mul(a, b):
    return lax.dot_general(a, b, (((1,), (0,)), ((), ())), preferred_element_type=f32)


def mul_t(a, b):
    return lax.dot_general(a, b, (((1,), (1,)), ((), ())), preferred_element_type=f32)


def wide(form, left, right):
    left_high, left_low = split(left)
    right_high, right_low = split(right)
    return form(left_high, right_high) + (
        form(left_high, right_low) + form(left_low, right_high)
    )


def block_grid(rows, cols):
    row_block = lax.broadcasted_iota(jnp.int32, (rows, cols), 0) // HEAD_DIM
    col_block = lax.broadcasted_iota(jnp.int32, (rows, cols), 1) // HEAD_DIM
    return row_block == col_block


def spread(x, blocks):
    count = blocks.shape[0] // x.shape[0]
    return jnp.where(blocks, jnp.concatenate([x] * count, axis=0), jnp.zeros_like(x[:1, :1]))


def fold(x, blocks):
    kept = jnp.where(blocks, x, jnp.zeros_like(x[:1, :1]))
    rows = HEAD_DIM
    out = kept[:rows]
    for n in range(1, x.shape[0] // rows):
        out = out + kept[n * rows : (n + 1) * rows]
    return out


def pack_mul(left, right, blocks):
    left_high, left_low = split(left)
    right_high, right_low = split(right)
    right_high, right_low = spread_low(right_high, blocks), spread_low(right_low, blocks)
    return mul(left_high, right_high) + (mul(left_high, right_low) + mul(left_low, right_high))


def pack_mul_t(left, right, blocks):
    left_high, left_low = split(left)
    right_high, right_low = split(right)
    right_high, right_low = spread_low(right_high, blocks), spread_low(right_low, blocks)
    return mul_t(left_high, right_high) + (mul_t(left_high, right_low) + mul_t(left_low, right_high))


def spread_low(x, blocks):
    return spread(x.astype(f32), blocks).astype(low)


def slot_bounds(len_ref, s, slots):
    start = jnp.int32(0)
    for n in range(slots):
        start = start + jnp.where(n < s, len_ref[n], 0)
    return start, start + len_ref[s]


def eye_pack(width):
    row = lax.broadcasted_iota(jnp.int32, (HEAD_DIM, width), 0)
    col = lax.broadcasted_iota(jnp.int32, (HEAD_DIM, width), 1) % HEAD_DIM
    return jnp.where(row == col, 1.0, 0.0).astype(f32)


def lane_mask(start, end, at, width):
    tok = at + lax.broadcasted_iota(jnp.int32, (1, width), 1)
    return (tok >= start) & (tok < end)


def band(taps_row, width):
    row = lax.broadcasted_iota(jnp.int32, (SUB, 3 * SUB), 0)
    col = lax.broadcasted_iota(jnp.int32, (SUB, 3 * SUB), 1)
    off = col - row - (SUB - width // 2)
    out = jnp.zeros((SUB, 3 * SUB), f32)
    for n in range(width):
        out = jnp.where(off == n, taps_row[:, n : n + 1], out)
    return out


def slot_marks(len_ref, at, slots, marks, width):
    rows = slots * marks
    row = lax.broadcasted_iota(jnp.int32, (rows, 1), 0)
    slot = row // marks
    mark = row % marks
    start = jnp.zeros((rows, 1), jnp.int32)
    length = jnp.zeros((rows, 1), jnp.int32)
    for n in range(slots):
        start = start + jnp.where(slot > n, len_ref[n], 0)
        length = jnp.where(slot == n, len_ref[n], length)
    lower = start + (mark * length) // marks
    upper = start + ((mark + 1) * length) // marks
    inv_count = 1.0 / jnp.maximum((upper - lower).astype(f32), 1.0)
    tok = at + lax.broadcasted_iota(jnp.int32, (rows, width), 1)
    member = jnp.where((tok >= lower) & (tok < upper), 1.0, 0.0)
    return member, inv_count


def mix_forward_kernel(
    slots, marks, taps,
    len_ref, tok_ref, weight_ref, bias_ref, conv_ref,
    qkv_ref, first_ref, last_ref, mixed_ref, mark_ref, value_ref, inner_ref,
    denom_ref, middle_ref, steps_ref, inverse_ref, bound_ref,
    vpad, scores, vsum,
):
    step = pl.program_id(0)
    width = first_ref.shape[0]
    heads = width // HEAD_DIM
    tok_count = qkv_ref.shape[1]
    tiles = tok_count // TILE
    packed = slots * marks
    at = pl.multiple_of(step * TILE, TILE)

    @pl.when(step == 0)
    def _():
        mark_ref[...] = jnp.zeros_like(mark_ref)
        vsum[...] = jnp.zeros_like(vsum)
        vpad[:, :SUB] = jnp.zeros((width, SUB), low)
        vpad[:, tok_count + SUB :] = jnp.zeros((width, SUB), low)

    rows = (mul_t(weight_ref[...], tok_ref[...]) + bias_ref[...]).astype(low)
    qkv_ref[:, pl.ds(at, TILE)] = rows
    vpad[:, pl.ds(pl.multiple_of(at + SUB, SUB), TILE)] = rows[2 * width :]
    member, inv_count = slot_marks(len_ref, at, slots, marks, TILE)
    mark_ref[...] += mul_t(member.astype(low), rows[: 2 * width])
    vsum[...] += mul_t(jnp.ones((8, TILE), low), rows[2 * width :])
    first_ref[:, pl.ds(at, TILE)] = jnp.zeros((width, TILE), low)
    last_ref[:, pl.ds(at, TILE)] = jnp.zeros((width, TILE), low)
    mixed_ref[:, pl.ds(at, TILE)] = jnp.zeros((width, TILE), low)

    @pl.when(step == tiles - 1)
    def _():
        mark_ref[...] = mark_ref[...] * inv_count
        head_blocks = block_grid(width, width)
        slot_blocks = block_grid(packed, packed)
        eye = eye_pack(packed)
        scale = HEAD_DIM ** -0.5

        middles, inverses_t, products = [], [], []
        bound_total = jnp.zeros((1, 1), f32)
        lane_slot = lax.broadcasted_iota(jnp.int32, (1, packed), 1) // marks
        for h in range(heads):
            q_marks = mark_ref[:, h * HEAD_DIM : (h + 1) * HEAD_DIM]
            k_marks = mark_ref[:, width + h * HEAD_DIM : width + (h + 1) * HEAD_DIM]
            sim = wide(mul_t, q_marks, k_marks) * scale
            sim = jnp.where(slot_blocks, sim, -1e30)
            sim = jnp.exp(sim - jnp.max(sim, axis=1, keepdims=True))
            sim = sim / jnp.sum(sim, axis=1, keepdims=True)
            middle = fold(sim, slot_blocks)
            col_sums = jnp.sum(middle, axis=0, keepdims=True)
            bound = jnp.zeros((1, packed), f32)
            for s in range(slots):
                top = jnp.max(jnp.where(lane_slot == s, col_sums, 0.0), axis=1, keepdims=True)
                bound = jnp.where(lane_slot == s, top, bound)
                bound_total += jnp.where(len_ref[s] > 0, top, 0.0)
            middle_ref[h] = middle
            middles.append(middle)
            inverses_t.append(middle / bound)
            products.append(pack_mul_t(middle, middle, slot_blocks) / bound)
        bound_ref[...] = jnp.broadcast_to(bound_total, bound_ref.shape)

        def newton(n, carry):
            out = []
            for h in range(heads):
                inverse_t, product = carry[h]
                square = pack_mul(product, product, slot_blocks)
                cube = pack_mul(product, square, slot_blocks)
                fourth = pack_mul(square, square, slot_blocks)
                second = 15.0 * eye - 7.0 * product + square
                third = 13.0 * eye - 15.0 * product + 7.0 * square - cube
                steps_ref[n, 0, h] = product
                steps_ref[n, 1, h] = second
                steps_ref[n, 2, h] = third
                steps_ref[n, 3, h] = inverse_t
                out.append(
                    (
                        0.25 * pack_mul(third, inverse_t, slot_blocks),
                        0.25 * (13.0 * product - 15.0 * square + 7.0 * cube - fourth),
                    )
                )
            return tuple(out)

        final = lax.fori_loop(0, PINV_ITERS, newton, tuple(zip(inverses_t, products)))
        for h in range(heads):
            inverse_ref[h] = final[h][0]

        def one_slot(s, _):
            start, end = slot_bounds(len_ref, s, slots)
            lo, hi = start // TILE, (end + TILE - 1) // TILE
            hi = jnp.where(end > start, hi, lo)
            own = mark_ref[pl.ds(pl.multiple_of(s * marks, marks), marks), :] * scale
            q_block = spread(own[:, :width], head_blocks).astype(low)
            k_block = spread(own[:, width:], head_blocks).astype(low)

            def score_tile(n, top):
                t = pl.multiple_of(n * TILE, TILE)
                mask = lane_mask(start, end, t, TILE)
                sim = mul(k_block, qkv_ref[:width, pl.ds(t, TILE)])
                sim = sim.reshape(heads, marks, TILE)
                sim = jnp.exp(sim - jnp.max(sim, axis=1, keepdims=True))
                sim = sim / jnp.sum(sim, axis=1, keepdims=True)
                sim = sim.reshape(width, TILE)
                old = first_ref[:, pl.ds(t, TILE)].astype(f32)
                first_ref[:, pl.ds(t, TILE)] = jnp.where(mask, sim, old).astype(low)
                sim = mul(q_block, qkv_ref[width : 2 * width, pl.ds(t, TILE)])
                sim = jnp.where(mask, sim, mask_fill)
                scores[:, pl.ds(t, TILE)] = sim
                for c in range(TILE // SUB):
                    top = jnp.maximum(top, sim[:, c * SUB : (c + 1) * SUB])
                return top

            top = lax.fori_loop(lo, hi, score_tile, jnp.full((width, SUB), mask_fill, f32))
            top = jnp.max(top, axis=1, keepdims=True)

            def value_tile(n, carry):
                denom, total = carry
                t = pl.multiple_of(n * TILE, TILE)
                mask = lane_mask(start, end, t, TILE)
                part = jnp.exp(scores[:, pl.ds(t, TILE)] - top)
                old = last_ref[:, pl.ds(t, TILE)].astype(f32)
                last_ref[:, pl.ds(t, TILE)] = jnp.where(mask, part, old).astype(low)
                total = total + mul_t(part.astype(low), qkv_ref[2 * width :, pl.ds(t, TILE)])
                for c in range(TILE // SUB):
                    denom = denom + part[:, c * SUB : (c + 1) * SUB]
                return denom, total

            denom, total = lax.fori_loop(
                lo, hi, value_tile,
                (jnp.zeros((width, SUB), f32), jnp.zeros((width, width), f32)),
            )
            denom = jnp.sum(denom, axis=1, keepdims=True)
            inv = 1.0 / jnp.where(denom > 0.0, denom, 1.0)
            denom_ref[s] = inv
            values = fold(total * inv, head_blocks)
            values = jnp.where(end > start, values, vsum[:1] / tok_count)
            value_ref[pl.ds(pl.multiple_of(s * marks, marks), marks), :] = values
            return 0

        lax.fori_loop(0, slots, one_slot, 0)

        lane_head = lax.broadcasted_iota(jnp.int32, (1, width), 1) // HEAD_DIM
        inner = jnp.zeros((packed, width), f32)
        for h in range(heads):
            inverse = pack_mul_t(eye, final[h][0], slot_blocks)
            own_values = jnp.where(lane_head == h, value_ref[...], 0.0)
            inner = inner + wide(mul, spread(inverse, slot_blocks), own_values)
        inner_ref[...] = inner

        bands = [band(conv_ref[h : h + 1, :], taps).astype(low) for h in range(heads)]

        def out_slot(s, _):
            start, end = slot_bounds(len_ref, s, slots)
            lo, hi = start // TILE, (end + TILE - 1) // TILE
            hi = jnp.where(end > start, hi, lo)
            own = inner_ref[pl.ds(pl.multiple_of(s * marks, marks), marks), :]
            a_block = jnp.transpose(spread(own, head_blocks)).astype(low)

            def out_tile(n, _):
                t = pl.multiple_of(n * TILE, TILE)
                mask = lane_mask(start, end, t, TILE)
                rows = mul(a_block, first_ref[:, pl.ds(t, TILE)])
                rows = rows + convolve(vpad, bands, start, end, t, heads)
                old = mixed_ref[:, pl.ds(t, TILE)].astype(f32)
                mixed_ref[:, pl.ds(t, TILE)] = jnp.where(mask, rows, old).astype(low)
                return 0

            return lax.fori_loop(lo, hi, out_tile, 0)

        lax.fori_loop(0, slots, out_slot, 0)


def windows(padded, start, end, t):
    full = padded[:, pl.ds(t, TILE + 2 * SUB)]
    keep = lane_mask(start, end, t - SUB, TILE + 2 * SUB)
    return jnp.where(keep, full.astype(f32), 0.0).astype(low)


def convolve(padded, bands, start, end, t, heads):
    full = windows(padded, start, end, t)
    out = []
    count = TILE // SUB
    for h in range(heads):
        own = full[h * HEAD_DIM : (h + 1) * HEAD_DIM]
        stack = jnp.concatenate(
            [own[:, c * SUB : (c + 3) * SUB] for c in range(count)], axis=0
        )
        res = mul_t(stack, bands[h])
        out.append(
            jnp.concatenate(
                [res[c * HEAD_DIM : (c + 1) * HEAD_DIM] for c in range(count)], axis=1
            )
        )
    return jnp.concatenate(out, axis=0)


def mix_backward_kernel(
    slots, marks, taps,
    len_ref, grad_ref, qkv_ref, first_ref, last_ref, mark_ref, value_ref, inner_ref,
    denom_ref, middle_ref, steps_ref, inverse_ref, conv_ref,
    out_ref, bias_ref, conv_out_ref,
    gpad, vpad, ds_first, ds_last, conv_grad, d_inner, d_k, d_q, d_value,
):
    width = first_ref.shape[0]
    heads = width // HEAD_DIM
    tok_count = qkv_ref.shape[1]
    packed = slots * marks
    scale = HEAD_DIM ** -0.5
    head_blocks = block_grid(width, width)
    slot_blocks = block_grid(packed, packed)
    eye = eye_pack(packed)
    count = TILE // SUB

    for padded, source in ((gpad, grad_ref[...]), (vpad, qkv_ref[2 * width :, :])):
        padded[:, :SUB] = jnp.zeros((width, SUB), low)
        padded[:, tok_count + SUB :] = jnp.zeros((width, SUB), low)
        padded[:, SUB : tok_count + SUB] = source
    out_ref[...] = jnp.zeros_like(out_ref)
    ds_first[...] = jnp.zeros_like(ds_first)
    ds_last[...] = jnp.zeros_like(ds_last)
    conv_grad[...] = jnp.zeros_like(conv_grad)

    def reach(s):
        start, end = slot_bounds(len_ref, s, slots)
        lo, hi = start // TILE, (end + TILE - 1) // TILE
        return start, end, lo, jnp.where(end > start, hi, lo)

    def own_rows(s):
        return pl.ds(pl.multiple_of(s * marks, marks), marks)

    def first_slot(s, _):
        start, end, lo, hi = reach(s)
        a_block = spread(inner_ref[own_rows(s), :], head_blocks).astype(low)

        def tile(n, carry):
            inner_total, key_total = carry
            t = pl.multiple_of(n * TILE, TILE)
            mask = lane_mask(start, end, t, TILE)
            own_grad = grad_ref[:, pl.ds(t, TILE)]
            kernel_rows = jnp.where(mask, first_ref[:, pl.ds(t, TILE)].astype(f32), 0.0)
            d_kernel = mul(a_block, own_grad)
            prod = (kernel_rows * d_kernel).reshape(heads, marks, TILE)
            row_sum = jnp.sum(prod, axis=1, keepdims=True)
            d_sim = prod - kernel_rows.reshape(heads, marks, TILE) * row_sum
            d_sim = d_sim.reshape(width, TILE)
            d_sim_low = d_sim.astype(low)
            old = ds_first[:, pl.ds(t, TILE)].astype(f32)
            ds_first[:, pl.ds(t, TILE)] = jnp.where(mask, d_sim, old).astype(low)
            inner_total = inner_total + mul_t(kernel_rows.astype(low), own_grad)
            key_total = key_total + mul_t(d_sim_low, qkv_ref[:width, pl.ds(t, TILE)])
            full = windows(vpad, start, end, t)
            grad_own = jnp.where(mask, own_grad.astype(f32), 0.0).astype(low)
            for h in range(heads):
                sel = slice(h * HEAD_DIM, (h + 1) * HEAD_DIM)
                left = jnp.concatenate(
                    [grad_own[sel, c * SUB : (c + 1) * SUB] for c in range(count)], axis=0
                )
                right = jnp.concatenate(
                    [full[sel, c * SUB : (c + 3) * SUB] for c in range(count)], axis=0
                )
                conv_grad[h] += lax.dot_general(
                    left, right, (((0,), (0,)), ((), ())), preferred_element_type=f32
                )
            return inner_total, key_total

        zero = jnp.zeros((width, width), f32)
        inner_total, key_total = lax.fori_loop(lo, hi, tile, (zero, zero))
        d_inner[own_rows(s), :] = fold(inner_total, head_blocks)
        d_k[own_rows(s), :] = fold(key_total, head_blocks) * scale
        return 0

    lax.fori_loop(0, slots, first_slot, 0)

    row = lax.broadcasted_iota(jnp.int32, (SUB, 3 * SUB), 0)
    col = lax.broadcasted_iota(jnp.int32, (SUB, 3 * SUB), 1)
    off = col - row - (SUB - taps // 2)
    tap_lane = lax.broadcasted_iota(jnp.int32, (1, SUB), 1)
    for h in range(heads):
        found = jnp.zeros((1, SUB), f32)
        square = conv_grad[h]
        for n in range(taps):
            part = jnp.sum(jnp.where(off == n, square, 0.0), axis=0, keepdims=True)
            part = jnp.sum(part, axis=1, keepdims=True)
            found = jnp.where(tap_lane == n, part, found)
        conv_out_ref[h : h + 1, :] = found

    lane_head = lax.broadcasted_iota(jnp.int32, (1, width), 1) // HEAD_DIM
    value_total = jnp.zeros((packed, width), f32)
    d_inverses = []
    for h in range(heads):
        own = jnp.where(lane_head == h, d_inner[...], 0.0)
        value_total = value_total + wide(mul, spread(inverse_ref[h], slot_blocks), own)
        d_inverses.append(fold(wide(mul_t, own, value_ref[...]), slot_blocks))
    d_value[...] = value_total

    middles_t = [pack_mul_t(eye, middle_ref[h], slot_blocks) for h in range(heads)]

    def newton(k, carry):
        n = PINV_ITERS - 1 - k
        out = []
        for h in range(heads):
            d_inverse, d_middle = carry[h]
            product = steps_ref[n, 0, h]
            second = steps_ref[n, 1, h]
            third = steps_ref[n, 2, h]
            inverse_t = steps_ref[n, 3, h]
            middle_t = middles_t[h]
            d_third = 0.25 * pack_mul(inverse_t, d_inverse, slot_blocks)
            d_second = -pack_mul(product, d_third, slot_blocks)
            d_first = -pack_mul(product, d_second, slot_blocks)
            d_product = (
                -pack_mul(d_third, second, slot_blocks)
                - pack_mul(d_second, 7.0 * eye - product, slot_blocks)
                - d_first
            )
            d_middle = d_middle + pack_mul(d_product, inverse_t, slot_blocks)
            d_inverse = 0.25 * pack_mul(d_inverse, third, slot_blocks) + pack_mul(
                middle_t, d_product, slot_blocks
            )
            out.append((d_inverse, d_middle))
        return tuple(out)

    zero = jnp.zeros((HEAD_DIM, packed), f32)
    final = lax.fori_loop(0, PINV_ITERS, newton, tuple((x, zero) for x in d_inverses))
    lane_slot = lax.broadcasted_iota(jnp.int32, (1, packed), 1) // marks
    dq_total = jnp.zeros((packed, width), f32)
    dk_total = jnp.zeros((packed, width), f32)
    for h in range(heads):
        d_inverse, d_middle = final[h]
        middle = middle_ref[h]
        first_t = steps_ref[0, 3, h]
        d_inverse_t = pack_mul_t(eye, d_inverse, slot_blocks)
        col_sums = jnp.sum(middle, axis=0, keepdims=True)
        share = jnp.sum(d_inverse_t * first_t, axis=0, keepdims=True)
        bound = jnp.zeros((1, packed), f32)
        d_bound = jnp.zeros((1, packed), f32)
        hits = jnp.zeros((1, packed), f32)
        for s in range(slots):
            mine = lane_slot == s
            top = jnp.max(jnp.where(mine, col_sums, 0.0), axis=1, keepdims=True)
            total = jnp.sum(jnp.where(mine, share, 0.0), axis=1, keepdims=True)
            number = jnp.sum(
                jnp.where(mine & (col_sums == top), 1.0, 0.0), axis=1, keepdims=True
            )
            bound = jnp.where(mine, top, bound)
            d_bound = jnp.where(mine, -total / top, d_bound)
            hits = jnp.where(mine, number, hits)
        d_middle = d_middle + d_inverse_t / bound
        d_middle = d_middle + jnp.where(col_sums == bound, d_bound / hits, 0.0)
        prod = spread(middle * d_middle, slot_blocks)
        d_sim = prod - spread(middle, slot_blocks) * jnp.sum(prod, axis=1, keepdims=True)
        d_sim = d_sim * scale
        own = lane_head == h
        q_marks = jnp.where(own, mark_ref[:, :width], 0.0)
        k_marks = jnp.where(own, mark_ref[:, width:], 0.0)
        dq_total = dq_total + wide(mul, d_sim, k_marks)
        dk_total = dk_total + wide(mul, jnp.transpose(d_sim), q_marks)
    d_q[...] = dq_total
    d_k[...] += dk_total

    flipped = []
    for h in range(heads):
        flipped.append(
            band(
                jnp.concatenate(
                    [conv_ref[h : h + 1, n : n + 1] for n in reversed(range(taps))], axis=1
                ),
                taps,
            ).astype(low)
        )

    def last_slot(s, _):
        start, end, lo, hi = reach(s)
        inv = denom_ref[s]
        own_d = d_value[own_rows(s), :]
        own_v = value_ref[own_rows(s), :]
        d_block = spread(own_d, head_blocks)
        row_sum = jnp.sum(
            d_block * jnp.concatenate([own_v] * heads, axis=0), axis=1, keepdims=True
        )
        row_sum = row_sum * inv
        d_block = d_block * inv
        d_block_t = jnp.transpose(d_block).astype(low)
        d_block = d_block.astype(low)

        def tile(n, query_total):
            t = pl.multiple_of(n * TILE, TILE)
            mask = lane_mask(start, end, t, TILE)
            kernel_rows = jnp.where(mask, last_ref[:, pl.ds(t, TILE)].astype(f32), 0.0)
            v_rows = qkv_ref[2 * width :, pl.ds(t, TILE)]
            d_sim = kernel_rows * (mul(d_block, v_rows) - row_sum)
            d_low = d_sim.astype(low)
            old = ds_last[:, pl.ds(t, TILE)].astype(f32)
            ds_last[:, pl.ds(t, TILE)] = jnp.where(mask, d_sim, old).astype(low)
            dv = mul(d_block_t, kernel_rows.astype(low))
            dv = dv + convolve(gpad, flipped, start, end, t, heads)
            old = out_ref[2 * width :, pl.ds(t, TILE)].astype(f32)
            out_ref[2 * width :, pl.ds(t, TILE)] = jnp.where(mask, dv, old).astype(low)
            return query_total + mul_t(d_low, qkv_ref[width : 2 * width, pl.ds(t, TILE)])

        query_total = lax.fori_loop(lo, hi, tile, jnp.zeros((width, width), f32))
        d_q[own_rows(s), :] += fold(query_total, head_blocks) * scale
        return 0

    lax.fori_loop(0, slots, last_slot, 0)

    inv_count = slot_marks(len_ref, 0, slots, marks, SUB)[1]
    d_q[...] = d_q[...] * inv_count
    d_k[...] = d_k[...] * inv_count

    def final_slot(s, _):
        start, end, lo, hi = reach(s)
        length = end - start
        own = mark_ref[own_rows(s), :] * scale

        def left(block, d_mark):
            wide_rows = jnp.concatenate([spread(block, head_blocks), d_mark], axis=0)
            return jnp.transpose(wide_rows).astype(low)

        q_left = left(own[:, width:], d_q[own_rows(s), :])
        k_left = left(own[:, :width], d_k[own_rows(s), :])
        mark = lax.broadcasted_iota(jnp.int32, (marks, 1), 0)
        lower = start + (mark * length) // marks
        upper = start + ((mark + 1) * length) // marks

        def tile(n, _):
            t = pl.multiple_of(n * TILE, TILE)
            mask = lane_mask(start, end, t, TILE)
            tok = t + lax.broadcasted_iota(jnp.int32, (marks, TILE), 1)
            member = jnp.where((tok >= lower) & (tok < upper), 1.0, 0.0).astype(low)
            for at, lhs, source in ((0, q_left, ds_first), (width, k_left, ds_last)):
                rhs = jnp.concatenate([source[:, pl.ds(t, TILE)], member], axis=0)
                rows = mul(lhs, rhs)
                old = out_ref[at : at + width, pl.ds(t, TILE)].astype(f32)
                out_ref[at : at + width, pl.ds(t, TILE)] = jnp.where(mask, rows, old).astype(low)
            return 0

        return lax.fori_loop(lo, hi, tile, 0)

    lax.fori_loop(0, slots, final_slot, 0)

    def bias_tile(n, carry):
        t = pl.multiple_of(n * TILE, TILE)
        q_sum, v_sum = carry
        q_rows = out_ref[:width, pl.ds(t, TILE)].astype(f32)
        v_rows = out_ref[2 * width :, pl.ds(t, TILE)].astype(f32)
        for c in range(count):
            q_sum = q_sum + q_rows[:, c * SUB : (c + 1) * SUB]
            v_sum = v_sum + v_rows[:, c * SUB : (c + 1) * SUB]
        return q_sum, v_sum

    zero = jnp.zeros((width, SUB), f32)
    q_sum, v_sum = lax.fori_loop(0, tok_count // TILE, bias_tile, (zero, zero))
    bias_ref[:, 0:1] = jnp.sum(q_sum, axis=1, keepdims=True)
    bias_ref[:, 1:2] = jnp.sum(v_sum, axis=1, keepdims=True)


def mix_forward(seq_lengths, tokens, weight_t, bias_col, conv_own, slots, marks):
    tok_count, model = tokens.shape
    width = weight_t.shape[0] // 3
    heads = width // HEAD_DIM
    packed = slots * marks
    taps = conv_own.shape[1]
    whole = lambda *shape: pl.BlockSpec(shape, lambda i, lens: (0,) * len(shape))
    shapes = [
        ((3 * width, tok_count), low),
        ((width, tok_count), low),
        ((width, tok_count), low),
        ((width, tok_count), low),
        ((packed, 2 * width), f32),
        ((packed, width), f32),
        ((packed, width), f32),
        ((slots, width, 1), f32),
        ((heads, HEAD_DIM, packed), f32),
        ((PINV_ITERS, 4, heads, HEAD_DIM, packed), f32),
        ((heads, HEAD_DIM, packed), f32),
        ((8, 128), f32),
    ]
    return pl.pallas_call(
        partial(mix_forward_kernel, slots, marks, taps),
        out_shape=[jax.ShapeDtypeStruct(s, t) for s, t in shapes],
        grid_spec=pltpu.PrefetchScalarGridSpec(
            num_scalar_prefetch=1,
            grid=(tok_count // TILE,),
            in_specs=[
                pl.BlockSpec((TILE, model), lambda i, lens: (i, 0)),
                whole(3 * width, model),
                whole(3 * width, 1),
                whole(heads, taps),
            ],
            out_specs=[whole(*s) for s, _ in shapes],
            scratch_shapes=[
                pltpu.VMEM((width, tok_count + 2 * SUB), low),
                pltpu.VMEM((width, tok_count), f32),
                pltpu.VMEM((8, width), f32),
            ],
        ),
        compiler_params=pltpu.CompilerParams(vmem_limit_bytes=56 * 1024 * 1024),
        cost_estimate=pl.CostEstimate(
            flops=20 * 10**9, bytes_accessed=30 * 10**6, transcendentals=10**6
        ),
        name="mix_forward",
    )(seq_lengths, tokens, weight_t, bias_col, conv_own)


def mix_backward(seq_lengths, grad_t, saved, conv_own, slots, marks):
    qkv_t, first, last, mark, value, inner, denom, middle, steps, inverse = saved
    width, tok_count = grad_t.shape
    heads = width // HEAD_DIM
    packed = slots * marks
    taps = conv_own.shape[1]
    args = (grad_t, qkv_t, first, last, mark, value, inner, denom, middle, steps, inverse, conv_own)
    whole = lambda shape: pl.BlockSpec(
        shape, lambda i, lens: (0,) * len(shape), pipeline_mode=pl.Buffered(1)
    )
    shapes = [((3 * width, tok_count), low), ((width, 2), f32), ((heads, SUB), f32)]
    square = pltpu.VMEM((packed, width), f32)
    return pl.pallas_call(
        partial(mix_backward_kernel, slots, marks, taps),
        out_shape=[jax.ShapeDtypeStruct(s, t) for s, t in shapes],
        grid_spec=pltpu.PrefetchScalarGridSpec(
            num_scalar_prefetch=1,
            grid=(1,),
            in_specs=[whole(x.shape) for x in args],
            out_specs=[whole(s) for s, _ in shapes],
            scratch_shapes=[
                pltpu.VMEM((width, tok_count + 2 * SUB), low),
                pltpu.VMEM((width, tok_count + 2 * SUB), low),
                pltpu.VMEM((width, tok_count), low),
                pltpu.VMEM((width, tok_count), low),
                pltpu.VMEM((heads, SUB, 3 * SUB), f32),
                square, square, square, square,
            ],
        ),
        compiler_params=pltpu.CompilerParams(vmem_limit_bytes=56 * 1024 * 1024),
        cost_estimate=pl.CostEstimate(
            flops=20 * 10**9, bytes_accessed=30 * 10**6, transcendentals=10**6
        ),
        name="mix_backward",
    )(seq_lengths, *args)


contract_rows = (((0,), (0,)), ((), ()))
contract_cols = (((1,), (1,)), ((), ()))
norm_eps = 1e-05


def split_up(x, dim, peers):
    before, after = (x.shape[:dim], x.shape[dim + 1 :])
    return jnp.moveaxis(x.reshape(*before, peers, -1, *after), dim, 0)


def sum_at_owner(x, axis, dim):
    peers = lax.axis_size(axis)
    tiles = lax.all_to_all(split_up(x, dim, peers), axis, 0, 0, tiled=True)
    return jnp.sum(tiles.astype(f32), axis=0)


def layer_norm(row_data, gain_vec, shift_vec):
    centre = row_data - jnp.mean(row_data, axis=1, keepdims=True)
    spread_row = jnp.mean(centre * centre, axis=1, keepdims=True)
    return centre * lax.rsqrt(spread_row + norm_eps) * gain_vec[None, :] + shift_vec[None, :]


def gelu_exact(values):
    return jax.nn.gelu(values, approximate=False)


def body(
    tokens,
    qkv_weight,
    qv_bias,
    conv_weight,
    out_weight,
    out_bias,
    norm1_gain,
    norm1_bias,
    ffn_in_weight,
    ffn_in_bias,
    ffn_out_weight,
    ffn_out_bias,
    norm2_gain,
    norm2_bias,
    cotangent,
    seq_lengths,
    segment_ids,
    landmark_bounds,
):
    tok_count, model_width = tokens.shape
    head_width = qkv_weight.shape[2]
    heads_here = head_width // HEAD_DIM
    head_total = conv_weight.shape[0]
    kernel_taps = conv_weight.shape[1]
    slots, marks = landmark_bounds.shape
    quarter = tok_count // lax.axis_size("heads")
    head_index = lax.axis_index("heads")
    own_start = head_index * quarter
    both = ("batch", "heads")
    own_rows_low = lax.dynamic_slice_in_dim(tokens, own_start, quarter, 0)
    own_tokens = own_rows_low.astype(f32)
    conv_own = lax.dynamic_slice_in_dim(conv_weight, head_index * heads_here, heads_here, 0)
    qv_own = lax.dynamic_slice_in_dim(qv_bias, head_index * head_width, head_width, 1)
    flat_qkv = qkv_weight.reshape(model_width, 3 * head_width)
    bias_col = jnp.concatenate([qv_own[0], jnp.zeros_like(qv_own[0]), qv_own[1]])[:, None]
    forward = mix_forward(
        seq_lengths, tokens, jnp.transpose(flat_qkv), bias_col, conv_own, slots, marks
    )
    qkv_t, first, last, mixed_t, mark, value, inner, denom, middle, steps, inverse, bound = forward
    bound_total = bound[0, 0]
    attn_part = lax.psum_scatter(
        lax.dot_general(mixed_t, out_weight, contract_rows, preferred_element_type=f32).astype(low),
        "heads",
        scatter_dimension=0,
        tiled=True,
    ).astype(f32)
    live_count = jnp.sum((seq_lengths > 0).astype(f32)) * heads_here
    first_res = own_tokens + attn_part + out_bias[None, :]
    norm1_out, norm1_pull = jax.vjp(layer_norm, first_res, norm1_gain, norm1_bias)
    norm1_low = norm1_out.astype(low)
    ff_own = ffn_out_weight.shape[0]
    bias_row = jnp.zeros((16, model_width), low).at[0, :ff_own].set(ffn_in_bias)
    whole_in = lax.all_gather(ffn_in_weight, both, axis=1, tiled=True)
    out_pack = lax.all_gather(jnp.concatenate([ffn_out_weight, bias_row], axis=0), both, axis=0)
    whole_out = out_pack[:, :ff_own].reshape(-1, model_width)
    whole_in_bias = out_pack[:, ff_own, :ff_own].reshape(-1)
    pre_act = (
        jnp.dot(norm1_low, whole_in, preferred_element_type=f32)
        + whole_in_bias.astype(f32)[None, :]
    )
    hidden_act, gelu_pull = jax.vjp(gelu_exact, pre_act)
    hidden_low = hidden_act.astype(low)
    ffn_result = jnp.dot(hidden_low, whole_out, preferred_element_type=f32) + ffn_out_bias[None, :]
    final_out, norm2_pull = jax.vjp(layer_norm, norm1_out + ffn_result, norm2_gain, norm2_bias)
    grad_second, grad_gain_two, grad_shift_two = norm2_pull(cotangent.astype(f32))
    grad_ffn_low = grad_second.astype(low)
    grad_ffn_bias = jnp.sum(grad_ffn_low.astype(f32), axis=0)
    down_term = lax.dot_general(
        hidden_low, grad_ffn_low, contract_rows, preferred_element_type=f32
    ).astype(low)
    grad_hidden = lax.dot_general(
        grad_ffn_low, whole_out, contract_cols, preferred_element_type=f32
    )
    grad_pre = gelu_pull(grad_hidden)[0].astype(low)
    grad_in_bias = jnp.sum(grad_pre.astype(f32), axis=0)
    up_term = lax.dot_general(
        norm1_low, grad_pre, contract_rows, preferred_element_type=f32
    ).astype(low)
    grad_norm1 = grad_second + lax.dot_general(
        grad_pre, whole_in, contract_cols, preferred_element_type=f32
    )
    grad_first, grad_gain_one, grad_shift_one = norm1_pull(grad_norm1)
    grad_attn_low = grad_first.astype(low)
    grad_out_bias = jnp.sum(grad_attn_low.astype(f32), axis=0)
    piece_rows = lax.all_gather(grad_attn_low, "heads", axis=0, tiled=True)
    grad_mix_t = lax.dot_general(
        out_weight, piece_rows, contract_cols, preferred_element_type=f32
    ).astype(low)
    grad_mix_t, down_term, up_term = lax.optimization_barrier((grad_mix_t, down_term, up_term))
    up_share = lax.psum_scatter(up_term, both, scatter_dimension=1, tiled=True).astype(f32)
    down_share = lax.psum_scatter(down_term, both, scatter_dimension=0, tiled=True).astype(f32)
    saved = (qkv_t, first, last, mark, value, inner, denom, middle, steps, inverse)
    grad_t, grad_bias, grad_conv = mix_backward(
        seq_lengths, grad_mix_t, saved, conv_own, slots, marks
    )
    out_part = lax.dot_general(
        mixed_t, piece_rows, (((1,), (0,)), ((), ())), preferred_element_type=f32
    )
    grad_qv_own = jnp.transpose(grad_bias)
    qkv_part = lax.dot_general(
        tokens, grad_t, (((0,), (1,)), ((), ())), preferred_element_type=f32
    ).reshape(model_width, 3, head_width)
    input_part = lax.psum_scatter(
        lax.dot_general(
            grad_t, flat_qkv, (((0,), (1,)), ((), ())), preferred_element_type=f32
        ).astype(low),
        "heads",
        scatter_dimension=0,
        tiled=True,
    ).astype(f32)
    input_grad = grad_first + input_part
    conv_full = lax.dynamic_update_slice_in_dim(
        jnp.zeros((head_total, kernel_taps), f32),
        grad_conv[:, :kernel_taps],
        head_index * heads_here,
        0,
    )
    bias_full = lax.dynamic_update_slice_in_dim(
        jnp.zeros((2, head_total * HEAD_DIM), f32), grad_qv_own, head_index * head_width, 1
    )
    qkv_share, out_share = (
        sum_at_owner(qkv_part.astype(low), "batch", 0),
        sum_at_owner(out_part.astype(low), "batch", 1),
    )
    vector_all = jnp.stack(
        [grad_ffn_bias, grad_gain_two, grad_shift_two, grad_gain_one, grad_shift_one, grad_out_bias]
    )
    in_bias_share, vector_share = (
        lax.psum_scatter(grad_in_bias, both, scatter_dimension=0, tiled=True),
        lax.psum_scatter(vector_all, both, scatter_dimension=1, tiled=True),
    )
    conv_sum, bias_sum, bound_all, count_all = lax.psum(
        (conv_full, bias_full, bound_total, live_count), both
    )
    conv_out = lax.dynamic_slice_in_dim(conv_sum, head_index * heads_here, heads_here, 0)
    bias_out = lax.dynamic_slice_in_dim(bias_sum, head_index * head_width, head_width, 1)
    condition = bound_all / count_all
    return (
        final_out.astype(low),
        input_grad,
        qkv_share,
        bias_out,
        conv_out,
        out_share,
        up_share,
        in_bias_share,
        down_share,
        vector_share,
        condition,
    )


def place():
    b, z = lax.axis_index("batch"), lax.axis_index("heads")
    core, x, y = b % 2, (b // 2) % 2, b // 4
    return b, z, b + 1 - 2 * core, b + 2 - 4 * x, b + 4 - 8 * y


def remote(src, dst, send, recv, device):
    return pltpu.make_async_remote_copy(
        src_ref=src,
        dst_ref=dst,
        send_sem=send,
        recv_sem=recv,
        device_id=device,
        device_id_type=pl.DeviceIdType.MESH,
    )


def greet(devices):
    barrier = pltpu.get_barrier_semaphore()
    for device in devices:
        pl.semaphore_signal(
            barrier, inc=1, device_id=device, device_id_type=pl.DeviceIdType.MESH
        )
    pl.semaphore_wait(barrier, len(devices))


def tail_kernel(
    part_ref, first_ref, down_ref, up_ref, outw_ref, qkvw_ref, small_ref,
    input_ref, down_own, up_own, outw_own, qkvw_own, small_out,
    up_in, down_in, core_down, core_up, core_outw, core_qkvw,
    one_down, one_up, one_outw, one_qkvw, two_down, two_up, two_outw, two_qkvw,
    z_down, z_up, z_outw, small_in,
    z_send, z_recv, c_send, c_recv, x_send, x_recv, e_send, e_recv, s_send, s_recv,
):
    b, z, bc, bx, by = place()
    both = bx + by - b
    flip = bc - b
    peers = [(b, lax.rem(z + i, 4)) for i in (1, 2, 3)]
    greet(peers + [(bc, z), (bx, z), (by, z)])
    chunks = up_in.shape[1]
    size = up_in.shape[2]
    issued = []

    fulls = (down_ref, up_ref, outw_ref, qkvw_ref)
    cores = (core_down, core_up, core_outw, core_qkvw)
    ones = (one_down, one_up, one_outw, one_qkvw)
    twos = (two_down, two_up, two_outw, two_qkvw)
    kinds = len(fulls)
    groups = (b, bx, by, both)

    def at(n, who):
        return fulls[n].at[:, who] if n == 2 else fulls[n].at[who]

    for slot, who in enumerate(groups):
        for n in range(kinds):
            copy = remote(
                at(n, who + flip), cores[n].at[slot], c_send.at[n, slot], c_recv.at[n, slot],
                (bc, z),
            )
            copy.start()
            issued.append(copy)

    def flow(up, owner, c):
        buf = up_in if up else down_in
        side = 0 if up else 1
        return remote(
            buf.at[owner, c], buf.at[owner, c], z_send.at[side, owner, c],
            z_recv.at[side, owner, c], (b, z + 1 if up else z - 1),
        )

    def flow_first(up, owner, c):
        buf = up_in if up else down_in
        side = 0 if up else 1
        return remote(
            part_ref.at[owner, c], buf.at[owner, c], z_send.at[side, owner, c],
            z_recv.at[side, owner, c], (b, z + 1 if up else z - 1),
        )

    def z_event(k, c):
        for up in (True, False):
            owner = 3 - k if up else k
            buf = up_in if up else down_in
            at_end = (z == 0) if up else (z == 3)
            inner = ((z > 0) & (z < owner)) if up else ((z < 3) & (z > owner))

            @pl.when(at_end)
            def _():
                flow_first(up, owner, c).start()

            @pl.when(inner)
            def _():
                flow(up, owner, c).wait_recv()
                buf[owner, c] = (
                    buf[owner, c].astype(f32) + part_ref[owner, c].astype(f32)
                ).astype(low)
                flow(up, owner, c).start()

    def core_event(n):
        for slot, who in enumerate(groups):
            ref = cores[n].at[slot]
            remote(ref, ref, c_send.at[n, slot], c_recv.at[n, slot], (bc, z)).wait_recv()
            mine = fulls[n][:, who] if n == 2 else fulls[n][who]
            cores[n][slot] = (cores[n][slot].astype(f32) + mine.astype(f32)).astype(low)
        first, second = (2, 1) if n % 2 == 0 else (1, 2)
        partner = by if n % 2 == 0 else bx
        for i, (src, dst) in enumerate(((first, 0), (3, 1))):
            copy = remote(
                cores[n].at[src], ones[n].at[dst], x_send.at[n, i], x_recv.at[n, i], (partner, z)
            )
            copy.start()
            issued.append(copy)

    def one_event(n):
        first, second = (2, 1) if n % 2 == 0 else (1, 2)
        partner, other = (by, bx) if n % 2 == 0 else (bx, by)
        for i, slot in ((0, 0), (1, second)):
            ref = ones[n].at[i]
            remote(ref, ref, x_send.at[n, i], x_recv.at[n, i], (partner, z)).wait_recv()
            ones[n][i] = (ones[n][i].astype(f32) + cores[n][slot].astype(f32)).astype(low)
        copy = remote(
            ones[n].at[1], twos[n], x_send.at[n, 2], x_recv.at[n, 2], (other, z)
        )
        copy.start()
        issued.append(copy)

    z_bufs = (z_down, z_up, z_outw)

    def two_event(n):
        other = bx if n % 2 == 0 else by
        ref = twos[n]
        remote(ref, ref, x_send.at[n, 2], x_recv.at[n, 2], (other, z)).wait_recv()
        if n == 3:
            qkvw_own[...] = twos[n][...].astype(f32) + ones[n][0].astype(f32)
            return
        twos[n][...] = (twos[n][...].astype(f32) + ones[n][0].astype(f32)).astype(low)
        for i, (_, to) in enumerate(peers):
            copy = remote(
                twos[n].at[to], z_bufs[n].at[i], e_send.at[n, i], e_recv.at[n, i], (b, to)
            )
            copy.start()
            issued.append(copy)

    def end_event(n):
        total = twos[n][z].astype(f32)
        for i in range(3):
            source = lax.rem(z + 3 - i, 4)
            ref = z_bufs[n].at[i]
            remote(ref, ref, e_send.at[n, i], e_recv.at[n, i], (b, source)).wait_recv()
            total = total + z_bufs[n][i].astype(f32)
        (down_own, up_own, outw_own)[n][...] = total

    zf = z + 1 - 2 * (z % 2)
    zg = z + 2 - 4 * (z // 2)
    partners = ((bc, z), (bx, z), (by, z), (b, zf), (b, zg))

    def small_start(k):
        copy = remote(
            small_out.at[k], small_in.at[k], s_send.at[k], s_recv.at[k], partners[k]
        )
        copy.start()
        issued.append(copy)

    def small_event(k):
        ref = small_in.at[k]
        remote(ref, ref, s_send.at[k], s_recv.at[k], partners[k]).wait_recv()
        small_out[k + 1] = small_out[k] + small_in[k]
        if k < 4:
            small_start(k + 1)

    small_out[0] = small_ref[...]
    small_start(0)

    z_list = [(k, c) for k in range(3) for c in range(chunks)]
    other = (
        [partial(core_event, n) for n in (0, 1, 2, 3)]
        + [partial(small_event, 0), partial(small_event, 1)]
        + [partial(one_event, n) for n in (0, 1, 2, 3)]
        + [partial(small_event, 2), partial(small_event, 3)]
        + [partial(two_event, n) for n in (0, 1, 2, 3)]
        + [partial(small_event, 4)]
    )
    lead = 2
    for k, c in z_list[:lead]:
        z_event(k, c)
    rest = z_list[lead:]
    for n in range(max(len(rest), len(other))):
        if n < len(other):
            other[n]()
        if n < len(rest):
            z_event(*rest[n])
    for n in (0, 1, 2):
        end_event(n)

    for c in range(chunks):
        rows = pl.ds(c * size, size)
        input_ref[rows] = first_ref[rows] + part_ref[z, c].astype(f32)

    for c in range(chunks):
        rows = pl.ds(c * size, size)
        for up in (True, False):
            buf = up_in if up else down_in

            @pl.when((z > 0) if up else (z < 3))
            def _():
                side = 0 if up else 1
                ref = buf.at[z, c]
                remote(
                    ref, ref, z_send.at[side, z, c], z_recv.at[side, z, c],
                    (b, z - 1 if up else z + 1),
                ).wait_recv()
                input_ref[rows] += buf[z, c].astype(f32)

    for k, c in z_list:
        for up in (True, False):
            owner = 3 - k if up else k

            @pl.when((z < owner) if up else (z > owner))
            def _():
                flow(up, owner, c).wait_send()

    for copy in issued:
        copy.wait_send()


def tail(part, first, down, up, outw, qkvw, small):
    quarter, model = first.shape
    chunks = 4
    size = quarter // chunks
    ff = down.shape[2]
    on, oh = outw.shape[2:]
    qn, qh = qkvw.shape[1:]
    blocks = ((4, ff, model), (4, ff, model), (4, on, oh), (qn, qh))
    own = lambda *s: jax.ShapeDtypeStruct(s, f32)
    vm = lambda *s: pltpu.VMEM(s, low)
    dma = pltpu.SemaphoreType.DMA
    return pl.pallas_call(
        tail_kernel,
        out_shape=[
            own(quarter, model), own(ff, model), own(ff, model), own(on, oh), own(qn, qh),
            own(6, *small.shape),
        ],
        in_specs=[pl.BlockSpec(memory_space=pltpu.VMEM)] * 7,
        out_specs=[pl.BlockSpec(memory_space=pltpu.VMEM)] * 6,
        scratch_shapes=[
            vm(4, chunks, size, model), vm(4, chunks, size, model),
            *[vm(4, *s) for s in blocks],
            *[vm(2, *s) for s in blocks],
            *[vm(*s) for s in blocks],
            *[vm(3, *s[1:]) for s in blocks[:3]],
            pltpu.VMEM((5, *small.shape), f32),
            dma((2, 4, chunks)), dma((2, 4, chunks)), dma((4, 4)), dma((4, 4)),
            dma((4, 3)), dma((4, 3)), dma((3, 3)), dma((3, 3)), dma((5,)), dma((5,)),
        ],
        compiler_params=pltpu.CompilerParams(
            collective_id=3, has_side_effects=True, vmem_limit_bytes=62 * 1024 * 1024
        ),
        name="tail",
    )(part.reshape(4, chunks, size, model), first, down, up, outw, qkvw, small)


def cumulative(x):
    t = 1.0 / (1.0 + 0.23164189 * jnp.abs(x))
    density = jnp.exp(-0.5 * x * x) * 0.3989422804
    poly = t * (
        0.319381530 + t * (-0.356563782 + t * (1.781477937 + t * (-1.821255978 + t * 1.330274429)))
    )
    upper = density * poly
    return jnp.where(x >= 0.0, 1.0 - upper, upper), density


def normed(x):
    centre = x - jnp.mean(x, axis=1, keepdims=True)
    scale = lax.rsqrt(jnp.mean(centre * centre, axis=1, keepdims=True) + norm_eps)
    return centre * scale, scale


def norm_back(grad, gain, rows, scale):
    e = grad * gain
    return scale * (
        e - jnp.mean(e, axis=1, keepdims=True) - rows * jnp.mean(e * rows, axis=1, keepdims=True)
    )


def middle_kernel(
    pieces, share,
    mixed_ref, own0, own1, own2, own3, tok_ref, cot_ref, vec_ref,
    out_ref, first_ref, attn_ref, hidden_ref, pre_ref, norm_ref, ffn_ref, all_ref, grad_ref,
    sums_ref, bin_ref,
    packs, wof, wo, slope, total, turned,
    a_send, a_recv, f_send, f_recv, p_send, p_recv, g_send, g_recv, own_sem, own_turn,
):
    b, z, bc, bx, by = place()
    both = bx + by - b
    peers = [(b, lax.rem(z + i, 4)) for i in (1, 2, 3)]
    greet(peers + [(bc, z), (bx, z), (by, z)])
    width, quarter = all_ref.shape[1:]
    model = tok_ref.shape[1]
    owns = (own0, own1, own2, own3)
    origins = [lax.rem(z + 4 - i, 4) for i in range(4)]
    issued = []

    def columns(n):
        return pl.ds(pl.multiple_of(n * quarter, quarter), quarter)

    for i, (_, to) in enumerate(peers):
        copy = remote(
            mixed_ref.at[:, columns(to)], all_ref.at[z], a_send.at[i], a_recv.at[i], (b, to)
        )
        copy.start()
        issued.append(copy)
    local = [
        pltpu.make_async_copy(own, packs.at[b, origin], own_sem.at[i])
        for i, (own, origin) in enumerate(zip(owns, origins))
    ]
    local.append(
        pltpu.make_async_copy(mixed_ref.at[:, columns(z)], all_ref.at[z], own_sem.at[4])
    )
    count = len(pieces)

    def near(n):
        return by if pieces[n][2] else bx

    def far(n):
        return bx if pieces[n][2] else by

    for n in range(count):
        rows = pl.ds(*pieces[n][:2])
        for i in range(4):
            copy = remote(
                owns[i].at[rows], packs.at[b, origins[i], rows],
                f_send.at[n, i], f_recv.at[n, i], (near(n), z),
            )
            copy.start()
            issued.append(copy)
    for copy in local:
        copy.start()

    def pair(n, slot, who, device):
        ref = packs.at[who, :, pl.ds(*pieces[n][:2])]
        return remote(ref, ref, p_send.at[n, slot], p_recv.at[n, slot], (device, z))

    def send(n, slot, who, device):
        copy = pair(n, slot, who, device)
        copy.start()
        issued.append(copy)

    for copy in local:
        copy.wait()
    for n in range(count):
        send(n, 0, b, far(n))
        send(n, 2, b, bc)
    for n in range(count):
        rows = pl.ds(*pieces[n][:2])
        for i in range(4):
            ref = packs.at[near(n), origins[i], rows]
            remote(ref, ref, f_send.at[n, i], f_recv.at[n, i], (near(n), z)).wait_recv()
        send(n, 1, near(n), far(n))
        send(n, 3, near(n), bc)
    for n in range(count):
        pair(n, 0, far(n), far(n)).wait_recv()
        send(n, 4, far(n), bc)
    for n in range(count):
        pair(n, 1, both, far(n)).wait_recv()
        send(n, 5, both, bc)
    flip = bc - b
    for n in range(count):
        pair(n, 2, bc, bc).wait_recv()
        pair(n, 3, near(n) + flip, bc).wait_recv()
        pair(n, 4, far(n) + flip, bc).wait_recv()
        pair(n, 5, both + flip, bc).wait_recv()
    for i in (1, 2, 3):
        ref = all_ref.at[origins[i]]
        remote(ref, ref, a_send.at[i - 1], a_recv.at[i - 1], (b, origins[i])).wait_recv()

    ff = (packs.shape[2] - 32) // 2
    group = 4 * ff
    for q in range(8):
        for s in range(4):
            wof[pl.ds(s * width + q * share, share), :] = packs[
                q, s, pl.ds(2 * ff, share), :
            ].astype(f32)
    wo[...] = wof[...].astype(low).reshape(wo.shape)
    ff_bias = []
    for q in range(8):
        row = jnp.zeros((1, group), f32)
        for s in range(4):
            row = row + packs[q, s, 2 * ff + share : 2 * ff + share + 1, :group].astype(f32)
        ff_bias.append(row)
    out_bias, gain1, shift1, down_bias, gain2, shift2 = [
        vec_ref[n : n + 1, :] for n in range(6)
    ]
    sums_ref[...] = jnp.zeros_like(sums_ref)
    bin_ref[...] = jnp.zeros_like(bin_ref)
    for q in range(8):
        bin_ref[1:2, q * group : (q + 1) * group] = ff_bias[q]
    size = turned.shape[2]
    span = 2 * group

    def weights(c, start):
        return jnp.concatenate(
            [
                packs[2 * c + n, :, pl.ds(start, ff), :].reshape(group, model)
                for n in range(2)
            ],
            axis=0,
        )

    def row_sum(n, x):
        sums_ref[n : n + 1, :] += jnp.sum(x, axis=0, keepdims=True)

    def turn_copy(r, i):
        to = lax.rem(z + i, 4)
        src = turned.at[r, pl.ds(pl.multiple_of(to * width, width), width)]
        dst = grad_ref.at[:, pl.ds(pl.multiple_of(z * quarter + r * size, size), size)]
        return remote(src, dst, g_send.at[r, i - 1], g_recv.at[r, i - 1], (b, to))

    def turn_own(r):
        src = turned.at[r, pl.ds(pl.multiple_of(z * width, width), width)]
        dst = grad_ref.at[:, pl.ds(pl.multiple_of(z * quarter + r * size, size), size)]
        return pltpu.make_async_copy(src, dst, own_turn.at[r])

    def row_tile(r, _):
        at = pl.multiple_of(r * size, size)
        rows = pl.ds(at, size)
        attn = jnp.zeros((size, model), f32)
        for s in range(4):
            attn = attn + lax.dot_general(
                all_ref[s, :, rows], wo[s], (((0,), (0,)), ((), ())), preferred_element_type=f32
            )
        n1, scale1 = normed(tok_ref[rows, :].astype(f32) + attn + out_bias)
        norm1 = n1 * gain1 + shift1
        norm_low = norm1.astype(low)
        norm_ref[rows, :] = norm_low
        total[...] = jnp.zeros_like(total)

        def forward(c, _):
            lanes = pl.ds(pl.multiple_of(c * span, span), span)
            act = mul_t(norm_low, weights(c, 0)) + bin_ref[1:2, lanes]
            phi, density = cumulative(act)
            hidden = (act * phi).astype(low)
            hidden_ref[rows, lanes] = hidden
            slope[:, lanes] = phi + act * density
            total[...] += mul(hidden, weights(c, ff))
            return 0

        lax.fori_loop(0, 4, forward, 0)
        n2, scale2 = normed(norm1 + total[...] + down_bias)
        out_ref[rows, :] = (n2 * gain2 + shift2).astype(low)
        cot = cot_ref[rows, :].astype(f32)
        row_sum(1, cot * n2)
        row_sum(2, cot)
        grad2 = norm_back(cot, gain2, n2, scale2)
        grad_low = grad2.astype(low)
        ffn_ref[rows, :] = grad_low
        row_sum(0, grad_low.astype(f32))
        total[...] = grad2

        def backward(c, _):
            lanes = pl.ds(pl.multiple_of(c * span, span), span)
            grad = (slope[:, lanes] * mul_t(grad_low, weights(c, ff))).astype(low)
            pre_ref[rows, lanes] = grad
            bin_ref[0:1, lanes] += jnp.sum(grad.astype(f32), axis=0, keepdims=True)
            total[...] += mul(grad, weights(c, 0))
            return 0

        lax.fori_loop(0, 4, backward, 0)
        grad1 = total[...]
        row_sum(3, grad1 * n1)
        row_sum(4, grad1)
        first = norm_back(grad1, gain1, n1, scale1)
        first_ref[rows, :] = first
        attn_low = first.astype(low)
        attn_ref[rows, :] = attn_low
        row_sum(5, attn_low.astype(f32))
        for s in range(4):
            turned[r, pl.ds(s * width, width), :] = mul_t(wo[s], attn_low).astype(low)
        for i in (1, 2, 3):
            turn_copy(r, i).start()
        turn_own(r).start()
        return 0

    tiles = quarter // size
    lax.fori_loop(0, tiles, row_tile, 0)

    def finish(r, _):
        for i in (1, 2, 3):
            source = origins[i]
            ref = grad_ref.at[:, pl.ds(pl.multiple_of(source * quarter + r * size, size), size)]
            remote(ref, ref, g_send.at[r, i - 1], g_recv.at[r, i - 1], (b, source)).wait_recv()
            turn_copy(r, i).wait_send()
        turn_own(r).wait()
        return 0

    lax.fori_loop(0, tiles, finish, 0)
    for copy in issued:
        copy.wait_send()


def ffn_middle(mixed_t, packs, tok, cot, vectors, ff, share):
    width, tok_count = mixed_t.shape
    quarter, model = tok.shape
    size = quarter // 3
    rows = packs[0].shape[0]
    half = ff // 2
    pieces = (
        (2 * ff, rows - 2 * ff, 0),
        (0, half, 0), (ff, half, 1), (half, half, 0), (ff + half, half, 1),
    )
    n = len(pieces)
    shape = jax.ShapeDtypeStruct
    vmem = pl.BlockSpec(memory_space=pltpu.VMEM)
    hbm = pl.BlockSpec(memory_space=pl.ANY)
    dma = pltpu.SemaphoreType.DMA
    return pl.pallas_call(
        partial(middle_kernel, pieces, share),
        out_shape=[
            shape((quarter, model), low),
            shape((quarter, model), f32),
            shape((quarter, model), low),
            shape((quarter, 32 * ff), low),
            shape((quarter, 32 * ff), low),
            shape((quarter, model), low),
            shape((quarter, model), low),
            shape((4, width, quarter), low),
            shape((width, tok_count), low),
            shape((8, model), f32),
            shape((8, 32 * ff), f32),
        ],
        in_specs=[hbm] + [vmem] * 7,
        out_specs=[vmem] * 8 + [hbm] + [vmem] * 2,
        scratch_shapes=[
            pltpu.VMEM((8, 4, rows, model), low),
            pltpu.VMEM((4 * width, model), f32),
            pltpu.VMEM((4, width, model), low),
            pltpu.VMEM((size, 32 * ff), f32),
            pltpu.VMEM((size, model), f32),
            pltpu.VMEM((3, 4 * width, size), low),
            dma((3,)), dma((3,)), dma((n, 4)), dma((n, 4)), dma((n, 6)), dma((n, 6)),
            dma((3, 3)), dma((3, 3)), dma((5,)), dma((3,)),
        ],
        compiler_params=pltpu.CompilerParams(
            collective_id=1, has_side_effects=True, vmem_limit_bytes=62 * 1024 * 1024
        ),
        name="middle",
    )(mixed_t, *packs, tok, cot, vectors)


def slice_body(
    tokens,
    qkv_weight,
    qv_bias,
    conv_weight,
    out_weight,
    out_bias,
    norm1_gain,
    norm1_bias,
    ffn_in_weight,
    ffn_in_bias,
    ffn_out_weight,
    ffn_out_bias,
    norm2_gain,
    norm2_bias,
    cotangent,
    seq_lengths,
    segment_ids,
    landmark_bounds,
):
    tok_count, model = tokens.shape
    width = qkv_weight.shape[2]
    heads_here = width // HEAD_DIM
    kernel_taps = conv_weight.shape[1]
    slots, marks = landmark_bounds.shape
    quarter = tok_count // 4
    z = lax.axis_index("heads")
    b = lax.axis_index("batch")
    own_low = lax.dynamic_slice_in_dim(tokens, z * quarter, quarter, 0)
    conv_own = lax.dynamic_slice_in_dim(conv_weight, z * heads_here, heads_here, 0)
    qv_own = lax.dynamic_slice_in_dim(qv_bias, z * width, width, 1)
    flat_qkv = qkv_weight.reshape(model, 3 * width)
    bias_col = jnp.concatenate([qv_own[0], jnp.zeros_like(qv_own[0]), qv_own[1]])[:, None]
    ff_own = ffn_out_weight.shape[0]
    share = width // 8
    bias_row = lax.dynamic_update_slice_in_dim(
        jnp.zeros((4 * ff_own,), low), ffn_in_bias, z * ff_own, 0
    )
    misc_own = jnp.concatenate(
        [
            lax.dynamic_slice_in_dim(out_weight, b * share, share, 0),
            jnp.zeros((32 - share, model), low).at[0, : 4 * ff_own].set(bias_row),
        ],
        axis=0,
    )
    pack = jnp.concatenate([jnp.transpose(ffn_in_weight), ffn_out_weight, misc_own], axis=0)
    packs = [pack] + [
        lax.ppermute(pack, "heads", [(n, (n + i) % 4) for n in range(4)]) for i in (1, 2, 3)
    ]
    forward = mix_forward(
        seq_lengths, tokens, jnp.transpose(flat_qkv), bias_col, conv_own, slots, marks
    )
    qkv_t, first, last, mixed_t, mark, value, inner, denom, middle, steps, inverse, bound = forward
    vectors = jnp.concatenate(
        [
            jnp.stack(
                [out_bias, norm1_gain, norm1_bias, ffn_out_bias, norm2_gain, norm2_bias]
            ),
            jnp.zeros((2, model), f32),
        ]
    )
    (
        final_low, grad_first, grad_attn_low, hidden_low, grad_pre, norm1_low, grad_ffn_low,
        mixed_all, grad_mix_t, vector_sums, bias_sums,
    ) = ffn_middle(mixed_t, packs, own_low, cotangent, vectors, ff_own, share)
    grad_in_bias = bias_sums[0]
    saved = (qkv_t, first, last, mark, value, inner, denom, middle, steps, inverse)
    grad_t, grad_bias, grad_conv = mix_backward(
        seq_lengths, grad_mix_t, saved, conv_own, slots, marks
    )
    part = lax.dot_general(
        grad_t, flat_qkv, (((0,), (1,)), ((), ())), preferred_element_type=f32
    ).astype(low)
    down_term = lax.dot_general(
        hidden_low, grad_ffn_low, contract_rows, preferred_element_type=f32
    ).astype(low)
    up_term = lax.dot_general(
        grad_pre, norm1_low, contract_rows, preferred_element_type=f32
    ).astype(low)
    out_term = lax.dot_general(
        grad_attn_low,
        mixed_all,
        (((0,), (2,)), ((), ())),
        preferred_element_type=f32,
    ).astype(low)
    out_term = jnp.swapaxes(out_term, 0, 1).reshape(4, 8, model // 8, width)
    qkv_term = lax.dot_general(
        tokens, grad_t, (((0,), (1,)), ((), ())), preferred_element_type=f32
    ).astype(low)

    flat = jnp.concatenate(
        [
            grad_in_bias,
            vector_sums[:6].reshape(-1),
        ]
    )
    head_total = conv_weight.shape[0]
    conv_full = lax.dynamic_update_slice_in_dim(
        jnp.zeros((head_total, kernel_taps), f32), grad_conv[:, :kernel_taps], z * heads_here, 0
    )
    bias_full = lax.dynamic_update_slice_in_dim(
        jnp.zeros((2, 4 * width), f32), jnp.transpose(grad_bias), z * width, 1
    )
    live_count = jnp.sum((seq_lengths > 0).astype(f32)) * heads_here
    scalars = jnp.stack([bound[0, 0], live_count])
    small = jnp.concatenate([flat, bias_full.reshape(-1), conv_full.reshape(-1), scalars])
    lanes = 768
    rows = -(-small.shape[0] // (8 * lanes)) * 8
    small = jnp.pad(small, (0, rows * lanes - small.shape[0])).reshape(rows, lanes)
    ff = ff_own * 32
    input_grad, down_share, up_share, out_share, qkv_share, sums = tail(
        part,
        grad_first,
        down_term.reshape(8, 4, ff_own, model),
        up_term.reshape(8, 4, ff_own, model),
        out_term,
        qkv_term.reshape(8, model // 8, 3 * width),
        small,
    )
    sums = sums[5].reshape(-1)
    index = b * 4 + z
    in_bias_share = lax.dynamic_slice_in_dim(sums, index * ff_own, ff_own, 0)
    vectors = sums[ff : ff + 6 * model].reshape(6, model)
    vector_share = lax.dynamic_slice_in_dim(vectors, index * (model // 32), model // 32, 1)
    at = ff + 6 * model
    bias_sum = sums[at : at + 8 * width].reshape(2, 4 * width)
    bias_out = lax.dynamic_slice_in_dim(bias_sum, z * width, width, 1)
    at = at + 8 * width
    conv_sum = sums[at : at + head_total * kernel_taps].reshape(head_total, kernel_taps)
    conv_out = lax.dynamic_slice_in_dim(conv_sum, z * heads_here, heads_here, 0)
    at = at + head_total * kernel_taps
    condition = sums[at] / sums[at + 1]
    return (
        final_low,
        input_grad,
        qkv_share.reshape(model // 8, 3, width),
        bias_out,
        conv_out,
        jnp.transpose(out_share),
        jnp.transpose(up_share),
        in_bias_share,
        down_share,
        vector_share,
        condition,
    )


def solution(mesh):
    chosen = slice_body if dict(mesh.shape) == {"batch": 8, "heads": 4} else body
    in_specs = (
        P("batch", None),
        P(None, None, "heads"),
        P(),
        P(),
        P("heads", None),
        P(),
        P(),
        P(),
        P(None, ("batch", "heads")),
        P(("batch", "heads")),
        P(("batch", "heads"), None),
        P(),
        P(),
        P(),
        P(("batch", "heads"), None),
        P("batch"),
        P("batch"),
        P("batch", None),
    )
    out_specs = (
        P(("batch", "heads"), None),
        P(("batch", "heads"), None),
        P("batch", None, "heads"),
        P(None, "heads"),
        P("heads", None),
        P("heads", "batch"),
        P(None, ("batch", "heads")),
        P(("batch", "heads")),
        P(("batch", "heads"), None),
        P(None, ("batch", "heads")),
        P(),
    )
    return jax.shard_map(chosen, mesh=mesh, in_specs=in_specs, out_specs=out_specs, check_vma=False)
```

```python
from functools import partial

import jax
import jax.numpy as jnp
from jax import lax
from jax.experimental import pallas as pl
from jax.experimental.pallas import tpu as pltpu
from jax.sharding import PartitionSpec as P

HEAD_DIM = 64
PINV_ITERS = 6
TILE = 512
SUB = 128

f32 = jnp.float32
low = jnp.bfloat16
mask_fill = -1000000000.0


def split(x):
    high = x.astype(low)
    return high, (x - high.astype(f32)).astype(low)


def mul(a, b):
    return lax.dot_general(a, b, (((1,), (0,)), ((), ())), preferred_element_type=f32)


def mul_t(a, b):
    return lax.dot_general(a, b, (((1,), (1,)), ((), ())), preferred_element_type=f32)


def wide(form, left, right):
    left_high, left_low = split(left)
    right_high, right_low = split(right)
    return form(left_high, right_high) + (
        form(left_high, right_low) + form(left_low, right_high)
    )


def block_grid(rows, cols):
    row_block = lax.broadcasted_iota(jnp.int32, (rows, cols), 0) // HEAD_DIM
    col_block = lax.broadcasted_iota(jnp.int32, (rows, cols), 1) // HEAD_DIM
    return row_block == col_block


def spread(x, blocks):
    count = blocks.shape[0] // x.shape[0]
    return jnp.where(blocks, jnp.concatenate([x] * count, axis=0), jnp.zeros_like(x[:1, :1]))


def fold(x, blocks):
    kept = jnp.where(blocks, x, jnp.zeros_like(x[:1, :1]))
    rows = HEAD_DIM
    out = kept[:rows]
    for n in range(1, x.shape[0] // rows):
        out = out + kept[n * rows : (n + 1) * rows]
    return out


def pack_mul(left, right, blocks):
    left_high, left_low = split(left)
    right_high, right_low = split(right)
    right_high, right_low = spread_low(right_high, blocks), spread_low(right_low, blocks)
    return mul(left_high, right_high) + (mul(left_high, right_low) + mul(left_low, right_high))


def pack_mul_t(left, right, blocks):
    left_high, left_low = split(left)
    right_high, right_low = split(right)
    right_high, right_low = spread_low(right_high, blocks), spread_low(right_low, blocks)
    return mul_t(left_high, right_high) + (mul_t(left_high, right_low) + mul_t(left_low, right_high))


def spread_low(x, blocks):
    return spread(x.astype(f32), blocks).astype(low)


def slot_bounds(len_ref, s, slots):
    start = jnp.int32(0)
    for n in range(slots):
        start = start + jnp.where(n < s, len_ref[n], 0)
    return start, start + len_ref[s]


def eye_pack(width):
    row = lax.broadcasted_iota(jnp.int32, (HEAD_DIM, width), 0)
    col = lax.broadcasted_iota(jnp.int32, (HEAD_DIM, width), 1) % HEAD_DIM
    return jnp.where(row == col, 1.0, 0.0).astype(f32)


def lane_mask(start, end, at, width):
    tok = at + lax.broadcasted_iota(jnp.int32, (1, width), 1)
    return (tok >= start) & (tok < end)


def band(taps_row, width):
    row = lax.broadcasted_iota(jnp.int32, (SUB, 3 * SUB), 0)
    col = lax.broadcasted_iota(jnp.int32, (SUB, 3 * SUB), 1)
    off = col - row - (SUB - width // 2)
    out = jnp.zeros((SUB, 3 * SUB), f32)
    for n in range(width):
        out = jnp.where(off == n, taps_row[:, n : n + 1], out)
    return out


def slot_marks(len_ref, at, slots, marks, width):
    rows = slots * marks
    row = lax.broadcasted_iota(jnp.int32, (rows, 1), 0)
    slot = row // marks
    mark = row % marks
    start = jnp.zeros((rows, 1), jnp.int32)
    length = jnp.zeros((rows, 1), jnp.int32)
    for n in range(slots):
        start = start + jnp.where(slot > n, len_ref[n], 0)
        length = jnp.where(slot == n, len_ref[n], length)
    lower = start + (mark * length) // marks
    upper = start + ((mark + 1) * length) // marks
    inv_count = 1.0 / jnp.maximum((upper - lower).astype(f32), 1.0)
    tok = at + lax.broadcasted_iota(jnp.int32, (rows, width), 1)
    member = jnp.where((tok >= lower) & (tok < upper), 1.0, 0.0)
    return member, inv_count


def mix_forward_kernel(
    slots, marks, taps,
    len_ref, tok_ref, weight_ref, bias_ref, conv_ref,
    qkv_ref, first_ref, last_ref, mixed_ref, mark_ref, value_ref, inner_ref,
    denom_ref, middle_ref, steps_ref, inverse_ref, bound_ref,
    vpad, scores, vsum,
):
    step = pl.program_id(0)
    width = first_ref.shape[0]
    heads = width // HEAD_DIM
    tok_count = qkv_ref.shape[1]
    tiles = tok_count // TILE
    packed = slots * marks
    at = pl.multiple_of(step * TILE, TILE)

    @pl.when(step == 0)
    def _():
        mark_ref[...] = jnp.zeros_like(mark_ref)
        vsum[...] = jnp.zeros_like(vsum)
        vpad[:, :SUB] = jnp.zeros((width, SUB), low)
        vpad[:, tok_count + SUB :] = jnp.zeros((width, SUB), low)

    rows = (mul_t(weight_ref[...], tok_ref[...]) + bias_ref[...]).astype(low)
    qkv_ref[:, pl.ds(at, TILE)] = rows
    vpad[:, pl.ds(pl.multiple_of(at + SUB, SUB), TILE)] = rows[2 * width :]
    member, inv_count = slot_marks(len_ref, at, slots, marks, TILE)
    mark_ref[...] += mul_t(member.astype(low), rows[: 2 * width])
    vsum[...] += mul_t(jnp.ones((8, TILE), low), rows[2 * width :])
    first_ref[:, pl.ds(at, TILE)] = jnp.zeros((width, TILE), low)
    last_ref[:, pl.ds(at, TILE)] = jnp.zeros((width, TILE), low)
    mixed_ref[:, pl.ds(at, TILE)] = jnp.zeros((width, TILE), low)

    @pl.when(step == tiles - 1)
    def _():
        mark_ref[...] = mark_ref[...] * inv_count
        head_blocks = block_grid(width, width)
        slot_blocks = block_grid(packed, packed)
        eye = eye_pack(packed)
        scale = HEAD_DIM ** -0.5

        middles, inverses_t, products = [], [], []
        bound_total = jnp.zeros((1, 1), f32)
        lane_slot = lax.broadcasted_iota(jnp.int32, (1, packed), 1) // marks
        for h in range(heads):
            q_marks = mark_ref[:, h * HEAD_DIM : (h + 1) * HEAD_DIM]
            k_marks = mark_ref[:, width + h * HEAD_DIM : width + (h + 1) * HEAD_DIM]
            sim = wide(mul_t, q_marks, k_marks) * scale
            sim = jnp.where(slot_blocks, sim, -1e30)
            sim = jnp.exp(sim - jnp.max(sim, axis=1, keepdims=True))
            sim = sim / jnp.sum(sim, axis=1, keepdims=True)
            middle = fold(sim, slot_blocks)
            col_sums = jnp.sum(middle, axis=0, keepdims=True)
            bound = jnp.zeros((1, packed), f32)
            for s in range(slots):
                top = jnp.max(jnp.where(lane_slot == s, col_sums, 0.0), axis=1, keepdims=True)
                bound = jnp.where(lane_slot == s, top, bound)
                bound_total += jnp.where(len_ref[s] > 0, top, 0.0)
            middle_ref[h] = middle
            middles.append(middle)
            inverses_t.append(middle / bound)
            products.append(pack_mul_t(middle, middle, slot_blocks) / bound)
        bound_ref[...] = jnp.broadcast_to(bound_total, bound_ref.shape)

        def newton(n, carry):
            out = []
            for h in range(heads):
                inverse_t, product = carry[h]
                square = pack_mul(product, product, slot_blocks)
                cube = pack_mul(product, square, slot_blocks)
                fourth = pack_mul(square, square, slot_blocks)
                second = 15.0 * eye - 7.0 * product + square
                third = 13.0 * eye - 15.0 * product + 7.0 * square - cube
                steps_ref[n, 0, h] = product
                steps_ref[n, 1, h] = second
                steps_ref[n, 2, h] = third
                steps_ref[n, 3, h] = inverse_t
                out.append(
                    (
                        0.25 * pack_mul(third, inverse_t, slot_blocks),
                        0.25 * (13.0 * product - 15.0 * square + 7.0 * cube - fourth),
                    )
                )
            return tuple(out)

        final = lax.fori_loop(0, PINV_ITERS, newton, tuple(zip(inverses_t, products)))
        for h in range(heads):
            inverse_ref[h] = final[h][0]

        def one_slot(s, _):
            start, end = slot_bounds(len_ref, s, slots)
            lo, hi = start // TILE, (end + TILE - 1) // TILE
            hi = jnp.where(end > start, hi, lo)
            own = mark_ref[pl.ds(pl.multiple_of(s * marks, marks), marks), :] * scale
            q_block = spread(own[:, :width], head_blocks).astype(low)
            k_block = spread(own[:, width:], head_blocks).astype(low)

            def score_tile(n, top):
                t = pl.multiple_of(n * TILE, TILE)
                mask = lane_mask(start, end, t, TILE)
                sim = mul(k_block, qkv_ref[:width, pl.ds(t, TILE)])
                sim = sim.reshape(heads, marks, TILE)
                sim = jnp.exp(sim - jnp.max(sim, axis=1, keepdims=True))
                sim = sim / jnp.sum(sim, axis=1, keepdims=True)
                sim = sim.reshape(width, TILE)
                old = first_ref[:, pl.ds(t, TILE)].astype(f32)
                first_ref[:, pl.ds(t, TILE)] = jnp.where(mask, sim, old).astype(low)
                sim = mul(q_block, qkv_ref[width : 2 * width, pl.ds(t, TILE)])
                sim = jnp.where(mask, sim, mask_fill)
                scores[:, pl.ds(t, TILE)] = sim
                for c in range(TILE // SUB):
                    top = jnp.maximum(top, sim[:, c * SUB : (c + 1) * SUB])
                return top

            top = lax.fori_loop(lo, hi, score_tile, jnp.full((width, SUB), mask_fill, f32))
            top = jnp.max(top, axis=1, keepdims=True)

            def value_tile(n, carry):
                denom, total = carry
                t = pl.multiple_of(n * TILE, TILE)
                mask = lane_mask(start, end, t, TILE)
                part = jnp.exp(scores[:, pl.ds(t, TILE)] - top)
                old = last_ref[:, pl.ds(t, TILE)].astype(f32)
                last_ref[:, pl.ds(t, TILE)] = jnp.where(mask, part, old).astype(low)
                total = total + mul_t(part.astype(low), qkv_ref[2 * width :, pl.ds(t, TILE)])
                for c in range(TILE // SUB):
                    denom = denom + part[:, c * SUB : (c + 1) * SUB]
                return denom, total

            denom, total = lax.fori_loop(
                lo, hi, value_tile,
                (jnp.zeros((width, SUB), f32), jnp.zeros((width, width), f32)),
            )
            denom = jnp.sum(denom, axis=1, keepdims=True)
            inv = 1.0 / jnp.where(denom > 0.0, denom, 1.0)
            denom_ref[s] = inv
            values = fold(total * inv, head_blocks)
            values = jnp.where(end > start, values, vsum[:1] / tok_count)
            value_ref[pl.ds(pl.multiple_of(s * marks, marks), marks), :] = values
            return 0

        lax.fori_loop(0, slots, one_slot, 0)

        lane_head = lax.broadcasted_iota(jnp.int32, (1, width), 1) // HEAD_DIM
        inner = jnp.zeros((packed, width), f32)
        for h in range(heads):
            inverse = pack_mul_t(eye, final[h][0], slot_blocks)
            own_values = jnp.where(lane_head == h, value_ref[...], 0.0)
            inner = inner + wide(mul, spread(inverse, slot_blocks), own_values)
        inner_ref[...] = inner

        bands = [band(conv_ref[h : h + 1, :], taps).astype(low) for h in range(heads)]

        def out_slot(s, _):
            start, end = slot_bounds(len_ref, s, slots)
            lo, hi = start // TILE, (end + TILE - 1) // TILE
            hi = jnp.where(end > start, hi, lo)
            own = inner_ref[pl.ds(pl.multiple_of(s * marks, marks), marks), :]
            a_block = jnp.transpose(spread(own, head_blocks)).astype(low)

            def out_tile(n, _):
                t = pl.multiple_of(n * TILE, TILE)
                mask = lane_mask(start, end, t, TILE)
                rows = mul(a_block, first_ref[:, pl.ds(t, TILE)])
                rows = rows + convolve(vpad, bands, start, end, t, heads)
                old = mixed_ref[:, pl.ds(t, TILE)].astype(f32)
                mixed_ref[:, pl.ds(t, TILE)] = jnp.where(mask, rows, old).astype(low)
                return 0

            return lax.fori_loop(lo, hi, out_tile, 0)

        lax.fori_loop(0, slots, out_slot, 0)


def windows(padded, start, end, t):
    full = padded[:, pl.ds(t, TILE + 2 * SUB)]
    keep = lane_mask(start, end, t - SUB, TILE + 2 * SUB)
    return jnp.where(keep, full.astype(f32), 0.0).astype(low)


def convolve(padded, bands, start, end, t, heads):
    full = windows(padded, start, end, t)
    out = []
    count = TILE // SUB
    for h in range(heads):
        own = full[h * HEAD_DIM : (h + 1) * HEAD_DIM]
        stack = jnp.concatenate(
            [own[:, c * SUB : (c + 3) * SUB] for c in range(count)], axis=0
        )
        res = mul_t(stack, bands[h])
        out.append(
            jnp.concatenate(
                [res[c * HEAD_DIM : (c + 1) * HEAD_DIM] for c in range(count)], axis=1
            )
        )
    return jnp.concatenate(out, axis=0)


def mix_backward_kernel(
    slots, marks, taps,
    len_ref, grad_ref, qkv_ref, first_ref, last_ref, mark_ref, value_ref, inner_ref,
    denom_ref, middle_ref, steps_ref, inverse_ref, conv_ref,
    out_ref, bias_ref, conv_out_ref,
    gpad, vpad, ds_first, ds_last, conv_grad, d_inner, d_k, d_q, d_value,
):
    width = first_ref.shape[0]
    heads = width // HEAD_DIM
    tok_count = qkv_ref.shape[1]
    packed = slots * marks
    scale = HEAD_DIM ** -0.5
    head_blocks = block_grid(width, width)
    slot_blocks = block_grid(packed, packed)
    eye = eye_pack(packed)
    count = TILE // SUB

    for padded, source in ((gpad, grad_ref[...]), (vpad, qkv_ref[2 * width :, :])):
        padded[:, :SUB] = jnp.zeros((width, SUB), low)
        padded[:, tok_count + SUB :] = jnp.zeros((width, SUB), low)
        padded[:, SUB : tok_count + SUB] = source
    out_ref[...] = jnp.zeros_like(out_ref)
    ds_first[...] = jnp.zeros_like(ds_first)
    ds_last[...] = jnp.zeros_like(ds_last)
    conv_grad[...] = jnp.zeros_like(conv_grad)

    def reach(s):
        start, end = slot_bounds(len_ref, s, slots)
        lo, hi = start // TILE, (end + TILE - 1) // TILE
        return start, end, lo, jnp.where(end > start, hi, lo)

    def own_rows(s):
        return pl.ds(pl.multiple_of(s * marks, marks), marks)

    def first_slot(s, _):
        start, end, lo, hi = reach(s)
        a_block = spread(inner_ref[own_rows(s), :], head_blocks).astype(low)

        def tile(n, carry):
            inner_total, key_total = carry
            t = pl.multiple_of(n * TILE, TILE)
            mask = lane_mask(start, end, t, TILE)
            own_grad = grad_ref[:, pl.ds(t, TILE)]
            kernel_rows = jnp.where(mask, first_ref[:, pl.ds(t, TILE)].astype(f32), 0.0)
            d_kernel = mul(a_block, own_grad)
            prod = (kernel_rows * d_kernel).reshape(heads, marks, TILE)
            row_sum = jnp.sum(prod, axis=1, keepdims=True)
            d_sim = prod - kernel_rows.reshape(heads, marks, TILE) * row_sum
            d_sim = d_sim.reshape(width, TILE)
            d_sim_low = d_sim.astype(low)
            old = ds_first[:, pl.ds(t, TILE)].astype(f32)
            ds_first[:, pl.ds(t, TILE)] = jnp.where(mask, d_sim, old).astype(low)
            inner_total = inner_total + mul_t(kernel_rows.astype(low), own_grad)
            key_total = key_total + mul_t(d_sim_low, qkv_ref[:width, pl.ds(t, TILE)])
            full = windows(vpad, start, end, t)
            grad_own = jnp.where(mask, own_grad.astype(f32), 0.0).astype(low)
            for h in range(heads):
                sel = slice(h * HEAD_DIM, (h + 1) * HEAD_DIM)
                left = jnp.concatenate(
                    [grad_own[sel, c * SUB : (c + 1) * SUB] for c in range(count)], axis=0
                )
                right = jnp.concatenate(
                    [full[sel, c * SUB : (c + 3) * SUB] for c in range(count)], axis=0
                )
                conv_grad[h] += lax.dot_general(
                    left, right, (((0,), (0,)), ((), ())), preferred_element_type=f32
                )
            return inner_total, key_total

        zero = jnp.zeros((width, width), f32)
        inner_total, key_total = lax.fori_loop(lo, hi, tile, (zero, zero))
        d_inner[own_rows(s), :] = fold(inner_total, head_blocks)
        d_k[own_rows(s), :] = fold(key_total, head_blocks) * scale
        return 0

    lax.fori_loop(0, slots, first_slot, 0)

    row = lax.broadcasted_iota(jnp.int32, (SUB, 3 * SUB), 0)
    col = lax.broadcasted_iota(jnp.int32, (SUB, 3 * SUB), 1)
    off = col - row - (SUB - taps // 2)
    tap_lane = lax.broadcasted_iota(jnp.int32, (1, SUB), 1)
    for h in range(heads):
        found = jnp.zeros((1, SUB), f32)
        square = conv_grad[h]
        for n in range(taps):
            part = jnp.sum(jnp.where(off == n, square, 0.0), axis=0, keepdims=True)
            part = jnp.sum(part, axis=1, keepdims=True)
            found = jnp.where(tap_lane == n, part, found)
        conv_out_ref[h : h + 1, :] = found

    lane_head = lax.broadcasted_iota(jnp.int32, (1, width), 1) // HEAD_DIM
    value_total = jnp.zeros((packed, width), f32)
    d_inverses = []
    for h in range(heads):
        own = jnp.where(lane_head == h, d_inner[...], 0.0)
        value_total = value_total + wide(mul, spread(inverse_ref[h], slot_blocks), own)
        d_inverses.append(fold(wide(mul_t, own, value_ref[...]), slot_blocks))
    d_value[...] = value_total

    middles_t = [pack_mul_t(eye, middle_ref[h], slot_blocks) for h in range(heads)]

    def newton(k, carry):
        n = PINV_ITERS - 1 - k
        out = []
        for h in range(heads):
            d_inverse, d_middle = carry[h]
            product = steps_ref[n, 0, h]
            second = steps_ref[n, 1, h]
            third = steps_ref[n, 2, h]
            inverse_t = steps_ref[n, 3, h]
            middle_t = middles_t[h]
            d_third = 0.25 * pack_mul(inverse_t, d_inverse, slot_blocks)
            d_second = -pack_mul(product, d_third, slot_blocks)
            d_first = -pack_mul(product, d_second, slot_blocks)
            d_product = (
                -pack_mul(d_third, second, slot_blocks)
                - pack_mul(d_second, 7.0 * eye - product, slot_blocks)
                - d_first
            )
            d_middle = d_middle + pack_mul(d_product, inverse_t, slot_blocks)
            d_inverse = 0.25 * pack_mul(d_inverse, third, slot_blocks) + pack_mul(
                middle_t, d_product, slot_blocks
            )
            out.append((d_inverse, d_middle))
        return tuple(out)

    zero = jnp.zeros((HEAD_DIM, packed), f32)
    final = lax.fori_loop(0, PINV_ITERS, newton, tuple((x, zero) for x in d_inverses))
    lane_slot = lax.broadcasted_iota(jnp.int32, (1, packed), 1) // marks
    dq_total = jnp.zeros((packed, width), f32)
    dk_total = jnp.zeros((packed, width), f32)
    for h in range(heads):
        d_inverse, d_middle = final[h]
        middle = middle_ref[h]
        first_t = steps_ref[0, 3, h]
        d_inverse_t = pack_mul_t(eye, d_inverse, slot_blocks)
        col_sums = jnp.sum(middle, axis=0, keepdims=True)
        share = jnp.sum(d_inverse_t * first_t, axis=0, keepdims=True)
        bound = jnp.zeros((1, packed), f32)
        d_bound = jnp.zeros((1, packed), f32)
        hits = jnp.zeros((1, packed), f32)
        for s in range(slots):
            mine = lane_slot == s
            top = jnp.max(jnp.where(mine, col_sums, 0.0), axis=1, keepdims=True)
            total = jnp.sum(jnp.where(mine, share, 0.0), axis=1, keepdims=True)
            number = jnp.sum(
                jnp.where(mine & (col_sums == top), 1.0, 0.0), axis=1, keepdims=True
            )
            bound = jnp.where(mine, top, bound)
            d_bound = jnp.where(mine, -total / top, d_bound)
            hits = jnp.where(mine, number, hits)
        d_middle = d_middle + d_inverse_t / bound
        d_middle = d_middle + jnp.where(col_sums == bound, d_bound / hits, 0.0)
        prod = spread(middle * d_middle, slot_blocks)
        d_sim = prod - spread(middle, slot_blocks) * jnp.sum(prod, axis=1, keepdims=True)
        d_sim = d_sim * scale
        own = lane_head == h
        q_marks = jnp.where(own, mark_ref[:, :width], 0.0)
        k_marks = jnp.where(own, mark_ref[:, width:], 0.0)
        dq_total = dq_total + wide(mul, d_sim, k_marks)
        dk_total = dk_total + wide(mul, jnp.transpose(d_sim), q_marks)
    d_q[...] = dq_total
    d_k[...] += dk_total

    flipped = []
    for h in range(heads):
        flipped.append(
            band(
                jnp.concatenate(
                    [conv_ref[h : h + 1, n : n + 1] for n in reversed(range(taps))], axis=1
                ),
                taps,
            ).astype(low)
        )

    def last_slot(s, _):
        start, end, lo, hi = reach(s)
        inv = denom_ref[s]
        own_d = d_value[own_rows(s), :]
        own_v = value_ref[own_rows(s), :]
        d_block = spread(own_d, head_blocks)
        row_sum = jnp.sum(
            d_block * jnp.concatenate([own_v] * heads, axis=0), axis=1, keepdims=True
        )
        row_sum = row_sum * inv
        d_block = d_block * inv
        d_block_t = jnp.transpose(d_block).astype(low)
        d_block = d_block.astype(low)

        def tile(n, query_total):
            t = pl.multiple_of(n * TILE, TILE)
            mask = lane_mask(start, end, t, TILE)
            kernel_rows = jnp.where(mask, last_ref[:, pl.ds(t, TILE)].astype(f32), 0.0)
            v_rows = qkv_ref[2 * width :, pl.ds(t, TILE)]
            d_sim = kernel_rows * (mul(d_block, v_rows) - row_sum)
            d_low = d_sim.astype(low)
            old = ds_last[:, pl.ds(t, TILE)].astype(f32)
            ds_last[:, pl.ds(t, TILE)] = jnp.where(mask, d_sim, old).astype(low)
            dv = mul(d_block_t, kernel_rows.astype(low))
            dv = dv + convolve(gpad, flipped, start, end, t, heads)
            old = out_ref[2 * width :, pl.ds(t, TILE)].astype(f32)
            out_ref[2 * width :, pl.ds(t, TILE)] = jnp.where(mask, dv, old).astype(low)
            return query_total + mul_t(d_low, qkv_ref[width : 2 * width, pl.ds(t, TILE)])

        query_total = lax.fori_loop(lo, hi, tile, jnp.zeros((width, width), f32))
        d_q[own_rows(s), :] += fold(query_total, head_blocks) * scale
        return 0

    lax.fori_loop(0, slots, last_slot, 0)

    inv_count = slot_marks(len_ref, 0, slots, marks, SUB)[1]
    d_q[...] = d_q[...] * inv_count
    d_k[...] = d_k[...] * inv_count

    def final_slot(s, _):
        start, end, lo, hi = reach(s)
        length = end - start
        own = mark_ref[own_rows(s), :] * scale

        def left(block, d_mark):
            wide_rows = jnp.concatenate([spread(block, head_blocks), d_mark], axis=0)
            return jnp.transpose(wide_rows).astype(low)

        q_left = left(own[:, width:], d_q[own_rows(s), :])
        k_left = left(own[:, :width], d_k[own_rows(s), :])
        mark = lax.broadcasted_iota(jnp.int32, (marks, 1), 0)
        lower = start + (mark * length) // marks
        upper = start + ((mark + 1) * length) // marks

        def tile(n, _):
            t = pl.multiple_of(n * TILE, TILE)
            mask = lane_mask(start, end, t, TILE)
            tok = t + lax.broadcasted_iota(jnp.int32, (marks, TILE), 1)
            member = jnp.where((tok >= lower) & (tok < upper), 1.0, 0.0).astype(low)
            for at, lhs, source in ((0, q_left, ds_first), (width, k_left, ds_last)):
                rhs = jnp.concatenate([source[:, pl.ds(t, TILE)], member], axis=0)
                rows = mul(lhs, rhs)
                old = out_ref[at : at + width, pl.ds(t, TILE)].astype(f32)
                out_ref[at : at + width, pl.ds(t, TILE)] = jnp.where(mask, rows, old).astype(low)
            return 0

        return lax.fori_loop(lo, hi, tile, 0)

    lax.fori_loop(0, slots, final_slot, 0)

    def bias_tile(n, carry):
        t = pl.multiple_of(n * TILE, TILE)
        q_sum, v_sum = carry
        q_rows = out_ref[:width, pl.ds(t, TILE)].astype(f32)
        v_rows = out_ref[2 * width :, pl.ds(t, TILE)].astype(f32)
        for c in range(count):
            q_sum = q_sum + q_rows[:, c * SUB : (c + 1) * SUB]
            v_sum = v_sum + v_rows[:, c * SUB : (c + 1) * SUB]
        return q_sum, v_sum

    zero = jnp.zeros((width, SUB), f32)
    q_sum, v_sum = lax.fori_loop(0, tok_count // TILE, bias_tile, (zero, zero))
    bias_ref[...] = jnp.zeros_like(bias_ref)
    bias_ref[0:1, :] = jnp.sum(jnp.transpose(q_sum), axis=0, keepdims=True)
    bias_ref[1:2, :] = jnp.sum(jnp.transpose(v_sum), axis=0, keepdims=True)


def mix_forward(seq_lengths, tokens, weight_t, bias_col, conv_own, slots, marks):
    tok_count, model = tokens.shape
    width = weight_t.shape[0] // 3
    heads = width // HEAD_DIM
    packed = slots * marks
    taps = conv_own.shape[1]
    whole = lambda *shape: pl.BlockSpec(shape, lambda i, lens: (0,) * len(shape))
    shapes = [
        ((3 * width, tok_count), low),
        ((width, tok_count), low),
        ((width, tok_count), low),
        ((width, tok_count), low),
        ((packed, 2 * width), f32),
        ((packed, width), f32),
        ((packed, width), f32),
        ((slots, width, 1), f32),
        ((heads, HEAD_DIM, packed), f32),
        ((PINV_ITERS, 4, heads, HEAD_DIM, packed), f32),
        ((heads, HEAD_DIM, packed), f32),
        ((8, 128), f32),
    ]
    return pl.pallas_call(
        partial(mix_forward_kernel, slots, marks, taps),
        out_shape=[jax.ShapeDtypeStruct(s, t) for s, t in shapes],
        grid_spec=pltpu.PrefetchScalarGridSpec(
            num_scalar_prefetch=1,
            grid=(tok_count // TILE,),
            in_specs=[
                pl.BlockSpec((TILE, model), lambda i, lens: (i, 0)),
                whole(3 * width, model),
                whole(3 * width, 1),
                whole(heads, taps),
            ],
            out_specs=[whole(*s) for s, _ in shapes],
            scratch_shapes=[
                pltpu.VMEM((width, tok_count + 2 * SUB), low),
                pltpu.VMEM((width, tok_count), f32),
                pltpu.VMEM((8, width), f32),
            ],
        ),
        compiler_params=pltpu.CompilerParams(vmem_limit_bytes=56 * 1024 * 1024),
        cost_estimate=pl.CostEstimate(
            flops=20 * 10**9, bytes_accessed=30 * 10**6, transcendentals=10**6
        ),
        name="mix_forward",
    )(seq_lengths, tokens, weight_t, bias_col, conv_own)


def mix_backward(seq_lengths, grad_t, saved, conv_own, slots, marks):
    qkv_t, first, last, mark, value, inner, denom, middle, steps, inverse = saved
    width, tok_count = grad_t.shape
    heads = width // HEAD_DIM
    packed = slots * marks
    taps = conv_own.shape[1]
    args = (grad_t, qkv_t, first, last, mark, value, inner, denom, middle, steps, inverse, conv_own)
    whole = lambda shape: pl.BlockSpec(
        shape, lambda i, lens: (0,) * len(shape), pipeline_mode=pl.Buffered(1)
    )
    shapes = [((3 * width, tok_count), low), ((8, width), f32), ((heads, SUB), f32)]
    square = pltpu.VMEM((packed, width), f32)
    return pl.pallas_call(
        partial(mix_backward_kernel, slots, marks, taps),
        out_shape=[jax.ShapeDtypeStruct(s, t) for s, t in shapes],
        grid_spec=pltpu.PrefetchScalarGridSpec(
            num_scalar_prefetch=1,
            grid=(1,),
            in_specs=[whole(x.shape) for x in args],
            out_specs=[whole(s) for s, _ in shapes],
            scratch_shapes=[
                pltpu.VMEM((width, tok_count + 2 * SUB), low),
                pltpu.VMEM((width, tok_count + 2 * SUB), low),
                pltpu.VMEM((width, tok_count), low),
                pltpu.VMEM((width, tok_count), low),
                pltpu.VMEM((heads, SUB, 3 * SUB), f32),
                square, square, square, square,
            ],
        ),
        compiler_params=pltpu.CompilerParams(vmem_limit_bytes=56 * 1024 * 1024),
        cost_estimate=pl.CostEstimate(
            flops=20 * 10**9, bytes_accessed=30 * 10**6, transcendentals=10**6
        ),
        name="mix_backward",
    )(seq_lengths, *args)


contract_rows = (((0,), (0,)), ((), ()))
contract_cols = (((1,), (1,)), ((), ()))
norm_eps = 1e-05


def split_up(x, dim, peers):
    before, after = (x.shape[:dim], x.shape[dim + 1 :])
    return jnp.moveaxis(x.reshape(*before, peers, -1, *after), dim, 0)


def sum_at_owner(x, axis, dim):
    peers = lax.axis_size(axis)
    tiles = lax.all_to_all(split_up(x, dim, peers), axis, 0, 0, tiled=True)
    return jnp.sum(tiles.astype(f32), axis=0)


def layer_norm(row_data, gain_vec, shift_vec):
    centre = row_data - jnp.mean(row_data, axis=1, keepdims=True)
    spread_row = jnp.mean(centre * centre, axis=1, keepdims=True)
    return centre * lax.rsqrt(spread_row + norm_eps) * gain_vec[None, :] + shift_vec[None, :]


def gelu_exact(values):
    return jax.nn.gelu(values, approximate=False)


def body(
    tokens,
    qkv_weight,
    qv_bias,
    conv_weight,
    out_weight,
    out_bias,
    norm1_gain,
    norm1_bias,
    ffn_in_weight,
    ffn_in_bias,
    ffn_out_weight,
    ffn_out_bias,
    norm2_gain,
    norm2_bias,
    cotangent,
    seq_lengths,
    segment_ids,
    landmark_bounds,
):
    tok_count, model_width = tokens.shape
    head_width = qkv_weight.shape[2]
    heads_here = head_width // HEAD_DIM
    head_total = conv_weight.shape[0]
    kernel_taps = conv_weight.shape[1]
    slots, marks = landmark_bounds.shape
    quarter = tok_count // lax.axis_size("heads")
    head_index = lax.axis_index("heads")
    own_start = head_index * quarter
    both = ("batch", "heads")
    own_rows_low = lax.dynamic_slice_in_dim(tokens, own_start, quarter, 0)
    own_tokens = own_rows_low.astype(f32)
    conv_own = lax.dynamic_slice_in_dim(conv_weight, head_index * heads_here, heads_here, 0)
    qv_own = lax.dynamic_slice_in_dim(qv_bias, head_index * head_width, head_width, 1)
    flat_qkv = qkv_weight.reshape(model_width, 3 * head_width)
    bias_col = jnp.concatenate([qv_own[0], jnp.zeros_like(qv_own[0]), qv_own[1]])[:, None]
    forward = mix_forward(
        seq_lengths, tokens, jnp.transpose(flat_qkv), bias_col, conv_own, slots, marks
    )
    qkv_t, first, last, mixed_t, mark, value, inner, denom, middle, steps, inverse, bound = forward
    bound_total = bound[0, 0]
    attn_part = lax.psum_scatter(
        lax.dot_general(mixed_t, out_weight, contract_rows, preferred_element_type=f32).astype(low),
        "heads",
        scatter_dimension=0,
        tiled=True,
    ).astype(f32)
    live_count = jnp.sum((seq_lengths > 0).astype(f32)) * heads_here
    first_res = own_tokens + attn_part + out_bias[None, :]
    norm1_out, norm1_pull = jax.vjp(layer_norm, first_res, norm1_gain, norm1_bias)
    norm1_low = norm1_out.astype(low)
    ff_own = ffn_out_weight.shape[0]
    bias_row = jnp.zeros((16, model_width), low).at[0, :ff_own].set(ffn_in_bias)
    whole_in = lax.all_gather(ffn_in_weight, both, axis=1, tiled=True)
    out_pack = lax.all_gather(jnp.concatenate([ffn_out_weight, bias_row], axis=0), both, axis=0)
    whole_out = out_pack[:, :ff_own].reshape(-1, model_width)
    whole_in_bias = out_pack[:, ff_own, :ff_own].reshape(-1)
    pre_act = (
        jnp.dot(norm1_low, whole_in, preferred_element_type=f32)
        + whole_in_bias.astype(f32)[None, :]
    )
    hidden_act, gelu_pull = jax.vjp(gelu_exact, pre_act)
    hidden_low = hidden_act.astype(low)
    ffn_result = jnp.dot(hidden_low, whole_out, preferred_element_type=f32) + ffn_out_bias[None, :]
    final_out, norm2_pull = jax.vjp(layer_norm, norm1_out + ffn_result, norm2_gain, norm2_bias)
    grad_second, grad_gain_two, grad_shift_two = norm2_pull(cotangent.astype(f32))
    grad_ffn_low = grad_second.astype(low)
    grad_ffn_bias = jnp.sum(grad_ffn_low.astype(f32), axis=0)
    down_term = lax.dot_general(
        hidden_low, grad_ffn_low, contract_rows, preferred_element_type=f32
    ).astype(low)
    grad_hidden = lax.dot_general(
        grad_ffn_low, whole_out, contract_cols, preferred_element_type=f32
    )
    grad_pre = gelu_pull(grad_hidden)[0].astype(low)
    grad_in_bias = jnp.sum(grad_pre.astype(f32), axis=0)
    up_term = lax.dot_general(
        norm1_low, grad_pre, contract_rows, preferred_element_type=f32
    ).astype(low)
    grad_norm1 = grad_second + lax.dot_general(
        grad_pre, whole_in, contract_cols, preferred_element_type=f32
    )
    grad_first, grad_gain_one, grad_shift_one = norm1_pull(grad_norm1)
    grad_attn_low = grad_first.astype(low)
    grad_out_bias = jnp.sum(grad_attn_low.astype(f32), axis=0)
    piece_rows = lax.all_gather(grad_attn_low, "heads", axis=0, tiled=True)
    grad_mix_t = lax.dot_general(
        out_weight, piece_rows, contract_cols, preferred_element_type=f32
    ).astype(low)
    grad_mix_t, down_term, up_term = lax.optimization_barrier((grad_mix_t, down_term, up_term))
    up_share = lax.psum_scatter(up_term, both, scatter_dimension=1, tiled=True).astype(f32)
    down_share = lax.psum_scatter(down_term, both, scatter_dimension=0, tiled=True).astype(f32)
    saved = (qkv_t, first, last, mark, value, inner, denom, middle, steps, inverse)
    grad_t, grad_bias, grad_conv = mix_backward(
        seq_lengths, grad_mix_t, saved, conv_own, slots, marks
    )
    out_part = lax.dot_general(
        mixed_t, piece_rows, (((1,), (0,)), ((), ())), preferred_element_type=f32
    )
    grad_qv_own = grad_bias[:2]
    qkv_part = lax.dot_general(
        tokens, grad_t, (((0,), (1,)), ((), ())), preferred_element_type=f32
    ).reshape(model_width, 3, head_width)
    input_part = lax.psum_scatter(
        lax.dot_general(
            grad_t, flat_qkv, (((0,), (1,)), ((), ())), preferred_element_type=f32
        ).astype(low),
        "heads",
        scatter_dimension=0,
        tiled=True,
    ).astype(f32)
    input_grad = grad_first + input_part
    conv_full = lax.dynamic_update_slice_in_dim(
        jnp.zeros((head_total, kernel_taps), f32),
        grad_conv[:, :kernel_taps],
        head_index * heads_here,
        0,
    )
    bias_full = lax.dynamic_update_slice_in_dim(
        jnp.zeros((2, head_total * HEAD_DIM), f32), grad_qv_own, head_index * head_width, 1
    )
    qkv_share, out_share = (
        sum_at_owner(qkv_part.astype(low), "batch", 0),
        sum_at_owner(out_part.astype(low), "batch", 1),
    )
    vector_all = jnp.stack(
        [grad_ffn_bias, grad_gain_two, grad_shift_two, grad_gain_one, grad_shift_one, grad_out_bias]
    )
    in_bias_share, vector_share = (
        lax.psum_scatter(grad_in_bias, both, scatter_dimension=0, tiled=True),
        lax.psum_scatter(vector_all, both, scatter_dimension=1, tiled=True),
    )
    conv_sum, bias_sum, bound_all, count_all = lax.psum(
        (conv_full, bias_full, bound_total, live_count), both
    )
    conv_out = lax.dynamic_slice_in_dim(conv_sum, head_index * heads_here, heads_here, 0)
    bias_out = lax.dynamic_slice_in_dim(bias_sum, head_index * head_width, head_width, 1)
    condition = bound_all / count_all
    return (
        final_out.astype(low),
        input_grad,
        qkv_share,
        bias_out,
        conv_out,
        out_share,
        up_share,
        in_bias_share,
        down_share,
        vector_share,
        condition,
    )


def place():
    b, z = lax.axis_index("batch"), lax.axis_index("heads")
    core, x, y = b % 2, (b // 2) % 2, b // 4
    return b, z, b + 1 - 2 * core, b + 2 - 4 * x, b + 4 - 8 * y


def remote(src, dst, send, recv, device):
    return pltpu.make_async_remote_copy(
        src_ref=src,
        dst_ref=dst,
        send_sem=send,
        recv_sem=recv,
        device_id=device,
        device_id_type=pl.DeviceIdType.MESH,
    )


def greet(devices):
    barrier = pltpu.get_barrier_semaphore()
    for device in devices:
        pl.semaphore_signal(
            barrier, inc=1, device_id=device, device_id_type=pl.DeviceIdType.MESH
        )
    pl.semaphore_wait(barrier, len(devices))


def tail_kernel(
    len_ref,
    gt_hbm, wq_hbm, we_hbm, hid_hbm, pre_hbm, n1_hbm, gf_hbm, ga_hbm, mx_hbm, tok_hbm, first_hbm,
    sums_ref, bin_ref, qv_ref, conv_ref, bound_ref,
    input_ref, down_own, up_own, outw_own, qkvw_own, in_bias, vector_own, qv_own, conv_own, ratio,
    small_out,
    gt, wq, we, hid, pre, n1, gf, ga, mx, tok,
    q_in, r_out, r_in, s_in, out_down, out_up, full_outw, full_qkvw, acc_qkvw,
    core_down, core_up, core_outw, core_qkvw,
    one_down, one_up, one_outw, one_qkvw, two_down, two_up, two_outw, two_qkvw,
    z_down, z_up, z_outw, small_in,
    load_sem, q_send, q_recv, r_send, r_recv, t_send, t_recv, c_send, c_recv, x_send, x_recv, e_send, e_recv, s_send, s_recv,
):
    b, z, bc, bx, by = place()
    both = bx + by - b
    flip = bc - b
    peers = [(b, lax.rem(z + i, 4)) for i in (1, 2, 3)]
    issued = []
    loads = [
        pltpu.make_async_copy(src, dst, load_sem.at[n])
        for n, (src, dst) in enumerate(
            (
                (gt_hbm, gt), (wq_hbm, wq), (pre_hbm, pre), (n1_hbm, n1), (hid_hbm, hid),
                (gf_hbm, gf), (we_hbm, we), (mx_hbm, mx), (ga_hbm, ga), (tok_hbm, tok),
                (first_hbm, input_ref),
            )
        )
    ]
    for copy in loads:
        copy.start()
    greet(peers + [(bc, z), (bx, z), (by, z)])
    chunks, size = r_in.shape[1:3]
    quarter = chunks * size
    ff = down_own.shape[0]
    group = 4 * ff

    zf = z + 1 - 2 * (z % 2)
    zg = z + 2 - 4 * (z // 2)
    partners = ((bc, z), (bx, z), (by, z), (b, zf), (b, zg))

    def small_start(k):
        copy = remote(
            small_out.at[k], small_in.at[k], s_send.at[k], s_recv.at[k], partners[k]
        )
        copy.start()
        issued.append(copy)

    def small_event(k):
        ref = small_in.at[k]
        remote(ref, ref, s_send.at[k], s_recv.at[k], partners[k]).wait_recv()
        small_out[k + 1] = small_out[k] + small_in[k]
        if k < 4:
            small_start(k + 1)

    model = input_ref.shape[1]
    bias_rows = bin_ref.shape[1] // model
    at_vec, at_qv = bias_rows, bias_rows + 6
    heads, taps = conv_own.shape
    at_conv = at_qv + 8
    at_end = at_conv + 4 * heads
    width = qv_own.shape[1]
    small_out[0] = jnp.zeros(small_out.shape[1:], f32)
    for n in range(bias_rows):
        small_out[0, n : n + 1, :] = bin_ref[0:1, n * model : (n + 1) * model]
    small_out[0, at_vec : at_vec + 6, :] = sums_ref[0:6, :]
    live = jnp.int32(0)
    for n in range(len_ref.shape[0]):
        live = live + jnp.where(len_ref[n] > 0, heads, 0)
    lane = lax.broadcasted_iota(jnp.int32, (1, 128), 1)
    small_out[0, at_end : at_end + 1, 0:128] = jnp.where(
        lane == 0, bound_ref[0:1, :], jnp.where(lane == 1, live.astype(f32), 0.0)
    )
    for n in range(4):

        @pl.when(z == n)
        def _():
            for r in range(2):
                row = at_qv + 2 * n + r
                small_out[0, row : row + 1, :width] = qv_ref[r : r + 1, :]
            for r in range(heads):
                row = at_conv + heads * n + r
                small_out[0, row : row + 1, 0:128] = conv_ref[r : r + 1, :]

    small_start(0)

    is_end = (z == 0) | (z == 3)
    low_side = z < 2
    to_inner = jnp.where(low_side, 1, 2)
    across = jnp.where(z == 1, 2, 1)
    to_end = jnp.where(low_side, 0, 3)

    def owner(k):
        return jnp.where(low_side, 3 - k, k)

    def columns(who, c):
        return pl.ds(pl.multiple_of(who * quarter + c * size, size), size)

    def times(x, w):
        return lax.dot_general(x, w, (((0,), (0,)), ((), ())), preferred_element_type=f32)

    def part(who, c):
        return times(gt[:, columns(who, c)], wq[...])

    def q_copy(k, c):
        return remote(
            gt.at[:, columns(owner(k), c)], q_in.at[k, c], q_send.at[k, c], q_recv.at[k, c],
            (b, to_inner),
        )

    def q_wait(k, c):
        ref = q_in.at[k, c]
        remote(ref, ref, q_send.at[k, c], q_recv.at[k, c], (b, to_end)).wait_recv()

    def r_copy(k, c):
        return remote(
            r_out.at[k, c], r_in.at[k, c], r_send.at[k, c], r_recv.at[k, c], (b, across)
        )

    def t_copy(c):
        return remote(r_in.at[0, c], s_in.at[c], t_send.at[c], t_recv.at[c], (b, to_end))

    def first_hop(k, c):
        @pl.when(jnp.logical_not(is_end))
        def _():
            own = part(owner(k), c)
            q_wait(k, c)
            r_out[k, c] = (own + times(q_in[k, c], we[...])).astype(low)
            r_copy(k, c).start()

    def last_hop(c):
        @pl.when(jnp.logical_not(is_end))
        def _():
            own = part(to_end, c)
            r_copy(0, c).wait_recv()
            r_in[0, c] = (r_in[0, c].astype(f32) + own).astype(low)
            t_copy(c).start()

    cores = (core_down, core_up, core_outw, core_qkvw)
    ones = (one_down, one_up, one_outw, one_qkvw)
    twos = (two_down, two_up, two_outw, two_qkvw)
    outs = (out_down, out_up)
    left = (hid, pre)
    right = (gf, n1)

    def who(slot):
        return b + (slot % 2) * (bx - b) + (slot // 2) * (by - b)

    def term(n, owner):
        at = pl.ds(pl.multiple_of(owner * group, group), group)
        return lax.dot_general(
            left[n][:, at], right[n][...], (((0,), (0,)), ((), ())), preferred_element_type=f32
        )

    def core_copy(n, slot):
        if n < 2:
            src = outs[n].at[slot]
        elif n == 2:
            src = full_outw.at[:, who(slot) + flip]
        else:
            src = full_qkvw.at[who(slot) + flip]
        return remote(src, cores[n].at[slot], c_send.at[n, slot], c_recv.at[n, slot], (bc, z))

    def give(n, slot):
        if n < 2:
            value = term(n, who(slot) + flip).astype(low)
            outs[n][slot] = value.reshape(outs[n].shape[1:])
        core_copy(n, slot).start()

    def keep(n, slot):
        if n < 2:
            own = term(n, who(slot)).reshape(outs[n].shape[1:])
        elif n == 2:
            own = full_outw[:, who(slot)].astype(f32)
        else:
            own = full_qkvw[who(slot)].astype(f32)
        core_copy(n, slot).wait_recv()
        cores[n][slot] = (cores[n][slot].astype(f32) + own).astype(low)

    def side_copy(n, dst, src):
        partner = by if n % 2 == 0 else bx
        return remote(
            cores[n].at[src], ones[n].at[dst], x_send.at[n, dst], x_recv.at[n, dst], (partner, z)
        )

    def small_group(n):
        def one(i, _):
            give(n, 3 - i)
            return 0

        lax.fori_loop(0, 4, one, 0)

    def small_keep(n):
        def one(i, _):
            keep(n, 3 - i)
            return 0

        lax.fori_loop(0, 4, one, 0)
        side_copy(n, 1, 3).start()
        side_copy(n, 0, 2 if n % 2 == 0 else 1).start()

    def half(h, _):
        def out(i, _):
            give(1, 3 - 2 * i - h)
            give(0, 3 - i - 2 * h)
            return 0

        lax.fori_loop(0, 2, out, 0)

        @pl.when(h == 1)
        def _():
            first_hop(0, 1)

        def own(i, _):
            slot_up, slot_down = 3 - 2 * i - h, 3 - i - 2 * h
            keep(1, slot_up)

            @pl.when(h == 0)
            def _():
                side_copy(1, 1 - i, slot_up).start()

            keep(0, slot_down)

            @pl.when(h == 0)
            def _():
                side_copy(0, 1 - i, slot_down).start()

            return 0

        lax.fori_loop(0, 2, own, 0)
        return 0

    def one_event(n):
        second = 1 if n % 2 == 0 else 2
        partner, other = (by, bx) if n % 2 == 0 else (bx, by)
        ref = ones[n].at[1]
        remote(ref, ref, x_send.at[n, 1], x_recv.at[n, 1], (partner, z)).wait_recv()
        ones[n][1] = (ones[n][1].astype(f32) + cores[n][second].astype(f32)).astype(low)
        copy = remote(ones[n].at[1], twos[n], x_send.at[n, 2], x_recv.at[n, 2], (other, z))
        copy.start()
        issued.append(copy)

    z_bufs = (z_down, z_up, z_outw)

    def two_event(n):
        partner, other = (by, bx) if n % 2 == 0 else (bx, by)
        ref = ones[n].at[0]
        remote(ref, ref, x_send.at[n, 0], x_recv.at[n, 0], (partner, z)).wait_recv()
        ref = twos[n]
        remote(ref, ref, x_send.at[n, 2], x_recv.at[n, 2], (other, z)).wait_recv()
        own = ones[n][0].astype(f32) + cores[n][0].astype(f32)
        if n == 3:
            qkvw_own[...] = twos[n][...].astype(f32) + own
            return
        twos[n][...] = (twos[n][...].astype(f32) + own).astype(low)
        for i, (_, to) in enumerate(peers):
            copy = remote(
                twos[n].at[to], z_bufs[n].at[i], e_send.at[n, i], e_recv.at[n, i], (b, to)
            )
            copy.start()
            issued.append(copy)

    def end_event(n):
        total = twos[n][z].astype(f32)
        for i in range(3):
            source = lax.rem(z + 3 - i, 4)
            ref = z_bufs[n].at[i]
            remote(ref, ref, e_send.at[n, i], e_recv.at[n, i], (b, source)).wait_recv()
            total = total + z_bufs[n][i].astype(f32)
        if n > 0:
            total = jnp.transpose(total)
        (down_own, up_own, outw_own)[n][...] = total

    def projections():
        on, oh = full_outw.shape[2:]
        for s in range(4):
            value = jnp.transpose(mul(mx[s], ga[...]))
            full_outw[s] = value.astype(low).reshape(full_outw.shape[1:])
        acc_qkvw[...] = jnp.zeros_like(acc_qkvw)
        span = quarter

        def one(n, _):
            at = pl.ds(pl.multiple_of(n * span, span), span)
            acc_qkvw[...] += mul(gt[:, at], tok[at, :])
            return 0

        lax.fori_loop(0, 4, one, 0)
        full_qkvw[...] = jnp.transpose(acc_qkvw[...]).astype(low).reshape(full_qkvw.shape)

    loads[0].wait()

    @pl.when(is_end)
    def _():
        for k in range(3):
            for c in range(chunks):
                q_copy(k, c).start()

    for n in range(1, 7):
        loads[n].wait()

    def both_halves(h, _):
        half(h, 0)

        @pl.when(h == 0)
        def _():
            first_hop(0, 0)

        return 0

    lax.fori_loop(0, 2, both_halves, 0)
    first_hop(0, 2)
    last_hop(0)
    one_event(1)
    one_event(0)
    for n in (7, 8, 9):
        loads[n].wait()
    projections()
    first_hop(1, 0)
    last_hop(1)
    small_group(2)
    small_group(3)
    small_event(0)
    first_hop(1, 1)
    last_hop(2)
    small_keep(2)
    small_keep(3)
    small_event(1)
    first_hop(1, 2)
    two_event(1)
    two_event(0)
    small_event(2)
    one_event(2)
    one_event(3)
    small_event(3)
    two_event(2)
    two_event(3)
    small_event(4)
    loads[10].wait()

    def own_rows(c, _):
        rows = pl.ds(pl.multiple_of(c * size, size), size)
        input_ref[rows, :] += part(z, c)

        @pl.when(is_end)
        def _():
            ref = s_in.at[c]
            remote(ref, ref, t_send.at[c], t_recv.at[c], (b, to_inner)).wait_recv()
            input_ref[rows, :] += s_in[c].astype(f32)

        @pl.when(jnp.logical_not(is_end))
        def _():
            r_copy(1, c).wait_recv()
            q_wait(2, c)
            input_ref[rows, :] += r_in[1, c].astype(f32) + times(q_in[2, c], we[...])

        return 0

    lax.fori_loop(0, chunks, own_rows, 0)
    for n in (1, 0, 2):
        end_event(n)

    @pl.when(is_end)
    def _():
        for k in range(3):
            for c in range(chunks):
                q_copy(k, c).wait_send()

    @pl.when(jnp.logical_not(is_end))
    def _():
        for c in range(chunks):
            r_copy(0, c).wait_send()
            r_copy(1, c).wait_send()
            t_copy(c).wait_send()

    final = small_out.at[5]
    in_bias[...] = jnp.zeros_like(in_bias)
    index = b * 4 + z
    per_row = model // ff
    for n in range(bias_rows):

        @pl.when(index // per_row == n)
        def _():
            row = pltpu.roll(final[n : n + 1, :], (model - (index % per_row) * ff) % model, 1)
            in_bias[...] = row[:, :ff]

    share = vector_own.shape[1]
    vectors = final[at_vec : at_vec + 6, :]
    vector_own[...] = pltpu.roll(vectors, (model - index * share) % model, 1)[:, :share]
    for n in range(4):

        @pl.when(z == n)
        def _():
            qv_own[...] = final[at_qv + 2 * n : at_qv + 2 * n + 2, :width]
            conv_own[...] = final[at_conv + heads * n : at_conv + heads * (n + 1), :taps]

    ratio[...] = final[at_end : at_end + 1, 0:1] / final[at_end : at_end + 1, 1:2]

    for n in range(4):
        for dst in range(2):
            side_copy(n, dst, dst).wait_send()
        for slot in range(4):
            core_copy(n, slot).wait_send()
    for copy in issued:
        copy.wait_send()


def tail(
    lengths, gt, wq, we, hid, pre, n1, gf, ga, mx, tok, first, sums, bins, qv_grad, conv_grad, bound,
    taps,
):
    quarter, model = first.shape
    chunks = 3
    size = quarter // chunks
    ff = hid.shape[1] // 32
    width = mx.shape[1]
    heads = width // HEAD_DIM
    on, oh = model // 8, width
    qn, qh = model // 8, gt.shape[0]
    blocks = ((4, ff, model), (4, ff, model), (4, on, oh), (qn, qh))
    own = lambda *s: jax.ShapeDtypeStruct(s, f32)
    vm = lambda *s: pltpu.VMEM(s, low)
    dma = pltpu.SemaphoreType.DMA
    sources = (gt, wq, we, hid, pre, n1, gf, ga, mx, tok)
    small = -(-(bins.shape[1] // model + 15 + 4 * heads) // 8) * 8
    vmem = pl.BlockSpec(memory_space=pltpu.VMEM)
    return pl.pallas_call(
        tail_kernel,
        out_shape=[
            own(quarter, model), own(ff, model), own(model, ff), own(oh, on), own(qn, qh),
            own(1, ff), own(6, model // 32), own(2, width), own(heads, taps), own(1, 1),
        ],
        in_specs=[pl.BlockSpec(memory_space=pltpu.SMEM)]
        + [pl.BlockSpec(memory_space=pl.ANY)] * 11
        + [vmem] * 5,
        out_specs=[vmem] * 10,
        scratch_shapes=[
            pltpu.VMEM((6, small, model), f32),
            *[vm(*x.shape) for x in sources],
            vm(3, chunks, qh, size), vm(2, chunks, size, model), vm(2, chunks, size, model),
            vm(chunks, size, model),
            vm(4, *blocks[0]), vm(4, *blocks[1]),
            vm(4, 8, on, oh), vm(8, qn, qh), pltpu.VMEM((qh, model), f32),
            *[vm(4, *s) for s in blocks],
            *[vm(2, *s) for s in blocks],
            *[vm(*s) for s in blocks],
            *[vm(3, *s[1:]) for s in blocks[:3]],
            pltpu.VMEM((5, small, model), f32),
            dma((11,)),
            dma((3, chunks)), dma((3, chunks)), dma((2, chunks)), dma((2, chunks)),
            dma((chunks,)), dma((chunks,)), dma((4, 4)), dma((4, 4)),
            dma((4, 3)), dma((4, 3)), dma((3, 3)), dma((3, 3)), dma((5,)), dma((5,)),
        ],
        compiler_params=pltpu.CompilerParams(
            collective_id=3, has_side_effects=True, vmem_limit_bytes=63 * 1024 * 1024
        ),
        name="tail",
    )(lengths, *sources, first, sums, bins, qv_grad, conv_grad, bound)


def cumulative(x):
    t = 1.0 / (1.0 + 0.23164189 * jnp.abs(x))
    density = jnp.exp(-0.5 * x * x) * 0.3989422804
    poly = t * (
        0.319381530 + t * (-0.356563782 + t * (1.781477937 + t * (-1.821255978 + t * 1.330274429)))
    )
    upper = density * poly
    return jnp.where(x >= 0.0, 1.0 - upper, upper), density


def normed(x):
    centre = x - jnp.mean(x, axis=1, keepdims=True)
    scale = lax.rsqrt(jnp.mean(centre * centre, axis=1, keepdims=True) + norm_eps)
    return centre * scale, scale


def norm_back(grad, gain, rows, scale):
    e = grad * gain
    return scale * (
        e - jnp.mean(e, axis=1, keepdims=True) - rows * jnp.mean(e * rows, axis=1, keepdims=True)
    )


def middle_kernel(
    pieces, share,
    mixed_ref, own0, own1, own2, own3, tok_hbm, cot_ref,
    out_bias_ref, gain1_ref, shift1_ref, down_bias_ref, gain2_ref, shift2_ref,
    out_ref, first_ref, attn_ref, hidden_ref, pre_ref, norm_ref, ffn_ref, all_ref, grad_ref,
    sums_ref, bin_ref,
    tok_ref, packs, wof, wo, slope, total, turned,
    a_send, a_recv, f_send, f_recv, p_send, p_recv, g_send, g_recv, own_sem, own_turn,
):
    b, z, bc, bx, by = place()
    both = bx + by - b
    peers = [(b, lax.rem(z + i, 4)) for i in (1, 2, 3)]
    greet(peers + [(bc, z), (bx, z), (by, z)])
    width, quarter = all_ref.shape[1:]
    model = tok_hbm.shape[1]
    owns = (own0, own1, own2, own3)
    origins = [lax.rem(z + 4 - i, 4) for i in range(4)]
    issued = []

    def columns(n):
        return pl.ds(pl.multiple_of(n * quarter, quarter), quarter)

    for i, (_, to) in enumerate(peers):
        copy = remote(
            mixed_ref.at[:, columns(to)], all_ref.at[z], a_send.at[i], a_recv.at[i], (b, to)
        )
        copy.start()
        issued.append(copy)
    local = [
        pltpu.make_async_copy(own, packs.at[b, origin], own_sem.at[i])
        for i, (own, origin) in enumerate(zip(owns, origins))
    ]
    local.append(
        pltpu.make_async_copy(mixed_ref.at[:, columns(z)], all_ref.at[z], own_sem.at[4])
    )
    local.append(
        pltpu.make_async_copy(
            tok_hbm.at[pl.ds(pl.multiple_of(z * quarter, quarter), quarter)], tok_ref, own_sem.at[5]
        )
    )
    count = len(pieces)

    def near(n):
        return by if pieces[n][2] else bx

    def far(n):
        return bx if pieces[n][2] else by

    for n in range(count):
        rows = pl.ds(*pieces[n][:2])
        for i in range(4):
            copy = remote(
                owns[i].at[rows], packs.at[b, origins[i], rows],
                f_send.at[n, i], f_recv.at[n, i], (near(n), z),
            )
            copy.start()
            issued.append(copy)
    for copy in local:
        copy.start()

    def pair(n, slot, who, device):
        ref = packs.at[who, :, pl.ds(*pieces[n][:2])]
        return remote(ref, ref, p_send.at[n, slot], p_recv.at[n, slot], (device, z))

    def send(n, slot, who, device):
        copy = pair(n, slot, who, device)
        copy.start()
        issued.append(copy)

    for copy in local:
        copy.wait()
    for n in range(count):
        send(n, 0, b, far(n))
        send(n, 2, b, bc)
    for n in range(count):
        rows = pl.ds(*pieces[n][:2])
        for i in range(4):
            ref = packs.at[near(n), origins[i], rows]
            remote(ref, ref, f_send.at[n, i], f_recv.at[n, i], (near(n), z)).wait_recv()
        send(n, 1, near(n), far(n))
        send(n, 3, near(n), bc)
    for n in range(count):
        pair(n, 0, far(n), far(n)).wait_recv()
        send(n, 4, far(n), bc)
    for n in range(count):
        pair(n, 1, both, far(n)).wait_recv()
        send(n, 5, both, bc)
    flip = bc - b
    for n in range(count):
        pair(n, 2, bc, bc).wait_recv()
        pair(n, 3, near(n) + flip, bc).wait_recv()
        pair(n, 4, far(n) + flip, bc).wait_recv()
        pair(n, 5, both + flip, bc).wait_recv()
    for i in (1, 2, 3):
        ref = all_ref.at[origins[i]]
        remote(ref, ref, a_send.at[i - 1], a_recv.at[i - 1], (b, origins[i])).wait_recv()

    ff = (packs.shape[2] - 32) // 2
    group = 4 * ff
    for q in range(8):
        for s in range(4):
            wof[pl.ds(s * width + q * share, share), :] = packs[
                q, s, pl.ds(2 * ff, share), :
            ].astype(f32)
    wo[...] = wof[...].astype(low).reshape(wo.shape)
    ff_bias = []
    for q in range(8):
        row = jnp.zeros((1, group), f32)
        for s in range(4):
            row = row + packs[q, s, 2 * ff + share : 2 * ff + share + 1, :group].astype(f32)
        ff_bias.append(row)
    out_bias, gain1, shift1 = out_bias_ref[...], gain1_ref[...], shift1_ref[...]
    down_bias, gain2, shift2 = down_bias_ref[...], gain2_ref[...], shift2_ref[...]
    sums_ref[...] = jnp.zeros_like(sums_ref)
    bin_ref[...] = jnp.zeros_like(bin_ref)
    for q in range(8):
        bin_ref[1:2, q * group : (q + 1) * group] = ff_bias[q]
    size = turned.shape[2]
    span = 2 * group

    def weights(c, start):
        return jnp.concatenate(
            [
                packs[2 * c + n, :, pl.ds(start, ff), :].reshape(group, model)
                for n in range(2)
            ],
            axis=0,
        )

    def row_sum(n, x):
        sums_ref[n : n + 1, :] += jnp.sum(x, axis=0, keepdims=True)

    def turn_copy(r, i):
        to = lax.rem(z + i, 4)
        src = turned.at[r, pl.ds(pl.multiple_of(to * width, width), width)]
        dst = grad_ref.at[:, pl.ds(pl.multiple_of(z * quarter + r * size, size), size)]
        return remote(src, dst, g_send.at[r, i - 1], g_recv.at[r, i - 1], (b, to))

    def turn_own(r):
        src = turned.at[r, pl.ds(pl.multiple_of(z * width, width), width)]
        dst = grad_ref.at[:, pl.ds(pl.multiple_of(z * quarter + r * size, size), size)]
        return pltpu.make_async_copy(src, dst, own_turn.at[r])

    def row_tile(r, _):
        at = pl.multiple_of(r * size, size)
        rows = pl.ds(at, size)
        attn = jnp.zeros((size, model), f32)
        for s in range(4):
            attn = attn + lax.dot_general(
                all_ref[s, :, rows], wo[s], (((0,), (0,)), ((), ())), preferred_element_type=f32
            )
        n1, scale1 = normed(tok_ref[rows, :].astype(f32) + attn + out_bias)
        norm1 = n1 * gain1 + shift1
        norm_low = norm1.astype(low)
        norm_ref[rows, :] = norm_low
        total[...] = jnp.zeros_like(total)

        def forward(c, _):
            lanes = pl.ds(pl.multiple_of(c * span, span), span)
            act = mul_t(norm_low, weights(c, 0)) + bin_ref[1:2, lanes]
            phi, density = cumulative(act)
            hidden = (act * phi).astype(low)
            hidden_ref[rows, lanes] = hidden
            slope[:, lanes] = phi + act * density
            total[...] += mul(hidden, weights(c, ff))
            return 0

        lax.fori_loop(0, 4, forward, 0)
        n2, scale2 = normed(norm1 + total[...] + down_bias)
        out_ref[rows, :] = (n2 * gain2 + shift2).astype(low)
        cot = cot_ref[rows, :].astype(f32)
        row_sum(1, cot * n2)
        row_sum(2, cot)
        grad2 = norm_back(cot, gain2, n2, scale2)
        grad_low = grad2.astype(low)
        ffn_ref[rows, :] = grad_low
        row_sum(0, grad_low.astype(f32))
        total[...] = grad2

        def backward(c, _):
            lanes = pl.ds(pl.multiple_of(c * span, span), span)
            grad = (slope[:, lanes] * mul_t(grad_low, weights(c, ff))).astype(low)
            pre_ref[rows, lanes] = grad
            bin_ref[0:1, lanes] += jnp.sum(grad.astype(f32), axis=0, keepdims=True)
            total[...] += mul(grad, weights(c, 0))
            return 0

        lax.fori_loop(0, 4, backward, 0)
        grad1 = total[...]
        row_sum(3, grad1 * n1)
        row_sum(4, grad1)
        first = norm_back(grad1, gain1, n1, scale1)
        first_ref[rows, :] = first
        attn_low = first.astype(low)
        attn_ref[rows, :] = attn_low
        row_sum(5, attn_low.astype(f32))
        for s in range(4):
            turned[r, pl.ds(s * width, width), :] = mul_t(wo[s], attn_low).astype(low)
        for i in (1, 2, 3):
            turn_copy(r, i).start()
        turn_own(r).start()
        return 0

    tiles = quarter // size
    lax.fori_loop(0, tiles, row_tile, 0)

    def finish(r, _):
        for i in (1, 2, 3):
            source = origins[i]
            ref = grad_ref.at[:, pl.ds(pl.multiple_of(source * quarter + r * size, size), size)]
            remote(ref, ref, g_send.at[r, i - 1], g_recv.at[r, i - 1], (b, source)).wait_recv()
            turn_copy(r, i).wait_send()
        turn_own(r).wait()
        return 0

    lax.fori_loop(0, tiles, finish, 0)
    for copy in issued:
        copy.wait_send()


def ffn_middle(mixed_t, packs, tokens, cot, vectors, ff, share):
    width, tok_count = mixed_t.shape
    quarter, model = tok_count // 4, tokens.shape[1]
    size = quarter // 3
    rows = packs[0].shape[0]
    half = ff // 2
    pieces = (
        (2 * ff, rows - 2 * ff, 0),
        (0, half, 0), (ff, half, 1), (half, half, 0), (ff + half, half, 1),
    )
    n = len(pieces)
    shape = jax.ShapeDtypeStruct
    vmem = pl.BlockSpec(memory_space=pltpu.VMEM)
    hbm = pl.BlockSpec(memory_space=pl.ANY)
    dma = pltpu.SemaphoreType.DMA
    return pl.pallas_call(
        partial(middle_kernel, pieces, share),
        out_shape=[
            shape((quarter, model), low),
            shape((quarter, model), f32),
            shape((quarter, model), low),
            shape((quarter, 32 * ff), low),
            shape((quarter, 32 * ff), low),
            shape((quarter, model), low),
            shape((quarter, model), low),
            shape((4, width, quarter), low),
            shape((width, tok_count), low),
            shape((8, model), f32),
            shape((8, 32 * ff), f32),
        ],
        in_specs=[hbm] + [vmem] * 4 + [hbm] + [vmem] * 7,
        out_specs=[vmem] * 8 + [hbm] + [vmem] * 2,
        scratch_shapes=[
            pltpu.VMEM((quarter, model), low),
            pltpu.VMEM((8, 4, rows, model), low),
            pltpu.VMEM((4 * width, model), f32),
            pltpu.VMEM((4, width, model), low),
            pltpu.VMEM((size, 32 * ff), f32),
            pltpu.VMEM((size, model), f32),
            pltpu.VMEM((3, 4 * width, size), low),
            dma((3,)), dma((3,)), dma((n, 4)), dma((n, 4)), dma((n, 6)), dma((n, 6)),
            dma((3, 3)), dma((3, 3)), dma((6,)), dma((3,)),
        ],
        compiler_params=pltpu.CompilerParams(
            collective_id=1, has_side_effects=True, vmem_limit_bytes=62 * 1024 * 1024
        ),
        name="middle",
    )(mixed_t, *packs, tokens, cot, *vectors)


def slice_body(
    tokens,
    qkv_weight,
    qv_bias,
    conv_weight,
    out_weight,
    out_bias,
    norm1_gain,
    norm1_bias,
    ffn_in_weight,
    ffn_in_bias,
    ffn_out_weight,
    ffn_out_bias,
    norm2_gain,
    norm2_bias,
    cotangent,
    seq_lengths,
    segment_ids,
    landmark_bounds,
):
    model = tokens.shape[1]
    width = qkv_weight.shape[2]
    heads_here = width // HEAD_DIM
    kernel_taps = conv_weight.shape[1]
    slots, marks = landmark_bounds.shape
    z = lax.axis_index("heads")
    b = lax.axis_index("batch")
    conv_own = lax.dynamic_slice_in_dim(conv_weight, z * heads_here, heads_here, 0)
    qv_own = lax.dynamic_slice_in_dim(qv_bias, z * width, width, 1)
    weight_t = jnp.transpose(qkv_weight.reshape(model, 3 * width))
    bias_col = jnp.concatenate([qv_own[0], jnp.zeros_like(qv_own[0]), qv_own[1]])[:, None]
    ff_own = ffn_out_weight.shape[0]
    share = width // 8
    bias_row = lax.dynamic_update_slice_in_dim(
        jnp.zeros((4 * ff_own,), low), ffn_in_bias, z * ff_own, 0
    )
    misc_own = jnp.concatenate(
        [
            lax.dynamic_slice_in_dim(out_weight, b * share, share, 0),
            jnp.zeros((32 - share, model), low).at[0, : 4 * ff_own].set(bias_row),
        ],
        axis=0,
    )
    pack = jnp.concatenate([jnp.transpose(ffn_in_weight), ffn_out_weight, misc_own], axis=0)
    packs = [pack] + [
        lax.ppermute(pack, "heads", [(n, (n + i) % 4) for n in range(4)]) for i in (1, 2, 3)
    ]
    forward = mix_forward(
        seq_lengths, tokens, weight_t, bias_col, conv_own, slots, marks
    )
    qkv_t, first, last, mixed_t, mark, value, inner, denom, middle, steps, inverse, bound = forward
    vectors = [
        v[None, :]
        for v in (out_bias, norm1_gain, norm1_bias, ffn_out_bias, norm2_gain, norm2_bias)
    ]
    (
        final_low, grad_first, grad_attn_low, hidden_low, grad_pre, norm1_low, grad_ffn_low,
        mixed_all, grad_mix_t, vector_sums, bias_sums,
    ) = ffn_middle(mixed_t, packs, tokens, cotangent, vectors, ff_own, share)
    saved = (qkv_t, first, last, mark, value, inner, denom, middle, steps, inverse)
    held, grad_mix_t = lax.optimization_barrier((weight_t, grad_mix_t))
    weight_end = lax.ppermute(held, "heads", [(0, 1), (3, 2)])
    grad_t, grad_bias, grad_conv = mix_backward(
        seq_lengths, grad_mix_t, saved, conv_own, slots, marks
    )
    (
        input_grad, down_share, up_share, out_share, qkv_share,
        in_bias_share, vector_share, bias_out, conv_out, condition,
    ) = tail(
        seq_lengths, grad_t, weight_t, weight_end, hidden_low, grad_pre, norm1_low, grad_ffn_low,
        grad_attn_low, mixed_all, tokens, grad_first, vector_sums, bias_sums, grad_bias,
        grad_conv, bound, kernel_taps,
    )
    return (
        final_low,
        input_grad,
        qkv_share.reshape(model // 8, 3, width),
        bias_out,
        conv_out,
        out_share,
        up_share,
        in_bias_share.reshape(ff_own),
        down_share,
        vector_share,
        condition.reshape(()),
    )


def solution(mesh):
    chosen = slice_body if dict(mesh.shape) == {"batch": 8, "heads": 4} else body
    in_specs = (
        P("batch", None),
        P(None, None, "heads"),
        P(),
        P(),
        P("heads", None),
        P(),
        P(),
        P(),
        P(None, ("batch", "heads")),
        P(("batch", "heads")),
        P(("batch", "heads"), None),
        P(),
        P(),
        P(),
        P(("batch", "heads"), None),
        P("batch"),
        P("batch"),
        P("batch", None),
    )
    out_specs = (
        P(("batch", "heads"), None),
        P(("batch", "heads"), None),
        P("batch", None, "heads"),
        P(None, "heads"),
        P("heads", None),
        P("heads", "batch"),
        P(None, ("batch", "heads")),
        P(("batch", "heads")),
        P(("batch", "heads"), None),
        P(None, ("batch", "heads")),
        P(),
    )
    return jax.shard_map(chosen, mesh=mesh, in_specs=in_specs, out_specs=out_specs, check_vma=False)
```

```python
from functools import partial

import jax
import jax.numpy as jnp
from jax import lax
from jax.experimental import pallas as pl
from jax.experimental.pallas import tpu as pltpu
from jax.sharding import PartitionSpec as P

HEAD_DIM = 64
PINV_ITERS = 6
TILE = 512
SUB = 128

f32 = jnp.float32
low = jnp.bfloat16
mask_fill = -1000000000.0


def split(x):
    high = x.astype(low)
    return high, (x - high.astype(f32)).astype(low)


def mul(a, b):
    return lax.dot_general(a, b, (((1,), (0,)), ((), ())), preferred_element_type=f32)


def mul_t(a, b):
    return lax.dot_general(a, b, (((1,), (1,)), ((), ())), preferred_element_type=f32)


def wide(form, left, right):
    left_high, left_low = split(left)
    right_high, right_low = split(right)
    return form(left_high, right_high) + (
        form(left_high, right_low) + form(left_low, right_high)
    )


def block_grid(rows, cols):
    row_block = lax.broadcasted_iota(jnp.int32, (rows, cols), 0) // HEAD_DIM
    col_block = lax.broadcasted_iota(jnp.int32, (rows, cols), 1) // HEAD_DIM
    return row_block == col_block


def spread(x, blocks):
    count = blocks.shape[0] // x.shape[0]
    return jnp.where(blocks, jnp.concatenate([x] * count, axis=0), jnp.zeros_like(x[:1, :1]))


def fold(x, blocks):
    kept = jnp.where(blocks, x, jnp.zeros_like(x[:1, :1]))
    rows = HEAD_DIM
    out = kept[:rows]
    for n in range(1, x.shape[0] // rows):
        out = out + kept[n * rows : (n + 1) * rows]
    return out


def pack_mul(left, right, blocks):
    left_high, left_low = split(left)
    right_high, right_low = split(right)
    right_high, right_low = spread_low(right_high, blocks), spread_low(right_low, blocks)
    return mul(left_high, right_high) + (mul(left_high, right_low) + mul(left_low, right_high))


def pack_mul_t(left, right, blocks):
    left_high, left_low = split(left)
    right_high, right_low = split(right)
    right_high, right_low = spread_low(right_high, blocks), spread_low(right_low, blocks)
    return mul_t(left_high, right_high) + (mul_t(left_high, right_low) + mul_t(left_low, right_high))


def spread_low(x, blocks):
    return spread(x.astype(f32), blocks).astype(low)


def slot_bounds(len_ref, s, slots):
    start = jnp.int32(0)
    for n in range(slots):
        start = start + jnp.where(n < s, len_ref[n], 0)
    return start, start + len_ref[s]


def eye_pack(width):
    row = lax.broadcasted_iota(jnp.int32, (HEAD_DIM, width), 0)
    col = lax.broadcasted_iota(jnp.int32, (HEAD_DIM, width), 1) % HEAD_DIM
    return jnp.where(row == col, 1.0, 0.0).astype(f32)


def lane_mask(start, end, at, width):
    tok = at + lax.broadcasted_iota(jnp.int32, (1, width), 1)
    return (tok >= start) & (tok < end)


def band(taps_row, width):
    row = lax.broadcasted_iota(jnp.int32, (SUB, 3 * SUB), 0)
    col = lax.broadcasted_iota(jnp.int32, (SUB, 3 * SUB), 1)
    off = col - row - (SUB - width // 2)
    out = jnp.zeros((SUB, 3 * SUB), f32)
    for n in range(width):
        out = jnp.where(off == n, taps_row[:, n : n + 1], out)
    return out


def slot_marks(len_ref, at, slots, marks, width):
    rows = slots * marks
    row = lax.broadcasted_iota(jnp.int32, (rows, 1), 0)
    slot = row // marks
    mark = row % marks
    start = jnp.zeros((rows, 1), jnp.int32)
    length = jnp.zeros((rows, 1), jnp.int32)
    for n in range(slots):
        start = start + jnp.where(slot > n, len_ref[n], 0)
        length = jnp.where(slot == n, len_ref[n], length)
    lower = start + (mark * length) // marks
    upper = start + ((mark + 1) * length) // marks
    inv_count = 1.0 / jnp.maximum((upper - lower).astype(f32), 1.0)
    tok = at + lax.broadcasted_iota(jnp.int32, (rows, width), 1)
    member = jnp.where((tok >= lower) & (tok < upper), 1.0, 0.0)
    return member, inv_count


def mix_forward_kernel(
    slots, marks, taps,
    len_ref, tok_ref, weight_ref, bias_ref, conv_ref,
    qkv_ref, first_ref, last_ref, mixed_ref, mark_ref, value_ref, inner_ref,
    denom_ref, middle_ref, steps_ref, inverse_ref, bound_ref,
    vpad, scores, vsum, bias_col, conv_own,
):
    step = pl.program_id(0)
    width = first_ref.shape[0]
    heads = width // HEAD_DIM
    tok_count = qkv_ref.shape[1]
    tiles = tok_count // TILE
    packed = slots * marks
    at = pl.multiple_of(step * TILE, TILE)

    @pl.when(step == 0)
    def _():
        z = lax.axis_index("heads")
        own_taps(conv_own, conv_ref, z)
        columns = jnp.transpose(jnp.concatenate([bias_ref[...], bias_ref[...]], axis=0))
        bias_col[: bias_ref.shape[1], :] = columns
        mark_ref[...] = jnp.zeros_like(mark_ref)
        vsum[...] = jnp.zeros_like(vsum)
        vpad[:, :SUB] = jnp.zeros((width, SUB), low)
        vpad[:, tok_count + SUB :] = jnp.zeros((width, SUB), low)

    at_head = pl.ds(pl.multiple_of(lax.axis_index("heads") * width, HEAD_DIM), width)
    rows = mul_t(weight_ref[...], tok_ref[...])
    rows = jnp.concatenate(
        [
            rows[:width] + bias_col[at_head, 0:1],
            rows[width : 2 * width],
            rows[2 * width :] + bias_col[at_head, 1:2],
        ],
        axis=0,
    ).astype(low)
    qkv_ref[:, pl.ds(at, TILE)] = rows
    vpad[:, pl.ds(pl.multiple_of(at + SUB, SUB), TILE)] = rows[2 * width :]
    member, inv_count = slot_marks(len_ref, at, slots, marks, TILE)
    mark_ref[...] += mul_t(member.astype(low), rows[: 2 * width])
    vsum[...] += mul_t(jnp.ones((8, TILE), low), rows[2 * width :])
    first_ref[:, pl.ds(at, TILE)] = jnp.zeros((width, TILE), low)
    last_ref[:, pl.ds(at, TILE)] = jnp.zeros((width, TILE), low)
    mixed_ref[:, pl.ds(at, TILE)] = jnp.zeros((width, TILE), low)

    @pl.when(step == tiles - 1)
    def _():
        mark_ref[...] = mark_ref[...] * inv_count
        head_blocks = block_grid(width, width)
        slot_blocks = block_grid(packed, packed)
        eye = eye_pack(packed)
        scale = HEAD_DIM ** -0.5

        middles, inverses_t, products = [], [], []
        bound_total = jnp.zeros((1, 1), f32)
        lane_slot = lax.broadcasted_iota(jnp.int32, (1, packed), 1) // marks
        for h in range(heads):
            q_marks = mark_ref[:, h * HEAD_DIM : (h + 1) * HEAD_DIM]
            k_marks = mark_ref[:, width + h * HEAD_DIM : width + (h + 1) * HEAD_DIM]
            sim = wide(mul_t, q_marks, k_marks) * scale
            sim = jnp.where(slot_blocks, sim, -1e30)
            sim = jnp.exp(sim - jnp.max(sim, axis=1, keepdims=True))
            sim = sim / jnp.sum(sim, axis=1, keepdims=True)
            middle = fold(sim, slot_blocks)
            col_sums = jnp.sum(middle, axis=0, keepdims=True)
            bound = jnp.zeros((1, packed), f32)
            for s in range(slots):
                top = jnp.max(jnp.where(lane_slot == s, col_sums, 0.0), axis=1, keepdims=True)
                bound = jnp.where(lane_slot == s, top, bound)
                bound_total += jnp.where(len_ref[s] > 0, top, 0.0)
            middle_ref[h] = middle
            middles.append(middle)
            inverses_t.append(middle / bound)
            products.append(pack_mul_t(middle, middle, slot_blocks) / bound)
        bound_ref[...] = jnp.broadcast_to(bound_total, bound_ref.shape)

        def newton(n, carry):
            out = []
            for h in range(heads):
                inverse_t, product = carry[h]
                square = pack_mul(product, product, slot_blocks)
                cube = pack_mul(product, square, slot_blocks)
                fourth = pack_mul(square, square, slot_blocks)
                second = 15.0 * eye - 7.0 * product + square
                third = 13.0 * eye - 15.0 * product + 7.0 * square - cube
                steps_ref[n, 0, h] = product
                steps_ref[n, 1, h] = second
                steps_ref[n, 2, h] = third
                steps_ref[n, 3, h] = inverse_t
                out.append(
                    (
                        0.25 * pack_mul(third, inverse_t, slot_blocks),
                        0.25 * (13.0 * product - 15.0 * square + 7.0 * cube - fourth),
                    )
                )
            return tuple(out)

        final = lax.fori_loop(0, PINV_ITERS, newton, tuple(zip(inverses_t, products)))
        for h in range(heads):
            inverse_ref[h] = final[h][0]

        def one_slot(s, _):
            start, end = slot_bounds(len_ref, s, slots)
            lo, hi = start // TILE, (end + TILE - 1) // TILE
            hi = jnp.where(end > start, hi, lo)
            own = mark_ref[pl.ds(pl.multiple_of(s * marks, marks), marks), :] * scale
            q_block = spread(own[:, :width], head_blocks).astype(low)
            k_block = spread(own[:, width:], head_blocks).astype(low)

            def score_tile(n, top):
                t = pl.multiple_of(n * TILE, TILE)
                mask = lane_mask(start, end, t, TILE)
                sim = mul(k_block, qkv_ref[:width, pl.ds(t, TILE)])
                sim = sim.reshape(heads, marks, TILE)
                sim = jnp.exp(sim - jnp.max(sim, axis=1, keepdims=True))
                sim = sim / jnp.sum(sim, axis=1, keepdims=True)
                sim = sim.reshape(width, TILE)
                old = first_ref[:, pl.ds(t, TILE)].astype(f32)
                first_ref[:, pl.ds(t, TILE)] = jnp.where(mask, sim, old).astype(low)
                sim = mul(q_block, qkv_ref[width : 2 * width, pl.ds(t, TILE)])
                sim = jnp.where(mask, sim, mask_fill)
                scores[:, pl.ds(t, TILE)] = sim
                for c in range(TILE // SUB):
                    top = jnp.maximum(top, sim[:, c * SUB : (c + 1) * SUB])
                return top

            top = lax.fori_loop(lo, hi, score_tile, jnp.full((width, SUB), mask_fill, f32))
            top = jnp.max(top, axis=1, keepdims=True)

            def value_tile(n, carry):
                denom, total = carry
                t = pl.multiple_of(n * TILE, TILE)
                mask = lane_mask(start, end, t, TILE)
                part = jnp.exp(scores[:, pl.ds(t, TILE)] - top)
                old = last_ref[:, pl.ds(t, TILE)].astype(f32)
                last_ref[:, pl.ds(t, TILE)] = jnp.where(mask, part, old).astype(low)
                total = total + mul_t(part.astype(low), qkv_ref[2 * width :, pl.ds(t, TILE)])
                for c in range(TILE // SUB):
                    denom = denom + part[:, c * SUB : (c + 1) * SUB]
                return denom, total

            denom, total = lax.fori_loop(
                lo, hi, value_tile,
                (jnp.zeros((width, SUB), f32), jnp.zeros((width, width), f32)),
            )
            denom = jnp.sum(denom, axis=1, keepdims=True)
            inv = 1.0 / jnp.where(denom > 0.0, denom, 1.0)
            denom_ref[s] = inv
            values = fold(total * inv, head_blocks)
            values = jnp.where(end > start, values, vsum[:1] / tok_count)
            value_ref[pl.ds(pl.multiple_of(s * marks, marks), marks), :] = values
            return 0

        lax.fori_loop(0, slots, one_slot, 0)

        lane_head = lax.broadcasted_iota(jnp.int32, (1, width), 1) // HEAD_DIM
        inner = jnp.zeros((packed, width), f32)
        for h in range(heads):
            inverse = pack_mul_t(eye, final[h][0], slot_blocks)
            own_values = jnp.where(lane_head == h, value_ref[...], 0.0)
            inner = inner + wide(mul, spread(inverse, slot_blocks), own_values)
        inner_ref[...] = inner

        bands = [band(conv_own[h : h + 1, :], taps).astype(low) for h in range(heads)]

        def out_slot(s, _):
            start, end = slot_bounds(len_ref, s, slots)
            lo, hi = start // TILE, (end + TILE - 1) // TILE
            hi = jnp.where(end > start, hi, lo)
            own = inner_ref[pl.ds(pl.multiple_of(s * marks, marks), marks), :]
            a_block = jnp.transpose(spread(own, head_blocks)).astype(low)

            def out_tile(n, _):
                t = pl.multiple_of(n * TILE, TILE)
                mask = lane_mask(start, end, t, TILE)
                rows = mul(a_block, first_ref[:, pl.ds(t, TILE)])
                rows = rows + convolve(vpad, bands, start, end, t, heads)
                old = mixed_ref[:, pl.ds(t, TILE)].astype(f32)
                mixed_ref[:, pl.ds(t, TILE)] = jnp.where(mask, rows, old).astype(low)
                return 0

            return lax.fori_loop(lo, hi, out_tile, 0)

        lax.fori_loop(0, slots, out_slot, 0)


def own_taps(own_ref, all_ref, z):
    heads = own_ref.shape[0]
    for n in range(all_ref.shape[0] // heads):

        @pl.when(z == n)
        def _():
            own_ref[...] = all_ref[n * heads : (n + 1) * heads, :]


def windows(padded, start, end, t):
    full = padded[:, pl.ds(t, TILE + 2 * SUB)]
    keep = lane_mask(start, end, t - SUB, TILE + 2 * SUB)
    return jnp.where(keep, full.astype(f32), 0.0).astype(low)


def convolve(padded, bands, start, end, t, heads):
    full = windows(padded, start, end, t)
    out = []
    count = TILE // SUB
    for h in range(heads):
        own = full[h * HEAD_DIM : (h + 1) * HEAD_DIM]
        stack = jnp.concatenate(
            [own[:, c * SUB : (c + 3) * SUB] for c in range(count)], axis=0
        )
        res = mul_t(stack, bands[h])
        out.append(
            jnp.concatenate(
                [res[c * HEAD_DIM : (c + 1) * HEAD_DIM] for c in range(count)], axis=1
            )
        )
    return jnp.concatenate(out, axis=0)


def mix_backward_kernel(
    slots, marks, taps,
    len_ref, grad_ref, qkv_ref, first_ref, last_ref, mark_ref, value_ref, inner_ref,
    denom_ref, middle_ref, steps_ref, inverse_ref, conv_ref,
    out_ref, bias_ref, conv_out_ref,
    gpad, vpad, ds_first, ds_last, conv_grad, d_inner, d_k, d_q, d_value, conv_own,
):
    width = first_ref.shape[0]
    heads = width // HEAD_DIM
    tok_count = qkv_ref.shape[1]
    packed = slots * marks
    scale = HEAD_DIM ** -0.5
    head_blocks = block_grid(width, width)
    slot_blocks = block_grid(packed, packed)
    eye = eye_pack(packed)
    count = TILE // SUB

    for padded, source in ((gpad, grad_ref[...]), (vpad, qkv_ref[2 * width :, :])):
        padded[:, :SUB] = jnp.zeros((width, SUB), low)
        padded[:, tok_count + SUB :] = jnp.zeros((width, SUB), low)
        padded[:, SUB : tok_count + SUB] = source
    out_ref[...] = jnp.zeros_like(out_ref)
    ds_first[...] = jnp.zeros_like(ds_first)
    ds_last[...] = jnp.zeros_like(ds_last)
    conv_grad[...] = jnp.zeros_like(conv_grad)

    own_taps(conv_own, conv_ref, lax.axis_index("heads"))

    def reach(s):
        start, end = slot_bounds(len_ref, s, slots)
        lo, hi = start // TILE, (end + TILE - 1) // TILE
        return start, end, lo, jnp.where(end > start, hi, lo)

    def own_rows(s):
        return pl.ds(pl.multiple_of(s * marks, marks), marks)

    def first_slot(s, _):
        start, end, lo, hi = reach(s)
        a_block = spread(inner_ref[own_rows(s), :], head_blocks).astype(low)

        def tile(n, carry):
            inner_total, key_total = carry
            t = pl.multiple_of(n * TILE, TILE)
            mask = lane_mask(start, end, t, TILE)
            own_grad = grad_ref[:, pl.ds(t, TILE)]
            kernel_rows = jnp.where(mask, first_ref[:, pl.ds(t, TILE)].astype(f32), 0.0)
            d_kernel = mul(a_block, own_grad)
            prod = (kernel_rows * d_kernel).reshape(heads, marks, TILE)
            row_sum = jnp.sum(prod, axis=1, keepdims=True)
            d_sim = prod - kernel_rows.reshape(heads, marks, TILE) * row_sum
            d_sim = d_sim.reshape(width, TILE)
            d_sim_low = d_sim.astype(low)
            old = ds_first[:, pl.ds(t, TILE)].astype(f32)
            ds_first[:, pl.ds(t, TILE)] = jnp.where(mask, d_sim, old).astype(low)
            inner_total = inner_total + mul_t(kernel_rows.astype(low), own_grad)
            key_total = key_total + mul_t(d_sim_low, qkv_ref[:width, pl.ds(t, TILE)])
            full = windows(vpad, start, end, t)
            grad_own = jnp.where(mask, own_grad.astype(f32), 0.0).astype(low)
            for h in range(heads):
                sel = slice(h * HEAD_DIM, (h + 1) * HEAD_DIM)
                left = jnp.concatenate(
                    [grad_own[sel, c * SUB : (c + 1) * SUB] for c in range(count)], axis=0
                )
                right = jnp.concatenate(
                    [full[sel, c * SUB : (c + 3) * SUB] for c in range(count)], axis=0
                )
                conv_grad[h] += lax.dot_general(
                    left, right, (((0,), (0,)), ((), ())), preferred_element_type=f32
                )
            return inner_total, key_total

        zero = jnp.zeros((width, width), f32)
        inner_total, key_total = lax.fori_loop(lo, hi, tile, (zero, zero))
        d_inner[own_rows(s), :] = fold(inner_total, head_blocks)
        d_k[own_rows(s), :] = fold(key_total, head_blocks) * scale
        return 0

    lax.fori_loop(0, slots, first_slot, 0)

    row = lax.broadcasted_iota(jnp.int32, (SUB, 3 * SUB), 0)
    col = lax.broadcasted_iota(jnp.int32, (SUB, 3 * SUB), 1)
    off = col - row - (SUB - taps // 2)
    tap_lane = lax.broadcasted_iota(jnp.int32, (1, SUB), 1)
    for h in range(heads):
        found = jnp.zeros((1, SUB), f32)
        square = conv_grad[h]
        for n in range(taps):
            part = jnp.sum(jnp.where(off == n, square, 0.0), axis=0, keepdims=True)
            part = jnp.sum(part, axis=1, keepdims=True)
            found = jnp.where(tap_lane == n, part, found)
        conv_out_ref[h : h + 1, :] = found

    lane_head = lax.broadcasted_iota(jnp.int32, (1, width), 1) // HEAD_DIM
    value_total = jnp.zeros((packed, width), f32)
    d_inverses = []
    for h in range(heads):
        own = jnp.where(lane_head == h, d_inner[...], 0.0)
        value_total = value_total + wide(mul, spread(inverse_ref[h], slot_blocks), own)
        d_inverses.append(fold(wide(mul_t, own, value_ref[...]), slot_blocks))
    d_value[...] = value_total

    middles_t = [pack_mul_t(eye, middle_ref[h], slot_blocks) for h in range(heads)]

    def newton(k, carry):
        n = PINV_ITERS - 1 - k
        out = []
        for h in range(heads):
            d_inverse, d_middle = carry[h]
            product = steps_ref[n, 0, h]
            second = steps_ref[n, 1, h]
            third = steps_ref[n, 2, h]
            inverse_t = steps_ref[n, 3, h]
            middle_t = middles_t[h]
            d_third = 0.25 * pack_mul(inverse_t, d_inverse, slot_blocks)
            d_second = -pack_mul(product, d_third, slot_blocks)
            d_first = -pack_mul(product, d_second, slot_blocks)
            d_product = (
                -pack_mul(d_third, second, slot_blocks)
                - pack_mul(d_second, 7.0 * eye - product, slot_blocks)
                - d_first
            )
            d_middle = d_middle + pack_mul(d_product, inverse_t, slot_blocks)
            d_inverse = 0.25 * pack_mul(d_inverse, third, slot_blocks) + pack_mul(
                middle_t, d_product, slot_blocks
            )
            out.append((d_inverse, d_middle))
        return tuple(out)

    zero = jnp.zeros((HEAD_DIM, packed), f32)
    final = lax.fori_loop(0, PINV_ITERS, newton, tuple((x, zero) for x in d_inverses))
    lane_slot = lax.broadcasted_iota(jnp.int32, (1, packed), 1) // marks
    dq_total = jnp.zeros((packed, width), f32)
    dk_total = jnp.zeros((packed, width), f32)
    for h in range(heads):
        d_inverse, d_middle = final[h]
        middle = middle_ref[h]
        first_t = steps_ref[0, 3, h]
        d_inverse_t = pack_mul_t(eye, d_inverse, slot_blocks)
        col_sums = jnp.sum(middle, axis=0, keepdims=True)
        share = jnp.sum(d_inverse_t * first_t, axis=0, keepdims=True)
        bound = jnp.zeros((1, packed), f32)
        d_bound = jnp.zeros((1, packed), f32)
        hits = jnp.zeros((1, packed), f32)
        for s in range(slots):
            mine = lane_slot == s
            top = jnp.max(jnp.where(mine, col_sums, 0.0), axis=1, keepdims=True)
            total = jnp.sum(jnp.where(mine, share, 0.0), axis=1, keepdims=True)
            number = jnp.sum(
                jnp.where(mine & (col_sums == top), 1.0, 0.0), axis=1, keepdims=True
            )
            bound = jnp.where(mine, top, bound)
            d_bound = jnp.where(mine, -total / top, d_bound)
            hits = jnp.where(mine, number, hits)
        d_middle = d_middle + d_inverse_t / bound
        d_middle = d_middle + jnp.where(col_sums == bound, d_bound / hits, 0.0)
        prod = spread(middle * d_middle, slot_blocks)
        d_sim = prod - spread(middle, slot_blocks) * jnp.sum(prod, axis=1, keepdims=True)
        d_sim = d_sim * scale
        own = lane_head == h
        q_marks = jnp.where(own, mark_ref[:, :width], 0.0)
        k_marks = jnp.where(own, mark_ref[:, width:], 0.0)
        dq_total = dq_total + wide(mul, d_sim, k_marks)
        dk_total = dk_total + wide(mul, jnp.transpose(d_sim), q_marks)
    d_q[...] = dq_total
    d_k[...] += dk_total

    flipped = []
    for h in range(heads):
        flipped.append(
            band(
                jnp.concatenate(
                    [conv_own[h : h + 1, n : n + 1] for n in reversed(range(taps))], axis=1
                ),
                taps,
            ).astype(low)
        )

    def last_slot(s, _):
        start, end, lo, hi = reach(s)
        inv = denom_ref[s]
        own_d = d_value[own_rows(s), :]
        own_v = value_ref[own_rows(s), :]
        d_block = spread(own_d, head_blocks)
        row_sum = jnp.sum(
            d_block * jnp.concatenate([own_v] * heads, axis=0), axis=1, keepdims=True
        )
        row_sum = row_sum * inv
        d_block = d_block * inv
        d_block_t = jnp.transpose(d_block).astype(low)
        d_block = d_block.astype(low)

        def tile(n, query_total):
            t = pl.multiple_of(n * TILE, TILE)
            mask = lane_mask(start, end, t, TILE)
            kernel_rows = jnp.where(mask, last_ref[:, pl.ds(t, TILE)].astype(f32), 0.0)
            v_rows = qkv_ref[2 * width :, pl.ds(t, TILE)]
            d_sim = kernel_rows * (mul(d_block, v_rows) - row_sum)
            d_low = d_sim.astype(low)
            old = ds_last[:, pl.ds(t, TILE)].astype(f32)
            ds_last[:, pl.ds(t, TILE)] = jnp.where(mask, d_sim, old).astype(low)
            dv = mul(d_block_t, kernel_rows.astype(low))
            dv = dv + convolve(gpad, flipped, start, end, t, heads)
            old = out_ref[2 * width :, pl.ds(t, TILE)].astype(f32)
            out_ref[2 * width :, pl.ds(t, TILE)] = jnp.where(mask, dv, old).astype(low)
            return query_total + mul_t(d_low, qkv_ref[width : 2 * width, pl.ds(t, TILE)])

        query_total = lax.fori_loop(lo, hi, tile, jnp.zeros((width, width), f32))
        d_q[own_rows(s), :] += fold(query_total, head_blocks) * scale
        return 0

    lax.fori_loop(0, slots, last_slot, 0)

    inv_count = slot_marks(len_ref, 0, slots, marks, SUB)[1]
    d_q[...] = d_q[...] * inv_count
    d_k[...] = d_k[...] * inv_count

    def final_slot(s, _):
        start, end, lo, hi = reach(s)
        length = end - start
        own = mark_ref[own_rows(s), :] * scale

        def left(block, d_mark):
            wide_rows = jnp.concatenate([spread(block, head_blocks), d_mark], axis=0)
            return jnp.transpose(wide_rows).astype(low)

        q_left = left(own[:, width:], d_q[own_rows(s), :])
        k_left = left(own[:, :width], d_k[own_rows(s), :])
        mark = lax.broadcasted_iota(jnp.int32, (marks, 1), 0)
        lower = start + (mark * length) // marks
        upper = start + ((mark + 1) * length) // marks

        def tile(n, _):
            t = pl.multiple_of(n * TILE, TILE)
            mask = lane_mask(start, end, t, TILE)
            tok = t + lax.broadcasted_iota(jnp.int32, (marks, TILE), 1)
            member = jnp.where((tok >= lower) & (tok < upper), 1.0, 0.0).astype(low)
            for at, lhs, source in ((0, q_left, ds_first), (width, k_left, ds_last)):
                rhs = jnp.concatenate([source[:, pl.ds(t, TILE)], member], axis=0)
                rows = mul(lhs, rhs)
                old = out_ref[at : at + width, pl.ds(t, TILE)].astype(f32)
                out_ref[at : at + width, pl.ds(t, TILE)] = jnp.where(mask, rows, old).astype(low)
            return 0

        return lax.fori_loop(lo, hi, tile, 0)

    lax.fori_loop(0, slots, final_slot, 0)

    def bias_tile(n, carry):
        t = pl.multiple_of(n * TILE, TILE)
        q_sum, v_sum = carry
        q_rows = out_ref[:width, pl.ds(t, TILE)].astype(f32)
        v_rows = out_ref[2 * width :, pl.ds(t, TILE)].astype(f32)
        for c in range(count):
            q_sum = q_sum + q_rows[:, c * SUB : (c + 1) * SUB]
            v_sum = v_sum + v_rows[:, c * SUB : (c + 1) * SUB]
        return q_sum, v_sum

    zero = jnp.zeros((width, SUB), f32)
    q_sum, v_sum = lax.fori_loop(0, tok_count // TILE, bias_tile, (zero, zero))
    bias_ref[...] = jnp.zeros_like(bias_ref)
    bias_ref[0:1, :] = jnp.sum(jnp.transpose(q_sum), axis=0, keepdims=True)
    bias_ref[1:2, :] = jnp.sum(jnp.transpose(v_sum), axis=0, keepdims=True)


def mix_forward(seq_lengths, tokens, weight_t, bias, conv, slots, marks):
    tok_count, model = tokens.shape
    width = weight_t.shape[0] // 3
    heads = width // HEAD_DIM
    packed = slots * marks
    taps = conv.shape[1]
    whole = lambda *shape: pl.BlockSpec(shape, lambda i, lens: (0,) * len(shape))
    shapes = [
        ((3 * width, tok_count), low),
        ((width, tok_count), low),
        ((width, tok_count), low),
        ((width, tok_count), low),
        ((packed, 2 * width), f32),
        ((packed, width), f32),
        ((packed, width), f32),
        ((slots, width, 1), f32),
        ((heads, HEAD_DIM, packed), f32),
        ((PINV_ITERS, 4, heads, HEAD_DIM, packed), f32),
        ((heads, HEAD_DIM, packed), f32),
        ((8, 128), f32),
    ]
    return pl.pallas_call(
        partial(mix_forward_kernel, slots, marks, taps),
        out_shape=[jax.ShapeDtypeStruct(s, t) for s, t in shapes],
        grid_spec=pltpu.PrefetchScalarGridSpec(
            num_scalar_prefetch=1,
            grid=(tok_count // TILE,),
            in_specs=[
                pl.BlockSpec((TILE, model), lambda i, lens: (i, 0)),
                whole(3 * width, model),
                whole(*bias.shape),
                whole(*conv.shape),
            ],
            out_specs=[whole(*s) for s, _ in shapes],
            scratch_shapes=[
                pltpu.VMEM((width, tok_count + 2 * SUB), low),
                pltpu.VMEM((width, tok_count), f32),
                pltpu.VMEM((8, width), f32),
                pltpu.VMEM((bias.shape[1], 2 * bias.shape[0]), f32),
                pltpu.VMEM((heads, taps), f32),
            ],
        ),
        compiler_params=pltpu.CompilerParams(vmem_limit_bytes=56 * 1024 * 1024),
        cost_estimate=pl.CostEstimate(
            flops=20 * 10**9, bytes_accessed=30 * 10**6, transcendentals=10**6
        ),
        name="mix_forward",
    )(seq_lengths, tokens, weight_t, bias, conv)


def mix_backward(seq_lengths, grad_t, saved, conv, slots, marks):
    qkv_t, first, last, mark, value, inner, denom, middle, steps, inverse = saved
    width, tok_count = grad_t.shape
    heads = width // HEAD_DIM
    packed = slots * marks
    taps = conv.shape[1]
    args = (grad_t, qkv_t, first, last, mark, value, inner, denom, middle, steps, inverse, conv)
    whole = lambda shape: pl.BlockSpec(
        shape, lambda i, lens: (0,) * len(shape), pipeline_mode=pl.Buffered(1)
    )
    shapes = [((3 * width, tok_count), low), ((8, width), f32), ((heads, SUB), f32)]
    square = pltpu.VMEM((packed, width), f32)
    return pl.pallas_call(
        partial(mix_backward_kernel, slots, marks, taps),
        out_shape=[jax.ShapeDtypeStruct(s, t) for s, t in shapes],
        grid_spec=pltpu.PrefetchScalarGridSpec(
            num_scalar_prefetch=1,
            grid=(1,),
            in_specs=[whole(x.shape) for x in args],
            out_specs=[whole(s) for s, _ in shapes],
            scratch_shapes=[
                pltpu.VMEM((width, tok_count + 2 * SUB), low),
                pltpu.VMEM((width, tok_count + 2 * SUB), low),
                pltpu.VMEM((width, tok_count), low),
                pltpu.VMEM((width, tok_count), low),
                pltpu.VMEM((heads, SUB, 3 * SUB), f32),
                square, square, square, square,
                pltpu.VMEM((heads, taps), f32),
            ],
        ),
        compiler_params=pltpu.CompilerParams(vmem_limit_bytes=56 * 1024 * 1024),
        cost_estimate=pl.CostEstimate(
            flops=20 * 10**9, bytes_accessed=30 * 10**6, transcendentals=10**6
        ),
        name="mix_backward",
    )(seq_lengths, *args)


contract_rows = (((0,), (0,)), ((), ()))
contract_cols = (((1,), (1,)), ((), ()))
norm_eps = 1e-05


def split_up(x, dim, peers):
    before, after = (x.shape[:dim], x.shape[dim + 1 :])
    return jnp.moveaxis(x.reshape(*before, peers, -1, *after), dim, 0)


def sum_at_owner(x, axis, dim):
    peers = lax.axis_size(axis)
    tiles = lax.all_to_all(split_up(x, dim, peers), axis, 0, 0, tiled=True)
    return jnp.sum(tiles.astype(f32), axis=0)


def layer_norm(row_data, gain_vec, shift_vec):
    centre = row_data - jnp.mean(row_data, axis=1, keepdims=True)
    spread_row = jnp.mean(centre * centre, axis=1, keepdims=True)
    return centre * lax.rsqrt(spread_row + norm_eps) * gain_vec[None, :] + shift_vec[None, :]


def gelu_exact(values):
    return jax.nn.gelu(values, approximate=False)


def body(
    tokens,
    qkv_weight,
    qv_bias,
    conv_weight,
    out_weight,
    out_bias,
    norm1_gain,
    norm1_bias,
    ffn_in_weight,
    ffn_in_bias,
    ffn_out_weight,
    ffn_out_bias,
    norm2_gain,
    norm2_bias,
    cotangent,
    seq_lengths,
    segment_ids,
    landmark_bounds,
):
    tok_count, model_width = tokens.shape
    head_width = qkv_weight.shape[2]
    heads_here = head_width // HEAD_DIM
    head_total = conv_weight.shape[0]
    kernel_taps = conv_weight.shape[1]
    slots, marks = landmark_bounds.shape
    quarter = tok_count // lax.axis_size("heads")
    head_index = lax.axis_index("heads")
    own_start = head_index * quarter
    both = ("batch", "heads")
    own_rows_low = lax.dynamic_slice_in_dim(tokens, own_start, quarter, 0)
    own_tokens = own_rows_low.astype(f32)
    flat_qkv = qkv_weight.reshape(model_width, 3 * head_width)
    forward = mix_forward(
        seq_lengths, tokens, jnp.transpose(flat_qkv), qv_bias, conv_weight, slots, marks
    )
    qkv_t, first, last, mixed_t, mark, value, inner, denom, middle, steps, inverse, bound = forward
    bound_total = bound[0, 0]
    attn_part = lax.psum_scatter(
        lax.dot_general(mixed_t, out_weight, contract_rows, preferred_element_type=f32).astype(low),
        "heads",
        scatter_dimension=0,
        tiled=True,
    ).astype(f32)
    live_count = jnp.sum((seq_lengths > 0).astype(f32)) * heads_here
    first_res = own_tokens + attn_part + out_bias[None, :]
    norm1_out, norm1_pull = jax.vjp(layer_norm, first_res, norm1_gain, norm1_bias)
    norm1_low = norm1_out.astype(low)
    ff_own = ffn_out_weight.shape[0]
    bias_row = jnp.zeros((16, model_width), low).at[0, :ff_own].set(ffn_in_bias)
    whole_in = lax.all_gather(ffn_in_weight, both, axis=1, tiled=True)
    out_pack = lax.all_gather(jnp.concatenate([ffn_out_weight, bias_row], axis=0), both, axis=0)
    whole_out = out_pack[:, :ff_own].reshape(-1, model_width)
    whole_in_bias = out_pack[:, ff_own, :ff_own].reshape(-1)
    pre_act = (
        jnp.dot(norm1_low, whole_in, preferred_element_type=f32)
        + whole_in_bias.astype(f32)[None, :]
    )
    hidden_act, gelu_pull = jax.vjp(gelu_exact, pre_act)
    hidden_low = hidden_act.astype(low)
    ffn_result = jnp.dot(hidden_low, whole_out, preferred_element_type=f32) + ffn_out_bias[None, :]
    final_out, norm2_pull = jax.vjp(layer_norm, norm1_out + ffn_result, norm2_gain, norm2_bias)
    grad_second, grad_gain_two, grad_shift_two = norm2_pull(cotangent.astype(f32))
    grad_ffn_low = grad_second.astype(low)
    grad_ffn_bias = jnp.sum(grad_ffn_low.astype(f32), axis=0)
    down_term = lax.dot_general(
        hidden_low, grad_ffn_low, contract_rows, preferred_element_type=f32
    ).astype(low)
    grad_hidden = lax.dot_general(
        grad_ffn_low, whole_out, contract_cols, preferred_element_type=f32
    )
    grad_pre = gelu_pull(grad_hidden)[0].astype(low)
    grad_in_bias = jnp.sum(grad_pre.astype(f32), axis=0)
    up_term = lax.dot_general(
        norm1_low, grad_pre, contract_rows, preferred_element_type=f32
    ).astype(low)
    grad_norm1 = grad_second + lax.dot_general(
        grad_pre, whole_in, contract_cols, preferred_element_type=f32
    )
    grad_first, grad_gain_one, grad_shift_one = norm1_pull(grad_norm1)
    grad_attn_low = grad_first.astype(low)
    grad_out_bias = jnp.sum(grad_attn_low.astype(f32), axis=0)
    piece_rows = lax.all_gather(grad_attn_low, "heads", axis=0, tiled=True)
    grad_mix_t = lax.dot_general(
        out_weight, piece_rows, contract_cols, preferred_element_type=f32
    ).astype(low)
    grad_mix_t, down_term, up_term = lax.optimization_barrier((grad_mix_t, down_term, up_term))
    up_share = lax.psum_scatter(up_term, both, scatter_dimension=1, tiled=True).astype(f32)
    down_share = lax.psum_scatter(down_term, both, scatter_dimension=0, tiled=True).astype(f32)
    saved = (qkv_t, first, last, mark, value, inner, denom, middle, steps, inverse)
    grad_t, grad_bias, grad_conv = mix_backward(
        seq_lengths, grad_mix_t, saved, conv_weight, slots, marks
    )
    out_part = lax.dot_general(
        mixed_t, piece_rows, (((1,), (0,)), ((), ())), preferred_element_type=f32
    )
    grad_qv_own = grad_bias[:2]
    qkv_part = lax.dot_general(
        tokens, grad_t, (((0,), (1,)), ((), ())), preferred_element_type=f32
    ).reshape(model_width, 3, head_width)
    input_part = lax.psum_scatter(
        lax.dot_general(
            grad_t, flat_qkv, (((0,), (1,)), ((), ())), preferred_element_type=f32
        ).astype(low),
        "heads",
        scatter_dimension=0,
        tiled=True,
    ).astype(f32)
    input_grad = grad_first + input_part
    conv_full = lax.dynamic_update_slice_in_dim(
        jnp.zeros((head_total, kernel_taps), f32),
        grad_conv[:, :kernel_taps],
        head_index * heads_here,
        0,
    )
    bias_full = lax.dynamic_update_slice_in_dim(
        jnp.zeros((2, head_total * HEAD_DIM), f32), grad_qv_own, head_index * head_width, 1
    )
    qkv_share, out_share = (
        sum_at_owner(qkv_part.astype(low), "batch", 0),
        sum_at_owner(out_part.astype(low), "batch", 1),
    )
    vector_all = jnp.stack(
        [grad_ffn_bias, grad_gain_two, grad_shift_two, grad_gain_one, grad_shift_one, grad_out_bias]
    )
    in_bias_share, vector_share = (
        lax.psum_scatter(grad_in_bias, both, scatter_dimension=0, tiled=True),
        lax.psum_scatter(vector_all, both, scatter_dimension=1, tiled=True),
    )
    conv_sum, bias_sum, bound_all, count_all = lax.psum(
        (conv_full, bias_full, bound_total, live_count), both
    )
    conv_out = lax.dynamic_slice_in_dim(conv_sum, head_index * heads_here, heads_here, 0)
    bias_out = lax.dynamic_slice_in_dim(bias_sum, head_index * head_width, head_width, 1)
    condition = bound_all / count_all
    return (
        final_out.astype(low),
        input_grad,
        qkv_share,
        bias_out,
        conv_out,
        out_share,
        up_share,
        in_bias_share,
        down_share,
        vector_share,
        condition,
    )


def place():
    b, z = lax.axis_index("batch"), lax.axis_index("heads")
    core, x, y = b % 2, (b // 2) % 2, b // 4
    return b, z, b + 1 - 2 * core, b + 2 - 4 * x, b + 4 - 8 * y


def remote(src, dst, send, recv, device):
    return pltpu.make_async_remote_copy(
        src_ref=src,
        dst_ref=dst,
        send_sem=send,
        recv_sem=recv,
        device_id=device,
        device_id_type=pl.DeviceIdType.MESH,
    )


def greet(devices):
    barrier = pltpu.get_barrier_semaphore()
    for device in devices:
        pl.semaphore_signal(
            barrier, inc=1, device_id=device, device_id_type=pl.DeviceIdType.MESH
        )
    pl.semaphore_wait(barrier, len(devices))


def tail_kernel(
    len_ref,
    gt_hbm, wq_hbm, we_hbm, hid_hbm, pre_hbm, n1_hbm, gf_hbm, ga_hbm, mx_hbm, tok_hbm, first_hbm,
    sums_ref, bin_ref, qv_ref, conv_ref, bound_ref,
    input_ref, down_own, up_own, outw_own, qkvw_own, in_bias, vector_own, qv_own, conv_own, ratio,
    small_out,
    gt, wq, we, hid, pre, n1, gf, ga, mx, tok,
    q_in, r_out, r_in, s_in, out_down, out_up, full_outw, full_qkvw, acc_qkvw,
    core_down, core_up, core_outw, core_qkvw,
    one_down, one_up, one_outw, one_qkvw, two_down, two_up, two_outw, two_qkvw,
    e_down, e_up, e_outw, g_down, g_up, g_outw, h_down, h_up, h_outw, small_in,
    load_sem, q_send, q_recv, r_send, r_recv, t_send, t_recv, c_send, c_recv, x_send, x_recv, e_send, e_recv,
    g_send, g_recv, h_send, h_recv, s_send, s_recv,
):
    b, z, bc, bx, by = place()
    both = bx + by - b
    flip = bc - b
    peers = [(b, lax.rem(z + i, 4)) for i in (1, 2, 3)]
    issued = []
    loads = [
        pltpu.make_async_copy(src, dst, load_sem.at[n])
        for n, (src, dst) in enumerate(
            (
                (pre_hbm, pre), (n1_hbm, n1), (hid_hbm, hid), (gf_hbm, gf), (gt_hbm, gt),
                (wq_hbm, wq), (we_hbm, we), (mx_hbm, mx), (ga_hbm, ga), (tok_hbm, tok),
                (first_hbm, input_ref),
            )
        )
    ]
    for copy in loads:
        copy.start()
    greet(peers + [(bc, z), (bx, z), (by, z)])
    chunks, size = r_in.shape[1:3]
    quarter = chunks * size
    ff = down_own.shape[0]
    group = 4 * ff

    zf = z + 1 - 2 * (z % 2)
    zg = z + 2 - 4 * (z // 2)
    partners = ((bc, z), (bx, z), (by, z), (b, zf), (b, zg))

    def small_start(k):
        copy = remote(
            small_out.at[k], small_in.at[k], s_send.at[k], s_recv.at[k], partners[k]
        )
        copy.start()
        issued.append(copy)

    def small_event(k):
        ref = small_in.at[k]
        remote(ref, ref, s_send.at[k], s_recv.at[k], partners[k]).wait_recv()
        small_out[k + 1] = small_out[k] + small_in[k]
        if k < 4:
            small_start(k + 1)

    model = input_ref.shape[1]
    bias_rows = bin_ref.shape[1] // model
    at_vec, at_qv = bias_rows, bias_rows + 6
    heads, taps = conv_own.shape
    at_conv = at_qv + 8
    at_end = at_conv + 4 * heads
    width = qv_own.shape[1]
    small_out[0] = jnp.zeros(small_out.shape[1:], f32)
    for n in range(bias_rows):
        small_out[0, n : n + 1, :] = bin_ref[0:1, n * model : (n + 1) * model]
    small_out[0, at_vec : at_vec + 6, :] = sums_ref[0:6, :]
    live = jnp.int32(0)
    for n in range(len_ref.shape[0]):
        live = live + jnp.where(len_ref[n] > 0, heads, 0)
    lane = lax.broadcasted_iota(jnp.int32, (1, 128), 1)
    small_out[0, at_end : at_end + 1, 0:128] = jnp.where(
        lane == 0, bound_ref[0:1, :], jnp.where(lane == 1, live.astype(f32), 0.0)
    )
    for n in range(4):

        @pl.when(z == n)
        def _():
            for r in range(2):
                row = at_qv + 2 * n + r
                small_out[0, row : row + 1, :width] = qv_ref[r : r + 1, :]
            for r in range(heads):
                row = at_conv + heads * n + r
                small_out[0, row : row + 1, 0:128] = conv_ref[r : r + 1, :]

    small_start(0)

    is_end = (z == 0) | (z == 3)
    low_side = z < 2
    to_inner = jnp.where(low_side, 1, 2)
    across = jnp.where(z == 1, 2, 1)
    to_end = jnp.where(low_side, 0, 3)

    def owner(k):
        return jnp.where(low_side, 3 - k, k)

    def columns(who, c):
        return pl.ds(pl.multiple_of(who * quarter + c * size, size), size)

    def times(x, w):
        return lax.dot_general(x, w, (((0,), (0,)), ((), ())), preferred_element_type=f32)

    def part(who, c):
        return times(gt[:, columns(who, c)], wq[...])

    def q_copy(k, c):
        return remote(
            gt_hbm.at[:, columns(owner(k), c)], q_in.at[k, c], q_send.at[k, c], q_recv.at[k, c],
            (b, to_inner),
        )

    def q_wait(k, c):
        ref = q_in.at[k, c]
        remote(ref, ref, q_send.at[k, c], q_recv.at[k, c], (b, to_end)).wait_recv()

    def r_copy(k, c):
        return remote(
            r_out.at[k, c], r_in.at[k, c], r_send.at[k, c], r_recv.at[k, c], (b, across)
        )

    def t_copy(c):
        return remote(r_in.at[0, c], s_in.at[c], t_send.at[c], t_recv.at[c], (b, to_end))

    def first_hop(k, c):
        @pl.when(jnp.logical_not(is_end))
        def _():
            own = part(owner(k), c)
            q_wait(k, c)
            r_out[k, c] = (own + times(q_in[k, c], we[...])).astype(low)
            r_copy(k, c).start()

    def last_hop(c):
        @pl.when(jnp.logical_not(is_end))
        def _():
            own = part(to_end, c)
            r_copy(0, c).wait_recv()
            r_in[0, c] = (r_in[0, c].astype(f32) + own).astype(low)
            t_copy(c).start()

    cores = (core_down, core_up, core_outw, core_qkvw)
    ones = (one_down, one_up, one_outw, one_qkvw)
    twos = (two_down, two_up, two_outw, two_qkvw)
    outs = (out_down, out_up)
    left = (hid, pre)
    right = (gf, n1)

    def who(slot):
        return b + (slot % 2) * (bx - b) + (slot // 2) * (by - b)

    def term(n, owner):
        at = pl.ds(pl.multiple_of(owner * group, group), group)
        return lax.dot_general(
            left[n][:, at], right[n][...], (((0,), (0,)), ((), ())), preferred_element_type=f32
        )

    def core_copy(n, slot):
        if n < 2:
            src = outs[n].at[slot]
        elif n == 2:
            src = full_outw.at[:, who(slot) + flip]
        else:
            src = full_qkvw.at[who(slot) + flip]
        return remote(src, cores[n].at[slot], c_send.at[n, slot], c_recv.at[n, slot], (bc, z))

    def give(n, slot):
        if n < 2:
            value = term(n, who(slot) + flip).astype(low)
            outs[n][slot] = value.reshape(outs[n].shape[1:])
        core_copy(n, slot).start()

    def keep(n, slot):
        if n < 2:
            own = term(n, who(slot)).reshape(outs[n].shape[1:])
        elif n == 2:
            own = full_outw[:, who(slot)].astype(f32)
        else:
            own = full_qkvw[who(slot)].astype(f32)
        core_copy(n, slot).wait_recv()
        cores[n][slot] = (cores[n][slot].astype(f32) + own).astype(low)

    def side_copy(n, dst, src):
        partner = by if n % 2 == 0 else bx
        return remote(
            cores[n].at[src], ones[n].at[dst], x_send.at[n, dst], x_recv.at[n, dst], (partner, z)
        )

    def small_group(n):
        def one(i, _):
            give(n, 3 - i)
            return 0

        lax.fori_loop(0, 4, one, 0)

    def small_keep(n):
        def one(i, _):
            keep(n, 3 - i)
            return 0

        lax.fori_loop(0, 4, one, 0)
        side_copy(n, 1, 3).start()
        side_copy(n, 0, 2 if n % 2 == 0 else 1).start()

    def half(h, _):
        def one(i, _):
            slot_up, slot_down = 3 - 2 * i - h, 3 - i - 2 * h
            give(1, slot_up)
            give(0, slot_down)
            keep(1, slot_up)

            @pl.when(h == 0)
            def _():
                side_copy(1, 1 - i, slot_up).start()

            keep(0, slot_down)

            @pl.when(h == 0)
            def _():
                side_copy(0, 1 - i, slot_down).start()

            return 0

        lax.fori_loop(0, 2, one, 0)

        @pl.when(h == 0)
        def _():
            for n in (4, 5, 6):
                loads[n].wait()
            first_hop(0, 0)

        return 0

    def one_event(n):
        second = 1 if n % 2 == 0 else 2
        partner, other = (by, bx) if n % 2 == 0 else (bx, by)
        ref = ones[n].at[1]
        remote(ref, ref, x_send.at[n, 1], x_recv.at[n, 1], (partner, z)).wait_recv()
        ones[n][1] = (ones[n][1].astype(f32) + cores[n][second].astype(f32)).astype(low)
        copy = remote(ones[n].at[1], twos[n], x_send.at[n, 2], x_recv.at[n, 2], (other, z))
        copy.start()
        issued.append(copy)

    e_bufs = (e_down, e_up, e_outw)
    g_bufs = (g_down, g_up, g_outw)
    h_bufs = (h_down, h_up, h_outw)

    def e_copy(n, k):
        return remote(
            twos[n].at[owner(k)], e_bufs[n].at[k], e_send.at[n, k], e_recv.at[n, k], (b, to_inner)
        )

    def e_wait(n, k):
        ref = e_bufs[n].at[k]
        remote(ref, ref, e_send.at[n, k], e_recv.at[n, k], (b, to_end)).wait_recv()

    def g_copy(n, k):
        return remote(
            e_bufs[n].at[k], g_bufs[n].at[k], g_send.at[n, k], g_recv.at[n, k], (b, across)
        )

    def h_copy(n):
        return remote(g_bufs[n].at[0], h_bufs[n], h_send.at[n], h_recv.at[n], (b, to_end))

    def two_event(n):
        partner, other = (by, bx) if n % 2 == 0 else (bx, by)
        ref = ones[n].at[0]
        remote(ref, ref, x_send.at[n, 0], x_recv.at[n, 0], (partner, z)).wait_recv()
        ref = twos[n]
        remote(ref, ref, x_send.at[n, 2], x_recv.at[n, 2], (other, z)).wait_recv()
        own = ones[n][0].astype(f32) + cores[n][0].astype(f32)
        if n == 3:
            qkvw_own[...] = twos[n][...].astype(f32) + own
            return
        twos[n][...] = (twos[n][...].astype(f32) + own).astype(low)

    def line_start(n, k):
        @pl.when(is_end)
        def _():
            e_copy(n, k).start()

    def line_across(n, k):
        @pl.when(jnp.logical_not(is_end))
        def _():
            e_wait(n, k)
            e_bufs[n][k] = (
                e_bufs[n][k].astype(f32) + twos[n][owner(k)].astype(f32)
            ).astype(low)
            g_copy(n, k).start()

    def line_back(n):
        @pl.when(jnp.logical_not(is_end))
        def _():
            g_copy(n, 0).wait_recv()
            g_bufs[n][0] = (
                g_bufs[n][0].astype(f32) + twos[n][to_end].astype(f32)
            ).astype(low)
            h_copy(n).start()

    def end_event(n):
        def write(value):
            out = (down_own, up_own, outw_own)[n]
            out[...] = jnp.transpose(value) if n > 0 else value

        @pl.when(is_end)
        def _():
            ref = h_bufs[n]
            remote(ref, ref, h_send.at[n], h_recv.at[n], (b, to_inner)).wait_recv()
            write(twos[n][z].astype(f32) + h_bufs[n][...].astype(f32))
            for k in range(3):
                e_copy(n, k).wait_send()

        @pl.when(jnp.logical_not(is_end))
        def _():
            g_copy(n, 1).wait_recv()
            e_wait(n, 2)
            write(
                twos[n][z].astype(f32)
                + g_bufs[n][1].astype(f32)
                + e_bufs[n][2].astype(f32)
            )
            for k in range(2):
                g_copy(n, k).wait_send()
            h_copy(n).wait_send()

    def projections():
        on, oh = full_outw.shape[2:]
        for s in range(4):
            value = jnp.transpose(mul(mx[s], ga[...]))
            full_outw[s] = value.astype(low).reshape(full_outw.shape[1:])
        acc_qkvw[...] = jnp.zeros_like(acc_qkvw)
        span = quarter

        def one(n, _):
            at = pl.ds(pl.multiple_of(n * span, span), span)
            acc_qkvw[...] += mul(gt[:, at], tok[at, :])
            return 0

        lax.fori_loop(0, 4, one, 0)
        full_qkvw[...] = jnp.transpose(acc_qkvw[...]).astype(low).reshape(full_qkvw.shape)

    @pl.when(is_end)
    def _():
        for k in range(3):
            for c in range(chunks):
                q_copy(k, c).start()

    for n in range(4):
        loads[n].wait()

    lax.fori_loop(0, 2, half, 0)
    first_hop(0, 1)
    one_event(1)
    one_event(0)
    first_hop(0, 2)
    last_hop(0)
    for n in (7, 8, 9):
        loads[n].wait()
    projections()
    first_hop(1, 0)
    last_hop(1)
    small_group(2)
    small_group(3)
    small_event(0)
    first_hop(1, 1)
    last_hop(2)
    small_keep(2)
    small_keep(3)
    small_event(1)
    first_hop(1, 2)
    two_event(1)
    line_start(1, 0)
    two_event(0)
    line_start(0, 0)
    line_start(1, 1)
    line_start(0, 1)
    small_event(2)
    one_event(2)
    one_event(3)
    small_event(3)
    two_event(2)
    for k in range(3):
        line_start(2, k)
    line_start(1, 2)
    line_start(0, 2)
    two_event(3)
    small_event(4)
    loads[10].wait()

    def own_rows(c, _):
        rows = pl.ds(pl.multiple_of(c * size, size), size)
        input_ref[rows, :] += part(z, c)

        @pl.when(is_end)
        def _():
            ref = s_in.at[c]
            remote(ref, ref, t_send.at[c], t_recv.at[c], (b, to_inner)).wait_recv()
            input_ref[rows, :] += s_in[c].astype(f32)

        @pl.when(jnp.logical_not(is_end))
        def _():
            r_copy(1, c).wait_recv()
            q_wait(2, c)
            input_ref[rows, :] += r_in[1, c].astype(f32) + times(q_in[2, c], we[...])

        return 0

    lax.fori_loop(0, chunks, own_rows, 0)
    for n, k in ((1, 0), (0, 0), (1, 1), (0, 1), (2, 0), (2, 1)):
        line_across(n, k)
        if k == 1:
            line_back(n)
    for n in (1, 0, 2):
        end_event(n)

    @pl.when(is_end)
    def _():
        for k in range(3):
            for c in range(chunks):
                q_copy(k, c).wait_send()

    @pl.when(jnp.logical_not(is_end))
    def _():
        for c in range(chunks):
            r_copy(0, c).wait_send()
            r_copy(1, c).wait_send()
            t_copy(c).wait_send()

    final = small_out.at[5]
    in_bias[...] = jnp.zeros_like(in_bias)
    index = b * 4 + z
    per_row = model // ff
    for n in range(bias_rows):

        @pl.when(index // per_row == n)
        def _():
            row = pltpu.roll(final[n : n + 1, :], (model - (index % per_row) * ff) % model, 1)
            in_bias[...] = row[:, :ff]

    share = vector_own.shape[1]
    vectors = final[at_vec : at_vec + 6, :]
    vector_own[...] = pltpu.roll(vectors, (model - index * share) % model, 1)[:, :share]
    for n in range(4):

        @pl.when(z == n)
        def _():
            qv_own[...] = final[at_qv + 2 * n : at_qv + 2 * n + 2, :width]
            conv_own[...] = final[at_conv + heads * n : at_conv + heads * (n + 1), :taps]

    ratio[...] = final[at_end : at_end + 1, 0:1] / final[at_end : at_end + 1, 1:2]

    for n in range(4):
        for dst in range(2):
            side_copy(n, dst, dst).wait_send()
        for slot in range(4):
            core_copy(n, slot).wait_send()
    for copy in issued:
        copy.wait_send()


def tail(
    lengths, gt, wq, we, hid, pre, n1, gf, ga, mx, tok, first, sums, bins, qv_grad, conv_grad, bound,
    taps,
):
    quarter, model = first.shape
    chunks = 3
    size = quarter // chunks
    ff = hid.shape[1] // 32
    width = mx.shape[1]
    heads = width // HEAD_DIM
    on, oh = model // 8, width
    qn, qh = model // 8, gt.shape[0]
    blocks = ((4, ff, model), (4, ff, model), (4, on, oh), (qn, qh))
    own = lambda *s: jax.ShapeDtypeStruct(s, f32)
    vm = lambda *s: pltpu.VMEM(s, low)
    dma = pltpu.SemaphoreType.DMA
    sources = (gt, wq, we, hid, pre, n1, gf, ga, mx, tok)
    small = -(-(bins.shape[1] // model + 15 + 4 * heads) // 8) * 8
    vmem = pl.BlockSpec(memory_space=pltpu.VMEM)
    return pl.pallas_call(
        tail_kernel,
        out_shape=[
            own(quarter, model), own(ff, model), own(model, ff), own(oh, on), own(qn, qh),
            own(1, ff), own(6, model // 32), own(2, width), own(heads, taps), own(1, 1),
        ],
        in_specs=[pl.BlockSpec(memory_space=pltpu.SMEM)]
        + [pl.BlockSpec(memory_space=pl.ANY)] * 11
        + [vmem] * 5,
        out_specs=[vmem] * 10,
        scratch_shapes=[
            pltpu.VMEM((6, small, model), f32),
            *[vm(*x.shape) for x in sources],
            vm(3, chunks, qh, size), vm(2, chunks, size, model), vm(2, chunks, size, model),
            vm(chunks, size, model),
            vm(4, *blocks[0]), vm(4, *blocks[1]),
            vm(4, 8, on, oh), vm(8, qn, qh), pltpu.VMEM((qh, model), f32),
            *[vm(4, *s) for s in blocks],
            *[vm(2, *s) for s in blocks],
            *[vm(*s) for s in blocks],
            *[vm(3, *s[1:]) for s in blocks[:3]],
            *[vm(2, *s[1:]) for s in blocks[:3]],
            *[vm(*s[1:]) for s in blocks[:3]],
            pltpu.VMEM((5, small, model), f32),
            dma((11,)),
            dma((3, chunks)), dma((3, chunks)), dma((2, chunks)), dma((2, chunks)),
            dma((chunks,)), dma((chunks,)), dma((4, 4)), dma((4, 4)),
            dma((4, 3)), dma((4, 3)), dma((3, 3)), dma((3, 3)), dma((3, 2)), dma((3, 2)),
            dma((3,)), dma((3,)), dma((5,)), dma((5,)),
        ],
        compiler_params=pltpu.CompilerParams(
            collective_id=3, has_side_effects=True, vmem_limit_bytes=63 * 1024 * 1024
        ),
        name="tail",
    )(lengths, *sources, first, sums, bins, qv_grad, conv_grad, bound)


def cumulative(x):
    t = 1.0 / (1.0 + 0.23164189 * jnp.abs(x))
    density = jnp.exp(-0.5 * x * x) * 0.3989422804
    poly = t * (
        0.319381530 + t * (-0.356563782 + t * (1.781477937 + t * (-1.821255978 + t * 1.330274429)))
    )
    upper = density * poly
    return jnp.where(x >= 0.0, 1.0 - upper, upper), density


def normed(x):
    centre = x - jnp.mean(x, axis=1, keepdims=True)
    scale = lax.rsqrt(jnp.mean(centre * centre, axis=1, keepdims=True) + norm_eps)
    return centre * scale, scale


def norm_back(grad, gain, rows, scale):
    e = grad * gain
    return scale * (
        e - jnp.mean(e, axis=1, keepdims=True) - rows * jnp.mean(e * rows, axis=1, keepdims=True)
    )


def middle_kernel(
    share,
    mixed_ref, own0, own1, own2, own3, tok_hbm, cot_hbm,
    vec_ref,
    out_hbm, first_hbm, attn_hbm, hidden_hbm, pre_hbm, norm_hbm, ffn_hbm, all_ref, grad_ref,
    sums_ref, bin_ref,
    out_ref, first_ref, attn_ref, hidden_ref, pre_ref, norm_ref, ffn_ref, tok_ref, cot_ref,
    packs, wof, wo, slope, total, n1_ref, scale_ref, turned,
    a_send, a_recv, f_send, f_recv, s_send, s_recv, p_send, p_recv, g_send, g_recv,
    own_sem, own_turn, out_sem,
):
    b, z, bc, bx, by = place()
    both = bx + by - b
    flip = bc - b
    peers = [(b, lax.rem(z + i, 4)) for i in (1, 2, 3)]
    width, quarter = all_ref.shape[1:]
    model = tok_hbm.shape[1]
    owns = (own0, own1, own2, own3)
    origins = [lax.rem(z + 4 - i, 4) for i in range(4)]
    size = turned.shape[2]
    tiles = quarter // size
    issued = []

    def own_columns(n):
        return pl.ds(pl.multiple_of(n * quarter, quarter), quarter)

    local = [
        pltpu.make_async_copy(own, packs.at[b, origin], own_sem.at[i])
        for i, (own, origin) in enumerate(zip(owns, origins))
    ]
    local.append(
        pltpu.make_async_copy(mixed_ref.at[:, own_columns(z)], all_ref.at[z], own_sem.at[4])
    )
    local.append(
        pltpu.make_async_copy(
            tok_hbm.at[pl.ds(pl.multiple_of(z * quarter, quarter), quarter)], tok_ref, own_sem.at[5]
        )
    )
    cot_load = pltpu.make_async_copy(cot_hbm, cot_ref, own_sem.at[6])
    for copy in local:
        copy.start()
    cot_load.start()
    greet(peers + [(bc, z), (bx, z), (by, z)])

    ff = (packs.shape[2] - 32) // 2
    half = ff // 2
    pieces = ((2 * ff, 32), (0, half), (half, half), (ff, ff))
    through_y = (True, True, True, False)
    count = len(pieces)

    def rows_of(n):
        return pl.ds(*pieces[n])

    def mix_copy(r, i):
        to = lax.rem(z + i, 4)
        src = mixed_ref.at[:, pl.ds(pl.multiple_of(to * quarter + r * size, size), size)]
        return remote(
            src, all_ref.at[z, :, pl.ds(r * size, size)], a_send.at[r, i - 1], a_recv.at[r, i - 1],
            (b, to),
        )

    def side(n, axis):
        out = []
        for i in range(4):
            out.append(
                remote(
                    owns[i].at[rows_of(n)], packs.at[b, origins[i], rows_of(n)],
                    f_send.at[n, axis, i], f_recv.at[n, axis, i], (by if axis else bx, z),
                )
            )
        return out

    def side_start(n):
        for axis in (0, 1):
            for copy in side(n, axis):
                copy.start()
                issued.append(copy)

    def block(n, who):
        return packs.at[who, :, rows_of(n)]

    def corner(n):
        who, device = (bx, by) if through_y[n] else (by, bx)
        return remote(block(n, who), block(n, who), s_send.at[n], s_recv.at[n], (device, z))

    def mate(n, slot, who):
        return remote(
            block(n, who), block(n, who), p_send.at[n, slot], p_recv.at[n, slot], (bc, z)
        )

    def mate_start(n, slot, who):
        copy = mate(n, slot, who)
        copy.start()
        issued.append(copy)

    def side_wait(n, axis):
        who = by if axis else bx
        for i in range(4):
            ref = packs.at[who, origins[i], rows_of(n)]
            remote(
                ref, ref, f_send.at[n, axis, i], f_recv.at[n, axis, i], (who, z)
            ).wait_recv()
        if through_y[n] == (axis == 0):
            copy = corner(n)
            copy.start()
            issued.append(copy)
        mate_start(n, 1 + axis, who)

    def corner_wait(n):
        device = by if through_y[n] else bx
        ref = block(n, both)
        remote(ref, ref, s_send.at[n], s_recv.at[n], (device, z)).wait_recv()
        mate_start(n, 3, both)

    def mate_wait(n, slot, who):
        mate(n, slot, who + flip).wait_recv()

    side_start(0)
    side_start(1)
    for r in range(tiles):
        for i in (1, 2, 3):
            copy = mix_copy(r, i)
            copy.start()
            issued.append(copy)
    for copy in local:
        copy.wait()
    for n in range(count):
        mate_start(n, 0, b)
    out_bias, gain1, shift1, down_bias, gain2, shift2 = [
        vec_ref[n : n + 1, :] for n in range(6)
    ]
    sums_ref[...] = jnp.zeros_like(sums_ref)
    bin_ref[...] = jnp.zeros_like(bin_ref)
    total[...] = jnp.zeros_like(total)
    side_wait(0, 0)
    side_wait(0, 1)
    side_start(2)
    side_start(3)
    corner_wait(0)
    for slot, who in enumerate((b, bx, by, both)):
        mate_wait(0, slot, who)
    group = 4 * ff
    for q in range(8):
        for s in range(4):
            wof[pl.ds(s * width + q * share, share), :] = packs[
                q, s, pl.ds(2 * ff, share), :
            ].astype(f32)
    wo[...] = wof[...].astype(low).reshape(wo.shape)
    for q in range(8):
        row = jnp.zeros((1, group), f32)
        for s in range(4):
            row = row + packs[q, s, 2 * ff + share : 2 * ff + share + 1, :group].astype(f32)
        bin_ref[1:2, q * group : (q + 1) * group] = row

    def row_sum(n, x):
        sums_ref[n : n + 1, :] += jnp.sum(x, axis=0, keepdims=True)

    def first_rows(r):
        rows = pl.ds(r * size, size)
        for i in (1, 2, 3):
            ref = all_ref.at[origins[i], :, rows]
            remote(
                ref, ref, a_send.at[r, i - 1], a_recv.at[r, i - 1], (b, origins[i])
            ).wait_recv()
        attn = jnp.zeros((size, model), f32)
        for s in range(4):
            attn = attn + lax.dot_general(
                all_ref[s, :, rows], wo[s], (((0,), (0,)), ((), ())), preferred_element_type=f32
            )
        n1, scale1 = normed(tok_ref[rows, :].astype(f32) + attn + out_bias)
        n1_ref[rows, :] = n1
        scale_ref[rows, :] = jnp.broadcast_to(scale1, (size, scale_ref.shape[1]))
        norm_ref[rows, :] = (n1 * gain1 + shift1).astype(low)

    span = 2 * group

    def weights(c, start):
        return jnp.concatenate(
            [
                packs[2 * c + n, :, pl.ds(start, ff), :].reshape(group, model)
                for n in range(2)
            ],
            axis=0,
        )

    def tile_rows(r):
        return pl.ds(pl.multiple_of(r * size, size), size)

    def feed(who):
        c = who // 2
        lanes = pl.ds(pl.multiple_of(c * span, span), span)

        def one(r, _):
            rows = tile_rows(r)
            act = mul_t(norm_ref[rows, :], weights(c, 0)) + bin_ref[1:2, lanes]
            phi, density = cumulative(act)
            hidden = (act * phi).astype(low)
            hidden_ref[rows, lanes] = hidden
            slope[rows, lanes] = phi + act * density
            total[rows, :] += mul(hidden, weights(c, ff))
            return 0

        lax.fori_loop(0, tiles, one, 0)

    first_rows(0)
    for axis in (0, 1):
        side_wait(1, axis)
    first_rows(1)
    for axis in (0, 1):
        side_wait(2, axis)
    first_rows(2)
    for n in range(1, count):
        mate_wait(n, 0, b)
    feed(b)
    side_wait(3, 0)
    side_wait(3, 1)
    for n in range(1, count):
        mate_wait(n, 1, bx)
    feed(bx)
    corner_wait(1)
    for n in range(1, count):
        mate_wait(n, 2, by)
    feed(by)
    corner_wait(2)
    corner_wait(3)
    for n in range(1, count):
        mate_wait(n, 3, both)
    feed(both)

    def turn_copy(r, i):
        to = lax.rem(z + i, 4)
        src = turned.at[r, pl.ds(pl.multiple_of(to * width, width), width)]
        dst = grad_ref.at[:, pl.ds(pl.multiple_of(z * quarter + r * size, size), size)]
        return remote(src, dst, g_send.at[r, i - 1], g_recv.at[r, i - 1], (b, to))

    def turn_own(r):
        src = turned.at[r, pl.ds(pl.multiple_of(z * width, width), width)]
        dst = grad_ref.at[:, pl.ds(pl.multiple_of(z * quarter + r * size, size), size)]
        return pltpu.make_async_copy(src, dst, own_turn.at[r])

    stores = (
        (out_ref, out_hbm), (first_ref, first_hbm), (attn_ref, attn_hbm), (pre_ref, pre_hbm),
        (ffn_ref, ffn_hbm), (hidden_ref, hidden_hbm), (norm_ref, norm_hbm),
    )

    def store(r, n):
        src, dst = stores[n]
        rows = tile_rows(r)
        return pltpu.make_async_copy(src.at[rows], dst.at[rows], out_sem.at[r, n])

    cot_load.wait()

    def row_tile(r, _):
        rows = tile_rows(r)
        n1 = n1_ref[rows, :]
        norm1 = n1 * gain1 + shift1
        n2, scale2 = normed(norm1 + total[rows, :] + down_bias)
        out_ref[rows, :] = (n2 * gain2 + shift2).astype(low)
        cot = cot_ref[rows, :].astype(f32)
        row_sum(1, cot * n2)
        row_sum(2, cot)
        grad2 = norm_back(cot, gain2, n2, scale2)
        grad_low = grad2.astype(low)
        ffn_ref[rows, :] = grad_low
        row_sum(0, grad_low.astype(f32))
        total[rows, :] = grad2

        def backward(c, _):
            lanes = pl.ds(pl.multiple_of(c * span, span), span)
            grad = (slope[rows, lanes] * mul_t(grad_low, weights(c, ff))).astype(low)
            pre_ref[rows, lanes] = grad
            bin_ref[0:1, lanes] += jnp.sum(grad.astype(f32), axis=0, keepdims=True)
            total[rows, :] += mul(grad, weights(c, 0))
            return 0

        lax.fori_loop(0, 4, backward, 0, unroll=2)
        grad1 = total[rows, :]
        row_sum(3, grad1 * n1)
        row_sum(4, grad1)
        first = norm_back(grad1, gain1, n1, scale_ref[rows, 0:1])
        first_ref[rows, :] = first
        attn_low = first.astype(low)
        attn_ref[rows, :] = attn_low
        row_sum(5, attn_low.astype(f32))
        for s in range(4):
            turned[r, pl.ds(s * width, width), :] = mul_t(wo[s], attn_low).astype(low)
        for i in (1, 2, 3):
            turn_copy(r, i).start()
        turn_own(r).start()
        for n in range(len(stores)):
            store(r, n).start()
        return 0

    lax.fori_loop(0, tiles, row_tile, 0)

    def finish(r, _):
        for i in (1, 2, 3):
            source = origins[i]
            ref = grad_ref.at[:, pl.ds(pl.multiple_of(source * quarter + r * size, size), size)]
            remote(ref, ref, g_send.at[r, i - 1], g_recv.at[r, i - 1], (b, source)).wait_recv()
            turn_copy(r, i).wait_send()
        turn_own(r).wait()
        for n in range(len(stores)):
            store(r, n).wait()
        return 0

    lax.fori_loop(0, tiles, finish, 0)
    for copy in issued:
        copy.wait_send()


def ffn_middle(mixed_t, packs, tokens, cot, vectors, ff, share):
    width, tok_count = mixed_t.shape
    quarter, model = tok_count // 4, tokens.shape[1]
    size = quarter // 3
    rows = packs[0].shape[0]
    shape = jax.ShapeDtypeStruct
    vmem = pl.BlockSpec(memory_space=pltpu.VMEM)
    hbm = pl.BlockSpec(memory_space=pl.ANY)
    dma = pltpu.SemaphoreType.DMA
    kept = [
        ((quarter, model), low),
        ((quarter, model), f32),
        ((quarter, model), low),
        ((quarter, 32 * ff), low),
        ((quarter, 32 * ff), low),
        ((quarter, model), low),
        ((quarter, model), low),
    ]
    return pl.pallas_call(
        partial(middle_kernel, share),
        out_shape=[shape(*x) for x in kept]
        + [
            shape((4, width, quarter), low),
            shape((width, tok_count), low),
            shape((8, model), f32),
            shape((8, 32 * ff), f32),
        ],
        in_specs=[hbm] + [vmem] * 4 + [hbm] * 2 + [vmem],
        out_specs=[hbm] * 7 + [vmem, hbm, vmem, vmem],
        scratch_shapes=[pltpu.VMEM(*x) for x in kept]
        + [
            pltpu.VMEM((quarter, model), low),
            pltpu.VMEM((quarter, model), low),
            pltpu.VMEM((8, 4, rows, model), low),
            pltpu.VMEM((4 * width, model), f32),
            pltpu.VMEM((4, width, model), low),
            pltpu.VMEM((quarter, 32 * ff), f32),
            pltpu.VMEM((quarter, model), f32),
            pltpu.VMEM((quarter, model), f32),
            pltpu.VMEM((quarter, 128), f32),
            pltpu.VMEM((3, 4 * width, size), low),
            dma((3, 3)), dma((3, 3)), dma((4, 2, 4)), dma((4, 2, 4)), dma((4,)), dma((4,)),
            dma((4, 4)), dma((4, 4)), dma((3, 3)), dma((3, 3)),
            dma((7,)), dma((3,)), dma((3, 7)),
        ],
        compiler_params=pltpu.CompilerParams(
            collective_id=1, has_side_effects=True, vmem_limit_bytes=63 * 1024 * 1024
        ),
        name="middle",
    )(mixed_t, *packs, tokens, cot, vectors)


def settle_kernel(*refs):
    count = len(refs) // 2
    for n in range(count):
        refs[count + n][...] = refs[n][...]


def settle(*arrays):
    vmem = pl.BlockSpec(memory_space=pltpu.VMEM)
    return pl.pallas_call(
        settle_kernel,
        out_shape=[jax.ShapeDtypeStruct(x.shape, x.dtype) for x in arrays],
        in_specs=[vmem] * len(arrays),
        out_specs=[vmem] * len(arrays),
        name="settle",
    )(*arrays)


def slice_body(
    tokens,
    qkv_weight,
    qv_bias,
    conv_weight,
    out_weight,
    out_bias,
    norm1_gain,
    norm1_bias,
    ffn_in_weight,
    ffn_in_bias,
    ffn_out_weight,
    ffn_out_bias,
    norm2_gain,
    norm2_bias,
    cotangent,
    seq_lengths,
    segment_ids,
    landmark_bounds,
):
    model = tokens.shape[1]
    width = qkv_weight.shape[2]
    kernel_taps = conv_weight.shape[1]
    slots, marks = landmark_bounds.shape
    z = lax.axis_index("heads")
    b = lax.axis_index("batch")
    weight_t = jnp.transpose(qkv_weight.reshape(model, 3 * width))
    ff_own = ffn_out_weight.shape[0]
    share = width // 8
    bias_row = lax.dynamic_update_slice_in_dim(
        jnp.zeros((4 * ff_own,), low), ffn_in_bias, z * ff_own, 0
    )
    misc_own = jnp.concatenate(
        [
            lax.dynamic_slice_in_dim(out_weight, b * share, share, 0),
            jnp.zeros((32 - share, model), low).at[0, : 4 * ff_own].set(bias_row),
        ],
        axis=0,
    )
    pack = jnp.concatenate([jnp.transpose(ffn_in_weight), ffn_out_weight, misc_own], axis=0)
    packs = [pack] + [
        lax.ppermute(pack, "heads", [(n, (n + i) % 4) for n in range(4)]) for i in (1, 2, 3)
    ]
    forward = mix_forward(
        seq_lengths, tokens, weight_t, qv_bias, conv_weight, slots, marks
    )
    qkv_t, first, last, mixed_t, mark, value, inner, denom, middle, steps, inverse, bound = forward
    vectors = jnp.stack(
        [out_bias, norm1_gain, norm1_bias, ffn_out_bias, norm2_gain, norm2_bias]
    )
    (
        final_low, grad_first, grad_attn_low, hidden_low, grad_pre, norm1_low, grad_ffn_low,
        mixed_all, grad_mix_t, vector_sums, bias_sums,
    ) = ffn_middle(mixed_t, packs, tokens, cotangent, vectors, ff_own, share)
    saved = (qkv_t, first, last, mark, value, inner, denom, middle, steps, inverse)
    held, grad_mix_t = lax.optimization_barrier((weight_t, grad_mix_t))
    weight_end = lax.ppermute(held, "heads", [(0, 1), (3, 2)])
    grad_t, grad_bias, grad_conv = mix_backward(
        seq_lengths, grad_mix_t, saved, conv_weight, slots, marks
    )
    (
        input_grad, down_share, up_share, out_share, qkv_share,
        in_bias_share, vector_share, bias_out, conv_out, condition,
    ) = tail(
        seq_lengths, grad_t, weight_t, weight_end, hidden_low, grad_pre, norm1_low, grad_ffn_low,
        grad_attn_low, mixed_all, tokens, grad_first, vector_sums, bias_sums, grad_bias,
        grad_conv, bound, kernel_taps,
    )
    (
        final_low, input_grad, down_share, up_share, out_share, qkv_share,
        in_bias_share, vector_share, bias_out, conv_out, condition,
    ) = settle(
        final_low, input_grad, down_share, up_share, out_share, qkv_share,
        in_bias_share, vector_share, bias_out, conv_out, condition,
    )
    return (
        final_low,
        input_grad,
        qkv_share.reshape(model // 8, 3, width),
        bias_out,
        conv_out,
        out_share,
        up_share,
        in_bias_share.reshape(ff_own),
        down_share,
        vector_share,
        condition.reshape(()),
    )


def solution(mesh):
    chosen = slice_body if dict(mesh.shape) == {"batch": 8, "heads": 4} else body
    in_specs = (
        P("batch", None),
        P(None, None, "heads"),
        P(),
        P(),
        P("heads", None),
        P(),
        P(),
        P(),
        P(None, ("batch", "heads")),
        P(("batch", "heads")),
        P(("batch", "heads"), None),
        P(),
        P(),
        P(),
        P(("batch", "heads"), None),
        P("batch"),
        P("batch"),
        P("batch", None),
    )
    out_specs = (
        P(("batch", "heads"), None),
        P(("batch", "heads"), None),
        P("batch", None, "heads"),
        P(None, "heads"),
        P("heads", None),
        P("heads", "batch"),
        P(None, ("batch", "heads")),
        P(("batch", "heads")),
        P(("batch", "heads"), None),
        P(None, ("batch", "heads")),
        P(),
    )
    return jax.shard_map(chosen, mesh=mesh, in_specs=in_specs, out_specs=out_specs, check_vma=False)
```

```python
from functools import partial

import jax
import jax.numpy as jnp
from jax import lax
from jax.experimental import pallas as pl
from jax.experimental.pallas import tpu as pltpu
from jax.sharding import PartitionSpec as P

HEAD_DIM = 64
PINV_ITERS = 6
TILE = 512
SUB = 128

f32 = jnp.float32
low = jnp.bfloat16
mask_fill = -1000000000.0


def split(x):
    high = x.astype(low)
    return high, (x - high.astype(f32)).astype(low)


def mul(a, b):
    return lax.dot_general(a, b, (((1,), (0,)), ((), ())), preferred_element_type=f32)


def mul_t(a, b):
    return lax.dot_general(a, b, (((1,), (1,)), ((), ())), preferred_element_type=f32)


def wide(form, left, right):
    left_high, left_low = split(left)
    right_high, right_low = split(right)
    return form(left_high, right_high) + (
        form(left_high, right_low) + form(left_low, right_high)
    )


def block_grid(rows, cols):
    row_block = lax.broadcasted_iota(jnp.int32, (rows, cols), 0) // HEAD_DIM
    col_block = lax.broadcasted_iota(jnp.int32, (rows, cols), 1) // HEAD_DIM
    return row_block == col_block


def spread(x, blocks):
    count = blocks.shape[0] // x.shape[0]
    return jnp.where(blocks, jnp.concatenate([x] * count, axis=0), jnp.zeros_like(x[:1, :1]))


def fold(x, blocks):
    kept = jnp.where(blocks, x, jnp.zeros_like(x[:1, :1]))
    rows = HEAD_DIM
    out = kept[:rows]
    for n in range(1, x.shape[0] // rows):
        out = out + kept[n * rows : (n + 1) * rows]
    return out


def pack_mul(left, right, blocks):
    left_high, left_low = split(left)
    right_high, right_low = split(right)
    right_high, right_low = spread_low(right_high, blocks), spread_low(right_low, blocks)
    return mul(left_high, right_high) + (mul(left_high, right_low) + mul(left_low, right_high))


def pack_mul_t(left, right, blocks):
    left_high, left_low = split(left)
    right_high, right_low = split(right)
    right_high, right_low = spread_low(right_high, blocks), spread_low(right_low, blocks)
    return mul_t(left_high, right_high) + (mul_t(left_high, right_low) + mul_t(left_low, right_high))


def spread_low(x, blocks):
    return spread(x.astype(f32), blocks).astype(low)


def slot_bounds(len_ref, s, slots):
    start = jnp.int32(0)
    for n in range(slots):
        start = start + jnp.where(n < s, len_ref[n], 0)
    return start, start + len_ref[s]


def eye_pack(width):
    row = lax.broadcasted_iota(jnp.int32, (HEAD_DIM, width), 0)
    col = lax.broadcasted_iota(jnp.int32, (HEAD_DIM, width), 1) % HEAD_DIM
    return jnp.where(row == col, 1.0, 0.0).astype(f32)


def lane_mask(start, end, at, width):
    tok = at + lax.broadcasted_iota(jnp.int32, (1, width), 1)
    return (tok >= start) & (tok < end)


def band(taps_row, width):
    row = lax.broadcasted_iota(jnp.int32, (SUB, 3 * SUB), 0)
    col = lax.broadcasted_iota(jnp.int32, (SUB, 3 * SUB), 1)
    off = col - row - (SUB - width // 2)
    out = jnp.zeros((SUB, 3 * SUB), f32)
    for n in range(width):
        out = jnp.where(off == n, taps_row[:, n : n + 1], out)
    return out


def slot_marks(len_ref, at, slots, marks, width):
    rows = slots * marks
    row = lax.broadcasted_iota(jnp.int32, (rows, 1), 0)
    slot = row // marks
    mark = row % marks
    start = jnp.zeros((rows, 1), jnp.int32)
    length = jnp.zeros((rows, 1), jnp.int32)
    for n in range(slots):
        start = start + jnp.where(slot > n, len_ref[n], 0)
        length = jnp.where(slot == n, len_ref[n], length)
    lower = start + (mark * length) // marks
    upper = start + ((mark + 1) * length) // marks
    inv_count = 1.0 / jnp.maximum((upper - lower).astype(f32), 1.0)
    tok = at + lax.broadcasted_iota(jnp.int32, (rows, width), 1)
    member = jnp.where((tok >= lower) & (tok < upper), 1.0, 0.0)
    return member, inv_count


def mix_forward_kernel(
    slots, marks, taps,
    len_ref, tok_ref, weight_ref, bias_ref, conv_ref,
    qkv_ref, first_ref, last_ref, mixed_ref, mark_ref, value_ref, inner_ref,
    denom_ref, middle_ref, steps_ref, inverse_ref, bound_ref,
    vpad, scores, vsum, bias_col, conv_own,
):
    step = pl.program_id(0)
    width = first_ref.shape[0]
    heads = width // HEAD_DIM
    tok_count = qkv_ref.shape[1]
    tiles = tok_count // TILE
    packed = slots * marks
    at = pl.multiple_of(step * TILE, TILE)

    @pl.when(step == 0)
    def _():
        z = lax.axis_index("heads")
        own_taps(conv_own, conv_ref, z)
        columns = jnp.transpose(jnp.concatenate([bias_ref[...], bias_ref[...]], axis=0))
        bias_col[: bias_ref.shape[1], :] = columns
        mark_ref[...] = jnp.zeros_like(mark_ref)
        vsum[...] = jnp.zeros_like(vsum)
        vpad[:, :SUB] = jnp.zeros((width, SUB), low)
        vpad[:, tok_count + SUB :] = jnp.zeros((width, SUB), low)

    at_head = pl.ds(pl.multiple_of(lax.axis_index("heads") * width, HEAD_DIM), width)
    rows = mul_t(weight_ref[...], tok_ref[...])
    rows = jnp.concatenate(
        [
            rows[:width] + bias_col[at_head, 0:1],
            rows[width : 2 * width],
            rows[2 * width :] + bias_col[at_head, 1:2],
        ],
        axis=0,
    ).astype(low)
    qkv_ref[:, pl.ds(at, TILE)] = rows
    vpad[:, pl.ds(pl.multiple_of(at + SUB, SUB), TILE)] = rows[2 * width :]
    member, inv_count = slot_marks(len_ref, at, slots, marks, TILE)
    mark_ref[...] += mul_t(member.astype(low), rows[: 2 * width])
    vsum[...] += mul_t(jnp.ones((8, TILE), low), rows[2 * width :])
    first_ref[:, pl.ds(at, TILE)] = jnp.zeros((width, TILE), low)
    last_ref[:, pl.ds(at, TILE)] = jnp.zeros((width, TILE), low)
    mixed_ref[:, pl.ds(at, TILE)] = jnp.zeros((width, TILE), low)

    @pl.when(step == tiles - 1)
    def _():
        mark_ref[...] = mark_ref[...] * inv_count
        head_blocks = block_grid(width, width)
        slot_blocks = block_grid(packed, packed)
        eye = eye_pack(packed)
        scale = HEAD_DIM ** -0.5

        middles, inverses_t, products = [], [], []
        bound_total = jnp.zeros((1, 1), f32)
        lane_slot = lax.broadcasted_iota(jnp.int32, (1, packed), 1) // marks
        for h in range(heads):
            q_marks = mark_ref[:, h * HEAD_DIM : (h + 1) * HEAD_DIM]
            k_marks = mark_ref[:, width + h * HEAD_DIM : width + (h + 1) * HEAD_DIM]
            sim = wide(mul_t, q_marks, k_marks) * scale
            sim = jnp.where(slot_blocks, sim, -1e30)
            sim = jnp.exp(sim - jnp.max(sim, axis=1, keepdims=True))
            sim = sim / jnp.sum(sim, axis=1, keepdims=True)
            middle = fold(sim, slot_blocks)
            col_sums = jnp.sum(middle, axis=0, keepdims=True)
            bound = jnp.zeros((1, packed), f32)
            for s in range(slots):
                top = jnp.max(jnp.where(lane_slot == s, col_sums, 0.0), axis=1, keepdims=True)
                bound = jnp.where(lane_slot == s, top, bound)
                bound_total += jnp.where(len_ref[s] > 0, top, 0.0)
            middle_ref[h] = middle
            middles.append(middle)
            inverses_t.append(middle / bound)
            products.append(pack_mul_t(middle, middle, slot_blocks) / bound)
        bound_ref[...] = jnp.broadcast_to(bound_total, bound_ref.shape)

        def newton(n, carry):
            out = []
            for h in range(heads):
                inverse_t, product = carry[h]
                square = pack_mul(product, product, slot_blocks)
                cube = pack_mul(product, square, slot_blocks)
                fourth = pack_mul(square, square, slot_blocks)
                second = 15.0 * eye - 7.0 * product + square
                third = 13.0 * eye - 15.0 * product + 7.0 * square - cube
                steps_ref[n, 0, h] = product
                steps_ref[n, 1, h] = second
                steps_ref[n, 2, h] = third
                steps_ref[n, 3, h] = inverse_t
                out.append(
                    (
                        0.25 * pack_mul(third, inverse_t, slot_blocks),
                        0.25 * (13.0 * product - 15.0 * square + 7.0 * cube - fourth),
                    )
                )
            return tuple(out)

        final = lax.fori_loop(0, PINV_ITERS, newton, tuple(zip(inverses_t, products)))
        for h in range(heads):
            inverse_ref[h] = final[h][0]

        def one_slot(s, _):
            start, end = slot_bounds(len_ref, s, slots)
            lo, hi = start // TILE, (end + TILE - 1) // TILE
            hi = jnp.where(end > start, hi, lo)
            own = mark_ref[pl.ds(pl.multiple_of(s * marks, marks), marks), :] * scale
            q_block = spread(own[:, :width], head_blocks).astype(low)
            k_block = spread(own[:, width:], head_blocks).astype(low)

            def score_tile(n, top):
                t = pl.multiple_of(n * TILE, TILE)
                mask = lane_mask(start, end, t, TILE)
                sim = mul(k_block, qkv_ref[:width, pl.ds(t, TILE)])
                sim = sim.reshape(heads, marks, TILE)
                sim = jnp.exp(sim - jnp.max(sim, axis=1, keepdims=True))
                sim = sim / jnp.sum(sim, axis=1, keepdims=True)
                sim = sim.reshape(width, TILE)
                old = first_ref[:, pl.ds(t, TILE)].astype(f32)
                first_ref[:, pl.ds(t, TILE)] = jnp.where(mask, sim, old).astype(low)
                sim = mul(q_block, qkv_ref[width : 2 * width, pl.ds(t, TILE)])
                sim = jnp.where(mask, sim, mask_fill)
                scores[:, pl.ds(t, TILE)] = sim
                for c in range(TILE // SUB):
                    top = jnp.maximum(top, sim[:, c * SUB : (c + 1) * SUB])
                return top

            top = lax.fori_loop(lo, hi, score_tile, jnp.full((width, SUB), mask_fill, f32))
            top = jnp.max(top, axis=1, keepdims=True)

            def value_tile(n, carry):
                denom, total = carry
                t = pl.multiple_of(n * TILE, TILE)
                mask = lane_mask(start, end, t, TILE)
                part = jnp.exp(scores[:, pl.ds(t, TILE)] - top)
                old = last_ref[:, pl.ds(t, TILE)].astype(f32)
                last_ref[:, pl.ds(t, TILE)] = jnp.where(mask, part, old).astype(low)
                total = total + mul_t(part.astype(low), qkv_ref[2 * width :, pl.ds(t, TILE)])
                for c in range(TILE // SUB):
                    denom = denom + part[:, c * SUB : (c + 1) * SUB]
                return denom, total

            denom, total = lax.fori_loop(
                lo, hi, value_tile,
                (jnp.zeros((width, SUB), f32), jnp.zeros((width, width), f32)),
            )
            denom = jnp.sum(denom, axis=1, keepdims=True)
            inv = 1.0 / jnp.where(denom > 0.0, denom, 1.0)
            denom_ref[s] = inv
            values = fold(total * inv, head_blocks)
            values = jnp.where(end > start, values, vsum[:1] / tok_count)
            value_ref[pl.ds(pl.multiple_of(s * marks, marks), marks), :] = values
            return 0

        lax.fori_loop(0, slots, one_slot, 0)

        lane_head = lax.broadcasted_iota(jnp.int32, (1, width), 1) // HEAD_DIM
        inner = jnp.zeros((packed, width), f32)
        for h in range(heads):
            inverse = pack_mul_t(eye, final[h][0], slot_blocks)
            own_values = jnp.where(lane_head == h, value_ref[...], 0.0)
            inner = inner + wide(mul, spread(inverse, slot_blocks), own_values)
        inner_ref[...] = inner

        bands = [band(conv_own[h : h + 1, :], taps).astype(low) for h in range(heads)]

        def out_slot(s, _):
            start, end = slot_bounds(len_ref, s, slots)
            lo, hi = start // TILE, (end + TILE - 1) // TILE
            hi = jnp.where(end > start, hi, lo)
            own = inner_ref[pl.ds(pl.multiple_of(s * marks, marks), marks), :]
            a_block = jnp.transpose(spread(own, head_blocks)).astype(low)

            def out_tile(n, _):
                t = pl.multiple_of(n * TILE, TILE)
                mask = lane_mask(start, end, t, TILE)
                rows = mul(a_block, first_ref[:, pl.ds(t, TILE)])
                rows = rows + convolve(vpad, bands, start, end, t, heads)
                old = mixed_ref[:, pl.ds(t, TILE)].astype(f32)
                mixed_ref[:, pl.ds(t, TILE)] = jnp.where(mask, rows, old).astype(low)
                return 0

            return lax.fori_loop(lo, hi, out_tile, 0)

        lax.fori_loop(0, slots, out_slot, 0)


def own_taps(own_ref, all_ref, z):
    heads = own_ref.shape[0]
    for n in range(all_ref.shape[0] // heads):

        @pl.when(z == n)
        def _():
            own_ref[...] = all_ref[n * heads : (n + 1) * heads, :]


def windows(padded, start, end, t):
    full = padded[:, pl.ds(t, TILE + 2 * SUB)]
    keep = lane_mask(start, end, t - SUB, TILE + 2 * SUB)
    return jnp.where(keep, full.astype(f32), 0.0).astype(low)


def convolve(padded, bands, start, end, t, heads):
    full = windows(padded, start, end, t)
    out = []
    count = TILE // SUB
    for h in range(heads):
        own = full[h * HEAD_DIM : (h + 1) * HEAD_DIM]
        stack = jnp.concatenate(
            [own[:, c * SUB : (c + 3) * SUB] for c in range(count)], axis=0
        )
        res = mul_t(stack, bands[h])
        out.append(
            jnp.concatenate(
                [res[c * HEAD_DIM : (c + 1) * HEAD_DIM] for c in range(count)], axis=1
            )
        )
    return jnp.concatenate(out, axis=0)


def mix_backward_kernel(
    slots, marks, taps,
    len_ref, grad_ref, qkv_ref, first_ref, last_ref, mark_ref, value_ref, inner_ref,
    denom_ref, middle_ref, steps_ref, inverse_ref, conv_ref,
    out_ref, bias_ref, conv_out_ref,
    gpad, vpad, ds_first, ds_last, conv_grad, d_inner, d_k, d_q, d_value, conv_own,
):
    width = first_ref.shape[0]
    heads = width // HEAD_DIM
    tok_count = qkv_ref.shape[1]
    packed = slots * marks
    scale = HEAD_DIM ** -0.5
    head_blocks = block_grid(width, width)
    slot_blocks = block_grid(packed, packed)
    eye = eye_pack(packed)
    count = TILE // SUB

    for padded, source in ((gpad, grad_ref[...]), (vpad, qkv_ref[2 * width :, :])):
        padded[:, :SUB] = jnp.zeros((width, SUB), low)
        padded[:, tok_count + SUB :] = jnp.zeros((width, SUB), low)
        padded[:, SUB : tok_count + SUB] = source
    out_ref[...] = jnp.zeros_like(out_ref)
    ds_first[...] = jnp.zeros_like(ds_first)
    ds_last[...] = jnp.zeros_like(ds_last)
    conv_grad[...] = jnp.zeros_like(conv_grad)

    own_taps(conv_own, conv_ref, lax.axis_index("heads"))

    def reach(s):
        start, end = slot_bounds(len_ref, s, slots)
        lo, hi = start // TILE, (end + TILE - 1) // TILE
        return start, end, lo, jnp.where(end > start, hi, lo)

    def own_rows(s):
        return pl.ds(pl.multiple_of(s * marks, marks), marks)

    def first_slot(s, _):
        start, end, lo, hi = reach(s)
        a_block = spread(inner_ref[own_rows(s), :], head_blocks).astype(low)

        def tile(n, carry):
            inner_total, key_total = carry
            t = pl.multiple_of(n * TILE, TILE)
            mask = lane_mask(start, end, t, TILE)
            own_grad = grad_ref[:, pl.ds(t, TILE)]
            kernel_rows = jnp.where(mask, first_ref[:, pl.ds(t, TILE)].astype(f32), 0.0)
            d_kernel = mul(a_block, own_grad)
            prod = (kernel_rows * d_kernel).reshape(heads, marks, TILE)
            row_sum = jnp.sum(prod, axis=1, keepdims=True)
            d_sim = prod - kernel_rows.reshape(heads, marks, TILE) * row_sum
            d_sim = d_sim.reshape(width, TILE)
            d_sim_low = d_sim.astype(low)
            old = ds_first[:, pl.ds(t, TILE)].astype(f32)
            ds_first[:, pl.ds(t, TILE)] = jnp.where(mask, d_sim, old).astype(low)
            inner_total = inner_total + mul_t(kernel_rows.astype(low), own_grad)
            key_total = key_total + mul_t(d_sim_low, qkv_ref[:width, pl.ds(t, TILE)])
            full = windows(vpad, start, end, t)
            grad_own = jnp.where(mask, own_grad.astype(f32), 0.0).astype(low)
            for h in range(heads):
                sel = slice(h * HEAD_DIM, (h + 1) * HEAD_DIM)
                left = jnp.concatenate(
                    [grad_own[sel, c * SUB : (c + 1) * SUB] for c in range(count)], axis=0
                )
                right = jnp.concatenate(
                    [full[sel, c * SUB : (c + 3) * SUB] for c in range(count)], axis=0
                )
                conv_grad[h] += lax.dot_general(
                    left, right, (((0,), (0,)), ((), ())), preferred_element_type=f32
                )
            return inner_total, key_total

        zero = jnp.zeros((width, width), f32)
        inner_total, key_total = lax.fori_loop(lo, hi, tile, (zero, zero))
        d_inner[own_rows(s), :] = fold(inner_total, head_blocks)
        d_k[own_rows(s), :] = fold(key_total, head_blocks) * scale
        return 0

    lax.fori_loop(0, slots, first_slot, 0)

    row = lax.broadcasted_iota(jnp.int32, (SUB, 3 * SUB), 0)
    col = lax.broadcasted_iota(jnp.int32, (SUB, 3 * SUB), 1)
    off = col - row - (SUB - taps // 2)
    tap_lane = lax.broadcasted_iota(jnp.int32, (1, SUB), 1)
    for h in range(heads):
        found = jnp.zeros((1, SUB), f32)
        square = conv_grad[h]
        for n in range(taps):
            part = jnp.sum(jnp.where(off == n, square, 0.0), axis=0, keepdims=True)
            part = jnp.sum(part, axis=1, keepdims=True)
            found = jnp.where(tap_lane == n, part, found)
        conv_out_ref[h : h + 1, :] = found

    lane_head = lax.broadcasted_iota(jnp.int32, (1, width), 1) // HEAD_DIM
    value_total = jnp.zeros((packed, width), f32)
    d_inverses = []
    for h in range(heads):
        own = jnp.where(lane_head == h, d_inner[...], 0.0)
        value_total = value_total + wide(mul, spread(inverse_ref[h], slot_blocks), own)
        d_inverses.append(fold(wide(mul_t, own, value_ref[...]), slot_blocks))
    d_value[...] = value_total

    middles_t = [pack_mul_t(eye, middle_ref[h], slot_blocks) for h in range(heads)]

    def newton(k, carry):
        n = PINV_ITERS - 1 - k
        out = []
        for h in range(heads):
            d_inverse, d_middle = carry[h]
            product = steps_ref[n, 0, h]
            second = steps_ref[n, 1, h]
            third = steps_ref[n, 2, h]
            inverse_t = steps_ref[n, 3, h]
            middle_t = middles_t[h]
            d_third = 0.25 * pack_mul(inverse_t, d_inverse, slot_blocks)
            d_second = -pack_mul(product, d_third, slot_blocks)
            d_first = -pack_mul(product, d_second, slot_blocks)
            d_product = (
                -pack_mul(d_third, second, slot_blocks)
                - pack_mul(d_second, 7.0 * eye - product, slot_blocks)
                - d_first
            )
            d_middle = d_middle + pack_mul(d_product, inverse_t, slot_blocks)
            d_inverse = 0.25 * pack_mul(d_inverse, third, slot_blocks) + pack_mul(
                middle_t, d_product, slot_blocks
            )
            out.append((d_inverse, d_middle))
        return tuple(out)

    zero = jnp.zeros((HEAD_DIM, packed), f32)
    final = lax.fori_loop(0, PINV_ITERS, newton, tuple((x, zero) for x in d_inverses))
    lane_slot = lax.broadcasted_iota(jnp.int32, (1, packed), 1) // marks
    dq_total = jnp.zeros((packed, width), f32)
    dk_total = jnp.zeros((packed, width), f32)
    for h in range(heads):
        d_inverse, d_middle = final[h]
        middle = middle_ref[h]
        first_t = steps_ref[0, 3, h]
        d_inverse_t = pack_mul_t(eye, d_inverse, slot_blocks)
        col_sums = jnp.sum(middle, axis=0, keepdims=True)
        share = jnp.sum(d_inverse_t * first_t, axis=0, keepdims=True)
        bound = jnp.zeros((1, packed), f32)
        d_bound = jnp.zeros((1, packed), f32)
        hits = jnp.zeros((1, packed), f32)
        for s in range(slots):
            mine = lane_slot == s
            top = jnp.max(jnp.where(mine, col_sums, 0.0), axis=1, keepdims=True)
            total = jnp.sum(jnp.where(mine, share, 0.0), axis=1, keepdims=True)
            number = jnp.sum(
                jnp.where(mine & (col_sums == top), 1.0, 0.0), axis=1, keepdims=True
            )
            bound = jnp.where(mine, top, bound)
            d_bound = jnp.where(mine, -total / top, d_bound)
            hits = jnp.where(mine, number, hits)
        d_middle = d_middle + d_inverse_t / bound
        d_middle = d_middle + jnp.where(col_sums == bound, d_bound / hits, 0.0)
        prod = spread(middle * d_middle, slot_blocks)
        d_sim = prod - spread(middle, slot_blocks) * jnp.sum(prod, axis=1, keepdims=True)
        d_sim = d_sim * scale
        own = lane_head == h
        q_marks = jnp.where(own, mark_ref[:, :width], 0.0)
        k_marks = jnp.where(own, mark_ref[:, width:], 0.0)
        dq_total = dq_total + wide(mul, d_sim, k_marks)
        dk_total = dk_total + wide(mul, jnp.transpose(d_sim), q_marks)
    d_q[...] = dq_total
    d_k[...] += dk_total

    flipped = []
    for h in range(heads):
        flipped.append(
            band(
                jnp.concatenate(
                    [conv_own[h : h + 1, n : n + 1] for n in reversed(range(taps))], axis=1
                ),
                taps,
            ).astype(low)
        )

    def last_slot(s, _):
        start, end, lo, hi = reach(s)
        inv = denom_ref[s]
        own_d = d_value[own_rows(s), :]
        own_v = value_ref[own_rows(s), :]
        d_block = spread(own_d, head_blocks)
        row_sum = jnp.sum(
            d_block * jnp.concatenate([own_v] * heads, axis=0), axis=1, keepdims=True
        )
        row_sum = row_sum * inv
        d_block = d_block * inv
        d_block_t = jnp.transpose(d_block).astype(low)
        d_block = d_block.astype(low)

        def tile(n, query_total):
            t = pl.multiple_of(n * TILE, TILE)
            mask = lane_mask(start, end, t, TILE)
            kernel_rows = jnp.where(mask, last_ref[:, pl.ds(t, TILE)].astype(f32), 0.0)
            v_rows = qkv_ref[2 * width :, pl.ds(t, TILE)]
            d_sim = kernel_rows * (mul(d_block, v_rows) - row_sum)
            d_low = d_sim.astype(low)
            old = ds_last[:, pl.ds(t, TILE)].astype(f32)
            ds_last[:, pl.ds(t, TILE)] = jnp.where(mask, d_sim, old).astype(low)
            dv = mul(d_block_t, kernel_rows.astype(low))
            dv = dv + convolve(gpad, flipped, start, end, t, heads)
            old = out_ref[2 * width :, pl.ds(t, TILE)].astype(f32)
            out_ref[2 * width :, pl.ds(t, TILE)] = jnp.where(mask, dv, old).astype(low)
            return query_total + mul_t(d_low, qkv_ref[width : 2 * width, pl.ds(t, TILE)])

        query_total = lax.fori_loop(lo, hi, tile, jnp.zeros((width, width), f32))
        d_q[own_rows(s), :] += fold(query_total, head_blocks) * scale
        return 0

    lax.fori_loop(0, slots, last_slot, 0)

    inv_count = slot_marks(len_ref, 0, slots, marks, SUB)[1]
    d_q[...] = d_q[...] * inv_count
    d_k[...] = d_k[...] * inv_count

    def final_slot(s, _):
        start, end, lo, hi = reach(s)
        length = end - start
        own = mark_ref[own_rows(s), :] * scale

        def left(block, d_mark):
            wide_rows = jnp.concatenate([spread(block, head_blocks), d_mark], axis=0)
            return jnp.transpose(wide_rows).astype(low)

        q_left = left(own[:, width:], d_q[own_rows(s), :])
        k_left = left(own[:, :width], d_k[own_rows(s), :])
        mark = lax.broadcasted_iota(jnp.int32, (marks, 1), 0)
        lower = start + (mark * length) // marks
        upper = start + ((mark + 1) * length) // marks

        def tile(n, _):
            t = pl.multiple_of(n * TILE, TILE)
            mask = lane_mask(start, end, t, TILE)
            tok = t + lax.broadcasted_iota(jnp.int32, (marks, TILE), 1)
            member = jnp.where((tok >= lower) & (tok < upper), 1.0, 0.0).astype(low)
            for at, lhs, source in ((0, q_left, ds_first), (width, k_left, ds_last)):
                rhs = jnp.concatenate([source[:, pl.ds(t, TILE)], member], axis=0)
                rows = mul(lhs, rhs)
                old = out_ref[at : at + width, pl.ds(t, TILE)].astype(f32)
                out_ref[at : at + width, pl.ds(t, TILE)] = jnp.where(mask, rows, old).astype(low)
            return 0

        return lax.fori_loop(lo, hi, tile, 0)

    lax.fori_loop(0, slots, final_slot, 0)

    def bias_tile(n, carry):
        t = pl.multiple_of(n * TILE, TILE)
        q_sum, v_sum = carry
        q_rows = out_ref[:width, pl.ds(t, TILE)].astype(f32)
        v_rows = out_ref[2 * width :, pl.ds(t, TILE)].astype(f32)
        for c in range(count):
            q_sum = q_sum + q_rows[:, c * SUB : (c + 1) * SUB]
            v_sum = v_sum + v_rows[:, c * SUB : (c + 1) * SUB]
        return q_sum, v_sum

    zero = jnp.zeros((width, SUB), f32)
    q_sum, v_sum = lax.fori_loop(0, tok_count // TILE, bias_tile, (zero, zero))
    bias_ref[...] = jnp.zeros_like(bias_ref)
    bias_ref[0:1, :] = jnp.sum(jnp.transpose(q_sum), axis=0, keepdims=True)
    bias_ref[1:2, :] = jnp.sum(jnp.transpose(v_sum), axis=0, keepdims=True)


def mix_forward(seq_lengths, tokens, weight_t, bias, conv, slots, marks):
    tok_count, model = tokens.shape
    width = weight_t.shape[0] // 3
    heads = width // HEAD_DIM
    packed = slots * marks
    taps = conv.shape[1]
    whole = lambda *shape: pl.BlockSpec(shape, lambda i, lens: (0,) * len(shape))
    shapes = [
        ((3 * width, tok_count), low),
        ((width, tok_count), low),
        ((width, tok_count), low),
        ((width, tok_count), low),
        ((packed, 2 * width), f32),
        ((packed, width), f32),
        ((packed, width), f32),
        ((slots, width, 1), f32),
        ((heads, HEAD_DIM, packed), f32),
        ((PINV_ITERS, 4, heads, HEAD_DIM, packed), f32),
        ((heads, HEAD_DIM, packed), f32),
        ((8, 128), f32),
    ]
    return pl.pallas_call(
        partial(mix_forward_kernel, slots, marks, taps),
        out_shape=[jax.ShapeDtypeStruct(s, t) for s, t in shapes],
        grid_spec=pltpu.PrefetchScalarGridSpec(
            num_scalar_prefetch=1,
            grid=(tok_count // TILE,),
            in_specs=[
                pl.BlockSpec((TILE, model), lambda i, lens: (i, 0)),
                whole(3 * width, model),
                whole(*bias.shape),
                whole(*conv.shape),
            ],
            out_specs=[whole(*s) for s, _ in shapes],
            scratch_shapes=[
                pltpu.VMEM((width, tok_count + 2 * SUB), low),
                pltpu.VMEM((width, tok_count), f32),
                pltpu.VMEM((8, width), f32),
                pltpu.VMEM((bias.shape[1], 2 * bias.shape[0]), f32),
                pltpu.VMEM((heads, taps), f32),
            ],
        ),
        compiler_params=pltpu.CompilerParams(vmem_limit_bytes=56 * 1024 * 1024),
        cost_estimate=pl.CostEstimate(
            flops=20 * 10**9, bytes_accessed=30 * 10**6, transcendentals=10**6
        ),
        name="mix_forward",
    )(seq_lengths, tokens, weight_t, bias, conv)


def mix_backward(seq_lengths, grad_t, saved, conv, slots, marks):
    qkv_t, first, last, mark, value, inner, denom, middle, steps, inverse = saved
    width, tok_count = grad_t.shape
    heads = width // HEAD_DIM
    packed = slots * marks
    taps = conv.shape[1]
    args = (grad_t, qkv_t, first, last, mark, value, inner, denom, middle, steps, inverse, conv)
    whole = lambda shape: pl.BlockSpec(
        shape, lambda i, lens: (0,) * len(shape), pipeline_mode=pl.Buffered(1)
    )
    shapes = [((3 * width, tok_count), low), ((8, width), f32), ((heads, SUB), f32)]
    square = pltpu.VMEM((packed, width), f32)
    return pl.pallas_call(
        partial(mix_backward_kernel, slots, marks, taps),
        out_shape=[jax.ShapeDtypeStruct(s, t) for s, t in shapes],
        grid_spec=pltpu.PrefetchScalarGridSpec(
            num_scalar_prefetch=1,
            grid=(1,),
            in_specs=[whole(x.shape) for x in args],
            out_specs=[whole(s) for s, _ in shapes],
            scratch_shapes=[
                pltpu.VMEM((width, tok_count + 2 * SUB), low),
                pltpu.VMEM((width, tok_count + 2 * SUB), low),
                pltpu.VMEM((width, tok_count), low),
                pltpu.VMEM((width, tok_count), low),
                pltpu.VMEM((heads, SUB, 3 * SUB), f32),
                square, square, square, square,
                pltpu.VMEM((heads, taps), f32),
            ],
        ),
        compiler_params=pltpu.CompilerParams(vmem_limit_bytes=56 * 1024 * 1024),
        cost_estimate=pl.CostEstimate(
            flops=20 * 10**9, bytes_accessed=30 * 10**6, transcendentals=10**6
        ),
        name="mix_backward",
    )(seq_lengths, *args)


contract_rows = (((0,), (0,)), ((), ()))
contract_cols = (((1,), (1,)), ((), ()))
norm_eps = 1e-05


def split_up(x, dim, peers):
    before, after = (x.shape[:dim], x.shape[dim + 1 :])
    return jnp.moveaxis(x.reshape(*before, peers, -1, *after), dim, 0)


def sum_at_owner(x, axis, dim):
    peers = lax.axis_size(axis)
    tiles = lax.all_to_all(split_up(x, dim, peers), axis, 0, 0, tiled=True)
    return jnp.sum(tiles.astype(f32), axis=0)


def layer_norm(row_data, gain_vec, shift_vec):
    centre = row_data - jnp.mean(row_data, axis=1, keepdims=True)
    spread_row = jnp.mean(centre * centre, axis=1, keepdims=True)
    return centre * lax.rsqrt(spread_row + norm_eps) * gain_vec[None, :] + shift_vec[None, :]


def gelu_exact(values):
    return jax.nn.gelu(values, approximate=False)


def body(
    tokens,
    qkv_weight,
    qv_bias,
    conv_weight,
    out_weight,
    out_bias,
    norm1_gain,
    norm1_bias,
    ffn_in_weight,
    ffn_in_bias,
    ffn_out_weight,
    ffn_out_bias,
    norm2_gain,
    norm2_bias,
    cotangent,
    seq_lengths,
    segment_ids,
    landmark_bounds,
):
    tok_count, model_width = tokens.shape
    head_width = qkv_weight.shape[2]
    heads_here = head_width // HEAD_DIM
    head_total = conv_weight.shape[0]
    kernel_taps = conv_weight.shape[1]
    slots, marks = landmark_bounds.shape
    quarter = tok_count // lax.axis_size("heads")
    head_index = lax.axis_index("heads")
    own_start = head_index * quarter
    both = ("batch", "heads")
    own_rows_low = lax.dynamic_slice_in_dim(tokens, own_start, quarter, 0)
    own_tokens = own_rows_low.astype(f32)
    flat_qkv = qkv_weight.reshape(model_width, 3 * head_width)
    forward = mix_forward(
        seq_lengths, tokens, jnp.transpose(flat_qkv), qv_bias, conv_weight, slots, marks
    )
    qkv_t, first, last, mixed_t, mark, value, inner, denom, middle, steps, inverse, bound = forward
    bound_total = bound[0, 0]
    attn_part = lax.psum_scatter(
        lax.dot_general(mixed_t, out_weight, contract_rows, preferred_element_type=f32).astype(low),
        "heads",
        scatter_dimension=0,
        tiled=True,
    ).astype(f32)
    live_count = jnp.sum((seq_lengths > 0).astype(f32)) * heads_here
    first_res = own_tokens + attn_part + out_bias[None, :]
    norm1_out, norm1_pull = jax.vjp(layer_norm, first_res, norm1_gain, norm1_bias)
    norm1_low = norm1_out.astype(low)
    ff_own = ffn_out_weight.shape[0]
    bias_row = jnp.zeros((16, model_width), low).at[0, :ff_own].set(ffn_in_bias)
    whole_in = lax.all_gather(ffn_in_weight, both, axis=1, tiled=True)
    out_pack = lax.all_gather(jnp.concatenate([ffn_out_weight, bias_row], axis=0), both, axis=0)
    whole_out = out_pack[:, :ff_own].reshape(-1, model_width)
    whole_in_bias = out_pack[:, ff_own, :ff_own].reshape(-1)
    pre_act = (
        jnp.dot(norm1_low, whole_in, preferred_element_type=f32)
        + whole_in_bias.astype(f32)[None, :]
    )
    hidden_act, gelu_pull = jax.vjp(gelu_exact, pre_act)
    hidden_low = hidden_act.astype(low)
    ffn_result = jnp.dot(hidden_low, whole_out, preferred_element_type=f32) + ffn_out_bias[None, :]
    final_out, norm2_pull = jax.vjp(layer_norm, norm1_out + ffn_result, norm2_gain, norm2_bias)
    grad_second, grad_gain_two, grad_shift_two = norm2_pull(cotangent.astype(f32))
    grad_ffn_low = grad_second.astype(low)
    grad_ffn_bias = jnp.sum(grad_ffn_low.astype(f32), axis=0)
    down_term = lax.dot_general(
        hidden_low, grad_ffn_low, contract_rows, preferred_element_type=f32
    ).astype(low)
    grad_hidden = lax.dot_general(
        grad_ffn_low, whole_out, contract_cols, preferred_element_type=f32
    )
    grad_pre = gelu_pull(grad_hidden)[0].astype(low)
    grad_in_bias = jnp.sum(grad_pre.astype(f32), axis=0)
    up_term = lax.dot_general(
        norm1_low, grad_pre, contract_rows, preferred_element_type=f32
    ).astype(low)
    grad_norm1 = grad_second + lax.dot_general(
        grad_pre, whole_in, contract_cols, preferred_element_type=f32
    )
    grad_first, grad_gain_one, grad_shift_one = norm1_pull(grad_norm1)
    grad_attn_low = grad_first.astype(low)
    grad_out_bias = jnp.sum(grad_attn_low.astype(f32), axis=0)
    piece_rows = lax.all_gather(grad_attn_low, "heads", axis=0, tiled=True)
    grad_mix_t = lax.dot_general(
        out_weight, piece_rows, contract_cols, preferred_element_type=f32
    ).astype(low)
    grad_mix_t, down_term, up_term = lax.optimization_barrier((grad_mix_t, down_term, up_term))
    up_share = lax.psum_scatter(up_term, both, scatter_dimension=1, tiled=True).astype(f32)
    down_share = lax.psum_scatter(down_term, both, scatter_dimension=0, tiled=True).astype(f32)
    saved = (qkv_t, first, last, mark, value, inner, denom, middle, steps, inverse)
    grad_t, grad_bias, grad_conv = mix_backward(
        seq_lengths, grad_mix_t, saved, conv_weight, slots, marks
    )
    out_part = lax.dot_general(
        mixed_t, piece_rows, (((1,), (0,)), ((), ())), preferred_element_type=f32
    )
    grad_qv_own = grad_bias[:2]
    qkv_part = lax.dot_general(
        tokens, grad_t, (((0,), (1,)), ((), ())), preferred_element_type=f32
    ).reshape(model_width, 3, head_width)
    input_part = lax.psum_scatter(
        lax.dot_general(
            grad_t, flat_qkv, (((0,), (1,)), ((), ())), preferred_element_type=f32
        ).astype(low),
        "heads",
        scatter_dimension=0,
        tiled=True,
    ).astype(f32)
    input_grad = grad_first + input_part
    conv_full = lax.dynamic_update_slice_in_dim(
        jnp.zeros((head_total, kernel_taps), f32),
        grad_conv[:, :kernel_taps],
        head_index * heads_here,
        0,
    )
    bias_full = lax.dynamic_update_slice_in_dim(
        jnp.zeros((2, head_total * HEAD_DIM), f32), grad_qv_own, head_index * head_width, 1
    )
    qkv_share, out_share = (
        sum_at_owner(qkv_part.astype(low), "batch", 0),
        sum_at_owner(out_part.astype(low), "batch", 1),
    )
    vector_all = jnp.stack(
        [grad_ffn_bias, grad_gain_two, grad_shift_two, grad_gain_one, grad_shift_one, grad_out_bias]
    )
    in_bias_share, vector_share = (
        lax.psum_scatter(grad_in_bias, both, scatter_dimension=0, tiled=True),
        lax.psum_scatter(vector_all, both, scatter_dimension=1, tiled=True),
    )
    conv_sum, bias_sum, bound_all, count_all = lax.psum(
        (conv_full, bias_full, bound_total, live_count), both
    )
    conv_out = lax.dynamic_slice_in_dim(conv_sum, head_index * heads_here, heads_here, 0)
    bias_out = lax.dynamic_slice_in_dim(bias_sum, head_index * head_width, head_width, 1)
    condition = bound_all / count_all
    return (
        final_out.astype(low),
        input_grad,
        qkv_share,
        bias_out,
        conv_out,
        out_share,
        up_share,
        in_bias_share,
        down_share,
        vector_share,
        condition,
    )


def place():
    b, z = lax.axis_index("batch"), lax.axis_index("heads")
    core, x, y = b % 2, (b // 2) % 2, b // 4
    return b, z, b + 1 - 2 * core, b + 2 - 4 * x, b + 4 - 8 * y


def remote(src, dst, send, recv, device):
    return pltpu.make_async_remote_copy(
        src_ref=src,
        dst_ref=dst,
        send_sem=send,
        recv_sem=recv,
        device_id=device,
        device_id_type=pl.DeviceIdType.MESH,
    )


def greet(devices):
    barrier = pltpu.get_barrier_semaphore()
    for device in devices:
        pl.semaphore_signal(
            barrier, inc=1, device_id=device, device_id_type=pl.DeviceIdType.MESH
        )
    pl.semaphore_wait(barrier, len(devices))


def tail_kernel(
    len_ref,
    gt_hbm, wq_hbm, we_hbm, hid_hbm, pre_hbm, n1_hbm, gf_hbm, ga_hbm, mx_hbm, tok_hbm, first_hbm,
    sums_ref, bin_ref, qv_ref, conv_ref, bound_ref,
    input_ref, down_own, up_own, outw_own, qkvw_own, in_bias, vector_own, qv_own, conv_own, ratio,
    small_out,
    gt, wq, we, hid, pre, n1, gf, ga, mx, tok,
    q_in, r_out, r_in, s_in, out_down, out_up, full_outw, full_qkvw, acc_qkvw,
    core_down, core_up, core_outw, core_qkvw,
    one_down, one_up, one_outw, one_qkvw, two_down, two_up, two_outw, two_qkvw,
    e_down, e_up, e_outw, g_down, g_up, g_outw, h_down, h_up, h_outw, small_in,
    load_sem, q_send, q_recv, r_send, r_recv, t_send, t_recv, c_send, c_recv, x_send, x_recv, e_send, e_recv,
    g_send, g_recv, h_send, h_recv, s_send, s_recv,
):
    b, z, bc, bx, by = place()
    both = bx + by - b
    flip = bc - b
    peers = [(b, lax.rem(z + i, 4)) for i in (1, 2, 3)]
    issued = []
    loads = [
        pltpu.make_async_copy(src, dst, load_sem.at[n])
        for n, (src, dst) in enumerate(
            (
                (pre_hbm, pre), (n1_hbm, n1), (hid_hbm, hid), (gf_hbm, gf), (gt_hbm, gt),
                (wq_hbm, wq), (we_hbm, we), (mx_hbm, mx), (ga_hbm, ga), (tok_hbm, tok),
                (first_hbm, input_ref),
            )
        )
    ]
    for copy in loads:
        copy.start()
    greet(peers + [(bc, z), (bx, z), (by, z)])
    chunks, size = r_in.shape[1:3]
    quarter = chunks * size
    ff = down_own.shape[0]
    group = 4 * ff

    zf = z + 1 - 2 * (z % 2)
    zg = z + 2 - 4 * (z // 2)
    partners = ((bc, z), (bx, z), (by, z), (b, zf), (b, zg))

    def small_start(k):
        copy = remote(
            small_out.at[k], small_in.at[k], s_send.at[k], s_recv.at[k], partners[k]
        )
        copy.start()
        issued.append(copy)

    def small_event(k):
        ref = small_in.at[k]
        remote(ref, ref, s_send.at[k], s_recv.at[k], partners[k]).wait_recv()
        small_out[k + 1] = small_out[k] + small_in[k]
        if k < 4:
            small_start(k + 1)

    model = input_ref.shape[1]
    bias_rows = bin_ref.shape[1] // model
    at_vec, at_qv = bias_rows, bias_rows + 6
    heads, taps = conv_own.shape
    at_conv = at_qv + 8
    at_end = at_conv + 4 * heads
    width = qv_own.shape[1]
    small_out[0] = jnp.zeros(small_out.shape[1:], f32)
    for n in range(bias_rows):
        small_out[0, n : n + 1, :] = bin_ref[0:1, n * model : (n + 1) * model]
    small_out[0, at_vec : at_vec + 6, :] = sums_ref[0:6, :]
    live = jnp.int32(0)
    for n in range(len_ref.shape[0]):
        live = live + jnp.where(len_ref[n] > 0, heads, 0)
    lane = lax.broadcasted_iota(jnp.int32, (1, 128), 1)
    small_out[0, at_end : at_end + 1, 0:128] = jnp.where(
        lane == 0, bound_ref[0:1, :], jnp.where(lane == 1, live.astype(f32), 0.0)
    )
    for n in range(4):

        @pl.when(z == n)
        def _():
            for r in range(2):
                row = at_qv + 2 * n + r
                small_out[0, row : row + 1, :width] = qv_ref[r : r + 1, :]
            for r in range(heads):
                row = at_conv + heads * n + r
                small_out[0, row : row + 1, 0:128] = conv_ref[r : r + 1, :]

    small_start(0)

    is_end = (z == 0) | (z == 3)
    low_side = z < 2
    to_inner = jnp.where(low_side, 1, 2)
    across = jnp.where(z == 1, 2, 1)
    to_end = jnp.where(low_side, 0, 3)

    def owner(k):
        return jnp.where(low_side, 3 - k, k)

    def columns(who, c):
        return pl.ds(pl.multiple_of(who * quarter + c * size, size), size)

    def times(x, w):
        return lax.dot_general(x, w, (((0,), (0,)), ((), ())), preferred_element_type=f32)

    def part(who, c):
        return times(gt[:, columns(who, c)], wq[...])

    def q_copy(k, c):
        return remote(
            gt_hbm.at[:, columns(owner(k), c)], q_in.at[k, c], q_send.at[k, c], q_recv.at[k, c],
            (b, to_inner),
        )

    def q_wait(k, c):
        ref = q_in.at[k, c]
        remote(ref, ref, q_send.at[k, c], q_recv.at[k, c], (b, to_end)).wait_recv()

    def r_copy(k, c):
        return remote(
            r_out.at[k, c], r_in.at[k, c], r_send.at[k, c], r_recv.at[k, c], (b, across)
        )

    def t_copy(c):
        return remote(r_in.at[0, c], s_in.at[c], t_send.at[c], t_recv.at[c], (b, to_end))

    def first_hop(k, c):
        @pl.when(jnp.logical_not(is_end))
        def _():
            own = part(owner(k), c)
            q_wait(k, c)
            r_out[k, c] = (own + times(q_in[k, c], we[...])).astype(low)
            r_copy(k, c).start()

    def last_hop(c):
        @pl.when(jnp.logical_not(is_end))
        def _():
            own = part(to_end, c)
            r_copy(0, c).wait_recv()
            r_in[0, c] = (r_in[0, c].astype(f32) + own).astype(low)
            t_copy(c).start()

    cores = (core_down, core_up, core_outw, core_qkvw)
    ones = (one_down, one_up, one_outw, one_qkvw)
    twos = (two_down, two_up, two_outw, two_qkvw)
    outs = (out_down, out_up)
    left = (hid, pre)
    right = (gf, n1)

    def who(slot):
        return b + (slot % 2) * (bx - b) + (slot // 2) * (by - b)

    def term(n, owner):
        at = pl.ds(pl.multiple_of(owner * group, group), group)
        return lax.dot_general(
            left[n][:, at], right[n][...], (((0,), (0,)), ((), ())), preferred_element_type=f32
        )

    def core_copy(n, slot):
        if n < 2:
            src = outs[n].at[slot]
        elif n == 2:
            src = full_outw.at[:, who(slot) + flip]
        else:
            src = full_qkvw.at[who(slot) + flip]
        return remote(src, cores[n].at[slot], c_send.at[n, slot], c_recv.at[n, slot], (bc, z))

    def give(n, slot):
        if n < 2:
            value = term(n, who(slot) + flip).astype(low)
            outs[n][slot] = value.reshape(outs[n].shape[1:])
        core_copy(n, slot).start()

    def keep(n, slot):
        if n < 2:
            own = term(n, who(slot)).reshape(outs[n].shape[1:])
        elif n == 2:
            own = full_outw[:, who(slot)].astype(f32)
        else:
            own = full_qkvw[who(slot)].astype(f32)
        core_copy(n, slot).wait_recv()
        cores[n][slot] = (cores[n][slot].astype(f32) + own).astype(low)

    def side_copy(n, dst, src):
        partner = by if n % 2 == 0 else bx
        return remote(
            cores[n].at[src], ones[n].at[dst], x_send.at[n, dst], x_recv.at[n, dst], (partner, z)
        )

    def small_group(n):
        def one(i, _):
            give(n, 3 - i)
            return 0

        lax.fori_loop(0, 4, one, 0)

    def small_keep(n):
        def one(i, _):
            keep(n, 3 - i)
            return 0

        lax.fori_loop(0, 4, one, 0)
        side_copy(n, 1, 3).start()
        side_copy(n, 0, 2 if n % 2 == 0 else 1).start()

    def half(h, _):
        def one(i, _):
            slot_up, slot_down = 3 - 2 * i - h, 3 - i - 2 * h
            give(1, slot_up)
            give(0, slot_down)
            keep(1, slot_up)

            @pl.when(h == 0)
            def _():
                side_copy(1, 1 - i, slot_up).start()

            keep(0, slot_down)

            @pl.when(h == 0)
            def _():
                side_copy(0, 1 - i, slot_down).start()

            return 0

        lax.fori_loop(0, 2, one, 0)

        @pl.when(h == 0)
        def _():
            for n in (4, 5, 6):
                loads[n].wait()
            first_hop(0, 0)

        return 0

    def one_event(n):
        second = 1 if n % 2 == 0 else 2
        partner, other = (by, bx) if n % 2 == 0 else (bx, by)
        ref = ones[n].at[1]
        remote(ref, ref, x_send.at[n, 1], x_recv.at[n, 1], (partner, z)).wait_recv()
        ones[n][1] = (ones[n][1].astype(f32) + cores[n][second].astype(f32)).astype(low)
        copy = remote(ones[n].at[1], twos[n], x_send.at[n, 2], x_recv.at[n, 2], (other, z))
        copy.start()
        issued.append(copy)

    e_bufs = (e_down, e_up, e_outw)
    g_bufs = (g_down, g_up, g_outw)
    h_bufs = (h_down, h_up, h_outw)

    def e_copy(n, k):
        return remote(
            twos[n].at[owner(k)], e_bufs[n].at[k], e_send.at[n, k], e_recv.at[n, k], (b, to_inner)
        )

    def e_wait(n, k):
        ref = e_bufs[n].at[k]
        remote(ref, ref, e_send.at[n, k], e_recv.at[n, k], (b, to_end)).wait_recv()

    def g_copy(n, k):
        return remote(
            e_bufs[n].at[k], g_bufs[n].at[k], g_send.at[n, k], g_recv.at[n, k], (b, across)
        )

    def h_copy(n):
        return remote(g_bufs[n].at[0], h_bufs[n], h_send.at[n], h_recv.at[n], (b, to_end))

    def two_event(n):
        partner, other = (by, bx) if n % 2 == 0 else (bx, by)
        ref = ones[n].at[0]
        remote(ref, ref, x_send.at[n, 0], x_recv.at[n, 0], (partner, z)).wait_recv()
        ref = twos[n]
        remote(ref, ref, x_send.at[n, 2], x_recv.at[n, 2], (other, z)).wait_recv()
        own = ones[n][0].astype(f32) + cores[n][0].astype(f32)
        if n == 3:
            qkvw_own[...] = twos[n][...].astype(f32) + own
            return
        twos[n][...] = (twos[n][...].astype(f32) + own).astype(low)

    def line_start(n, k):
        @pl.when(is_end)
        def _():
            e_copy(n, k).start()

    def line_across(n, k):
        @pl.when(jnp.logical_not(is_end))
        def _():
            e_wait(n, k)
            e_bufs[n][k] = (
                e_bufs[n][k].astype(f32) + twos[n][owner(k)].astype(f32)
            ).astype(low)
            g_copy(n, k).start()

    def line_back(n):
        @pl.when(jnp.logical_not(is_end))
        def _():
            g_copy(n, 0).wait_recv()
            g_bufs[n][0] = (
                g_bufs[n][0].astype(f32) + twos[n][to_end].astype(f32)
            ).astype(low)
            h_copy(n).start()

    def end_event(n):
        def write(value):
            out = (down_own, up_own, outw_own)[n]
            out[...] = jnp.transpose(value) if n > 0 else value

        @pl.when(is_end)
        def _():
            ref = h_bufs[n]
            remote(ref, ref, h_send.at[n], h_recv.at[n], (b, to_inner)).wait_recv()
            write(twos[n][z].astype(f32) + h_bufs[n][...].astype(f32))
            for k in range(3):
                e_copy(n, k).wait_send()

        @pl.when(jnp.logical_not(is_end))
        def _():
            g_copy(n, 1).wait_recv()
            e_wait(n, 2)
            write(
                twos[n][z].astype(f32)
                + g_bufs[n][1].astype(f32)
                + e_bufs[n][2].astype(f32)
            )
            for k in range(2):
                g_copy(n, k).wait_send()
            h_copy(n).wait_send()

    def projections():
        on, oh = full_outw.shape[2:]
        for s in range(4):
            value = jnp.transpose(mul(mx[s], ga[...]))
            full_outw[s] = value.astype(low).reshape(full_outw.shape[1:])
        acc_qkvw[...] = jnp.zeros_like(acc_qkvw)
        span = quarter

        def one(n, _):
            at = pl.ds(pl.multiple_of(n * span, span), span)
            acc_qkvw[...] += mul(gt[:, at], tok[at, :])
            return 0

        lax.fori_loop(0, 4, one, 0)
        full_qkvw[...] = jnp.transpose(acc_qkvw[...]).astype(low).reshape(full_qkvw.shape)

    @pl.when(is_end)
    def _():
        for k in range(3):
            for c in range(chunks):
                q_copy(k, c).start()

    for n in range(4):
        loads[n].wait()

    lax.fori_loop(0, 2, half, 0)
    first_hop(0, 1)
    one_event(1)
    one_event(0)
    first_hop(0, 2)
    last_hop(0)
    for n in (7, 8, 9):
        loads[n].wait()
    projections()
    first_hop(1, 0)
    last_hop(1)
    small_group(2)
    small_group(3)
    small_event(0)
    first_hop(1, 1)
    last_hop(2)
    small_keep(2)
    small_keep(3)
    small_event(1)
    first_hop(1, 2)
    two_event(1)
    line_start(1, 0)
    two_event(0)
    line_start(0, 0)
    line_start(1, 1)
    line_start(0, 1)
    small_event(2)
    one_event(2)
    one_event(3)
    small_event(3)
    two_event(2)
    for k in range(3):
        line_start(2, k)
    line_start(1, 2)
    line_start(0, 2)
    two_event(3)
    small_event(4)
    loads[10].wait()

    def own_rows(c, _):
        rows = pl.ds(pl.multiple_of(c * size, size), size)
        input_ref[rows, :] += part(z, c)

        @pl.when(is_end)
        def _():
            ref = s_in.at[c]
            remote(ref, ref, t_send.at[c], t_recv.at[c], (b, to_inner)).wait_recv()
            input_ref[rows, :] += s_in[c].astype(f32)

        @pl.when(jnp.logical_not(is_end))
        def _():
            r_copy(1, c).wait_recv()
            q_wait(2, c)
            input_ref[rows, :] += r_in[1, c].astype(f32) + times(q_in[2, c], we[...])

        return 0

    lax.fori_loop(0, chunks, own_rows, 0)
    for n, k in ((1, 0), (0, 0), (1, 1), (0, 1), (2, 0), (2, 1)):
        line_across(n, k)
        if k == 1:
            line_back(n)
    for n in (1, 0, 2):
        end_event(n)

    @pl.when(is_end)
    def _():
        for k in range(3):
            for c in range(chunks):
                q_copy(k, c).wait_send()

    @pl.when(jnp.logical_not(is_end))
    def _():
        for c in range(chunks):
            r_copy(0, c).wait_send()
            r_copy(1, c).wait_send()
            t_copy(c).wait_send()

    final = small_out.at[5]
    in_bias[...] = jnp.zeros_like(in_bias)
    index = b * 4 + z
    per_row = model // ff
    for n in range(bias_rows):

        @pl.when(index // per_row == n)
        def _():
            row = pltpu.roll(final[n : n + 1, :], (model - (index % per_row) * ff) % model, 1)
            in_bias[...] = row[:, :ff]

    share = vector_own.shape[1]
    vectors = final[at_vec : at_vec + 6, :]
    vector_own[...] = pltpu.roll(vectors, (model - index * share) % model, 1)[:, :share]
    for n in range(4):

        @pl.when(z == n)
        def _():
            qv_own[...] = final[at_qv + 2 * n : at_qv + 2 * n + 2, :width]
            conv_own[...] = final[at_conv + heads * n : at_conv + heads * (n + 1), :taps]

    ratio[...] = final[at_end : at_end + 1, 0:1] / final[at_end : at_end + 1, 1:2]

    for n in range(4):
        for dst in range(2):
            side_copy(n, dst, dst).wait_send()
        for slot in range(4):
            core_copy(n, slot).wait_send()
    for copy in issued:
        copy.wait_send()


def tail(
    lengths, gt, wq, we, hid, pre, n1, gf, ga, mx, tok, first, sums, bins, qv_grad, conv_grad, bound,
    taps,
):
    quarter, model = first.shape
    chunks = 3
    size = quarter // chunks
    ff = hid.shape[1] // 32
    width = mx.shape[1]
    heads = width // HEAD_DIM
    on, oh = model // 8, width
    qn, qh = model // 8, gt.shape[0]
    blocks = ((4, ff, model), (4, ff, model), (4, on, oh), (qn, qh))
    own = lambda *s: jax.ShapeDtypeStruct(s, f32)
    vm = lambda *s: pltpu.VMEM(s, low)
    dma = pltpu.SemaphoreType.DMA
    sources = (gt, wq, we, hid, pre, n1, gf, ga, mx, tok)
    small = -(-(bins.shape[1] // model + 15 + 4 * heads) // 8) * 8
    vmem = pl.BlockSpec(memory_space=pltpu.VMEM)
    return pl.pallas_call(
        tail_kernel,
        out_shape=[
            own(quarter, model), own(ff, model), own(model, ff), own(oh, on), own(qn, qh),
            own(1, ff), own(6, model // 32), own(2, width), own(heads, taps), own(1, 1),
        ],
        in_specs=[pl.BlockSpec(memory_space=pltpu.SMEM)]
        + [pl.BlockSpec(memory_space=pl.ANY)] * 11
        + [vmem] * 5,
        out_specs=[vmem] * 10,
        scratch_shapes=[
            pltpu.VMEM((6, small, model), f32),
            *[vm(*x.shape) for x in sources],
            vm(3, chunks, qh, size), vm(2, chunks, size, model), vm(2, chunks, size, model),
            vm(chunks, size, model),
            vm(4, *blocks[0]), vm(4, *blocks[1]),
            vm(4, 8, on, oh), vm(8, qn, qh), pltpu.VMEM((qh, model), f32),
            *[vm(4, *s) for s in blocks],
            *[vm(2, *s) for s in blocks],
            *[vm(*s) for s in blocks],
            *[vm(3, *s[1:]) for s in blocks[:3]],
            *[vm(2, *s[1:]) for s in blocks[:3]],
            *[vm(*s[1:]) for s in blocks[:3]],
            pltpu.VMEM((5, small, model), f32),
            dma((11,)),
            dma((3, chunks)), dma((3, chunks)), dma((2, chunks)), dma((2, chunks)),
            dma((chunks,)), dma((chunks,)), dma((4, 4)), dma((4, 4)),
            dma((4, 3)), dma((4, 3)), dma((3, 3)), dma((3, 3)), dma((3, 2)), dma((3, 2)),
            dma((3,)), dma((3,)), dma((5,)), dma((5,)),
        ],
        compiler_params=pltpu.CompilerParams(
            collective_id=3, has_side_effects=True, vmem_limit_bytes=63 * 1024 * 1024
        ),
        name="tail",
    )(lengths, *sources, first, sums, bins, qv_grad, conv_grad, bound)


def cumulative(x):
    t = 1.0 / (1.0 + 0.23164189 * jnp.abs(x))
    density = jnp.exp(-0.5 * x * x) * 0.3989422804
    poly = t * (
        0.319381530 + t * (-0.356563782 + t * (1.781477937 + t * (-1.821255978 + t * 1.330274429)))
    )
    upper = density * poly
    return jnp.where(x >= 0.0, 1.0 - upper, upper), density


def normed(x):
    centre = x - jnp.mean(x, axis=1, keepdims=True)
    scale = lax.rsqrt(jnp.mean(centre * centre, axis=1, keepdims=True) + norm_eps)
    return centre * scale, scale


def norm_back(grad, gain, rows, scale):
    e = grad * gain
    return scale * (
        e - jnp.mean(e, axis=1, keepdims=True) - rows * jnp.mean(e * rows, axis=1, keepdims=True)
    )


def middle_kernel(
    share,
    mixed_ref, own0, own1, own2, own3, tok_hbm, cot_hbm,
    vec_ref,
    out_hbm, first_hbm, attn_hbm, hidden_hbm, pre_hbm, norm_hbm, ffn_hbm, all_ref, grad_ref,
    sums_ref, bin_ref,
    out_ref, first_ref, attn_ref, hidden_ref, pre_ref, norm_ref, ffn_ref, tok_ref, cot_ref,
    packs, wof, wo, slope, total, n1_ref, scale_ref, turned,
    a_send, a_recv, f_send, f_recv, s_send, s_recv, p_send, p_recv, g_send, g_recv,
    own_sem, own_turn, out_sem,
):
    b, z, bc, bx, by = place()
    both = bx + by - b
    flip = bc - b
    peers = [(b, lax.rem(z + i, 4)) for i in (1, 2, 3)]
    width, quarter = all_ref.shape[1:]
    model = tok_hbm.shape[1]
    owns = (own0, own1, own2, own3)
    origins = [lax.rem(z + 4 - i, 4) for i in range(4)]
    size = turned.shape[2]
    tiles = quarter // size
    issued = []

    def own_columns(n):
        return pl.ds(pl.multiple_of(n * quarter, quarter), quarter)

    local = [
        pltpu.make_async_copy(own, packs.at[b, origin], own_sem.at[i])
        for i, (own, origin) in enumerate(zip(owns, origins))
    ]
    local.append(
        pltpu.make_async_copy(mixed_ref.at[:, own_columns(z)], all_ref.at[z], own_sem.at[4])
    )
    local.append(
        pltpu.make_async_copy(
            tok_hbm.at[pl.ds(pl.multiple_of(z * quarter, quarter), quarter)], tok_ref, own_sem.at[5]
        )
    )
    cot_load = pltpu.make_async_copy(cot_hbm, cot_ref, own_sem.at[6])
    for copy in local:
        copy.start()
    cot_load.start()
    greet(peers + [(bc, z), (bx, z), (by, z)])

    ff = (packs.shape[2] - 32) // 2
    half = ff // 2
    pieces = ((2 * ff, 32), (0, half), (half, half), (ff, ff))
    through_y = (True, True, True, False)
    count = len(pieces)

    def rows_of(n):
        return pl.ds(*pieces[n])

    def mix_copy(r, i):
        to = lax.rem(z + i, 4)
        src = mixed_ref.at[:, pl.ds(pl.multiple_of(to * quarter + r * size, size), size)]
        return remote(
            src, all_ref.at[z, :, pl.ds(r * size, size)], a_send.at[r, i - 1], a_recv.at[r, i - 1],
            (b, to),
        )

    def side(n, axis):
        out = []
        for i in range(4):
            out.append(
                remote(
                    owns[i].at[rows_of(n)], packs.at[b, origins[i], rows_of(n)],
                    f_send.at[n, axis, i], f_recv.at[n, axis, i], (by if axis else bx, z),
                )
            )
        return out

    def side_start(n):
        for axis in (0, 1):
            for copy in side(n, axis):
                copy.start()
                issued.append(copy)

    def block(n, who):
        return packs.at[who, :, rows_of(n)]

    def corner(n):
        who, device = (bx, by) if through_y[n] else (by, bx)
        return remote(block(n, who), block(n, who), s_send.at[n], s_recv.at[n], (device, z))

    def mate(n, slot, who):
        return remote(
            block(n, who), block(n, who), p_send.at[n, slot], p_recv.at[n, slot], (bc, z)
        )

    def mate_start(n, slot, who):
        mate(n, slot, who).start()

    def side_wait(n, axis):
        who = by if axis else bx
        for i in range(4):
            ref = packs.at[who, origins[i], rows_of(n)]
            remote(
                ref, ref, f_send.at[n, axis, i], f_recv.at[n, axis, i], (who, z)
            ).wait_recv()
        if through_y[n] == (axis == 0):
            corner(n).start()
        mate_start(n, 1 + axis, who)

    def corner_wait(n):
        device = by if through_y[n] else bx
        ref = block(n, both)
        remote(ref, ref, s_send.at[n], s_recv.at[n], (device, z)).wait_recv()
        mate_start(n, 3, both)

    def mate_wait(n, slot, who):
        mate(n, slot, who + flip).wait_recv()

    side_start(0)
    side_start(1)
    for r in range(tiles):
        for i in (1, 2, 3):
            copy = mix_copy(r, i)
            copy.start()
            issued.append(copy)
    for copy in local:
        copy.wait()
    for n in range(count):
        mate_start(n, 0, b)
    out_bias, gain1, shift1, down_bias, gain2, shift2 = [
        vec_ref[n : n + 1, :] for n in range(6)
    ]
    sums_ref[...] = jnp.zeros_like(sums_ref)
    bin_ref[...] = jnp.zeros_like(bin_ref)
    total[...] = jnp.zeros_like(total)
    side_wait(0, 0)
    side_wait(0, 1)
    side_start(2)
    side_start(3)
    corner_wait(0)
    for slot, who in enumerate((b, bx, by, both)):
        mate_wait(0, slot, who)
    group = 4 * ff
    for q in range(8):
        for s in range(4):
            wof[pl.ds(s * width + q * share, share), :] = packs[
                q, s, pl.ds(2 * ff, share), :
            ].astype(f32)
    wo[...] = wof[...].astype(low).reshape(wo.shape)
    for q in range(8):
        row = jnp.zeros((1, group), f32)
        for s in range(4):
            row = row + packs[q, s, 2 * ff + share : 2 * ff + share + 1, :group].astype(f32)
        bin_ref[1:2, q * group : (q + 1) * group] = row

    def row_sum(n, x):
        sums_ref[n : n + 1, :] += jnp.sum(x, axis=0, keepdims=True)

    def first_rows(r, _):
        rows = pl.ds(pl.multiple_of(r * size, size), size)

        @pl.when(r == 1)
        def _():
            side_wait(1, 0)
            side_wait(1, 1)

        @pl.when(r == 2)
        def _():
            side_wait(2, 0)
            side_wait(2, 1)

        for i in (1, 2, 3):
            ref = all_ref.at[origins[i], :, rows]
            remote(
                ref, ref, a_send.at[r, i - 1], a_recv.at[r, i - 1], (b, origins[i])
            ).wait_recv()
        attn = jnp.zeros((size, model), f32)
        for s in range(4):
            attn = attn + lax.dot_general(
                all_ref[s, :, rows], wo[s], (((0,), (0,)), ((), ())), preferred_element_type=f32
            )
        n1, scale1 = normed(tok_ref[rows, :].astype(f32) + attn + out_bias)
        n1_ref[rows, :] = n1
        scale_ref[rows, :] = jnp.broadcast_to(scale1, (size, scale_ref.shape[1]))
        norm_ref[rows, :] = (n1 * gain1 + shift1).astype(low)
        return 0

    span = 2 * group

    def weights(c, start):
        return jnp.concatenate(
            [
                packs[2 * c + n, :, pl.ds(start, ff), :].reshape(group, model)
                for n in range(2)
            ],
            axis=0,
        )

    def tile_rows(r):
        return pl.ds(pl.multiple_of(r * size, size), size)

    def feed(who):
        c = who // 2
        lanes = pl.ds(pl.multiple_of(c * span, span), span)

        def one(r, _):
            rows = tile_rows(r)
            act = mul_t(norm_ref[rows, :], weights(c, 0)) + bin_ref[1:2, lanes]
            phi, density = cumulative(act)
            hidden = (act * phi).astype(low)
            hidden_ref[rows, lanes] = hidden
            slope[rows, lanes] = phi + act * density
            total[rows, :] += mul(hidden, weights(c, ff))
            return 0

        lax.fori_loop(0, tiles, one, 0)

    lax.fori_loop(0, tiles, first_rows, 0)

    def group_step(k, _):
        def mates(slot, who):
            for n in range(1, count):
                mate_wait(n, slot, who)

        @pl.when(k == 0)
        def _():
            mates(0, b)

        @pl.when(k == 1)
        def _():
            side_wait(3, 0)
            side_wait(3, 1)
            mates(1, bx)

        @pl.when(k == 2)
        def _():
            corner_wait(1)
            mates(2, by)

        @pl.when(k == 3)
        def _():
            corner_wait(2)
            corner_wait(3)
            mates(3, both)

        feed(b + (k % 2) * (bx - b) + (k // 2) * (by - b))
        return 0

    lax.fori_loop(0, 4, group_step, 0)

    def turn_copy(r, i):
        to = lax.rem(z + i, 4)
        src = turned.at[r, pl.ds(pl.multiple_of(to * width, width), width)]
        dst = grad_ref.at[:, pl.ds(pl.multiple_of(z * quarter + r * size, size), size)]
        return remote(src, dst, g_send.at[r, i - 1], g_recv.at[r, i - 1], (b, to))

    def turn_own(r):
        src = turned.at[r, pl.ds(pl.multiple_of(z * width, width), width)]
        dst = grad_ref.at[:, pl.ds(pl.multiple_of(z * quarter + r * size, size), size)]
        return pltpu.make_async_copy(src, dst, own_turn.at[r])

    stores = (
        (out_ref, out_hbm), (first_ref, first_hbm), (attn_ref, attn_hbm), (pre_ref, pre_hbm),
        (ffn_ref, ffn_hbm), (hidden_ref, hidden_hbm), (norm_ref, norm_hbm),
    )

    def store(r, n):
        src, dst = stores[n]
        rows = tile_rows(r)
        return pltpu.make_async_copy(src.at[rows], dst.at[rows], out_sem.at[r, n])

    cot_load.wait()

    def row_tile(r, _):
        rows = tile_rows(r)
        n1 = n1_ref[rows, :]
        norm1 = n1 * gain1 + shift1
        n2, scale2 = normed(norm1 + total[rows, :] + down_bias)
        out_ref[rows, :] = (n2 * gain2 + shift2).astype(low)
        cot = cot_ref[rows, :].astype(f32)
        row_sum(1, cot * n2)
        row_sum(2, cot)
        grad2 = norm_back(cot, gain2, n2, scale2)
        grad_low = grad2.astype(low)
        ffn_ref[rows, :] = grad_low
        row_sum(0, grad_low.astype(f32))
        total[rows, :] = grad2

        def backward(c, _):
            lanes = pl.ds(pl.multiple_of(c * span, span), span)
            grad = (slope[rows, lanes] * mul_t(grad_low, weights(c, ff))).astype(low)
            pre_ref[rows, lanes] = grad
            bin_ref[0:1, lanes] += jnp.sum(grad.astype(f32), axis=0, keepdims=True)
            total[rows, :] += mul(grad, weights(c, 0))
            return 0

        lax.fori_loop(0, 4, backward, 0)
        grad1 = total[rows, :]
        row_sum(3, grad1 * n1)
        row_sum(4, grad1)
        first = norm_back(grad1, gain1, n1, scale_ref[rows, 0:1])
        first_ref[rows, :] = first
        attn_low = first.astype(low)
        attn_ref[rows, :] = attn_low
        row_sum(5, attn_low.astype(f32))
        for s in range(4):
            turned[r, pl.ds(s * width, width), :] = mul_t(wo[s], attn_low).astype(low)
        for i in (1, 2, 3):
            turn_copy(r, i).start()
        turn_own(r).start()
        for n in range(len(stores)):
            store(r, n).start()
        return 0

    lax.fori_loop(0, tiles, row_tile, 0)

    def finish(r, _):
        for i in (1, 2, 3):
            source = origins[i]
            ref = grad_ref.at[:, pl.ds(pl.multiple_of(source * quarter + r * size, size), size)]
            remote(ref, ref, g_send.at[r, i - 1], g_recv.at[r, i - 1], (b, source)).wait_recv()
            turn_copy(r, i).wait_send()
        turn_own(r).wait()
        for n in range(len(stores)):
            store(r, n).wait()
        return 0

    lax.fori_loop(0, tiles, finish, 0)
    for n in range(count):
        corner(n).wait_send()
        for slot, who in enumerate((b, bx, by, both)):
            mate(n, slot, who).wait_send()
    for copy in issued:
        copy.wait_send()


def ffn_middle(mixed_t, packs, tokens, cot, vectors, ff, share):
    width, tok_count = mixed_t.shape
    quarter, model = tok_count // 4, tokens.shape[1]
    size = quarter // 3
    rows = packs[0].shape[0]
    shape = jax.ShapeDtypeStruct
    vmem = pl.BlockSpec(memory_space=pltpu.VMEM)
    hbm = pl.BlockSpec(memory_space=pl.ANY)
    dma = pltpu.SemaphoreType.DMA
    kept = [
        ((quarter, model), low),
        ((quarter, model), f32),
        ((quarter, model), low),
        ((quarter, 32 * ff), low),
        ((quarter, 32 * ff), low),
        ((quarter, model), low),
        ((quarter, model), low),
    ]
    return pl.pallas_call(
        partial(middle_kernel, share),
        out_shape=[shape(*x) for x in kept]
        + [
            shape((4, width, quarter), low),
            shape((width, tok_count), low),
            shape((8, model), f32),
            shape((8, 32 * ff), f32),
        ],
        in_specs=[hbm] + [vmem] * 4 + [hbm] * 2 + [vmem],
        out_specs=[hbm] * 7 + [vmem, hbm, vmem, vmem],
        scratch_shapes=[pltpu.VMEM(*x) for x in kept]
        + [
            pltpu.VMEM((quarter, model), low),
            pltpu.VMEM((quarter, model), low),
            pltpu.VMEM((8, 4, rows, model), low),
            pltpu.VMEM((4 * width, model), f32),
            pltpu.VMEM((4, width, model), low),
            pltpu.VMEM((quarter, 32 * ff), f32),
            pltpu.VMEM((quarter, model), f32),
            pltpu.VMEM((quarter, model), f32),
            pltpu.VMEM((quarter, 128), f32),
            pltpu.VMEM((3, 4 * width, size), low),
            dma((3, 3)), dma((3, 3)), dma((4, 2, 4)), dma((4, 2, 4)), dma((4,)), dma((4,)),
            dma((4, 4)), dma((4, 4)), dma((3, 3)), dma((3, 3)),
            dma((7,)), dma((3,)), dma((3, 7)),
        ],
        compiler_params=pltpu.CompilerParams(
            collective_id=1, has_side_effects=True, vmem_limit_bytes=63 * 1024 * 1024
        ),
        name="middle",
    )(mixed_t, *packs, tokens, cot, vectors)


def settle_kernel(*refs):
    count = len(refs) // 2
    for n in range(count):
        refs[count + n][...] = refs[n][...]


def settle(*arrays):
    vmem = pl.BlockSpec(memory_space=pltpu.VMEM)
    return pl.pallas_call(
        settle_kernel,
        out_shape=[jax.ShapeDtypeStruct(x.shape, x.dtype) for x in arrays],
        in_specs=[vmem] * len(arrays),
        out_specs=[vmem] * len(arrays),
        name="settle",
    )(*arrays)


def slice_body(
    tokens,
    qkv_weight,
    qv_bias,
    conv_weight,
    out_weight,
    out_bias,
    norm1_gain,
    norm1_bias,
    ffn_in_weight,
    ffn_in_bias,
    ffn_out_weight,
    ffn_out_bias,
    norm2_gain,
    norm2_bias,
    cotangent,
    seq_lengths,
    segment_ids,
    landmark_bounds,
):
    model = tokens.shape[1]
    width = qkv_weight.shape[2]
    kernel_taps = conv_weight.shape[1]
    slots, marks = landmark_bounds.shape
    z = lax.axis_index("heads")
    b = lax.axis_index("batch")
    weight_t = jnp.transpose(qkv_weight.reshape(model, 3 * width))
    ff_own = ffn_out_weight.shape[0]
    share = width // 8
    bias_row = lax.dynamic_update_slice_in_dim(
        jnp.zeros((4 * ff_own,), low), ffn_in_bias, z * ff_own, 0
    )
    misc_own = jnp.concatenate(
        [
            lax.dynamic_slice_in_dim(out_weight, b * share, share, 0),
            jnp.zeros((32 - share, model), low).at[0, : 4 * ff_own].set(bias_row),
        ],
        axis=0,
    )
    pack = jnp.concatenate([jnp.transpose(ffn_in_weight), ffn_out_weight, misc_own], axis=0)
    packs = [pack] + [
        lax.ppermute(pack, "heads", [(n, (n + i) % 4) for n in range(4)]) for i in (1, 2, 3)
    ]
    forward = mix_forward(
        seq_lengths, tokens, weight_t, qv_bias, conv_weight, slots, marks
    )
    qkv_t, first, last, mixed_t, mark, value, inner, denom, middle, steps, inverse, bound = forward
    vectors = jnp.stack(
        [out_bias, norm1_gain, norm1_bias, ffn_out_bias, norm2_gain, norm2_bias]
    )
    (
        final_low, grad_first, grad_attn_low, hidden_low, grad_pre, norm1_low, grad_ffn_low,
        mixed_all, grad_mix_t, vector_sums, bias_sums,
    ) = ffn_middle(mixed_t, packs, tokens, cotangent, vectors, ff_own, share)
    saved = (qkv_t, first, last, mark, value, inner, denom, middle, steps, inverse)
    held, grad_mix_t = lax.optimization_barrier((weight_t, grad_mix_t))
    weight_end = lax.ppermute(held, "heads", [(0, 1), (3, 2)])
    grad_t, grad_bias, grad_conv = mix_backward(
        seq_lengths, grad_mix_t, saved, conv_weight, slots, marks
    )
    (
        input_grad, down_share, up_share, out_share, qkv_share,
        in_bias_share, vector_share, bias_out, conv_out, condition,
    ) = tail(
        seq_lengths, grad_t, weight_t, weight_end, hidden_low, grad_pre, norm1_low, grad_ffn_low,
        grad_attn_low, mixed_all, tokens, grad_first, vector_sums, bias_sums, grad_bias,
        grad_conv, bound, kernel_taps,
    )
    (
        final_low, input_grad, down_share, up_share, out_share, qkv_share,
        in_bias_share, vector_share, bias_out, conv_out, condition,
    ) = settle(
        final_low, input_grad, down_share, up_share, out_share, qkv_share,
        in_bias_share, vector_share, bias_out, conv_out, condition,
    )
    return (
        final_low,
        input_grad,
        qkv_share.reshape(model // 8, 3, width),
        bias_out,
        conv_out,
        out_share,
        up_share,
        in_bias_share.reshape(ff_own),
        down_share,
        vector_share,
        condition.reshape(()),
    )


def solution(mesh):
    chosen = slice_body if dict(mesh.shape) == {"batch": 8, "heads": 4} else body
    in_specs = (
        P("batch", None),
        P(None, None, "heads"),
        P(),
        P(),
        P("heads", None),
        P(),
        P(),
        P(),
        P(None, ("batch", "heads")),
        P(("batch", "heads")),
        P(("batch", "heads"), None),
        P(),
        P(),
        P(),
        P(("batch", "heads"), None),
        P("batch"),
        P("batch"),
        P("batch", None),
    )
    out_specs = (
        P(("batch", "heads"), None),
        P(("batch", "heads"), None),
        P("batch", None, "heads"),
        P(None, "heads"),
        P("heads", None),
        P("heads", "batch"),
        P(None, ("batch", "heads")),
        P(("batch", "heads")),
        P(("batch", "heads"), None),
        P(None, ("batch", "heads")),
        P(),
    )
    return jax.shard_map(chosen, mesh=mesh, in_specs=in_specs, out_specs=out_specs, check_vma=False)
```

```python
from functools import partial

import jax
import jax.numpy as jnp
from jax import lax
from jax.experimental import pallas as pl
from jax.experimental.pallas import tpu as pltpu
from jax.sharding import PartitionSpec as P

HEAD_DIM = 64
PINV_ITERS = 6
TILE = 512
SUB = 128

f32 = jnp.float32
low = jnp.bfloat16
mask_fill = -1000000000.0


def split(x):
    high = x.astype(low)
    return high, (x - high.astype(f32)).astype(low)


def mul(a, b):
    return lax.dot_general(a, b, (((1,), (0,)), ((), ())), preferred_element_type=f32)


def mul_t(a, b):
    return lax.dot_general(a, b, (((1,), (1,)), ((), ())), preferred_element_type=f32)


def wide(form, left, right):
    left_high, left_low = split(left)
    right_high, right_low = split(right)
    return form(left_high, right_high) + (
        form(left_high, right_low) + form(left_low, right_high)
    )


def block_grid(rows, cols):
    row_block = lax.broadcasted_iota(jnp.int32, (rows, cols), 0) // HEAD_DIM
    col_block = lax.broadcasted_iota(jnp.int32, (rows, cols), 1) // HEAD_DIM
    return row_block == col_block


def spread(x, blocks):
    count = blocks.shape[0] // x.shape[0]
    return jnp.where(blocks, jnp.concatenate([x] * count, axis=0), jnp.zeros_like(x[:1, :1]))


def fold(x, blocks):
    kept = jnp.where(blocks, x, jnp.zeros_like(x[:1, :1]))
    rows = HEAD_DIM
    out = kept[:rows]
    for n in range(1, x.shape[0] // rows):
        out = out + kept[n * rows : (n + 1) * rows]
    return out


def ready(x, ones):
    count = ones.shape[0] // HEAD_DIM
    high, rest = split(x)
    return [jnp.concatenate([part] * count, axis=0) * ones for part in (high, rest)]


def pack_mul(lefts, right, form=mul):
    halves = [split(x) for x in lefts]
    high = [x[0] for x in halves]
    count = len(lefts)
    both_parts = form(jnp.concatenate(high + [x[1] for x in halves], axis=0), right[0])
    rest = form(jnp.concatenate(high, axis=0), right[1])
    out = []
    for n in range(count):
        at = slice(n * HEAD_DIM, (n + 1) * HEAD_DIM)
        more = slice((count + n) * HEAD_DIM, (count + n + 1) * HEAD_DIM)
        out.append(both_parts[at] + (both_parts[more] + rest[at]))
    return out


def block_ones(size):
    return jnp.where(block_grid(size, size), 1.0, 0.0).astype(low)


def slot_bounds(len_ref, s, slots):
    start = jnp.int32(0)
    for n in range(slots):
        start = start + jnp.where(n < s, len_ref[n], 0)
    return start, start + len_ref[s]


def eye_pack(width):
    row = lax.broadcasted_iota(jnp.int32, (HEAD_DIM, width), 0)
    col = lax.broadcasted_iota(jnp.int32, (HEAD_DIM, width), 1) % HEAD_DIM
    return jnp.where(row == col, 1.0, 0.0).astype(f32)


def lane_mask(start, end, at, width):
    tok = at + lax.broadcasted_iota(jnp.int32, (1, width), 1)
    return (tok >= start) & (tok < end)


def band(taps_row, width):
    row = lax.broadcasted_iota(jnp.int32, (SUB, 3 * SUB), 0)
    col = lax.broadcasted_iota(jnp.int32, (SUB, 3 * SUB), 1)
    off = col - row - (SUB - width // 2)
    out = jnp.zeros((SUB, 3 * SUB), f32)
    for n in range(width):
        out = jnp.where(off == n, taps_row[:, n : n + 1], out)
    return out


def slot_marks(len_ref, at, slots, marks, width):
    rows = slots * marks
    row = lax.broadcasted_iota(jnp.int32, (rows, 1), 0)
    slot = row // marks
    mark = row % marks
    start = jnp.zeros((rows, 1), jnp.int32)
    length = jnp.zeros((rows, 1), jnp.int32)
    for n in range(slots):
        start = start + jnp.where(slot > n, len_ref[n], 0)
        length = jnp.where(slot == n, len_ref[n], length)
    lower = start + (mark * length) // marks
    upper = start + ((mark + 1) * length) // marks
    inv_count = 1.0 / jnp.maximum((upper - lower).astype(f32), 1.0)
    tok = at + lax.broadcasted_iota(jnp.int32, (rows, width), 1)
    member = jnp.where((tok >= lower) & (tok < upper), 1.0, 0.0)
    return member, inv_count


def mix_forward_kernel(
    slots, marks, taps,
    len_ref, tok_ref, weight_ref, bias_ref, conv_ref,
    qkv_ref, first_ref, last_ref, mixed_ref, mark_ref, value_ref, inner_ref,
    denom_ref, middle_ref, steps_ref, inverse_ref, bound_ref,
    vpad, scores, vsum, bias_col, conv_own,
):
    step = pl.program_id(0)
    width = first_ref.shape[0]
    heads = width // HEAD_DIM
    tok_count = qkv_ref.shape[1]
    tiles = tok_count // TILE
    packed = slots * marks
    at = pl.multiple_of(step * TILE, TILE)

    @pl.when(step == 0)
    def _():
        z = lax.axis_index("heads")
        own_taps(conv_own, conv_ref, z)
        columns = jnp.transpose(jnp.concatenate([bias_ref[...], bias_ref[...]], axis=0))
        bias_col[: bias_ref.shape[1], :] = columns
        mark_ref[...] = jnp.zeros_like(mark_ref)
        vsum[...] = jnp.zeros_like(vsum)
        vpad[:, :SUB] = jnp.zeros((width, SUB), low)
        vpad[:, tok_count + SUB :] = jnp.zeros((width, SUB), low)

    at_head = pl.ds(pl.multiple_of(lax.axis_index("heads") * width, HEAD_DIM), width)
    rows = mul_t(weight_ref[...], tok_ref[...])
    rows = jnp.concatenate(
        [
            rows[:width] + bias_col[at_head, 0:1],
            rows[width : 2 * width],
            rows[2 * width :] + bias_col[at_head, 1:2],
        ],
        axis=0,
    ).astype(low)
    qkv_ref[:, pl.ds(at, TILE)] = rows
    vpad[:, pl.ds(pl.multiple_of(at + SUB, SUB), TILE)] = rows[2 * width :]
    member, inv_count = slot_marks(len_ref, at, slots, marks, TILE)
    mark_ref[...] += mul_t(member.astype(low), rows[: 2 * width])
    vsum[...] += mul_t(jnp.ones((8, TILE), low), rows[2 * width :])
    first_ref[:, pl.ds(at, TILE)] = jnp.zeros((width, TILE), low)
    last_ref[:, pl.ds(at, TILE)] = jnp.zeros((width, TILE), low)
    mixed_ref[:, pl.ds(at, TILE)] = jnp.zeros((width, TILE), low)

    @pl.when(step == tiles - 1)
    def _():
        mark_ref[...] = mark_ref[...] * inv_count
        head_blocks = block_grid(width, width)
        slot_blocks = block_grid(packed, packed)
        ones = block_ones(packed)
        eye = eye_pack(packed)
        scale = HEAD_DIM ** -0.5

        middles, inverses_t, products = [], [], []
        bound_total = jnp.zeros((1, 1), f32)
        lane_slot = lax.broadcasted_iota(jnp.int32, (1, packed), 1) // marks
        for h in range(heads):
            q_marks = mark_ref[:, h * HEAD_DIM : (h + 1) * HEAD_DIM]
            k_marks = mark_ref[:, width + h * HEAD_DIM : width + (h + 1) * HEAD_DIM]
            sim = wide(mul_t, q_marks, k_marks) * scale
            sim = jnp.where(slot_blocks, sim, -1e30)
            sim = jnp.exp(sim - jnp.max(sim, axis=1, keepdims=True))
            sim = sim / jnp.sum(sim, axis=1, keepdims=True)
            middle = fold(sim, slot_blocks)
            col_sums = jnp.sum(middle, axis=0, keepdims=True)
            bound = jnp.zeros((1, packed), f32)
            for s in range(slots):
                top = jnp.max(jnp.where(lane_slot == s, col_sums, 0.0), axis=1, keepdims=True)
                bound = jnp.where(lane_slot == s, top, bound)
                bound_total += jnp.where(len_ref[s] > 0, top, 0.0)
            middle_ref[h] = middle
            middles.append(middle)
            inverses_t.append(middle / bound)
            products.append(pack_mul([middle], ready(middle, ones), mul_t)[0] / bound)
        bound_ref[...] = jnp.broadcast_to(bound_total, bound_ref.shape)

        def newton(n, carry):
            out = []
            for h in range(heads):
                before_t, weight, product = carry[h]
                (inverse_t,) = pack_mul([0.25 * weight], ready(before_t, ones))
                (square,) = pack_mul([product], ready(product, ones))
                cube, fourth = pack_mul([product, square], ready(square, ones))
                third = 13.0 * eye - 15.0 * product + 7.0 * square - cube
                steps_ref[n, 0, h] = product
                steps_ref[n, 1, h] = square
                steps_ref[n, 2, h] = third
                steps_ref[n, 3, h] = inverse_t
                after = 0.25 * (13.0 * product - 15.0 * square + 7.0 * cube - fourth)
                out.append((inverse_t, third, after))
            return tuple(out)

        start = tuple((x, 4.0 * eye, p) for x, p in zip(inverses_t, products))
        final = lax.fori_loop(0, PINV_ITERS, newton, start)
        for h in range(heads):
            inverse_t, third, _ = final[h]
            inverse_ref[h] = pack_mul([0.25 * third], ready(inverse_t, ones))[0]

        def one_slot(s, _):
            start, end = slot_bounds(len_ref, s, slots)
            lo, hi = start // TILE, (end + TILE - 1) // TILE
            hi = jnp.where(end > start, hi, lo)
            own = mark_ref[pl.ds(pl.multiple_of(s * marks, marks), marks), :] * scale
            q_block = spread(own[:, :width], head_blocks).astype(low)
            k_block = spread(own[:, width:], head_blocks).astype(low)

            def score_tile(n, top):
                t = pl.multiple_of(n * TILE, TILE)
                mask = lane_mask(start, end, t, TILE)
                sim = mul(k_block, qkv_ref[:width, pl.ds(t, TILE)])
                sim = sim.reshape(heads, marks, TILE)
                sim = jnp.exp(sim - jnp.max(sim, axis=1, keepdims=True))
                sim = sim / jnp.sum(sim, axis=1, keepdims=True)
                sim = sim.reshape(width, TILE)
                old = first_ref[:, pl.ds(t, TILE)].astype(f32)
                first_ref[:, pl.ds(t, TILE)] = jnp.where(mask, sim, old).astype(low)
                sim = mul(q_block, qkv_ref[width : 2 * width, pl.ds(t, TILE)])
                sim = jnp.where(mask, sim, mask_fill)
                scores[:, pl.ds(t, TILE)] = sim
                for c in range(TILE // SUB):
                    top = jnp.maximum(top, sim[:, c * SUB : (c + 1) * SUB])
                return top

            top = lax.fori_loop(lo, hi, score_tile, jnp.full((width, SUB), mask_fill, f32))
            top = jnp.max(top, axis=1, keepdims=True)

            def value_tile(n, carry):
                denom, total = carry
                t = pl.multiple_of(n * TILE, TILE)
                mask = lane_mask(start, end, t, TILE)
                part = jnp.exp(scores[:, pl.ds(t, TILE)] - top)
                old = last_ref[:, pl.ds(t, TILE)].astype(f32)
                last_ref[:, pl.ds(t, TILE)] = jnp.where(mask, part, old).astype(low)
                total = total + mul_t(part.astype(low), qkv_ref[2 * width :, pl.ds(t, TILE)])
                for c in range(TILE // SUB):
                    denom = denom + part[:, c * SUB : (c + 1) * SUB]
                return denom, total

            denom, total = lax.fori_loop(
                lo, hi, value_tile,
                (jnp.zeros((width, SUB), f32), jnp.zeros((width, width), f32)),
            )
            denom = jnp.sum(denom, axis=1, keepdims=True)
            inv = 1.0 / jnp.where(denom > 0.0, denom, 1.0)
            denom_ref[s] = inv
            values = fold(total * inv, head_blocks)
            values = jnp.where(end > start, values, vsum[:1] / tok_count)
            value_ref[pl.ds(pl.multiple_of(s * marks, marks), marks), :] = values
            return 0

        lax.fori_loop(0, slots, one_slot, 0)

        lane_head = lax.broadcasted_iota(jnp.int32, (1, width), 1) // HEAD_DIM
        inner = jnp.zeros((packed, width), f32)
        for h in range(heads):
            (inverse,) = pack_mul([eye], ready(inverse_ref[h], ones), mul_t)
            own_values = jnp.where(lane_head == h, value_ref[...], 0.0)
            inner = inner + wide(mul, spread(inverse, slot_blocks), own_values)
        inner_ref[...] = inner

        bands = [band(conv_own[h : h + 1, :], taps).astype(low) for h in range(heads)]

        def out_slot(s, _):
            start, end = slot_bounds(len_ref, s, slots)
            lo, hi = start // TILE, (end + TILE - 1) // TILE
            hi = jnp.where(end > start, hi, lo)
            own = inner_ref[pl.ds(pl.multiple_of(s * marks, marks), marks), :]
            a_block = jnp.transpose(spread(own, head_blocks)).astype(low)

            def out_tile(n, _):
                t = pl.multiple_of(n * TILE, TILE)
                mask = lane_mask(start, end, t, TILE)
                rows = mul(a_block, first_ref[:, pl.ds(t, TILE)])
                rows = rows + convolve(vpad, bands, start, end, t, heads)
                old = mixed_ref[:, pl.ds(t, TILE)].astype(f32)
                mixed_ref[:, pl.ds(t, TILE)] = jnp.where(mask, rows, old).astype(low)
                return 0

            return lax.fori_loop(lo, hi, out_tile, 0)

        lax.fori_loop(0, slots, out_slot, 0)


def own_taps(own_ref, all_ref, z):
    heads = own_ref.shape[0]
    for n in range(all_ref.shape[0] // heads):

        @pl.when(z == n)
        def _():
            own_ref[...] = all_ref[n * heads : (n + 1) * heads, :]


def windows(padded, start, end, t):
    full = padded[:, pl.ds(t, TILE + 2 * SUB)]
    keep = lane_mask(start, end, t - SUB, TILE + 2 * SUB)
    return jnp.where(keep, full.astype(f32), 0.0).astype(low)


def convolve(padded, bands, start, end, t, heads):
    full = windows(padded, start, end, t)
    out = []
    count = TILE // SUB
    for h in range(heads):
        own = full[h * HEAD_DIM : (h + 1) * HEAD_DIM]
        stack = jnp.concatenate(
            [own[:, c * SUB : (c + 3) * SUB] for c in range(count)], axis=0
        )
        res = mul_t(stack, bands[h])
        out.append(
            jnp.concatenate(
                [res[c * HEAD_DIM : (c + 1) * HEAD_DIM] for c in range(count)], axis=1
            )
        )
    return jnp.concatenate(out, axis=0)


def mix_backward_kernel(
    slots, marks, taps,
    len_ref, grad_ref, qkv_ref, first_ref, last_ref, mark_ref, value_ref, inner_ref,
    denom_ref, middle_ref, steps_ref, inverse_ref, conv_ref,
    out_ref, bias_ref, conv_out_ref,
    gpad, vpad, ds_first, ds_last, conv_grad, d_inner, d_k, d_q, d_value, conv_own,
):
    width = first_ref.shape[0]
    heads = width // HEAD_DIM
    tok_count = qkv_ref.shape[1]
    packed = slots * marks
    scale = HEAD_DIM ** -0.5
    head_blocks = block_grid(width, width)
    slot_blocks = block_grid(packed, packed)
    ones = block_ones(packed)
    eye = eye_pack(packed)
    count = TILE // SUB

    for padded, source in ((gpad, grad_ref[...]), (vpad, qkv_ref[2 * width :, :])):
        padded[:, :SUB] = jnp.zeros((width, SUB), low)
        padded[:, tok_count + SUB :] = jnp.zeros((width, SUB), low)
        padded[:, SUB : tok_count + SUB] = source
    out_ref[...] = jnp.zeros_like(out_ref)
    ds_first[...] = jnp.zeros_like(ds_first)
    ds_last[...] = jnp.zeros_like(ds_last)
    conv_grad[...] = jnp.zeros_like(conv_grad)

    own_taps(conv_own, conv_ref, lax.axis_index("heads"))

    def reach(s):
        start, end = slot_bounds(len_ref, s, slots)
        lo, hi = start // TILE, (end + TILE - 1) // TILE
        return start, end, lo, jnp.where(end > start, hi, lo)

    def own_rows(s):
        return pl.ds(pl.multiple_of(s * marks, marks), marks)

    def first_slot(s, _):
        start, end, lo, hi = reach(s)
        a_block = spread(inner_ref[own_rows(s), :], head_blocks).astype(low)

        def tile(n, carry):
            inner_total, key_total = carry
            t = pl.multiple_of(n * TILE, TILE)
            mask = lane_mask(start, end, t, TILE)
            own_grad = grad_ref[:, pl.ds(t, TILE)]
            kernel_rows = jnp.where(mask, first_ref[:, pl.ds(t, TILE)].astype(f32), 0.0)
            d_kernel = mul(a_block, own_grad)
            prod = (kernel_rows * d_kernel).reshape(heads, marks, TILE)
            row_sum = jnp.sum(prod, axis=1, keepdims=True)
            d_sim = prod - kernel_rows.reshape(heads, marks, TILE) * row_sum
            d_sim = d_sim.reshape(width, TILE)
            d_sim_low = d_sim.astype(low)
            old = ds_first[:, pl.ds(t, TILE)].astype(f32)
            ds_first[:, pl.ds(t, TILE)] = jnp.where(mask, d_sim, old).astype(low)
            inner_total = inner_total + mul_t(kernel_rows.astype(low), own_grad)
            key_total = key_total + mul_t(d_sim_low, qkv_ref[:width, pl.ds(t, TILE)])
            full = windows(vpad, start, end, t)
            grad_own = jnp.where(mask, own_grad.astype(f32), 0.0).astype(low)
            for h in range(heads):
                sel = slice(h * HEAD_DIM, (h + 1) * HEAD_DIM)
                left = jnp.concatenate(
                    [grad_own[sel, c * SUB : (c + 1) * SUB] for c in range(count)], axis=0
                )
                right = jnp.concatenate(
                    [full[sel, c * SUB : (c + 3) * SUB] for c in range(count)], axis=0
                )
                conv_grad[h] += lax.dot_general(
                    left, right, (((0,), (0,)), ((), ())), preferred_element_type=f32
                )
            return inner_total, key_total

        zero = jnp.zeros((width, width), f32)
        inner_total, key_total = lax.fori_loop(lo, hi, tile, (zero, zero))
        d_inner[own_rows(s), :] = fold(inner_total, head_blocks)
        d_k[own_rows(s), :] = fold(key_total, head_blocks) * scale
        return 0

    lax.fori_loop(0, slots, first_slot, 0)

    row = lax.broadcasted_iota(jnp.int32, (SUB, 3 * SUB), 0)
    col = lax.broadcasted_iota(jnp.int32, (SUB, 3 * SUB), 1)
    off = col - row - (SUB - taps // 2)
    tap_lane = lax.broadcasted_iota(jnp.int32, (1, SUB), 1)
    for h in range(heads):
        found = jnp.zeros((1, SUB), f32)
        square = conv_grad[h]
        for n in range(taps):
            part = jnp.sum(jnp.where(off == n, square, 0.0), axis=0, keepdims=True)
            part = jnp.sum(part, axis=1, keepdims=True)
            found = jnp.where(tap_lane == n, part, found)
        conv_out_ref[h : h + 1, :] = found

    lane_head = lax.broadcasted_iota(jnp.int32, (1, width), 1) // HEAD_DIM
    value_total = jnp.zeros((packed, width), f32)
    d_inverses = []
    for h in range(heads):
        own = jnp.where(lane_head == h, d_inner[...], 0.0)
        value_total = value_total + wide(mul, spread(inverse_ref[h], slot_blocks), own)
        d_inverses.append(fold(wide(mul_t, own, value_ref[...]), slot_blocks))
    d_value[...] = value_total

    def before(n, h, d_inverse):
        third, inverse_t = steps_ref[n, 2, h], steps_ref[n, 3, h]
        (d_third,) = pack_mul([0.25 * inverse_t], ready(d_inverse, ones))
        (earlier,) = pack_mul([0.25 * d_inverse], ready(third, ones))
        return earlier, d_third

    def newton(k, carry):
        n = PINV_ITERS - 1 - k
        out = []
        for h in range(heads):
            d_inverse, d_third, grad = carry[h]
            product, square, third = [steps_ref[n, i, h] for i in range(3)]
            mixed = 7.0 * product - square
            by_third, by_one, by_two = pack_mul([third, product, square], ready(grad, ones))
            left_mixed, left_one = pack_mul([mixed, product], ready(d_third, ones))
            (right,) = pack_mul([grad], ready(third, ones))
            (more,) = pack_mul([0.25 * by_one + d_third], ready(mixed, ones))
            (less,) = pack_mul([0.25 * by_two + left_one], ready(product, ones))
            d_product = (
                0.25 * (right + by_third - 13.0 * grad) - 15.0 * d_third + left_mixed + more - less
            )
            earlier, d_before = before(jnp.maximum(n - 1, 0), h, d_inverse)
            last = n == 0
            out.append((jnp.where(last, d_inverse, earlier), d_before, d_product))
        return tuple(out)

    zero = jnp.zeros((HEAD_DIM, packed), f32)
    start = []
    for h in range(heads):
        start.append(before(PINV_ITERS - 1, h, d_inverses[h]) + (zero,))
    final = lax.fori_loop(0, PINV_ITERS, newton, tuple(start))
    lane_slot = lax.broadcasted_iota(jnp.int32, (1, packed), 1) // marks
    dq_total = jnp.zeros((packed, width), f32)
    dk_total = jnp.zeros((packed, width), f32)
    for h in range(heads):
        d_inverse, _, d_product = final[h]
        middle = middle_ref[h]
        first_t = steps_ref[0, 3, h]
        (d_inverse_t,) = pack_mul([eye], ready(d_inverse, ones), mul_t)
        (d_product_t,) = pack_mul([eye], ready(d_product, ones), mul_t)
        (d_middle,) = pack_mul([d_product + d_product_t], ready(middle, ones))
        col_sums = jnp.sum(middle, axis=0, keepdims=True)
        share = jnp.sum(
            d_inverse_t * first_t + d_product * steps_ref[0, 0, h], axis=0, keepdims=True
        )
        bound = jnp.zeros((1, packed), f32)
        d_bound = jnp.zeros((1, packed), f32)
        hits = jnp.zeros((1, packed), f32)
        for s in range(slots):
            mine = lane_slot == s
            top = jnp.max(jnp.where(mine, col_sums, 0.0), axis=1, keepdims=True)
            total = jnp.sum(jnp.where(mine, share, 0.0), axis=1, keepdims=True)
            number = jnp.sum(
                jnp.where(mine & (col_sums == top), 1.0, 0.0), axis=1, keepdims=True
            )
            bound = jnp.where(mine, top, bound)
            d_bound = jnp.where(mine, -total / top, d_bound)
            hits = jnp.where(mine, number, hits)
        d_middle = (d_middle + d_inverse_t) / bound
        d_middle = d_middle + jnp.where(col_sums == bound, d_bound / hits, 0.0)
        prod = spread(middle * d_middle, slot_blocks)
        d_sim = prod - spread(middle, slot_blocks) * jnp.sum(prod, axis=1, keepdims=True)
        d_sim = d_sim * scale
        own = lane_head == h
        q_marks = jnp.where(own, mark_ref[:, :width], 0.0)
        k_marks = jnp.where(own, mark_ref[:, width:], 0.0)
        dq_total = dq_total + wide(mul, d_sim, k_marks)
        dk_total = dk_total + wide(mul, jnp.transpose(d_sim), q_marks)
    d_q[...] = dq_total
    d_k[...] += dk_total

    flipped = []
    for h in range(heads):
        flipped.append(
            band(
                jnp.concatenate(
                    [conv_own[h : h + 1, n : n + 1] for n in reversed(range(taps))], axis=1
                ),
                taps,
            ).astype(low)
        )

    def last_slot(s, _):
        start, end, lo, hi = reach(s)
        inv = denom_ref[s]
        own_d = d_value[own_rows(s), :]
        own_v = value_ref[own_rows(s), :]
        d_block = spread(own_d, head_blocks)
        row_sum = jnp.sum(
            d_block * jnp.concatenate([own_v] * heads, axis=0), axis=1, keepdims=True
        )
        row_sum = row_sum * inv
        d_block = d_block * inv
        d_block_t = jnp.transpose(d_block).astype(low)
        d_block = d_block.astype(low)

        def tile(n, query_total):
            t = pl.multiple_of(n * TILE, TILE)
            mask = lane_mask(start, end, t, TILE)
            kernel_rows = jnp.where(mask, last_ref[:, pl.ds(t, TILE)].astype(f32), 0.0)
            v_rows = qkv_ref[2 * width :, pl.ds(t, TILE)]
            d_sim = kernel_rows * (mul(d_block, v_rows) - row_sum)
            d_low = d_sim.astype(low)
            old = ds_last[:, pl.ds(t, TILE)].astype(f32)
            ds_last[:, pl.ds(t, TILE)] = jnp.where(mask, d_sim, old).astype(low)
            dv = mul(d_block_t, kernel_rows.astype(low))
            dv = dv + convolve(gpad, flipped, start, end, t, heads)
            old = out_ref[2 * width :, pl.ds(t, TILE)].astype(f32)
            out_ref[2 * width :, pl.ds(t, TILE)] = jnp.where(mask, dv, old).astype(low)
            return query_total + mul_t(d_low, qkv_ref[width : 2 * width, pl.ds(t, TILE)])

        query_total = lax.fori_loop(lo, hi, tile, jnp.zeros((width, width), f32))
        d_q[own_rows(s), :] += fold(query_total, head_blocks) * scale
        return 0

    lax.fori_loop(0, slots, last_slot, 0)

    inv_count = slot_marks(len_ref, 0, slots, marks, SUB)[1]
    d_q[...] = d_q[...] * inv_count
    d_k[...] = d_k[...] * inv_count

    def final_slot(s, _):
        start, end, lo, hi = reach(s)
        length = end - start
        own = mark_ref[own_rows(s), :] * scale

        def left(block, d_mark):
            wide_rows = jnp.concatenate([spread(block, head_blocks), d_mark], axis=0)
            return jnp.transpose(wide_rows).astype(low)

        q_left = left(own[:, width:], d_q[own_rows(s), :])
        k_left = left(own[:, :width], d_k[own_rows(s), :])
        mark = lax.broadcasted_iota(jnp.int32, (marks, 1), 0)
        lower = start + (mark * length) // marks
        upper = start + ((mark + 1) * length) // marks

        def tile(n, _):
            t = pl.multiple_of(n * TILE, TILE)
            mask = lane_mask(start, end, t, TILE)
            tok = t + lax.broadcasted_iota(jnp.int32, (marks, TILE), 1)
            member = jnp.where((tok >= lower) & (tok < upper), 1.0, 0.0).astype(low)
            for at, lhs, source in ((0, q_left, ds_first), (width, k_left, ds_last)):
                rhs = jnp.concatenate([source[:, pl.ds(t, TILE)], member], axis=0)
                rows = mul(lhs, rhs)
                old = out_ref[at : at + width, pl.ds(t, TILE)].astype(f32)
                out_ref[at : at + width, pl.ds(t, TILE)] = jnp.where(mask, rows, old).astype(low)
            return 0

        return lax.fori_loop(lo, hi, tile, 0)

    lax.fori_loop(0, slots, final_slot, 0)

    def bias_tile(n, carry):
        t = pl.multiple_of(n * TILE, TILE)
        q_sum, v_sum = carry
        q_rows = out_ref[:width, pl.ds(t, TILE)].astype(f32)
        v_rows = out_ref[2 * width :, pl.ds(t, TILE)].astype(f32)
        for c in range(count):
            q_sum = q_sum + q_rows[:, c * SUB : (c + 1) * SUB]
            v_sum = v_sum + v_rows[:, c * SUB : (c + 1) * SUB]
        return q_sum, v_sum

    zero = jnp.zeros((width, SUB), f32)
    q_sum, v_sum = lax.fori_loop(0, tok_count // TILE, bias_tile, (zero, zero))
    bias_ref[...] = jnp.zeros_like(bias_ref)
    bias_ref[0:1, :] = jnp.sum(jnp.transpose(q_sum), axis=0, keepdims=True)
    bias_ref[1:2, :] = jnp.sum(jnp.transpose(v_sum), axis=0, keepdims=True)


def mix_forward(seq_lengths, tokens, weight_t, bias, conv, slots, marks):
    tok_count, model = tokens.shape
    width = weight_t.shape[0] // 3
    heads = width // HEAD_DIM
    packed = slots * marks
    taps = conv.shape[1]
    whole = lambda *shape: pl.BlockSpec(shape, lambda i, lens: (0,) * len(shape))
    shapes = [
        ((3 * width, tok_count), low),
        ((width, tok_count), low),
        ((width, tok_count), low),
        ((width, tok_count), low),
        ((packed, 2 * width), f32),
        ((packed, width), f32),
        ((packed, width), f32),
        ((slots, width, 1), f32),
        ((heads, HEAD_DIM, packed), f32),
        ((PINV_ITERS, 4, heads, HEAD_DIM, packed), f32),
        ((heads, HEAD_DIM, packed), f32),
        ((8, 128), f32),
    ]
    return pl.pallas_call(
        partial(mix_forward_kernel, slots, marks, taps),
        out_shape=[jax.ShapeDtypeStruct(s, t) for s, t in shapes],
        grid_spec=pltpu.PrefetchScalarGridSpec(
            num_scalar_prefetch=1,
            grid=(tok_count // TILE,),
            in_specs=[
                pl.BlockSpec((TILE, model), lambda i, lens: (i, 0)),
                whole(3 * width, model),
                whole(*bias.shape),
                whole(*conv.shape),
            ],
            out_specs=[whole(*s) for s, _ in shapes],
            scratch_shapes=[
                pltpu.VMEM((width, tok_count + 2 * SUB), low),
                pltpu.VMEM((width, tok_count), f32),
                pltpu.VMEM((8, width), f32),
                pltpu.VMEM((bias.shape[1], 2 * bias.shape[0]), f32),
                pltpu.VMEM((heads, taps), f32),
            ],
        ),
        compiler_params=pltpu.CompilerParams(vmem_limit_bytes=56 * 1024 * 1024),
        cost_estimate=pl.CostEstimate(
            flops=20 * 10**9, bytes_accessed=30 * 10**6, transcendentals=10**6
        ),
        name="mix_forward",
    )(seq_lengths, tokens, weight_t, bias, conv)


def mix_backward(seq_lengths, grad_t, saved, conv, slots, marks):
    qkv_t, first, last, mark, value, inner, denom, middle, steps, inverse = saved
    width, tok_count = grad_t.shape
    heads = width // HEAD_DIM
    packed = slots * marks
    taps = conv.shape[1]
    args = (grad_t, qkv_t, first, last, mark, value, inner, denom, middle, steps, inverse, conv)
    whole = lambda shape: pl.BlockSpec(
        shape, lambda i, lens: (0,) * len(shape), pipeline_mode=pl.Buffered(1)
    )
    shapes = [((3 * width, tok_count), low), ((8, width), f32), ((heads, SUB), f32)]
    square = pltpu.VMEM((packed, width), f32)
    return pl.pallas_call(
        partial(mix_backward_kernel, slots, marks, taps),
        out_shape=[jax.ShapeDtypeStruct(s, t) for s, t in shapes],
        grid_spec=pltpu.PrefetchScalarGridSpec(
            num_scalar_prefetch=1,
            grid=(1,),
            in_specs=[whole(x.shape) for x in args],
            out_specs=[whole(s) for s, _ in shapes],
            scratch_shapes=[
                pltpu.VMEM((width, tok_count + 2 * SUB), low),
                pltpu.VMEM((width, tok_count + 2 * SUB), low),
                pltpu.VMEM((width, tok_count), low),
                pltpu.VMEM((width, tok_count), low),
                pltpu.VMEM((heads, SUB, 3 * SUB), f32),
                square, square, square, square,
                pltpu.VMEM((heads, taps), f32),
            ],
        ),
        compiler_params=pltpu.CompilerParams(vmem_limit_bytes=56 * 1024 * 1024),
        cost_estimate=pl.CostEstimate(
            flops=20 * 10**9, bytes_accessed=30 * 10**6, transcendentals=10**6
        ),
        name="mix_backward",
    )(seq_lengths, *args)


contract_rows = (((0,), (0,)), ((), ()))
contract_cols = (((1,), (1,)), ((), ()))
norm_eps = 1e-05


def split_up(x, dim, peers):
    before, after = (x.shape[:dim], x.shape[dim + 1 :])
    return jnp.moveaxis(x.reshape(*before, peers, -1, *after), dim, 0)


def sum_at_owner(x, axis, dim):
    peers = lax.axis_size(axis)
    tiles = lax.all_to_all(split_up(x, dim, peers), axis, 0, 0, tiled=True)
    return jnp.sum(tiles.astype(f32), axis=0)


def layer_norm(row_data, gain_vec, shift_vec):
    centre = row_data - jnp.mean(row_data, axis=1, keepdims=True)
    spread_row = jnp.mean(centre * centre, axis=1, keepdims=True)
    return centre * lax.rsqrt(spread_row + norm_eps) * gain_vec[None, :] + shift_vec[None, :]


def gelu_exact(values):
    return jax.nn.gelu(values, approximate=False)


def body(
    tokens,
    qkv_weight,
    qv_bias,
    conv_weight,
    out_weight,
    out_bias,
    norm1_gain,
    norm1_bias,
    ffn_in_weight,
    ffn_in_bias,
    ffn_out_weight,
    ffn_out_bias,
    norm2_gain,
    norm2_bias,
    cotangent,
    seq_lengths,
    segment_ids,
    landmark_bounds,
):
    tok_count, model_width = tokens.shape
    head_width = qkv_weight.shape[2]
    heads_here = head_width // HEAD_DIM
    head_total = conv_weight.shape[0]
    kernel_taps = conv_weight.shape[1]
    slots, marks = landmark_bounds.shape
    quarter = tok_count // lax.axis_size("heads")
    head_index = lax.axis_index("heads")
    own_start = head_index * quarter
    both = ("batch", "heads")
    own_rows_low = lax.dynamic_slice_in_dim(tokens, own_start, quarter, 0)
    own_tokens = own_rows_low.astype(f32)
    flat_qkv = qkv_weight.reshape(model_width, 3 * head_width)
    forward = mix_forward(
        seq_lengths, tokens, jnp.transpose(flat_qkv), qv_bias, conv_weight, slots, marks
    )
    qkv_t, first, last, mixed_t, mark, value, inner, denom, middle, steps, inverse, bound = forward
    bound_total = bound[0, 0]
    attn_part = lax.psum_scatter(
        lax.dot_general(mixed_t, out_weight, contract_rows, preferred_element_type=f32).astype(low),
        "heads",
        scatter_dimension=0,
        tiled=True,
    ).astype(f32)
    live_count = jnp.sum((seq_lengths > 0).astype(f32)) * heads_here
    first_res = own_tokens + attn_part + out_bias[None, :]
    norm1_out, norm1_pull = jax.vjp(layer_norm, first_res, norm1_gain, norm1_bias)
    norm1_low = norm1_out.astype(low)
    ff_own = ffn_out_weight.shape[0]
    bias_row = jnp.zeros((16, model_width), low).at[0, :ff_own].set(ffn_in_bias)
    whole_in = lax.all_gather(ffn_in_weight, both, axis=1, tiled=True)
    out_pack = lax.all_gather(jnp.concatenate([ffn_out_weight, bias_row], axis=0), both, axis=0)
    whole_out = out_pack[:, :ff_own].reshape(-1, model_width)
    whole_in_bias = out_pack[:, ff_own, :ff_own].reshape(-1)
    pre_act = (
        jnp.dot(norm1_low, whole_in, preferred_element_type=f32)
        + whole_in_bias.astype(f32)[None, :]
    )
    hidden_act, gelu_pull = jax.vjp(gelu_exact, pre_act)
    hidden_low = hidden_act.astype(low)
    ffn_result = jnp.dot(hidden_low, whole_out, preferred_element_type=f32) + ffn_out_bias[None, :]
    final_out, norm2_pull = jax.vjp(layer_norm, norm1_out + ffn_result, norm2_gain, norm2_bias)
    grad_second, grad_gain_two, grad_shift_two = norm2_pull(cotangent.astype(f32))
    grad_ffn_low = grad_second.astype(low)
    grad_ffn_bias = jnp.sum(grad_ffn_low.astype(f32), axis=0)
    down_term = lax.dot_general(
        hidden_low, grad_ffn_low, contract_rows, preferred_element_type=f32
    ).astype(low)
    grad_hidden = lax.dot_general(
        grad_ffn_low, whole_out, contract_cols, preferred_element_type=f32
    )
    grad_pre = gelu_pull(grad_hidden)[0].astype(low)
    grad_in_bias = jnp.sum(grad_pre.astype(f32), axis=0)
    up_term = lax.dot_general(
        norm1_low, grad_pre, contract_rows, preferred_element_type=f32
    ).astype(low)
    grad_norm1 = grad_second + lax.dot_general(
        grad_pre, whole_in, contract_cols, preferred_element_type=f32
    )
    grad_first, grad_gain_one, grad_shift_one = norm1_pull(grad_norm1)
    grad_attn_low = grad_first.astype(low)
    grad_out_bias = jnp.sum(grad_attn_low.astype(f32), axis=0)
    piece_rows = lax.all_gather(grad_attn_low, "heads", axis=0, tiled=True)
    grad_mix_t = lax.dot_general(
        out_weight, piece_rows, contract_cols, preferred_element_type=f32
    ).astype(low)
    grad_mix_t, down_term, up_term = lax.optimization_barrier((grad_mix_t, down_term, up_term))
    up_share = lax.psum_scatter(up_term, both, scatter_dimension=1, tiled=True).astype(f32)
    down_share = lax.psum_scatter(down_term, both, scatter_dimension=0, tiled=True).astype(f32)
    saved = (qkv_t, first, last, mark, value, inner, denom, middle, steps, inverse)
    grad_t, grad_bias, grad_conv = mix_backward(
        seq_lengths, grad_mix_t, saved, conv_weight, slots, marks
    )
    out_part = lax.dot_general(
        mixed_t, piece_rows, (((1,), (0,)), ((), ())), preferred_element_type=f32
    )
    grad_qv_own = grad_bias[:2]
    qkv_part = lax.dot_general(
        tokens, grad_t, (((0,), (1,)), ((), ())), preferred_element_type=f32
    ).reshape(model_width, 3, head_width)
    input_part = lax.psum_scatter(
        lax.dot_general(
            grad_t, flat_qkv, (((0,), (1,)), ((), ())), preferred_element_type=f32
        ).astype(low),
        "heads",
        scatter_dimension=0,
        tiled=True,
    ).astype(f32)
    input_grad = grad_first + input_part
    conv_full = lax.dynamic_update_slice_in_dim(
        jnp.zeros((head_total, kernel_taps), f32),
        grad_conv[:, :kernel_taps],
        head_index * heads_here,
        0,
    )
    bias_full = lax.dynamic_update_slice_in_dim(
        jnp.zeros((2, head_total * HEAD_DIM), f32), grad_qv_own, head_index * head_width, 1
    )
    qkv_share, out_share = (
        sum_at_owner(qkv_part.astype(low), "batch", 0),
        sum_at_owner(out_part.astype(low), "batch", 1),
    )
    vector_all = jnp.stack(
        [grad_ffn_bias, grad_gain_two, grad_shift_two, grad_gain_one, grad_shift_one, grad_out_bias]
    )
    in_bias_share, vector_share = (
        lax.psum_scatter(grad_in_bias, both, scatter_dimension=0, tiled=True),
        lax.psum_scatter(vector_all, both, scatter_dimension=1, tiled=True),
    )
    conv_sum, bias_sum, bound_all, count_all = lax.psum(
        (conv_full, bias_full, bound_total, live_count), both
    )
    conv_out = lax.dynamic_slice_in_dim(conv_sum, head_index * heads_here, heads_here, 0)
    bias_out = lax.dynamic_slice_in_dim(bias_sum, head_index * head_width, head_width, 1)
    condition = bound_all / count_all
    return (
        final_out.astype(low),
        input_grad,
        qkv_share,
        bias_out,
        conv_out,
        out_share,
        up_share,
        in_bias_share,
        down_share,
        vector_share,
        condition,
    )


def place():
    b, z = lax.axis_index("batch"), lax.axis_index("heads")
    core, x, y = b % 2, (b // 2) % 2, b // 4
    return b, z, b + 1 - 2 * core, b + 2 - 4 * x, b + 4 - 8 * y


def remote(src, dst, send, recv, device):
    return pltpu.make_async_remote_copy(
        src_ref=src,
        dst_ref=dst,
        send_sem=send,
        recv_sem=recv,
        device_id=device,
        device_id_type=pl.DeviceIdType.MESH,
    )


def greet(devices):
    barrier = pltpu.get_barrier_semaphore()
    for device in devices:
        pl.semaphore_signal(
            barrier, inc=1, device_id=device, device_id_type=pl.DeviceIdType.MESH
        )
    pl.semaphore_wait(barrier, len(devices))


def tail_kernel(
    len_ref,
    gt_hbm, wq_hbm, we_hbm, hid_hbm, pre_hbm, n1_hbm, gf_hbm, ga_hbm, mx_hbm, tok_hbm, first_hbm,
    sums_ref, bin_ref, qv_ref, conv_ref, bound_ref,
    input_ref, down_own, up_own, outw_own, qkvw_own, in_bias, vector_own, qv_own, conv_own, ratio,
    small_out,
    gt, wq, we, hid, pre, n1, gf, ga, mx, tok,
    q_in, r_out, r_in, s_in, out_down, out_up, full_outw, full_qkvw, acc_qkvw,
    core_down, core_up, core_outw, core_qkvw,
    one_down, one_up, one_outw, one_qkvw, two_down, two_up, two_outw, two_qkvw,
    e_down, e_up, e_outw, g_down, g_up, g_outw, h_down, h_up, h_outw, small_in,
    load_sem, q_send, q_recv, r_send, r_recv, t_send, t_recv, c_send, c_recv, x_send, x_recv, e_send, e_recv,
    g_send, g_recv, h_send, h_recv, s_send, s_recv,
):
    b, z, bc, bx, by = place()
    both = bx + by - b
    flip = bc - b
    peers = [(b, lax.rem(z + i, 4)) for i in (1, 2, 3)]
    issued = []
    loads = [
        pltpu.make_async_copy(src, dst, load_sem.at[n])
        for n, (src, dst) in enumerate(
            (
                (pre_hbm, pre), (n1_hbm, n1), (hid_hbm, hid), (gf_hbm, gf), (gt_hbm, gt),
                (wq_hbm, wq), (we_hbm, we), (mx_hbm, mx), (ga_hbm, ga), (tok_hbm, tok),
                (first_hbm, input_ref),
            )
        )
    ]
    for copy in loads:
        copy.start()
    greet(peers + [(bc, z), (bx, z), (by, z)])
    chunks, size = r_in.shape[1:3]
    quarter = chunks * size
    ff = down_own.shape[0]
    group = 4 * ff

    zf = z + 1 - 2 * (z % 2)
    zg = z + 2 - 4 * (z // 2)
    partners = ((bc, z), (bx, z), (by, z), (b, zf), (b, zg))

    def small_start(k):
        copy = remote(
            small_out.at[k], small_in.at[k], s_send.at[k], s_recv.at[k], partners[k]
        )
        copy.start()
        issued.append(copy)

    def small_event(k):
        ref = small_in.at[k]
        remote(ref, ref, s_send.at[k], s_recv.at[k], partners[k]).wait_recv()
        small_out[k + 1] = small_out[k] + small_in[k]
        if k < 4:
            small_start(k + 1)

    model = input_ref.shape[1]
    bias_rows = bin_ref.shape[1] // model
    at_vec, at_qv = bias_rows, bias_rows + 6
    heads, taps = conv_own.shape
    at_conv = at_qv + 8
    at_end = at_conv + 4 * heads
    width = qv_own.shape[1]
    small_out[0] = jnp.zeros(small_out.shape[1:], f32)
    for n in range(bias_rows):
        small_out[0, n : n + 1, :] = bin_ref[0:1, n * model : (n + 1) * model]
    small_out[0, at_vec : at_vec + 6, :] = sums_ref[0:6, :]
    live = jnp.int32(0)
    for n in range(len_ref.shape[0]):
        live = live + jnp.where(len_ref[n] > 0, heads, 0)
    lane = lax.broadcasted_iota(jnp.int32, (1, 128), 1)
    small_out[0, at_end : at_end + 1, 0:128] = jnp.where(
        lane == 0, bound_ref[0:1, :], jnp.where(lane == 1, live.astype(f32), 0.0)
    )
    for n in range(4):

        @pl.when(z == n)
        def _():
            for r in range(2):
                row = at_qv + 2 * n + r
                small_out[0, row : row + 1, :width] = qv_ref[r : r + 1, :]
            for r in range(heads):
                row = at_conv + heads * n + r
                small_out[0, row : row + 1, 0:128] = conv_ref[r : r + 1, :]

    small_start(0)

    is_end = (z == 0) | (z == 3)
    low_side = z < 2
    to_inner = jnp.where(low_side, 1, 2)
    across = jnp.where(z == 1, 2, 1)
    to_end = jnp.where(low_side, 0, 3)

    def owner(k):
        return jnp.where(low_side, 3 - k, k)

    def columns(who, c):
        return pl.ds(pl.multiple_of(who * quarter + c * size, size), size)

    def times(x, w):
        return lax.dot_general(x, w, (((0,), (0,)), ((), ())), preferred_element_type=f32)

    def part(who, c):
        return times(gt[:, columns(who, c)], wq[...])

    def q_copy(k, c):
        return remote(
            gt_hbm.at[:, columns(owner(k), c)], q_in.at[k, c], q_send.at[k, c], q_recv.at[k, c],
            (b, to_inner),
        )

    def q_wait(k, c):
        ref = q_in.at[k, c]
        remote(ref, ref, q_send.at[k, c], q_recv.at[k, c], (b, to_end)).wait_recv()

    def r_copy(k, c):
        return remote(
            r_out.at[k, c], r_in.at[k, c], r_send.at[k, c], r_recv.at[k, c], (b, across)
        )

    def t_copy(c):
        return remote(r_in.at[0, c], s_in.at[c], t_send.at[c], t_recv.at[c], (b, to_end))

    def first_hop(k, c):
        @pl.when(jnp.logical_not(is_end))
        def _():
            own = part(owner(k), c)
            q_wait(k, c)
            r_out[k, c] = (own + times(q_in[k, c], we[...])).astype(low)
            r_copy(k, c).start()

    def last_hop(c):
        @pl.when(jnp.logical_not(is_end))
        def _():
            own = part(to_end, c)
            r_copy(0, c).wait_recv()
            r_in[0, c] = (r_in[0, c].astype(f32) + own).astype(low)
            t_copy(c).start()

    cores = (core_down, core_up, core_outw, core_qkvw)
    ones = (one_down, one_up, one_outw, one_qkvw)
    twos = (two_down, two_up, two_outw, two_qkvw)
    outs = (out_down, out_up)
    left = (hid, pre)
    right = (gf, n1)

    def who(slot):
        return b + (slot % 2) * (bx - b) + (slot // 2) * (by - b)

    def term(n, owner):
        at = pl.ds(pl.multiple_of(owner * group, group), group)
        return lax.dot_general(
            left[n][:, at], right[n][...], (((0,), (0,)), ((), ())), preferred_element_type=f32
        )

    def core_copy(n, slot):
        if n < 2:
            src = outs[n].at[slot]
        elif n == 2:
            src = full_outw.at[:, who(slot) + flip]
        else:
            src = full_qkvw.at[who(slot) + flip]
        return remote(src, cores[n].at[slot], c_send.at[n, slot], c_recv.at[n, slot], (bc, z))

    def give(n, slot):
        if n < 2:
            value = term(n, who(slot) + flip).astype(low)
            outs[n][slot] = value.reshape(outs[n].shape[1:])
        core_copy(n, slot).start()

    def keep(n, slot):
        if n < 2:
            own = term(n, who(slot)).reshape(outs[n].shape[1:])
        elif n == 2:
            own = full_outw[:, who(slot)].astype(f32)
        else:
            own = full_qkvw[who(slot)].astype(f32)
        core_copy(n, slot).wait_recv()
        cores[n][slot] = (cores[n][slot].astype(f32) + own).astype(low)

    def side_copy(n, dst, src):
        partner = by if n % 2 == 0 else bx
        return remote(
            cores[n].at[src], ones[n].at[dst], x_send.at[n, dst], x_recv.at[n, dst], (partner, z)
        )

    def small_group(n):
        def one(i, _):
            give(n, 3 - i)
            return 0

        lax.fori_loop(0, 4, one, 0)

    def small_keep(n):
        def one(i, _):
            keep(n, 3 - i)
            return 0

        lax.fori_loop(0, 4, one, 0)
        side_copy(n, 1, 3).start()
        side_copy(n, 0, 2 if n % 2 == 0 else 1).start()

    def half(h, _):
        def one(i, _):
            slot_up, slot_down = 3 - 2 * i - h, 3 - i - 2 * h
            give(1, slot_up)
            give(0, slot_down)
            keep(1, slot_up)

            @pl.when(h == 0)
            def _():
                side_copy(1, 1 - i, slot_up).start()

            keep(0, slot_down)

            @pl.when(h == 0)
            def _():
                side_copy(0, 1 - i, slot_down).start()

            return 0

        lax.fori_loop(0, 2, one, 0)

        @pl.when(h == 0)
        def _():
            for n in (4, 5, 6):
                loads[n].wait()
            first_hop(0, 0)

        return 0

    def one_event(n):
        second = 1 if n % 2 == 0 else 2
        partner, other = (by, bx) if n % 2 == 0 else (bx, by)
        ref = ones[n].at[1]
        remote(ref, ref, x_send.at[n, 1], x_recv.at[n, 1], (partner, z)).wait_recv()
        ones[n][1] = (ones[n][1].astype(f32) + cores[n][second].astype(f32)).astype(low)
        copy = remote(ones[n].at[1], twos[n], x_send.at[n, 2], x_recv.at[n, 2], (other, z))
        copy.start()
        issued.append(copy)

    e_bufs = (e_down, e_up, e_outw)
    g_bufs = (g_down, g_up, g_outw)
    h_bufs = (h_down, h_up, h_outw)

    def e_copy(n, k):
        return remote(
            twos[n].at[owner(k)], e_bufs[n].at[k], e_send.at[n, k], e_recv.at[n, k], (b, to_inner)
        )

    def e_wait(n, k):
        ref = e_bufs[n].at[k]
        remote(ref, ref, e_send.at[n, k], e_recv.at[n, k], (b, to_end)).wait_recv()

    def g_copy(n, k):
        return remote(
            e_bufs[n].at[k], g_bufs[n].at[k], g_send.at[n, k], g_recv.at[n, k], (b, across)
        )

    def h_copy(n):
        return remote(g_bufs[n].at[0], h_bufs[n], h_send.at[n], h_recv.at[n], (b, to_end))

    def two_event(n):
        partner, other = (by, bx) if n % 2 == 0 else (bx, by)
        ref = ones[n].at[0]
        remote(ref, ref, x_send.at[n, 0], x_recv.at[n, 0], (partner, z)).wait_recv()
        ref = twos[n]
        remote(ref, ref, x_send.at[n, 2], x_recv.at[n, 2], (other, z)).wait_recv()
        own = ones[n][0].astype(f32) + cores[n][0].astype(f32)
        if n == 3:
            own = twos[n][...].astype(f32) + own
            for i in range(3):
                qkvw_own[i] = own[:, i * width : (i + 1) * width]
            return
        twos[n][...] = (twos[n][...].astype(f32) + own).astype(low)

    def line_start(n, k):
        @pl.when(is_end)
        def _():
            e_copy(n, k).start()

    def line_across(n, k):
        @pl.when(jnp.logical_not(is_end))
        def _():
            e_wait(n, k)
            e_bufs[n][k] = (
                e_bufs[n][k].astype(f32) + twos[n][owner(k)].astype(f32)
            ).astype(low)
            g_copy(n, k).start()

    def line_back(n):
        @pl.when(jnp.logical_not(is_end))
        def _():
            g_copy(n, 0).wait_recv()
            g_bufs[n][0] = (
                g_bufs[n][0].astype(f32) + twos[n][to_end].astype(f32)
            ).astype(low)
            h_copy(n).start()

    def end_event(n):
        def write(value):
            out = (down_own, up_own, outw_own)[n]
            out[...] = jnp.transpose(value) if n == 2 else value

        @pl.when(is_end)
        def _():
            ref = h_bufs[n]
            remote(ref, ref, h_send.at[n], h_recv.at[n], (b, to_inner)).wait_recv()
            write(twos[n][z].astype(f32) + h_bufs[n][...].astype(f32))
            for k in range(3):
                e_copy(n, k).wait_send()

        @pl.when(jnp.logical_not(is_end))
        def _():
            g_copy(n, 1).wait_recv()
            e_wait(n, 2)
            write(
                twos[n][z].astype(f32)
                + g_bufs[n][1].astype(f32)
                + e_bufs[n][2].astype(f32)
            )
            for k in range(2):
                g_copy(n, k).wait_send()
            h_copy(n).wait_send()

    def projections():
        on, oh = full_outw.shape[2:]
        for s in range(4):
            value = jnp.transpose(mul(mx[s], ga[...]))
            full_outw[s] = value.astype(low).reshape(full_outw.shape[1:])
        acc_qkvw[...] = jnp.zeros_like(acc_qkvw)
        span = quarter

        def one(n, _):
            at = pl.ds(pl.multiple_of(n * span, span), span)
            acc_qkvw[...] += mul(gt[:, at], tok[at, :])
            return 0

        lax.fori_loop(0, 4, one, 0)
        full_qkvw[...] = jnp.transpose(acc_qkvw[...]).astype(low).reshape(full_qkvw.shape)

    @pl.when(is_end)
    def _():
        for k in range(3):
            for c in range(chunks):
                q_copy(k, c).start()

    for n in range(4):
        loads[n].wait()

    lax.fori_loop(0, 2, half, 0)
    first_hop(0, 1)
    one_event(1)
    one_event(0)
    first_hop(0, 2)
    last_hop(0)
    for n in (7, 8, 9):
        loads[n].wait()
    projections()
    first_hop(1, 0)
    last_hop(1)
    small_group(2)
    small_group(3)
    small_event(0)
    first_hop(1, 1)
    last_hop(2)
    small_keep(2)
    small_keep(3)
    small_event(1)
    first_hop(1, 2)
    two_event(1)
    line_start(1, 0)
    two_event(0)
    line_start(0, 0)
    line_start(1, 1)
    line_start(0, 1)
    small_event(2)
    one_event(2)
    one_event(3)
    small_event(3)
    two_event(2)
    for k in range(3):
        line_start(2, k)
    line_start(1, 2)
    line_start(0, 2)
    two_event(3)
    small_event(4)
    loads[10].wait()

    def own_rows(c, _):
        rows = pl.ds(pl.multiple_of(c * size, size), size)
        input_ref[rows, :] += part(z, c)

        @pl.when(is_end)
        def _():
            ref = s_in.at[c]
            remote(ref, ref, t_send.at[c], t_recv.at[c], (b, to_inner)).wait_recv()
            input_ref[rows, :] += s_in[c].astype(f32)

        @pl.when(jnp.logical_not(is_end))
        def _():
            r_copy(1, c).wait_recv()
            q_wait(2, c)
            input_ref[rows, :] += r_in[1, c].astype(f32) + times(q_in[2, c], we[...])

        return 0

    lax.fori_loop(0, chunks, own_rows, 0)
    for n, k in ((1, 0), (0, 0), (1, 1), (0, 1), (2, 0), (2, 1)):
        line_across(n, k)
        if k == 1:
            line_back(n)
    for n in (1, 0, 2):
        end_event(n)

    @pl.when(is_end)
    def _():
        for k in range(3):
            for c in range(chunks):
                q_copy(k, c).wait_send()

    @pl.when(jnp.logical_not(is_end))
    def _():
        for c in range(chunks):
            r_copy(0, c).wait_send()
            r_copy(1, c).wait_send()
            t_copy(c).wait_send()

    final = small_out.at[5]
    in_bias[...] = jnp.zeros_like(in_bias)
    index = b * 4 + z
    per_row = model // ff
    for n in range(bias_rows):

        @pl.when(index // per_row == n)
        def _():
            row = pltpu.roll(final[n : n + 1, :], (model - (index % per_row) * ff) % model, 1)
            in_bias[...] = row[:, :ff]

    share = vector_own.shape[1]
    vectors = final[at_vec : at_vec + 6, :]
    vector_own[...] = pltpu.roll(vectors, (model - index * share) % model, 1)[:, :share]
    for n in range(4):

        @pl.when(z == n)
        def _():
            qv_own[...] = final[at_qv + 2 * n : at_qv + 2 * n + 2, :width]
            conv_own[...] = final[at_conv + heads * n : at_conv + heads * (n + 1), :taps]

    ratio[...] = final[at_end : at_end + 1, 0:1] / final[at_end : at_end + 1, 1:2]

    for n in range(4):
        for dst in range(2):
            side_copy(n, dst, dst).wait_send()
        for slot in range(4):
            core_copy(n, slot).wait_send()
    for copy in issued:
        copy.wait_send()


def tail(
    lengths, gt, wq, we, hid, pre, n1, gf, ga, mx, tok, first, sums, bins, qv_grad, conv_grad, bound,
    taps,
):
    quarter, model = first.shape
    chunks = 3
    size = quarter // chunks
    ff = hid.shape[1] // 32
    width = mx.shape[1]
    heads = width // HEAD_DIM
    on, oh = model // 8, width
    qn, qh = model // 8, gt.shape[0]
    blocks = ((4, ff, model), (4, ff, model), (4, on, oh), (qn, qh))
    own = lambda *s: jax.ShapeDtypeStruct(s, f32)
    vm = lambda *s: pltpu.VMEM(s, low)
    dma = pltpu.SemaphoreType.DMA
    sources = (gt, wq, we, hid, pre, n1, gf, ga, mx, tok)
    small = -(-(bins.shape[1] // model + 15 + 4 * heads) // 8) * 8
    vmem = pl.BlockSpec(memory_space=pltpu.VMEM)
    return pl.pallas_call(
        tail_kernel,
        out_shape=[
            own(quarter, model), own(ff, model), own(ff, model), own(oh, on), own(3, qn, width),
            own(1, ff), own(6, model // 32), own(2, width), own(heads, taps), own(1, 1),
        ],
        in_specs=[pl.BlockSpec(memory_space=pltpu.SMEM)]
        + [pl.BlockSpec(memory_space=pl.ANY)] * 11
        + [vmem] * 5,
        out_specs=[vmem] * 10,
        scratch_shapes=[
            pltpu.VMEM((6, small, model), f32),
            *[vm(*x.shape) for x in sources],
            vm(3, chunks, qh, size), vm(2, chunks, size, model), vm(2, chunks, size, model),
            vm(chunks, size, model),
            vm(4, *blocks[0]), vm(4, *blocks[1]),
            vm(4, 8, on, oh), vm(8, qn, qh), pltpu.VMEM((qh, model), f32),
            *[vm(4, *s) for s in blocks],
            *[vm(2, *s) for s in blocks],
            *[vm(*s) for s in blocks],
            *[vm(3, *s[1:]) for s in blocks[:3]],
            *[vm(2, *s[1:]) for s in blocks[:3]],
            *[vm(*s[1:]) for s in blocks[:3]],
            pltpu.VMEM((5, small, model), f32),
            dma((11,)),
            dma((3, chunks)), dma((3, chunks)), dma((2, chunks)), dma((2, chunks)),
            dma((chunks,)), dma((chunks,)), dma((4, 4)), dma((4, 4)),
            dma((4, 3)), dma((4, 3)), dma((3, 3)), dma((3, 3)), dma((3, 2)), dma((3, 2)),
            dma((3,)), dma((3,)), dma((5,)), dma((5,)),
        ],
        compiler_params=pltpu.CompilerParams(
            collective_id=3, has_side_effects=True, vmem_limit_bytes=63 * 1024 * 1024
        ),
        name="tail",
    )(lengths, *sources, first, sums, bins, qv_grad, conv_grad, bound)


def cumulative(x):
    t = 1.0 / (1.0 + 0.23164189 * jnp.abs(x))
    density = jnp.exp(-0.5 * x * x) * 0.3989422804
    poly = t * (
        0.319381530 + t * (-0.356563782 + t * (1.781477937 + t * (-1.821255978 + t * 1.330274429)))
    )
    upper = density * poly
    return jnp.where(x >= 0.0, 1.0 - upper, upper), density


def normed(x):
    centre = x - jnp.mean(x, axis=1, keepdims=True)
    scale = lax.rsqrt(jnp.mean(centre * centre, axis=1, keepdims=True) + norm_eps)
    return centre * scale, scale


def norm_back(grad, gain, rows, scale):
    e = grad * gain
    return scale * (
        e - jnp.mean(e, axis=1, keepdims=True) - rows * jnp.mean(e * rows, axis=1, keepdims=True)
    )


def middle_kernel(
    share,
    mixed_ref, own0, own1, own2, own3, tok_hbm, cot_hbm, weight_hbm,
    vec_ref,
    out_hbm, first_hbm, attn_hbm, hidden_hbm, pre_hbm, norm_hbm, ffn_hbm, all_ref, grad_ref,
    sums_ref, bin_ref, end_hbm,
    out_ref, first_ref, attn_ref, hidden_ref, pre_ref, norm_ref, ffn_ref, tok_ref, cot_ref,
    packs, wof, wo, slope, total, n1_ref, scale_ref, turned,
    a_send, a_recv, f_send, f_recv, s_send, s_recv, p_send, p_recv, g_send, g_recv,
    own_sem, own_turn, out_sem, w_send, w_recv,
):
    b, z, bc, bx, by = place()
    both = bx + by - b
    flip = bc - b
    peers = [(b, lax.rem(z + i, 4)) for i in (1, 2, 3)]
    width, quarter = all_ref.shape[1:]
    model = tok_hbm.shape[1]
    owns = (own0, own1, own2, own3)
    origins = [lax.rem(z + 4 - i, 4) for i in range(4)]
    size = turned.shape[2]
    tiles = quarter // size
    issued = []

    def own_columns(n):
        return pl.ds(pl.multiple_of(n * quarter, quarter), quarter)

    local = [
        pltpu.make_async_copy(own, packs.at[b, origin], own_sem.at[i])
        for i, (own, origin) in enumerate(zip(owns, origins))
    ]
    local.append(
        pltpu.make_async_copy(mixed_ref.at[:, own_columns(z)], all_ref.at[z], own_sem.at[4])
    )
    local.append(
        pltpu.make_async_copy(
            tok_hbm.at[pl.ds(pl.multiple_of(z * quarter, quarter), quarter)], tok_ref, own_sem.at[5]
        )
    )
    cot_load = pltpu.make_async_copy(cot_hbm, cot_ref, own_sem.at[6])
    for copy in local:
        copy.start()
    cot_load.start()
    greet(peers + [(bc, z), (bx, z), (by, z)])

    ff = (packs.shape[2] - 32) // 2
    half = ff // 2
    pieces = ((2 * ff, 32), (0, half), (half, half), (ff, ff))
    through_y = (True, True, True, False)
    count = len(pieces)

    def rows_of(n):
        return pl.ds(*pieces[n])

    def mix_copy(r, i):
        to = lax.rem(z + i, 4)
        src = mixed_ref.at[:, pl.ds(pl.multiple_of(to * quarter + r * size, size), size)]
        return remote(
            src, all_ref.at[z, :, pl.ds(r * size, size)], a_send.at[r, i - 1], a_recv.at[r, i - 1],
            (b, to),
        )

    def side(n, axis):
        out = []
        for i in range(4):
            out.append(
                remote(
                    owns[i].at[rows_of(n)], packs.at[b, origins[i], rows_of(n)],
                    f_send.at[n, axis, i], f_recv.at[n, axis, i], (by if axis else bx, z),
                )
            )
        return out

    def side_start(n):
        for axis in (0, 1):
            for copy in side(n, axis):
                copy.start()
                issued.append(copy)

    def block(n, who):
        return packs.at[who, :, rows_of(n)]

    def corner(n):
        who, device = (bx, by) if through_y[n] else (by, bx)
        return remote(block(n, who), block(n, who), s_send.at[n], s_recv.at[n], (device, z))

    def mate(n, slot, who):
        return remote(
            block(n, who), block(n, who), p_send.at[n, slot], p_recv.at[n, slot], (bc, z)
        )

    def mate_start(n, slot, who):
        mate(n, slot, who).start()

    def side_wait(n, axis):
        who = by if axis else bx
        for i in range(4):
            ref = packs.at[who, origins[i], rows_of(n)]
            remote(
                ref, ref, f_send.at[n, axis, i], f_recv.at[n, axis, i], (who, z)
            ).wait_recv()
        if through_y[n] == (axis == 0):
            corner(n).start()
        mate_start(n, 1 + axis, who)

    def corner_wait(n):
        device = by if through_y[n] else bx
        ref = block(n, both)
        remote(ref, ref, s_send.at[n], s_recv.at[n], (device, z)).wait_recv()
        mate_start(n, 3, both)

    def mate_wait(n, slot, who):
        mate(n, slot, who + flip).wait_recv()

    side_start(0)
    side_start(1)
    for r in range(tiles):
        for i in (1, 2, 3):
            copy = mix_copy(r, i)
            copy.start()
            issued.append(copy)
    is_end = (z == 0) | (z == 3)
    end_copy = remote(
        weight_hbm, end_hbm, w_send.at[0], w_recv.at[0], (b, jnp.where(z < 2, 1, 2))
    )

    @pl.when(is_end)
    def _():
        end_copy.start()

    for copy in local:
        copy.wait()
    for n in range(count):
        mate_start(n, 0, b)
    out_bias, gain1, shift1, down_bias, gain2, shift2 = [
        vec_ref[n : n + 1, :] for n in range(6)
    ]
    sums_ref[...] = jnp.zeros_like(sums_ref)
    bin_ref[...] = jnp.zeros_like(bin_ref)
    total[...] = jnp.zeros_like(total)
    side_wait(0, 0)
    side_wait(0, 1)
    side_start(2)
    side_start(3)
    corner_wait(0)
    for slot, who in enumerate((b, bx, by, both)):
        mate_wait(0, slot, who)
    group = 4 * ff
    for q in range(8):
        for s in range(4):
            wof[pl.ds(s * width + q * share, share), :] = packs[
                q, s, pl.ds(2 * ff, share), :
            ].astype(f32)
    wo[...] = wof[...].astype(low).reshape(wo.shape)
    for q in range(8):
        row = jnp.zeros((1, group), f32)
        for s in range(4):
            row = row + packs[q, s, 2 * ff + share : 2 * ff + share + 1, :group].astype(f32)
        bin_ref[1:2, q * group : (q + 1) * group] = row

    def row_sum(n, x):
        sums_ref[n : n + 1, :] += jnp.sum(x, axis=0, keepdims=True)

    def first_rows(r, _):
        rows = pl.ds(pl.multiple_of(r * size, size), size)

        @pl.when(r == 1)
        def _():
            side_wait(1, 0)
            side_wait(1, 1)

        @pl.when(r == 2)
        def _():
            side_wait(2, 0)
            side_wait(2, 1)

        for i in (1, 2, 3):
            ref = all_ref.at[origins[i], :, rows]
            remote(
                ref, ref, a_send.at[r, i - 1], a_recv.at[r, i - 1], (b, origins[i])
            ).wait_recv()
        attn = jnp.zeros((size, model), f32)
        for s in range(4):
            attn = attn + lax.dot_general(
                all_ref[s, :, rows], wo[s], (((0,), (0,)), ((), ())), preferred_element_type=f32
            )
        n1, scale1 = normed(tok_ref[rows, :].astype(f32) + attn + out_bias)
        n1_ref[rows, :] = n1
        scale_ref[rows, :] = jnp.broadcast_to(scale1, (size, scale_ref.shape[1]))
        norm_ref[rows, :] = (n1 * gain1 + shift1).astype(low)
        return 0

    span = 2 * group

    def weights(c, start):
        return jnp.concatenate(
            [
                packs[2 * c + n, :, pl.ds(start, ff), :].reshape(group, model)
                for n in range(2)
            ],
            axis=0,
        )

    def tile_rows(r):
        return pl.ds(pl.multiple_of(r * size, size), size)

    def feed(who):
        c = who // 2
        lanes = pl.ds(pl.multiple_of(c * span, span), span)

        def one(r, _):
            rows = tile_rows(r)
            act = mul_t(norm_ref[rows, :], weights(c, 0)) + bin_ref[1:2, lanes]
            phi, density = cumulative(act)
            hidden = (act * phi).astype(low)
            hidden_ref[rows, lanes] = hidden
            slope[rows, lanes] = phi + act * density
            total[rows, :] += mul(hidden, weights(c, ff))
            return 0

        lax.fori_loop(0, tiles, one, 0)

    lax.fori_loop(0, tiles, first_rows, 0)

    def group_step(k, _):
        def mates(slot, who):
            for n in range(1, count):
                mate_wait(n, slot, who)

        @pl.when(k == 0)
        def _():
            mates(0, b)

        @pl.when(k == 1)
        def _():
            side_wait(3, 0)
            side_wait(3, 1)
            mates(1, bx)

        @pl.when(k == 2)
        def _():
            corner_wait(1)
            mates(2, by)

        @pl.when(k == 3)
        def _():
            corner_wait(2)
            corner_wait(3)
            mates(3, both)

        feed(b + (k % 2) * (bx - b) + (k // 2) * (by - b))
        return 0

    lax.fori_loop(0, 4, group_step, 0)

    def turn_copy(r, i):
        to = lax.rem(z + i, 4)
        src = turned.at[r, pl.ds(pl.multiple_of(to * width, width), width)]
        dst = grad_ref.at[:, pl.ds(pl.multiple_of(z * quarter + r * size, size), size)]
        return remote(src, dst, g_send.at[r, i - 1], g_recv.at[r, i - 1], (b, to))

    def turn_own(r):
        src = turned.at[r, pl.ds(pl.multiple_of(z * width, width), width)]
        dst = grad_ref.at[:, pl.ds(pl.multiple_of(z * quarter + r * size, size), size)]
        return pltpu.make_async_copy(src, dst, own_turn.at[r])

    stores = (
        (out_ref, out_hbm), (first_ref, first_hbm), (attn_ref, attn_hbm), (pre_ref, pre_hbm),
        (ffn_ref, ffn_hbm), (hidden_ref, hidden_hbm), (norm_ref, norm_hbm),
    )

    def store(r, n):
        src, dst = stores[n]
        rows = tile_rows(r)
        return pltpu.make_async_copy(src.at[rows], dst.at[rows], out_sem.at[r, n])

    cot_load.wait()

    def row_tile(r, _):
        rows = tile_rows(r)
        n1 = n1_ref[rows, :]
        norm1 = n1 * gain1 + shift1
        n2, scale2 = normed(norm1 + total[rows, :] + down_bias)
        out_ref[rows, :] = (n2 * gain2 + shift2).astype(low)
        cot = cot_ref[rows, :].astype(f32)
        row_sum(1, cot * n2)
        row_sum(2, cot)
        grad2 = norm_back(cot, gain2, n2, scale2)
        grad_low = grad2.astype(low)
        ffn_ref[rows, :] = grad_low
        row_sum(0, grad_low.astype(f32))
        total[rows, :] = grad2

        def backward(c, _):
            lanes = pl.ds(pl.multiple_of(c * span, span), span)
            grad = (slope[rows, lanes] * mul_t(grad_low, weights(c, ff))).astype(low)
            pre_ref[rows, lanes] = grad
            bin_ref[0:1, lanes] += jnp.sum(grad.astype(f32), axis=0, keepdims=True)
            total[rows, :] += mul(grad, weights(c, 0))
            return 0

        lax.fori_loop(0, 4, backward, 0)
        grad1 = total[rows, :]
        row_sum(3, grad1 * n1)
        row_sum(4, grad1)
        first = norm_back(grad1, gain1, n1, scale_ref[rows, 0:1])
        first_ref[rows, :] = first
        attn_low = first.astype(low)
        attn_ref[rows, :] = attn_low
        row_sum(5, attn_low.astype(f32))
        for s in range(4):
            turned[r, pl.ds(s * width, width), :] = mul_t(wo[s], attn_low).astype(low)
        for i in (1, 2, 3):
            turn_copy(r, i).start()
        turn_own(r).start()
        for n in range(len(stores)):
            store(r, n).start()
        return 0

    lax.fori_loop(0, tiles, row_tile, 0)

    def finish(r, _):
        for i in (1, 2, 3):
            source = origins[i]
            ref = grad_ref.at[:, pl.ds(pl.multiple_of(source * quarter + r * size, size), size)]
            remote(ref, ref, g_send.at[r, i - 1], g_recv.at[r, i - 1], (b, source)).wait_recv()
            turn_copy(r, i).wait_send()
        turn_own(r).wait()
        for n in range(len(stores)):
            store(r, n).wait()
        return 0

    lax.fori_loop(0, tiles, finish, 0)

    @pl.when(is_end)
    def _():
        end_copy.wait_send()

    @pl.when(jnp.logical_not(is_end))
    def _():
        remote(
            end_hbm, end_hbm, w_send.at[0], w_recv.at[0], (b, jnp.where(z < 2, 0, 3))
        ).wait_recv()

    for n in range(count):
        corner(n).wait_send()
        for slot, who in enumerate((b, bx, by, both)):
            mate(n, slot, who).wait_send()
    for copy in issued:
        copy.wait_send()


def ffn_middle(mixed_t, packs, tokens, cot, weight_t, vectors, ff, share):
    width, tok_count = mixed_t.shape
    quarter, model = tok_count // 4, tokens.shape[1]
    size = quarter // 3
    rows = packs[0].shape[0]
    shape = jax.ShapeDtypeStruct
    vmem = pl.BlockSpec(memory_space=pltpu.VMEM)
    hbm = pl.BlockSpec(memory_space=pl.ANY)
    dma = pltpu.SemaphoreType.DMA
    kept = [
        ((quarter, model), low),
        ((quarter, model), f32),
        ((quarter, model), low),
        ((quarter, 32 * ff), low),
        ((quarter, 32 * ff), low),
        ((quarter, model), low),
        ((quarter, model), low),
    ]
    return pl.pallas_call(
        partial(middle_kernel, share),
        out_shape=[shape(*x) for x in kept]
        + [
            shape((4, width, quarter), low),
            shape((width, tok_count), low),
            shape((8, model), f32),
            shape((8, 32 * ff), f32),
            shape(weight_t.shape, low),
        ],
        in_specs=[hbm] + [vmem] * 4 + [hbm] * 3 + [vmem],
        out_specs=[hbm] * 7 + [vmem, hbm, vmem, vmem, hbm],
        scratch_shapes=[pltpu.VMEM(*x) for x in kept]
        + [
            pltpu.VMEM((quarter, model), low),
            pltpu.VMEM((quarter, model), low),
            pltpu.VMEM((8, 4, rows, model), low),
            pltpu.VMEM((4 * width, model), f32),
            pltpu.VMEM((4, width, model), low),
            pltpu.VMEM((quarter, 32 * ff), f32),
            pltpu.VMEM((quarter, model), f32),
            pltpu.VMEM((quarter, model), f32),
            pltpu.VMEM((quarter, 128), f32),
            pltpu.VMEM((3, 4 * width, size), low),
            dma((3, 3)), dma((3, 3)), dma((4, 2, 4)), dma((4, 2, 4)), dma((4,)), dma((4,)),
            dma((4, 4)), dma((4, 4)), dma((3, 3)), dma((3, 3)),
            dma((7,)), dma((3,)), dma((3, 7)), dma((1,)), dma((1,)),
        ],
        compiler_params=pltpu.CompilerParams(
            collective_id=1, has_side_effects=True, vmem_limit_bytes=63 * 1024 * 1024
        ),
        name="middle",
    )(mixed_t, *packs, tokens, cot, weight_t, vectors)


def settle_kernel(*refs):
    count = len(refs) // 2
    for n in range(count):
        refs[count + n][...] = refs[n][...]


def settle(*arrays):
    steps = 4
    tall = arrays[0].shape[0]

    def spec(x):
        if x.shape[0] == tall:
            return pl.BlockSpec((tall // steps, *x.shape[1:]), lambda n: (n, 0))
        return pl.BlockSpec(x.shape, lambda n: (0,) * x.ndim)

    return pl.pallas_call(
        settle_kernel,
        grid=(steps,),
        out_shape=[jax.ShapeDtypeStruct(x.shape, x.dtype) for x in arrays],
        in_specs=[spec(x) for x in arrays],
        out_specs=[spec(x) for x in arrays],
        name="settle",
    )(*arrays)


def slice_body(
    tokens,
    qkv_weight,
    qv_bias,
    conv_weight,
    out_weight,
    out_bias,
    norm1_gain,
    norm1_bias,
    ffn_in_weight,
    ffn_in_bias,
    ffn_out_weight,
    ffn_out_bias,
    norm2_gain,
    norm2_bias,
    cotangent,
    seq_lengths,
    segment_ids,
    landmark_bounds,
):
    model = tokens.shape[1]
    width = qkv_weight.shape[2]
    kernel_taps = conv_weight.shape[1]
    slots, marks = landmark_bounds.shape
    z = lax.axis_index("heads")
    b = lax.axis_index("batch")
    weight_t = jnp.transpose(qkv_weight.reshape(model, 3 * width))
    ff_own = ffn_out_weight.shape[0]
    share = width // 8
    bias_row = lax.dynamic_update_slice_in_dim(
        jnp.zeros((4 * ff_own,), low), ffn_in_bias, z * ff_own, 0
    )
    misc_own = jnp.concatenate(
        [
            lax.dynamic_slice_in_dim(out_weight, b * share, share, 0),
            jnp.zeros((32 - share, model), low).at[0, : 4 * ff_own].set(bias_row),
        ],
        axis=0,
    )
    pack = jnp.concatenate([jnp.transpose(ffn_in_weight), ffn_out_weight, misc_own], axis=0)
    packs = [pack] + [
        lax.ppermute(pack, "heads", [(n, (n + i) % 4) for n in range(4)]) for i in (1, 2, 3)
    ]
    forward = mix_forward(
        seq_lengths, tokens, weight_t, qv_bias, conv_weight, slots, marks
    )
    qkv_t, first, last, mixed_t, mark, value, inner, denom, middle, steps, inverse, bound = forward
    vectors = jnp.stack(
        [out_bias, norm1_gain, norm1_bias, ffn_out_bias, norm2_gain, norm2_bias]
    )
    (
        final_low, grad_first, grad_attn_low, hidden_low, grad_pre, norm1_low, grad_ffn_low,
        mixed_all, grad_mix_t, vector_sums, bias_sums, weight_end,
    ) = ffn_middle(mixed_t, packs, tokens, cotangent, weight_t, vectors, ff_own, share)
    saved = (qkv_t, first, last, mark, value, inner, denom, middle, steps, inverse)
    grad_t, grad_bias, grad_conv = mix_backward(
        seq_lengths, grad_mix_t, saved, conv_weight, slots, marks
    )
    (
        input_grad, down_share, up_share, out_share, qkv_share,
        in_bias_share, vector_share, bias_out, conv_out, condition,
    ) = tail(
        seq_lengths, grad_t, weight_t, weight_end, hidden_low, grad_pre, norm1_low, grad_ffn_low,
        grad_attn_low, mixed_all, tokens, grad_first, vector_sums, bias_sums, grad_bias,
        grad_conv, bound, kernel_taps,
    )
    (
        final_low, input_grad, down_share, up_share, out_share, qkv_share,
        in_bias_share, vector_share, bias_out, conv_out, condition,
    ) = settle(
        final_low, input_grad, down_share, up_share, out_share, qkv_share,
        in_bias_share, vector_share, bias_out, conv_out, condition,
    )
    return (
        final_low,
        input_grad,
        jnp.swapaxes(qkv_share, 0, 1),
        bias_out,
        conv_out,
        out_share,
        jnp.transpose(up_share),
        in_bias_share.reshape(ff_own),
        down_share,
        vector_share,
        condition.reshape(()),
    )


def solution(mesh):
    chosen = slice_body if dict(mesh.shape) == {"batch": 8, "heads": 4} else body
    in_specs = (
        P("batch", None),
        P(None, None, "heads"),
        P(),
        P(),
        P("heads", None),
        P(),
        P(),
        P(),
        P(None, ("batch", "heads")),
        P(("batch", "heads")),
        P(("batch", "heads"), None),
        P(),
        P(),
        P(),
        P(("batch", "heads"), None),
        P("batch"),
        P("batch"),
        P("batch", None),
    )
    out_specs = (
        P(("batch", "heads"), None),
        P(("batch", "heads"), None),
        P("batch", None, "heads"),
        P(None, "heads"),
        P("heads", None),
        P("heads", "batch"),
        P(None, ("batch", "heads")),
        P(("batch", "heads")),
        P(("batch", "heads"), None),
        P(None, ("batch", "heads")),
        P(),
    )
    return jax.shard_map(chosen, mesh=mesh, in_specs=in_specs, out_specs=out_specs, check_vma=False)
```

```python
from functools import partial

import jax
import jax.numpy as jnp
from jax import lax
from jax.experimental import pallas as pl
from jax.experimental.pallas import tpu as pltpu
from jax.sharding import PartitionSpec as P

HEAD_DIM = 64
PINV_ITERS = 6
TILE = 512
SUB = 128

f32 = jnp.float32
low = jnp.bfloat16
mask_fill = -1000000000.0


def split(x):
    high = x.astype(low)
    return high, (x - high.astype(f32)).astype(low)


def mul(a, b):
    return lax.dot_general(a, b, (((1,), (0,)), ((), ())), preferred_element_type=f32)


def mul_t(a, b):
    return lax.dot_general(a, b, (((1,), (1,)), ((), ())), preferred_element_type=f32)


def wide(form, left, right):
    left_high, left_low = split(left)
    right_high, right_low = split(right)
    return form(left_high, right_high) + (
        form(left_high, right_low) + form(left_low, right_high)
    )


def block_grid(rows, cols):
    row_block = lax.broadcasted_iota(jnp.int32, (rows, cols), 0) // HEAD_DIM
    col_block = lax.broadcasted_iota(jnp.int32, (rows, cols), 1) // HEAD_DIM
    return row_block == col_block


def spread(x, blocks):
    count = blocks.shape[0] // x.shape[0]
    return jnp.where(blocks, jnp.concatenate([x] * count, axis=0), jnp.zeros_like(x[:1, :1]))


def fold(x, blocks):
    kept = jnp.where(blocks, x, jnp.zeros_like(x[:1, :1]))
    rows = HEAD_DIM
    out = kept[:rows]
    for n in range(1, x.shape[0] // rows):
        out = out + kept[n * rows : (n + 1) * rows]
    return out


def ready(x, ones):
    count = ones.shape[0] // HEAD_DIM
    high, rest = split(x)
    return [jnp.concatenate([part] * count, axis=0) * ones for part in (high, rest)]


def pack_mul(lefts, right, form=mul):
    halves = [split(x) for x in lefts]
    high = [x[0] for x in halves]
    count = len(lefts)
    both_parts = form(jnp.concatenate(high + [x[1] for x in halves], axis=0), right[0])
    rest = form(jnp.concatenate(high, axis=0), right[1])
    out = []
    for n in range(count):
        at = slice(n * HEAD_DIM, (n + 1) * HEAD_DIM)
        more = slice((count + n) * HEAD_DIM, (count + n + 1) * HEAD_DIM)
        out.append(both_parts[at] + (both_parts[more] + rest[at]))
    return out


def block_ones(size):
    return jnp.where(block_grid(size, size), 1.0, 0.0).astype(low)


def slot_bounds(len_ref, s, slots):
    start = jnp.int32(0)
    for n in range(slots):
        start = start + jnp.where(n < s, len_ref[n], 0)
    return start, start + len_ref[s]


def eye_pack(width):
    row = lax.broadcasted_iota(jnp.int32, (HEAD_DIM, width), 0)
    col = lax.broadcasted_iota(jnp.int32, (HEAD_DIM, width), 1) % HEAD_DIM
    return jnp.where(row == col, 1.0, 0.0).astype(f32)


def lane_mask(start, end, at, width):
    tok = at + lax.broadcasted_iota(jnp.int32, (1, width), 1)
    return (tok >= start) & (tok < end)


def band(taps_row, width):
    row = lax.broadcasted_iota(jnp.int32, (SUB, 3 * SUB), 0)
    col = lax.broadcasted_iota(jnp.int32, (SUB, 3 * SUB), 1)
    off = col - row - (SUB - width // 2)
    out = jnp.zeros((SUB, 3 * SUB), f32)
    for n in range(width):
        out = jnp.where(off == n, taps_row[:, n : n + 1], out)
    return out


def slot_marks(len_ref, at, slots, marks, width):
    rows = slots * marks
    row = lax.broadcasted_iota(jnp.int32, (rows, 1), 0)
    slot = row // marks
    mark = row % marks
    start = jnp.zeros((rows, 1), jnp.int32)
    length = jnp.zeros((rows, 1), jnp.int32)
    for n in range(slots):
        start = start + jnp.where(slot > n, len_ref[n], 0)
        length = jnp.where(slot == n, len_ref[n], length)
    lower = start + (mark * length) // marks
    upper = start + ((mark + 1) * length) // marks
    inv_count = 1.0 / jnp.maximum((upper - lower).astype(f32), 1.0)
    tok = at + lax.broadcasted_iota(jnp.int32, (rows, width), 1)
    member = jnp.where((tok >= lower) & (tok < upper), 1.0, 0.0)
    return member, inv_count


def mix_forward_kernel(
    slots, marks, taps,
    len_ref, tok_ref, weight_ref, bias_ref, conv_ref,
    qkv_hbm, first_hbm, last_hbm, mixed_ref, mark_ref, value_ref, inner_ref,
    denom_ref, middle_ref, steps_hbm, inverse_ref, bound_ref,
    qkv_ref, first_ref, last_ref, steps_ref,
    vpad, scores, vsum, bias_col, conv_own, out_sem,
):
    step = pl.program_id(0)
    width = first_ref.shape[0]
    heads = width // HEAD_DIM
    tok_count = qkv_ref.shape[1]
    tiles = tok_count // TILE
    packed = slots * marks
    at = pl.multiple_of(step * TILE, TILE)

    @pl.when(step == 0)
    def _():
        z = lax.axis_index("heads")
        own_taps(conv_own, conv_ref, z)
        columns = jnp.transpose(jnp.concatenate([bias_ref[...], bias_ref[...]], axis=0))
        bias_col[: bias_ref.shape[1], :] = columns
        mark_ref[...] = jnp.zeros_like(mark_ref)
        vsum[...] = jnp.zeros_like(vsum)
        vpad[:, :SUB] = jnp.zeros((width, SUB), low)
        vpad[:, tok_count + SUB :] = jnp.zeros((width, SUB), low)

    at_head = pl.ds(pl.multiple_of(lax.axis_index("heads") * width, HEAD_DIM), width)
    rows = mul_t(weight_ref[...], tok_ref[...])
    rows = jnp.concatenate(
        [
            rows[:width] + bias_col[at_head, 0:1],
            rows[width : 2 * width],
            rows[2 * width :] + bias_col[at_head, 1:2],
        ],
        axis=0,
    ).astype(low)
    qkv_ref[:, pl.ds(at, TILE)] = rows
    vpad[:, pl.ds(pl.multiple_of(at + SUB, SUB), TILE)] = rows[2 * width :]
    member, inv_count = slot_marks(len_ref, at, slots, marks, TILE)
    mark_ref[...] += mul_t(member.astype(low), rows[: 2 * width])
    vsum[...] += mul_t(jnp.ones((8, TILE), low), rows[2 * width :])
    first_ref[:, pl.ds(at, TILE)] = jnp.zeros((width, TILE), low)
    last_ref[:, pl.ds(at, TILE)] = jnp.zeros((width, TILE), low)
    mixed_ref[:, pl.ds(at, TILE)] = jnp.zeros((width, TILE), low)

    leaving = [
        pltpu.make_async_copy(src, dst, out_sem.at[n])
        for n, (src, dst) in enumerate(
            (
                (qkv_ref, qkv_hbm), (steps_ref, steps_hbm), (first_ref, first_hbm),
                (last_ref, last_hbm),
            )
        )
    ]

    @pl.when(step == tiles - 1)
    def _():
        leaving[0].start()
        mark_ref[...] = mark_ref[...] * inv_count
        head_blocks = block_grid(width, width)
        slot_blocks = block_grid(packed, packed)
        ones = block_ones(packed)
        eye = eye_pack(packed)
        scale = HEAD_DIM ** -0.5

        middles, inverses_t, products = [], [], []
        bound_total = jnp.zeros((1, 1), f32)
        lane_slot = lax.broadcasted_iota(jnp.int32, (1, packed), 1) // marks
        for h in range(heads):
            q_marks = mark_ref[:, h * HEAD_DIM : (h + 1) * HEAD_DIM]
            k_marks = mark_ref[:, width + h * HEAD_DIM : width + (h + 1) * HEAD_DIM]
            sim = wide(mul_t, q_marks, k_marks) * scale
            sim = jnp.where(slot_blocks, sim, -1e30)
            sim = jnp.exp(sim - jnp.max(sim, axis=1, keepdims=True))
            sim = sim / jnp.sum(sim, axis=1, keepdims=True)
            middle = fold(sim, slot_blocks)
            col_sums = jnp.sum(middle, axis=0, keepdims=True)
            bound = jnp.zeros((1, packed), f32)
            for s in range(slots):
                top = jnp.max(jnp.where(lane_slot == s, col_sums, 0.0), axis=1, keepdims=True)
                bound = jnp.where(lane_slot == s, top, bound)
                bound_total += jnp.where(len_ref[s] > 0, top, 0.0)
            middle_ref[h] = middle
            middles.append(middle)
            inverses_t.append(middle / bound)
            products.append(pack_mul([middle], ready(middle, ones), mul_t)[0] / bound)
        bound_ref[...] = jnp.broadcast_to(bound_total, bound_ref.shape)

        def newton(n, carry):
            out = []
            for h in range(heads):
                before_t, weight, product = carry[h]
                (inverse_t,) = pack_mul([0.25 * weight], ready(before_t, ones))
                (square,) = pack_mul([product], ready(product, ones))
                cube, fourth = pack_mul([product, square], ready(square, ones))
                third = 13.0 * eye - 15.0 * product + 7.0 * square - cube
                steps_ref[n, 0, h] = product
                steps_ref[n, 1, h] = square
                steps_ref[n, 2, h] = third
                steps_ref[n, 3, h] = inverse_t
                after = 0.25 * (13.0 * product - 15.0 * square + 7.0 * cube - fourth)
                out.append((inverse_t, third, after))
            return tuple(out)

        start = tuple((x, 4.0 * eye, p) for x, p in zip(inverses_t, products))
        final = lax.fori_loop(0, PINV_ITERS, newton, start)
        for h in range(heads):
            inverse_t, third, _ = final[h]
            inverse_ref[h] = pack_mul([0.25 * third], ready(inverse_t, ones))[0]
        leaving[1].start()

        def one_slot(s, _):
            start, end = slot_bounds(len_ref, s, slots)
            lo, hi = start // TILE, (end + TILE - 1) // TILE
            hi = jnp.where(end > start, hi, lo)
            own = mark_ref[pl.ds(pl.multiple_of(s * marks, marks), marks), :] * scale
            q_block = spread(own[:, :width], head_blocks).astype(low)
            k_block = spread(own[:, width:], head_blocks).astype(low)

            def score_tile(n, top):
                t = pl.multiple_of(n * TILE, TILE)
                mask = lane_mask(start, end, t, TILE)
                sim = mul(k_block, qkv_ref[:width, pl.ds(t, TILE)])
                sim = sim.reshape(heads, marks, TILE)
                sim = jnp.exp(sim - jnp.max(sim, axis=1, keepdims=True))
                sim = sim / jnp.sum(sim, axis=1, keepdims=True)
                sim = sim.reshape(width, TILE)
                old = first_ref[:, pl.ds(t, TILE)].astype(f32)
                first_ref[:, pl.ds(t, TILE)] = jnp.where(mask, sim, old).astype(low)
                sim = mul(q_block, qkv_ref[width : 2 * width, pl.ds(t, TILE)])
                sim = jnp.where(mask, sim, mask_fill)
                scores[:, pl.ds(t, TILE)] = sim
                for c in range(TILE // SUB):
                    top = jnp.maximum(top, sim[:, c * SUB : (c + 1) * SUB])
                return top

            top = lax.fori_loop(lo, hi, score_tile, jnp.full((width, SUB), mask_fill, f32))
            top = jnp.max(top, axis=1, keepdims=True)

            def value_tile(n, carry):
                denom, total = carry
                t = pl.multiple_of(n * TILE, TILE)
                mask = lane_mask(start, end, t, TILE)
                part = jnp.exp(scores[:, pl.ds(t, TILE)] - top)
                old = last_ref[:, pl.ds(t, TILE)].astype(f32)
                last_ref[:, pl.ds(t, TILE)] = jnp.where(mask, part, old).astype(low)
                total = total + mul_t(part.astype(low), qkv_ref[2 * width :, pl.ds(t, TILE)])
                for c in range(TILE // SUB):
                    denom = denom + part[:, c * SUB : (c + 1) * SUB]
                return denom, total

            denom, total = lax.fori_loop(
                lo, hi, value_tile,
                (jnp.zeros((width, SUB), f32), jnp.zeros((width, width), f32)),
            )
            denom = jnp.sum(denom, axis=1, keepdims=True)
            inv = 1.0 / jnp.where(denom > 0.0, denom, 1.0)
            denom_ref[s] = inv
            values = fold(total * inv, head_blocks)
            values = jnp.where(end > start, values, vsum[:1] / tok_count)
            value_ref[pl.ds(pl.multiple_of(s * marks, marks), marks), :] = values
            return 0

        lax.fori_loop(0, slots, one_slot, 0)
        leaving[2].start()
        leaving[3].start()

        lane_head = lax.broadcasted_iota(jnp.int32, (1, width), 1) // HEAD_DIM
        inner = jnp.zeros((packed, width), f32)
        for h in range(heads):
            (inverse,) = pack_mul([eye], ready(inverse_ref[h], ones), mul_t)
            own_values = jnp.where(lane_head == h, value_ref[...], 0.0)
            inner = inner + wide(mul, spread(inverse, slot_blocks), own_values)
        inner_ref[...] = inner

        bands = [band(conv_own[h : h + 1, :], taps).astype(low) for h in range(heads)]

        def out_slot(s, _):
            start, end = slot_bounds(len_ref, s, slots)
            lo, hi = start // TILE, (end + TILE - 1) // TILE
            hi = jnp.where(end > start, hi, lo)
            own = inner_ref[pl.ds(pl.multiple_of(s * marks, marks), marks), :]
            a_block = jnp.transpose(spread(own, head_blocks)).astype(low)

            def out_tile(n, _):
                t = pl.multiple_of(n * TILE, TILE)
                mask = lane_mask(start, end, t, TILE)
                rows = mul(a_block, first_ref[:, pl.ds(t, TILE)])
                rows = rows + convolve(vpad, bands, start, end, t, heads)
                old = mixed_ref[:, pl.ds(t, TILE)].astype(f32)
                mixed_ref[:, pl.ds(t, TILE)] = jnp.where(mask, rows, old).astype(low)
                return 0

            return lax.fori_loop(lo, hi, out_tile, 0)

        lax.fori_loop(0, slots, out_slot, 0)
        for copy in leaving:
            copy.wait()


def own_taps(own_ref, all_ref, z):
    heads = own_ref.shape[0]
    for n in range(all_ref.shape[0] // heads):

        @pl.when(z == n)
        def _():
            own_ref[...] = all_ref[n * heads : (n + 1) * heads, :]


def windows(padded, start, end, t):
    full = padded[:, pl.ds(t, TILE + 2 * SUB)]
    keep = lane_mask(start, end, t - SUB, TILE + 2 * SUB)
    return jnp.where(keep, full.astype(f32), 0.0).astype(low)


def convolve(padded, bands, start, end, t, heads):
    full = windows(padded, start, end, t)
    out = []
    count = TILE // SUB
    for h in range(heads):
        own = full[h * HEAD_DIM : (h + 1) * HEAD_DIM]
        stack = jnp.concatenate(
            [own[:, c * SUB : (c + 3) * SUB] for c in range(count)], axis=0
        )
        res = mul_t(stack, bands[h])
        out.append(
            jnp.concatenate(
                [res[c * HEAD_DIM : (c + 1) * HEAD_DIM] for c in range(count)], axis=1
            )
        )
    return jnp.concatenate(out, axis=0)


def mix_backward_kernel(
    slots, marks, taps,
    len_ref, grad_ref, qkv_ref, first_ref, last_hbm, mark_ref, value_ref, inner_ref,
    denom_ref, middle_ref, steps_hbm, inverse_ref, conv_ref,
    out_hbm, bias_ref, conv_out_ref,
    last_ref, steps_ref, out_ref, move_sem,
    gpad, vpad, ds_first, ds_last, conv_grad, d_inner, d_k, d_q, d_value, conv_own,
):
    width = first_ref.shape[0]
    heads = width // HEAD_DIM
    tok_count = qkv_ref.shape[1]
    packed = slots * marks
    scale = HEAD_DIM ** -0.5
    head_blocks = block_grid(width, width)
    slot_blocks = block_grid(packed, packed)
    ones = block_ones(packed)
    eye = eye_pack(packed)
    count = TILE // SUB
    last_in = pltpu.make_async_copy(last_hbm, last_ref, move_sem.at[0])
    steps_in = pltpu.make_async_copy(steps_hbm, steps_ref, move_sem.at[1])
    steps_in.start()
    last_in.start()

    for padded, source in ((gpad, grad_ref[...]), (vpad, qkv_ref[2 * width :, :])):
        padded[:, :SUB] = jnp.zeros((width, SUB), low)
        padded[:, tok_count + SUB :] = jnp.zeros((width, SUB), low)
        padded[:, SUB : tok_count + SUB] = source
    out_ref[...] = jnp.zeros_like(out_ref)
    ds_first[...] = jnp.zeros_like(ds_first)
    ds_last[...] = jnp.zeros_like(ds_last)
    conv_grad[...] = jnp.zeros_like(conv_grad)

    own_taps(conv_own, conv_ref, lax.axis_index("heads"))

    def reach(s):
        start, end = slot_bounds(len_ref, s, slots)
        lo, hi = start // TILE, (end + TILE - 1) // TILE
        return start, end, lo, jnp.where(end > start, hi, lo)

    def own_rows(s):
        return pl.ds(pl.multiple_of(s * marks, marks), marks)

    def first_slot(s, _):
        start, end, lo, hi = reach(s)
        a_block = spread(inner_ref[own_rows(s), :], head_blocks).astype(low)

        def tile(n, carry):
            inner_total, key_total = carry
            t = pl.multiple_of(n * TILE, TILE)
            mask = lane_mask(start, end, t, TILE)
            own_grad = grad_ref[:, pl.ds(t, TILE)]
            kernel_rows = jnp.where(mask, first_ref[:, pl.ds(t, TILE)].astype(f32), 0.0)
            d_kernel = mul(a_block, own_grad)
            prod = (kernel_rows * d_kernel).reshape(heads, marks, TILE)
            row_sum = jnp.sum(prod, axis=1, keepdims=True)
            d_sim = prod - kernel_rows.reshape(heads, marks, TILE) * row_sum
            d_sim = d_sim.reshape(width, TILE)
            d_sim_low = d_sim.astype(low)
            old = ds_first[:, pl.ds(t, TILE)].astype(f32)
            ds_first[:, pl.ds(t, TILE)] = jnp.where(mask, d_sim, old).astype(low)
            inner_total = inner_total + mul_t(kernel_rows.astype(low), own_grad)
            key_total = key_total + mul_t(d_sim_low, qkv_ref[:width, pl.ds(t, TILE)])
            full = windows(vpad, start, end, t)
            grad_own = jnp.where(mask, own_grad.astype(f32), 0.0).astype(low)
            for h in range(heads):
                sel = slice(h * HEAD_DIM, (h + 1) * HEAD_DIM)
                left = jnp.concatenate(
                    [grad_own[sel, c * SUB : (c + 1) * SUB] for c in range(count)], axis=0
                )
                right = jnp.concatenate(
                    [full[sel, c * SUB : (c + 3) * SUB] for c in range(count)], axis=0
                )
                conv_grad[h] += lax.dot_general(
                    left, right, (((0,), (0,)), ((), ())), preferred_element_type=f32
                )
            return inner_total, key_total

        zero = jnp.zeros((width, width), f32)
        inner_total, key_total = lax.fori_loop(lo, hi, tile, (zero, zero))
        d_inner[own_rows(s), :] = fold(inner_total, head_blocks)
        d_k[own_rows(s), :] = fold(key_total, head_blocks) * scale
        return 0

    lax.fori_loop(0, slots, first_slot, 0)

    row = lax.broadcasted_iota(jnp.int32, (SUB, 3 * SUB), 0)
    col = lax.broadcasted_iota(jnp.int32, (SUB, 3 * SUB), 1)
    off = col - row - (SUB - taps // 2)
    tap_lane = lax.broadcasted_iota(jnp.int32, (1, SUB), 1)
    for h in range(heads):
        found = jnp.zeros((1, SUB), f32)
        square = conv_grad[h]
        for n in range(taps):
            part = jnp.sum(jnp.where(off == n, square, 0.0), axis=0, keepdims=True)
            part = jnp.sum(part, axis=1, keepdims=True)
            found = jnp.where(tap_lane == n, part, found)
        conv_out_ref[h : h + 1, :] = found

    lane_head = lax.broadcasted_iota(jnp.int32, (1, width), 1) // HEAD_DIM
    value_total = jnp.zeros((packed, width), f32)
    d_inverses = []
    for h in range(heads):
        own = jnp.where(lane_head == h, d_inner[...], 0.0)
        value_total = value_total + wide(mul, spread(inverse_ref[h], slot_blocks), own)
        d_inverses.append(fold(wide(mul_t, own, value_ref[...]), slot_blocks))
    d_value[...] = value_total

    def before(n, h, d_inverse):
        third, inverse_t = steps_ref[n, 2, h], steps_ref[n, 3, h]
        (d_third,) = pack_mul([0.25 * inverse_t], ready(d_inverse, ones))
        (earlier,) = pack_mul([0.25 * d_inverse], ready(third, ones))
        return earlier, d_third

    def newton(k, carry):
        n = PINV_ITERS - 1 - k
        out = []
        for h in range(heads):
            d_inverse, d_third, grad = carry[h]
            product, square, third = [steps_ref[n, i, h] for i in range(3)]
            mixed = 7.0 * product - square
            by_third, by_one, by_two = pack_mul([third, product, square], ready(grad, ones))
            left_mixed, left_one = pack_mul([mixed, product], ready(d_third, ones))
            (right,) = pack_mul([grad], ready(third, ones))
            (more,) = pack_mul([0.25 * by_one + d_third], ready(mixed, ones))
            (less,) = pack_mul([0.25 * by_two + left_one], ready(product, ones))
            d_product = (
                0.25 * (right + by_third - 13.0 * grad) - 15.0 * d_third + left_mixed + more - less
            )
            earlier, d_before = before(jnp.maximum(n - 1, 0), h, d_inverse)
            last = n == 0
            out.append((jnp.where(last, d_inverse, earlier), d_before, d_product))
        return tuple(out)

    steps_in.wait()
    zero = jnp.zeros((HEAD_DIM, packed), f32)
    start = []
    for h in range(heads):
        start.append(before(PINV_ITERS - 1, h, d_inverses[h]) + (zero,))
    final = lax.fori_loop(0, PINV_ITERS, newton, tuple(start))
    lane_slot = lax.broadcasted_iota(jnp.int32, (1, packed), 1) // marks
    dq_total = jnp.zeros((packed, width), f32)
    dk_total = jnp.zeros((packed, width), f32)
    for h in range(heads):
        d_inverse, _, d_product = final[h]
        middle = middle_ref[h]
        first_t = steps_ref[0, 3, h]
        (d_inverse_t,) = pack_mul([eye], ready(d_inverse, ones), mul_t)
        (d_product_t,) = pack_mul([eye], ready(d_product, ones), mul_t)
        (d_middle,) = pack_mul([d_product + d_product_t], ready(middle, ones))
        col_sums = jnp.sum(middle, axis=0, keepdims=True)
        share = jnp.sum(
            d_inverse_t * first_t + d_product * steps_ref[0, 0, h], axis=0, keepdims=True
        )
        bound = jnp.zeros((1, packed), f32)
        d_bound = jnp.zeros((1, packed), f32)
        hits = jnp.zeros((1, packed), f32)
        for s in range(slots):
            mine = lane_slot == s
            top = jnp.max(jnp.where(mine, col_sums, 0.0), axis=1, keepdims=True)
            total = jnp.sum(jnp.where(mine, share, 0.0), axis=1, keepdims=True)
            number = jnp.sum(
                jnp.where(mine & (col_sums == top), 1.0, 0.0), axis=1, keepdims=True
            )
            bound = jnp.where(mine, top, bound)
            d_bound = jnp.where(mine, -total / top, d_bound)
            hits = jnp.where(mine, number, hits)
        d_middle = (d_middle + d_inverse_t) / bound
        d_middle = d_middle + jnp.where(col_sums == bound, d_bound / hits, 0.0)
        prod = spread(middle * d_middle, slot_blocks)
        d_sim = prod - spread(middle, slot_blocks) * jnp.sum(prod, axis=1, keepdims=True)
        d_sim = d_sim * scale
        own = lane_head == h
        q_marks = jnp.where(own, mark_ref[:, :width], 0.0)
        k_marks = jnp.where(own, mark_ref[:, width:], 0.0)
        dq_total = dq_total + wide(mul, d_sim, k_marks)
        dk_total = dk_total + wide(mul, jnp.transpose(d_sim), q_marks)
    d_q[...] = dq_total
    d_k[...] += dk_total

    flipped = []
    for h in range(heads):
        flipped.append(
            band(
                jnp.concatenate(
                    [conv_own[h : h + 1, n : n + 1] for n in reversed(range(taps))], axis=1
                ),
                taps,
            ).astype(low)
        )

    def last_slot(s, _):
        start, end, lo, hi = reach(s)
        inv = denom_ref[s]
        own_d = d_value[own_rows(s), :]
        own_v = value_ref[own_rows(s), :]
        d_block = spread(own_d, head_blocks)
        row_sum = jnp.sum(
            d_block * jnp.concatenate([own_v] * heads, axis=0), axis=1, keepdims=True
        )
        row_sum = row_sum * inv
        d_block = d_block * inv
        d_block_t = jnp.transpose(d_block).astype(low)
        d_block = d_block.astype(low)

        def tile(n, query_total):
            t = pl.multiple_of(n * TILE, TILE)
            mask = lane_mask(start, end, t, TILE)
            kernel_rows = jnp.where(mask, last_ref[:, pl.ds(t, TILE)].astype(f32), 0.0)
            v_rows = qkv_ref[2 * width :, pl.ds(t, TILE)]
            d_sim = kernel_rows * (mul(d_block, v_rows) - row_sum)
            d_low = d_sim.astype(low)
            old = ds_last[:, pl.ds(t, TILE)].astype(f32)
            ds_last[:, pl.ds(t, TILE)] = jnp.where(mask, d_sim, old).astype(low)
            dv = mul(d_block_t, kernel_rows.astype(low))
            dv = dv + convolve(gpad, flipped, start, end, t, heads)
            old = out_ref[2 * width :, pl.ds(t, TILE)].astype(f32)
            out_ref[2 * width :, pl.ds(t, TILE)] = jnp.where(mask, dv, old).astype(low)
            return query_total + mul_t(d_low, qkv_ref[width : 2 * width, pl.ds(t, TILE)])

        query_total = lax.fori_loop(lo, hi, tile, jnp.zeros((width, width), f32))
        d_q[own_rows(s), :] += fold(query_total, head_blocks) * scale
        return 0

    last_in.wait()
    lax.fori_loop(0, slots, last_slot, 0)
    values = pl.ds(2 * width, width)
    values_out = pltpu.make_async_copy(out_ref.at[values], out_hbm.at[values], move_sem.at[2])
    values_out.start()

    inv_count = slot_marks(len_ref, 0, slots, marks, SUB)[1]
    d_q[...] = d_q[...] * inv_count
    d_k[...] = d_k[...] * inv_count

    def final_slot(s, _):
        start, end, lo, hi = reach(s)
        length = end - start
        own = mark_ref[own_rows(s), :] * scale

        def left(block, d_mark):
            wide_rows = jnp.concatenate([spread(block, head_blocks), d_mark], axis=0)
            return jnp.transpose(wide_rows).astype(low)

        q_left = left(own[:, width:], d_q[own_rows(s), :])
        k_left = left(own[:, :width], d_k[own_rows(s), :])
        mark = lax.broadcasted_iota(jnp.int32, (marks, 1), 0)
        lower = start + (mark * length) // marks
        upper = start + ((mark + 1) * length) // marks

        def tile(n, _):
            t = pl.multiple_of(n * TILE, TILE)
            mask = lane_mask(start, end, t, TILE)
            tok = t + lax.broadcasted_iota(jnp.int32, (marks, TILE), 1)
            member = jnp.where((tok >= lower) & (tok < upper), 1.0, 0.0).astype(low)
            for at, lhs, source in ((0, q_left, ds_first), (width, k_left, ds_last)):
                rhs = jnp.concatenate([source[:, pl.ds(t, TILE)], member], axis=0)
                rows = mul(lhs, rhs)
                old = out_ref[at : at + width, pl.ds(t, TILE)].astype(f32)
                out_ref[at : at + width, pl.ds(t, TILE)] = jnp.where(mask, rows, old).astype(low)
            return 0

        return lax.fori_loop(lo, hi, tile, 0)

    lax.fori_loop(0, slots, final_slot, 0)
    others = pl.ds(0, 2 * width)
    others_out = pltpu.make_async_copy(out_ref.at[others], out_hbm.at[others], move_sem.at[3])
    others_out.start()

    def bias_tile(n, carry):
        t = pl.multiple_of(n * TILE, TILE)
        q_sum, v_sum = carry
        q_rows = out_ref[:width, pl.ds(t, TILE)].astype(f32)
        v_rows = out_ref[2 * width :, pl.ds(t, TILE)].astype(f32)
        for c in range(count):
            q_sum = q_sum + q_rows[:, c * SUB : (c + 1) * SUB]
            v_sum = v_sum + v_rows[:, c * SUB : (c + 1) * SUB]
        return q_sum, v_sum

    zero = jnp.zeros((width, SUB), f32)
    q_sum, v_sum = lax.fori_loop(0, tok_count // TILE, bias_tile, (zero, zero))
    bias_ref[...] = jnp.zeros_like(bias_ref)
    bias_ref[0:1, :] = jnp.sum(jnp.transpose(q_sum), axis=0, keepdims=True)
    bias_ref[1:2, :] = jnp.sum(jnp.transpose(v_sum), axis=0, keepdims=True)
    values_out.wait()
    others_out.wait()


def mix_forward(seq_lengths, tokens, weight_t, bias, conv, slots, marks):
    tok_count, model = tokens.shape
    width = weight_t.shape[0] // 3
    heads = width // HEAD_DIM
    packed = slots * marks
    taps = conv.shape[1]
    whole = lambda *shape: pl.BlockSpec(shape, lambda i, lens: (0,) * len(shape))
    shapes = [
        ((3 * width, tok_count), low),
        ((width, tok_count), low),
        ((width, tok_count), low),
        ((width, tok_count), low),
        ((packed, 2 * width), f32),
        ((packed, width), f32),
        ((packed, width), f32),
        ((slots, width, 1), f32),
        ((heads, HEAD_DIM, packed), f32),
        ((PINV_ITERS, 4, heads, HEAD_DIM, packed), f32),
        ((heads, HEAD_DIM, packed), f32),
        ((8, 128), f32),
    ]
    apart = (0, 1, 2, 9)
    return pl.pallas_call(
        partial(mix_forward_kernel, slots, marks, taps),
        out_shape=[jax.ShapeDtypeStruct(s, t) for s, t in shapes],
        grid_spec=pltpu.PrefetchScalarGridSpec(
            num_scalar_prefetch=1,
            grid=(tok_count // TILE,),
            in_specs=[
                pl.BlockSpec((TILE, model), lambda i, lens: (i, 0)),
                whole(3 * width, model),
                whole(*bias.shape),
                whole(*conv.shape),
            ],
            out_specs=[
                pl.BlockSpec(memory_space=pl.ANY) if n in apart else whole(*s)
                for n, (s, _) in enumerate(shapes)
            ],
            scratch_shapes=[pltpu.VMEM(*shapes[n]) for n in apart]
            + [
                pltpu.VMEM((width, tok_count + 2 * SUB), low),
                pltpu.VMEM((width, tok_count), f32),
                pltpu.VMEM((8, width), f32),
                pltpu.VMEM((bias.shape[1], 2 * bias.shape[0]), f32),
                pltpu.VMEM((heads, taps), f32),
                pltpu.SemaphoreType.DMA((len(apart),)),
            ],
        ),
        compiler_params=pltpu.CompilerParams(vmem_limit_bytes=56 * 1024 * 1024),
        cost_estimate=pl.CostEstimate(
            flops=20 * 10**9, bytes_accessed=30 * 10**6, transcendentals=10**6
        ),
        name="mix_forward",
    )(seq_lengths, tokens, weight_t, bias, conv)


def mix_backward(seq_lengths, grad_t, saved, conv, slots, marks):
    qkv_t, first, last, mark, value, inner, denom, middle, steps, inverse = saved
    width, tok_count = grad_t.shape
    heads = width // HEAD_DIM
    packed = slots * marks
    taps = conv.shape[1]
    args = (grad_t, qkv_t, first, last, mark, value, inner, denom, middle, steps, inverse, conv)
    whole = lambda shape: pl.BlockSpec(
        shape, lambda i, lens: (0,) * len(shape), pipeline_mode=pl.Buffered(1)
    )
    shapes = [((3 * width, tok_count), low), ((8, width), f32), ((heads, SUB), f32)]
    square = pltpu.VMEM((packed, width), f32)
    hbm = pl.BlockSpec(memory_space=pl.ANY)
    return pl.pallas_call(
        partial(mix_backward_kernel, slots, marks, taps),
        out_shape=[jax.ShapeDtypeStruct(s, t) for s, t in shapes],
        grid_spec=pltpu.PrefetchScalarGridSpec(
            num_scalar_prefetch=1,
            grid=(1,),
            in_specs=[hbm if n in (3, 9) else whole(x.shape) for n, x in enumerate(args)],
            out_specs=[hbm] + [whole(s) for s, _ in shapes[1:]],
            scratch_shapes=[
                pltpu.VMEM(last.shape, low),
                pltpu.VMEM(steps.shape, f32),
                pltpu.VMEM(*shapes[0]),
                pltpu.SemaphoreType.DMA((4,)),
                pltpu.VMEM((width, tok_count + 2 * SUB), low),
                pltpu.VMEM((width, tok_count + 2 * SUB), low),
                pltpu.VMEM((width, tok_count), low),
                pltpu.VMEM((width, tok_count), low),
                pltpu.VMEM((heads, SUB, 3 * SUB), f32),
                square, square, square, square,
                pltpu.VMEM((heads, taps), f32),
            ],
        ),
        compiler_params=pltpu.CompilerParams(vmem_limit_bytes=56 * 1024 * 1024),
        cost_estimate=pl.CostEstimate(
            flops=20 * 10**9, bytes_accessed=30 * 10**6, transcendentals=10**6
        ),
        name="mix_backward",
    )(seq_lengths, *args)


contract_rows = (((0,), (0,)), ((), ()))
contract_cols = (((1,), (1,)), ((), ()))
norm_eps = 1e-05


def split_up(x, dim, peers):
    before, after = (x.shape[:dim], x.shape[dim + 1 :])
    return jnp.moveaxis(x.reshape(*before, peers, -1, *after), dim, 0)


def sum_at_owner(x, axis, dim):
    peers = lax.axis_size(axis)
    tiles = lax.all_to_all(split_up(x, dim, peers), axis, 0, 0, tiled=True)
    return jnp.sum(tiles.astype(f32), axis=0)


def layer_norm(row_data, gain_vec, shift_vec):
    centre = row_data - jnp.mean(row_data, axis=1, keepdims=True)
    spread_row = jnp.mean(centre * centre, axis=1, keepdims=True)
    return centre * lax.rsqrt(spread_row + norm_eps) * gain_vec[None, :] + shift_vec[None, :]


def gelu_exact(values):
    return jax.nn.gelu(values, approximate=False)


def body(
    tokens,
    qkv_weight,
    qv_bias,
    conv_weight,
    out_weight,
    out_bias,
    norm1_gain,
    norm1_bias,
    ffn_in_weight,
    ffn_in_bias,
    ffn_out_weight,
    ffn_out_bias,
    norm2_gain,
    norm2_bias,
    cotangent,
    seq_lengths,
    segment_ids,
    landmark_bounds,
):
    tok_count, model_width = tokens.shape
    head_width = qkv_weight.shape[2]
    heads_here = head_width // HEAD_DIM
    head_total = conv_weight.shape[0]
    kernel_taps = conv_weight.shape[1]
    slots, marks = landmark_bounds.shape
    quarter = tok_count // lax.axis_size("heads")
    head_index = lax.axis_index("heads")
    own_start = head_index * quarter
    both = ("batch", "heads")
    own_rows_low = lax.dynamic_slice_in_dim(tokens, own_start, quarter, 0)
    own_tokens = own_rows_low.astype(f32)
    flat_qkv = qkv_weight.reshape(model_width, 3 * head_width)
    forward = mix_forward(
        seq_lengths, tokens, jnp.transpose(flat_qkv), qv_bias, conv_weight, slots, marks
    )
    qkv_t, first, last, mixed_t, mark, value, inner, denom, middle, steps, inverse, bound = forward
    bound_total = bound[0, 0]
    attn_part = lax.psum_scatter(
        lax.dot_general(mixed_t, out_weight, contract_rows, preferred_element_type=f32).astype(low),
        "heads",
        scatter_dimension=0,
        tiled=True,
    ).astype(f32)
    live_count = jnp.sum((seq_lengths > 0).astype(f32)) * heads_here
    first_res = own_tokens + attn_part + out_bias[None, :]
    norm1_out, norm1_pull = jax.vjp(layer_norm, first_res, norm1_gain, norm1_bias)
    norm1_low = norm1_out.astype(low)
    ff_own = ffn_out_weight.shape[0]
    bias_row = jnp.zeros((16, model_width), low).at[0, :ff_own].set(ffn_in_bias)
    whole_in = lax.all_gather(ffn_in_weight, both, axis=1, tiled=True)
    out_pack = lax.all_gather(jnp.concatenate([ffn_out_weight, bias_row], axis=0), both, axis=0)
    whole_out = out_pack[:, :ff_own].reshape(-1, model_width)
    whole_in_bias = out_pack[:, ff_own, :ff_own].reshape(-1)
    pre_act = (
        jnp.dot(norm1_low, whole_in, preferred_element_type=f32)
        + whole_in_bias.astype(f32)[None, :]
    )
    hidden_act, gelu_pull = jax.vjp(gelu_exact, pre_act)
    hidden_low = hidden_act.astype(low)
    ffn_result = jnp.dot(hidden_low, whole_out, preferred_element_type=f32) + ffn_out_bias[None, :]
    final_out, norm2_pull = jax.vjp(layer_norm, norm1_out + ffn_result, norm2_gain, norm2_bias)
    grad_second, grad_gain_two, grad_shift_two = norm2_pull(cotangent.astype(f32))
    grad_ffn_low = grad_second.astype(low)
    grad_ffn_bias = jnp.sum(grad_ffn_low.astype(f32), axis=0)
    down_term = lax.dot_general(
        hidden_low, grad_ffn_low, contract_rows, preferred_element_type=f32
    ).astype(low)
    grad_hidden = lax.dot_general(
        grad_ffn_low, whole_out, contract_cols, preferred_element_type=f32
    )
    grad_pre = gelu_pull(grad_hidden)[0].astype(low)
    grad_in_bias = jnp.sum(grad_pre.astype(f32), axis=0)
    up_term = lax.dot_general(
        norm1_low, grad_pre, contract_rows, preferred_element_type=f32
    ).astype(low)
    grad_norm1 = grad_second + lax.dot_general(
        grad_pre, whole_in, contract_cols, preferred_element_type=f32
    )
    grad_first, grad_gain_one, grad_shift_one = norm1_pull(grad_norm1)
    grad_attn_low = grad_first.astype(low)
    grad_out_bias = jnp.sum(grad_attn_low.astype(f32), axis=0)
    piece_rows = lax.all_gather(grad_attn_low, "heads", axis=0, tiled=True)
    grad_mix_t = lax.dot_general(
        out_weight, piece_rows, contract_cols, preferred_element_type=f32
    ).astype(low)
    grad_mix_t, down_term, up_term = lax.optimization_barrier((grad_mix_t, down_term, up_term))
    up_share = lax.psum_scatter(up_term, both, scatter_dimension=1, tiled=True).astype(f32)
    down_share = lax.psum_scatter(down_term, both, scatter_dimension=0, tiled=True).astype(f32)
    saved = (qkv_t, first, last, mark, value, inner, denom, middle, steps, inverse)
    grad_t, grad_bias, grad_conv = mix_backward(
        seq_lengths, grad_mix_t, saved, conv_weight, slots, marks
    )
    out_part = lax.dot_general(
        mixed_t, piece_rows, (((1,), (0,)), ((), ())), preferred_element_type=f32
    )
    grad_qv_own = grad_bias[:2]
    qkv_part = lax.dot_general(
        tokens, grad_t, (((0,), (1,)), ((), ())), preferred_element_type=f32
    ).reshape(model_width, 3, head_width)
    input_part = lax.psum_scatter(
        lax.dot_general(
            grad_t, flat_qkv, (((0,), (1,)), ((), ())), preferred_element_type=f32
        ).astype(low),
        "heads",
        scatter_dimension=0,
        tiled=True,
    ).astype(f32)
    input_grad = grad_first + input_part
    conv_full = lax.dynamic_update_slice_in_dim(
        jnp.zeros((head_total, kernel_taps), f32),
        grad_conv[:, :kernel_taps],
        head_index * heads_here,
        0,
    )
    bias_full = lax.dynamic_update_slice_in_dim(
        jnp.zeros((2, head_total * HEAD_DIM), f32), grad_qv_own, head_index * head_width, 1
    )
    qkv_share, out_share = (
        sum_at_owner(qkv_part.astype(low), "batch", 0),
        sum_at_owner(out_part.astype(low), "batch", 1),
    )
    vector_all = jnp.stack(
        [grad_ffn_bias, grad_gain_two, grad_shift_two, grad_gain_one, grad_shift_one, grad_out_bias]
    )
    in_bias_share, vector_share = (
        lax.psum_scatter(grad_in_bias, both, scatter_dimension=0, tiled=True),
        lax.psum_scatter(vector_all, both, scatter_dimension=1, tiled=True),
    )
    conv_sum, bias_sum, bound_all, count_all = lax.psum(
        (conv_full, bias_full, bound_total, live_count), both
    )
    conv_out = lax.dynamic_slice_in_dim(conv_sum, head_index * heads_here, heads_here, 0)
    bias_out = lax.dynamic_slice_in_dim(bias_sum, head_index * head_width, head_width, 1)
    condition = bound_all / count_all
    return (
        final_out.astype(low),
        input_grad,
        qkv_share,
        bias_out,
        conv_out,
        out_share,
        up_share,
        in_bias_share,
        down_share,
        vector_share,
        condition,
    )


def place():
    b, z = lax.axis_index("batch"), lax.axis_index("heads")
    core, x, y = b % 2, (b // 2) % 2, b // 4
    return b, z, b + 1 - 2 * core, b + 2 - 4 * x, b + 4 - 8 * y


def remote(src, dst, send, recv, device):
    return pltpu.make_async_remote_copy(
        src_ref=src,
        dst_ref=dst,
        send_sem=send,
        recv_sem=recv,
        device_id=device,
        device_id_type=pl.DeviceIdType.MESH,
    )


def greet(devices):
    barrier = pltpu.get_barrier_semaphore()
    for device in devices:
        pl.semaphore_signal(
            barrier, inc=1, device_id=device, device_id_type=pl.DeviceIdType.MESH
        )
    pl.semaphore_wait(barrier, len(devices))


def tail_kernel(
    len_ref,
    gt_hbm, wq_hbm, we_hbm, hid_hbm, pre_hbm, n1_hbm, gf_hbm, ga_hbm, mx_hbm, tok_hbm, first_hbm,
    sums_ref, bin_ref, qv_ref, conv_ref, bound_ref,
    input_ref, down_own, up_own, outw_own, qkvw_own, in_bias, vector_own, qv_own, conv_own, ratio,
    small_out,
    gt, wq, we, hid, pre, n1, gf, ga, mx, tok,
    q_in, r_out, r_in, s_in, out_down, out_up, full_outw, full_qkvw, acc_qkvw,
    core_down, core_up, core_outw, core_qkvw,
    one_down, one_up, one_outw, one_qkvw, two_down, two_up, two_outw, two_qkvw,
    e_down, e_up, e_outw, g_down, g_up, g_outw, h_down, h_up, h_outw, small_in,
    load_sem, q_send, q_recv, r_send, r_recv, t_send, t_recv, c_send, c_recv, x_send, x_recv, e_send, e_recv,
    g_send, g_recv, h_send, h_recv, s_send, s_recv,
):
    b, z, bc, bx, by = place()
    both = bx + by - b
    flip = bc - b
    peers = [(b, lax.rem(z + i, 4)) for i in (1, 2, 3)]
    issued = []
    loads = [
        pltpu.make_async_copy(src, dst, load_sem.at[n])
        for n, (src, dst) in enumerate(
            (
                (pre_hbm, pre), (n1_hbm, n1), (hid_hbm, hid), (gf_hbm, gf), (gt_hbm, gt),
                (wq_hbm, wq), (we_hbm, we), (mx_hbm, mx), (ga_hbm, ga), (tok_hbm, tok),
                (first_hbm, input_ref),
            )
        )
    ]
    for copy in loads:
        copy.start()
    greet(peers + [(bc, z), (bx, z), (by, z)])
    chunks, size = r_in.shape[1:3]
    quarter = chunks * size
    ff = down_own.shape[0]
    group = 4 * ff

    zf = z + 1 - 2 * (z % 2)
    zg = z + 2 - 4 * (z // 2)
    partners = ((bc, z), (bx, z), (by, z), (b, zf), (b, zg))

    def small_start(k):
        copy = remote(
            small_out.at[k], small_in.at[k], s_send.at[k], s_recv.at[k], partners[k]
        )
        copy.start()
        issued.append(copy)

    def small_event(k):
        ref = small_in.at[k]
        remote(ref, ref, s_send.at[k], s_recv.at[k], partners[k]).wait_recv()
        small_out[k + 1] = small_out[k] + small_in[k]
        if k < 4:
            small_start(k + 1)

    model = input_ref.shape[1]
    bias_rows = bin_ref.shape[1] // model
    at_vec, at_qv = bias_rows, bias_rows + 6
    heads, taps = conv_own.shape
    at_conv = at_qv + 8
    at_end = at_conv + 4 * heads
    width = qv_own.shape[1]
    small_out[0] = jnp.zeros(small_out.shape[1:], f32)
    for n in range(bias_rows):
        small_out[0, n : n + 1, :] = bin_ref[0:1, n * model : (n + 1) * model]
    small_out[0, at_vec : at_vec + 6, :] = sums_ref[0:6, :]
    live = jnp.int32(0)
    for n in range(len_ref.shape[0]):
        live = live + jnp.where(len_ref[n] > 0, heads, 0)
    lane = lax.broadcasted_iota(jnp.int32, (1, 128), 1)
    small_out[0, at_end : at_end + 1, 0:128] = jnp.where(
        lane == 0, bound_ref[0:1, :], jnp.where(lane == 1, live.astype(f32), 0.0)
    )
    for n in range(4):

        @pl.when(z == n)
        def _():
            for r in range(2):
                row = at_qv + 2 * n + r
                small_out[0, row : row + 1, :width] = qv_ref[r : r + 1, :]
            for r in range(heads):
                row = at_conv + heads * n + r
                small_out[0, row : row + 1, 0:128] = conv_ref[r : r + 1, :]

    small_start(0)

    is_end = (z == 0) | (z == 3)
    low_side = z < 2
    to_inner = jnp.where(low_side, 1, 2)
    across = jnp.where(z == 1, 2, 1)
    to_end = jnp.where(low_side, 0, 3)

    def owner(k):
        return jnp.where(low_side, 3 - k, k)

    def columns(who, c):
        return pl.ds(pl.multiple_of(who * quarter + c * size, size), size)

    def times(x, w):
        return lax.dot_general(x, w, (((0,), (0,)), ((), ())), preferred_element_type=f32)

    def part(who, c):
        return times(gt[:, columns(who, c)], wq[...])

    def q_copy(k, c):
        return remote(
            gt_hbm.at[:, columns(owner(k), c)], q_in.at[k, c], q_send.at[k, c], q_recv.at[k, c],
            (b, to_inner),
        )

    def q_wait(k, c):
        ref = q_in.at[k, c]
        remote(ref, ref, q_send.at[k, c], q_recv.at[k, c], (b, to_end)).wait_recv()

    def r_copy(k, c):
        return remote(
            r_out.at[k, c], r_in.at[k, c], r_send.at[k, c], r_recv.at[k, c], (b, across)
        )

    def t_copy(c):
        return remote(r_in.at[0, c], s_in.at[c], t_send.at[c], t_recv.at[c], (b, to_end))

    def first_hop(k, c):
        @pl.when(jnp.logical_not(is_end))
        def _():
            own = part(owner(k), c)
            q_wait(k, c)
            r_out[k, c] = (own + times(q_in[k, c], we[...])).astype(low)
            r_copy(k, c).start()

    def last_hop(c):
        @pl.when(jnp.logical_not(is_end))
        def _():
            own = part(to_end, c)
            r_copy(0, c).wait_recv()
            r_in[0, c] = (r_in[0, c].astype(f32) + own).astype(low)
            t_copy(c).start()

    cores = (core_down, core_up, core_outw, core_qkvw)
    ones = (one_down, one_up, one_outw, one_qkvw)
    twos = (two_down, two_up, two_outw, two_qkvw)
    outs = (out_down, out_up)
    left = (hid, pre)
    right = (gf, n1)

    def who(slot):
        return b + (slot % 2) * (bx - b) + (slot // 2) * (by - b)

    def term(n, owner):
        at = pl.ds(pl.multiple_of(owner * group, group), group)
        return lax.dot_general(
            left[n][:, at], right[n][...], (((0,), (0,)), ((), ())), preferred_element_type=f32
        )

    def core_copy(n, slot):
        if n < 2:
            src = outs[n].at[slot]
        elif n == 2:
            src = full_outw.at[:, who(slot) + flip]
        else:
            src = full_qkvw.at[who(slot) + flip]
        return remote(src, cores[n].at[slot], c_send.at[n, slot], c_recv.at[n, slot], (bc, z))

    def give(n, slot):
        if n < 2:
            value = term(n, who(slot) + flip).astype(low)
            outs[n][slot] = value.reshape(outs[n].shape[1:])
        core_copy(n, slot).start()

    def keep(n, slot):
        if n < 2:
            own = term(n, who(slot)).reshape(outs[n].shape[1:])
        elif n == 2:
            own = full_outw[:, who(slot)].astype(f32)
        else:
            own = full_qkvw[who(slot)].astype(f32)
        core_copy(n, slot).wait_recv()
        cores[n][slot] = (cores[n][slot].astype(f32) + own).astype(low)

    def side_copy(n, dst, src):
        partner = by if n % 2 == 0 else bx
        return remote(
            cores[n].at[src], ones[n].at[dst], x_send.at[n, dst], x_recv.at[n, dst], (partner, z)
        )

    def small_group(n):
        def one(i, _):
            give(n, 3 - i)
            return 0

        lax.fori_loop(0, 4, one, 0)

    def small_keep(n):
        def one(i, _):
            keep(n, 3 - i)
            return 0

        lax.fori_loop(0, 4, one, 0)
        side_copy(n, 1, 3).start()
        side_copy(n, 0, 2 if n % 2 == 0 else 1).start()

    def half(h, _):
        def one(i, _):
            slot_up, slot_down = 3 - 2 * i - h, 3 - i - 2 * h
            give(1, slot_up)
            give(0, slot_down)
            keep(1, slot_up)

            @pl.when(h == 0)
            def _():
                side_copy(1, 1 - i, slot_up).start()

            keep(0, slot_down)

            @pl.when(h == 0)
            def _():
                side_copy(0, 1 - i, slot_down).start()

            return 0

        lax.fori_loop(0, 2, one, 0)

        @pl.when(h == 0)
        def _():
            for n in (4, 5, 6):
                loads[n].wait()
            first_hop(0, 0)

        return 0

    def one_event(n):
        second = 1 if n % 2 == 0 else 2
        partner, other = (by, bx) if n % 2 == 0 else (bx, by)
        ref = ones[n].at[1]
        remote(ref, ref, x_send.at[n, 1], x_recv.at[n, 1], (partner, z)).wait_recv()
        ones[n][1] = (ones[n][1].astype(f32) + cores[n][second].astype(f32)).astype(low)
        copy = remote(ones[n].at[1], twos[n], x_send.at[n, 2], x_recv.at[n, 2], (other, z))
        copy.start()
        issued.append(copy)

    e_bufs = (e_down, e_up, e_outw)
    g_bufs = (g_down, g_up, g_outw)
    h_bufs = (h_down, h_up, h_outw)

    def e_copy(n, k):
        return remote(
            twos[n].at[owner(k)], e_bufs[n].at[k], e_send.at[n, k], e_recv.at[n, k], (b, to_inner)
        )

    def e_wait(n, k):
        ref = e_bufs[n].at[k]
        remote(ref, ref, e_send.at[n, k], e_recv.at[n, k], (b, to_end)).wait_recv()

    def g_copy(n, k):
        return remote(
            e_bufs[n].at[k], g_bufs[n].at[k], g_send.at[n, k], g_recv.at[n, k], (b, across)
        )

    def h_copy(n):
        return remote(g_bufs[n].at[0], h_bufs[n], h_send.at[n], h_recv.at[n], (b, to_end))

    def two_event(n):
        partner, other = (by, bx) if n % 2 == 0 else (bx, by)
        ref = ones[n].at[0]
        remote(ref, ref, x_send.at[n, 0], x_recv.at[n, 0], (partner, z)).wait_recv()
        ref = twos[n]
        remote(ref, ref, x_send.at[n, 2], x_recv.at[n, 2], (other, z)).wait_recv()
        own = ones[n][0].astype(f32) + cores[n][0].astype(f32)
        if n == 3:
            own = twos[n][...].astype(f32) + own
            for i in range(3):
                qkvw_own[i] = own[:, i * width : (i + 1) * width]
            return
        twos[n][...] = (twos[n][...].astype(f32) + own).astype(low)

    def line_start(n, k):
        @pl.when(is_end)
        def _():
            e_copy(n, k).start()

    def line_across(n, k):
        @pl.when(jnp.logical_not(is_end))
        def _():
            e_wait(n, k)
            e_bufs[n][k] = (
                e_bufs[n][k].astype(f32) + twos[n][owner(k)].astype(f32)
            ).astype(low)
            g_copy(n, k).start()

    def line_back(n):
        @pl.when(jnp.logical_not(is_end))
        def _():
            g_copy(n, 0).wait_recv()
            g_bufs[n][0] = (
                g_bufs[n][0].astype(f32) + twos[n][to_end].astype(f32)
            ).astype(low)
            h_copy(n).start()

    def end_event(n):
        def write(value):
            out = (down_own, up_own, outw_own)[n]
            out[...] = jnp.transpose(value) if n == 2 else value

        @pl.when(is_end)
        def _():
            ref = h_bufs[n]
            remote(ref, ref, h_send.at[n], h_recv.at[n], (b, to_inner)).wait_recv()
            write(twos[n][z].astype(f32) + h_bufs[n][...].astype(f32))
            for k in range(3):
                e_copy(n, k).wait_send()

        @pl.when(jnp.logical_not(is_end))
        def _():
            g_copy(n, 1).wait_recv()
            e_wait(n, 2)
            write(
                twos[n][z].astype(f32)
                + g_bufs[n][1].astype(f32)
                + e_bufs[n][2].astype(f32)
            )
            for k in range(2):
                g_copy(n, k).wait_send()
            h_copy(n).wait_send()

    def projections():
        on, oh = full_outw.shape[2:]
        for s in range(4):
            value = jnp.transpose(mul(mx[s], ga[...]))
            full_outw[s] = value.astype(low).reshape(full_outw.shape[1:])
        acc_qkvw[...] = jnp.zeros_like(acc_qkvw)
        span = quarter

        def one(n, _):
            at = pl.ds(pl.multiple_of(n * span, span), span)
            acc_qkvw[...] += mul(gt[:, at], tok[at, :])
            return 0

        lax.fori_loop(0, 4, one, 0)
        full_qkvw[...] = jnp.transpose(acc_qkvw[...]).astype(low).reshape(full_qkvw.shape)

    @pl.when(is_end)
    def _():
        for k in range(3):
            for c in range(chunks):
                q_copy(k, c).start()

    for n in range(4):
        loads[n].wait()

    lax.fori_loop(0, 2, half, 0)
    first_hop(0, 1)
    one_event(1)
    one_event(0)
    first_hop(0, 2)
    last_hop(0)
    for n in (7, 8, 9):
        loads[n].wait()
    projections()
    first_hop(1, 0)
    last_hop(1)
    small_group(2)
    small_group(3)
    small_event(0)
    first_hop(1, 1)
    last_hop(2)
    small_keep(2)
    small_keep(3)
    small_event(1)
    first_hop(1, 2)
    two_event(1)
    line_start(1, 0)
    two_event(0)
    line_start(0, 0)
    line_start(1, 1)
    line_start(0, 1)
    small_event(2)
    one_event(2)
    one_event(3)
    small_event(3)
    two_event(2)
    for k in range(3):
        line_start(2, k)
    line_start(1, 2)
    line_start(0, 2)
    two_event(3)
    small_event(4)
    loads[10].wait()

    def own_rows(c, _):
        rows = pl.ds(pl.multiple_of(c * size, size), size)
        input_ref[rows, :] += part(z, c)

        @pl.when(is_end)
        def _():
            ref = s_in.at[c]
            remote(ref, ref, t_send.at[c], t_recv.at[c], (b, to_inner)).wait_recv()
            input_ref[rows, :] += s_in[c].astype(f32)

        @pl.when(jnp.logical_not(is_end))
        def _():
            r_copy(1, c).wait_recv()
            q_wait(2, c)
            input_ref[rows, :] += r_in[1, c].astype(f32) + times(q_in[2, c], we[...])

        return 0

    lax.fori_loop(0, chunks, own_rows, 0)
    for n, k in ((1, 0), (0, 0), (1, 1), (0, 1), (2, 0), (2, 1)):
        line_across(n, k)
        if k == 1:
            line_back(n)
    for n in (1, 0, 2):
        end_event(n)

    @pl.when(is_end)
    def _():
        for k in range(3):
            for c in range(chunks):
                q_copy(k, c).wait_send()

    @pl.when(jnp.logical_not(is_end))
    def _():
        for c in range(chunks):
            r_copy(0, c).wait_send()
            r_copy(1, c).wait_send()
            t_copy(c).wait_send()

    final = small_out.at[5]
    in_bias[...] = jnp.zeros_like(in_bias)
    index = b * 4 + z
    per_row = model // ff
    for n in range(bias_rows):

        @pl.when(index // per_row == n)
        def _():
            row = pltpu.roll(final[n : n + 1, :], (model - (index % per_row) * ff) % model, 1)
            in_bias[...] = row[:, :ff]

    share = vector_own.shape[1]
    vectors = final[at_vec : at_vec + 6, :]
    vector_own[...] = pltpu.roll(vectors, (model - index * share) % model, 1)[:, :share]
    for n in range(4):

        @pl.when(z == n)
        def _():
            qv_own[...] = final[at_qv + 2 * n : at_qv + 2 * n + 2, :width]
            conv_own[...] = final[at_conv + heads * n : at_conv + heads * (n + 1), :taps]

    ratio[...] = final[at_end : at_end + 1, 0:1] / final[at_end : at_end + 1, 1:2]

    for n in range(4):
        for dst in range(2):
            side_copy(n, dst, dst).wait_send()
        for slot in range(4):
            core_copy(n, slot).wait_send()
    for copy in issued:
        copy.wait_send()


def tail(
    lengths, gt, wq, we, hid, pre, n1, gf, ga, mx, tok, first, sums, bins, qv_grad, conv_grad, bound,
    taps,
):
    quarter, model = first.shape
    chunks = 3
    size = quarter // chunks
    ff = hid.shape[1] // 32
    width = mx.shape[1]
    heads = width // HEAD_DIM
    on, oh = model // 8, width
    qn, qh = model // 8, gt.shape[0]
    blocks = ((4, ff, model), (4, ff, model), (4, on, oh), (qn, qh))
    own = lambda *s: jax.ShapeDtypeStruct(s, f32)
    vm = lambda *s: pltpu.VMEM(s, low)
    dma = pltpu.SemaphoreType.DMA
    sources = (gt, wq, we, hid, pre, n1, gf, ga, mx, tok)
    small = -(-(bins.shape[1] // model + 15 + 4 * heads) // 8) * 8
    vmem = pl.BlockSpec(memory_space=pltpu.VMEM)
    return pl.pallas_call(
        tail_kernel,
        out_shape=[
            own(quarter, model), own(ff, model), own(ff, model), own(oh, on), own(3, qn, width),
            own(1, ff), own(6, model // 32), own(2, width), own(heads, taps), own(1, 1),
        ],
        in_specs=[pl.BlockSpec(memory_space=pltpu.SMEM)]
        + [pl.BlockSpec(memory_space=pl.ANY)] * 11
        + [vmem] * 5,
        out_specs=[vmem] * 10,
        scratch_shapes=[
            pltpu.VMEM((6, small, model), f32),
            *[vm(*x.shape) for x in sources],
            vm(3, chunks, qh, size), vm(2, chunks, size, model), vm(2, chunks, size, model),
            vm(chunks, size, model),
            vm(4, *blocks[0]), vm(4, *blocks[1]),
            vm(4, 8, on, oh), vm(8, qn, qh), pltpu.VMEM((qh, model), f32),
            *[vm(4, *s) for s in blocks],
            *[vm(2, *s) for s in blocks],
            *[vm(*s) for s in blocks],
            *[vm(3, *s[1:]) for s in blocks[:3]],
            *[vm(2, *s[1:]) for s in blocks[:3]],
            *[vm(*s[1:]) for s in blocks[:3]],
            pltpu.VMEM((5, small, model), f32),
            dma((11,)),
            dma((3, chunks)), dma((3, chunks)), dma((2, chunks)), dma((2, chunks)),
            dma((chunks,)), dma((chunks,)), dma((4, 4)), dma((4, 4)),
            dma((4, 3)), dma((4, 3)), dma((3, 3)), dma((3, 3)), dma((3, 2)), dma((3, 2)),
            dma((3,)), dma((3,)), dma((5,)), dma((5,)),
        ],
        compiler_params=pltpu.CompilerParams(
            collective_id=3, has_side_effects=True, vmem_limit_bytes=63 * 1024 * 1024
        ),
        name="tail",
    )(lengths, *sources, first, sums, bins, qv_grad, conv_grad, bound)


def cumulative(x):
    t = 1.0 / (1.0 + 0.23164189 * jnp.abs(x))
    density = jnp.exp(-0.5 * x * x) * 0.3989422804
    poly = t * (
        0.319381530 + t * (-0.356563782 + t * (1.781477937 + t * (-1.821255978 + t * 1.330274429)))
    )
    upper = density * poly
    return jnp.where(x >= 0.0, 1.0 - upper, upper), density


def normed(x):
    centre = x - jnp.mean(x, axis=1, keepdims=True)
    scale = lax.rsqrt(jnp.mean(centre * centre, axis=1, keepdims=True) + norm_eps)
    return centre * scale, scale


def norm_back(grad, gain, rows, scale):
    e = grad * gain
    return scale * (
        e - jnp.mean(e, axis=1, keepdims=True) - rows * jnp.mean(e * rows, axis=1, keepdims=True)
    )


def middle_kernel(
    share,
    mixed_ref, own0, own1, own2, own3, tok_hbm, cot_hbm, weight_hbm,
    vec_ref,
    out_hbm, first_hbm, attn_hbm, hidden_hbm, pre_hbm, norm_hbm, ffn_hbm, all_ref, grad_ref,
    sums_ref, bin_ref, end_hbm,
    out_ref, first_ref, attn_ref, hidden_ref, pre_ref, norm_ref, ffn_ref, tok_ref, cot_ref,
    packs, wof, wo, slope, total, n1_ref, scale_ref, turned,
    a_send, a_recv, f_send, f_recv, s_send, s_recv, p_send, p_recv, g_send, g_recv,
    own_sem, own_turn, out_sem, w_send, w_recv,
):
    b, z, bc, bx, by = place()
    both = bx + by - b
    flip = bc - b
    peers = [(b, lax.rem(z + i, 4)) for i in (1, 2, 3)]
    width, quarter = all_ref.shape[1:]
    model = tok_hbm.shape[1]
    owns = (own0, own1, own2, own3)
    origins = [lax.rem(z + 4 - i, 4) for i in range(4)]
    size = turned.shape[2]
    tiles = quarter // size
    issued = []

    def own_columns(n):
        return pl.ds(pl.multiple_of(n * quarter, quarter), quarter)

    local = [
        pltpu.make_async_copy(own, packs.at[b, origin], own_sem.at[i])
        for i, (own, origin) in enumerate(zip(owns, origins))
    ]
    local.append(
        pltpu.make_async_copy(mixed_ref.at[:, own_columns(z)], all_ref.at[z], own_sem.at[4])
    )
    local.append(
        pltpu.make_async_copy(
            tok_hbm.at[pl.ds(pl.multiple_of(z * quarter, quarter), quarter)], tok_ref, own_sem.at[5]
        )
    )
    cot_load = pltpu.make_async_copy(cot_hbm, cot_ref, own_sem.at[6])
    for copy in local:
        copy.start()
    cot_load.start()
    greet(peers + [(bc, z), (bx, z), (by, z)])

    ff = (packs.shape[2] - 32) // 2
    half = ff // 2
    pieces = ((2 * ff, 32), (0, half), (half, half), (ff, ff))
    through_y = (True, True, True, False)
    count = len(pieces)

    def rows_of(n):
        return pl.ds(*pieces[n])

    def mix_copy(r, i):
        to = lax.rem(z + i, 4)
        src = mixed_ref.at[:, pl.ds(pl.multiple_of(to * quarter + r * size, size), size)]
        return remote(
            src, all_ref.at[z, :, pl.ds(r * size, size)], a_send.at[r, i - 1], a_recv.at[r, i - 1],
            (b, to),
        )

    def side(n, axis):
        out = []
        for i in range(4):
            out.append(
                remote(
                    owns[i].at[rows_of(n)], packs.at[b, origins[i], rows_of(n)],
                    f_send.at[n, axis, i], f_recv.at[n, axis, i], (by if axis else bx, z),
                )
            )
        return out

    def side_start(n):
        for axis in (0, 1):
            for copy in side(n, axis):
                copy.start()
                issued.append(copy)

    def block(n, who):
        return packs.at[who, :, rows_of(n)]

    def corner(n):
        who, device = (bx, by) if through_y[n] else (by, bx)
        return remote(block(n, who), block(n, who), s_send.at[n], s_recv.at[n], (device, z))

    def mate(n, slot, who):
        return remote(
            block(n, who), block(n, who), p_send.at[n, slot], p_recv.at[n, slot], (bc, z)
        )

    def mate_start(n, slot, who):
        mate(n, slot, who).start()

    def side_wait(n, axis):
        who = by if axis else bx
        for i in range(4):
            ref = packs.at[who, origins[i], rows_of(n)]
            remote(
                ref, ref, f_send.at[n, axis, i], f_recv.at[n, axis, i], (who, z)
            ).wait_recv()
        if through_y[n] == (axis == 0):
            corner(n).start()
        mate_start(n, 1 + axis, who)

    def corner_wait(n):
        device = by if through_y[n] else bx
        ref = block(n, both)
        remote(ref, ref, s_send.at[n], s_recv.at[n], (device, z)).wait_recv()
        mate_start(n, 3, both)

    def mate_wait(n, slot, who):
        mate(n, slot, who + flip).wait_recv()

    side_start(0)
    side_start(1)
    for r in range(tiles):
        for i in (1, 2, 3):
            copy = mix_copy(r, i)
            copy.start()
            issued.append(copy)
    is_end = (z == 0) | (z == 3)
    end_copy = remote(
        weight_hbm, end_hbm, w_send.at[0], w_recv.at[0], (b, jnp.where(z < 2, 1, 2))
    )

    @pl.when(is_end)
    def _():
        end_copy.start()

    for copy in local:
        copy.wait()
    for n in range(count):
        mate_start(n, 0, b)
    out_bias, gain1, shift1, down_bias, gain2, shift2 = [
        vec_ref[n : n + 1, :] for n in range(6)
    ]
    sums_ref[...] = jnp.zeros_like(sums_ref)
    bin_ref[...] = jnp.zeros_like(bin_ref)
    total[...] = jnp.zeros_like(total)
    side_wait(0, 0)
    side_wait(0, 1)
    side_start(2)
    side_start(3)
    corner_wait(0)
    for slot, who in enumerate((b, bx, by, both)):
        mate_wait(0, slot, who)
    group = 4 * ff
    for q in range(8):
        for s in range(4):
            wof[pl.ds(s * width + q * share, share), :] = packs[
                q, s, pl.ds(2 * ff, share), :
            ].astype(f32)
    wo[...] = wof[...].astype(low).reshape(wo.shape)
    for q in range(8):
        row = jnp.zeros((1, group), f32)
        for s in range(4):
            row = row + packs[q, s, 2 * ff + share : 2 * ff + share + 1, :group].astype(f32)
        bin_ref[1:2, q * group : (q + 1) * group] = row

    def row_sum(n, x):
        sums_ref[n : n + 1, :] += jnp.sum(x, axis=0, keepdims=True)

    def first_rows(r, _):
        rows = pl.ds(pl.multiple_of(r * size, size), size)

        @pl.when(r == 1)
        def _():
            side_wait(1, 0)
            side_wait(1, 1)

        @pl.when(r == 2)
        def _():
            side_wait(2, 0)
            side_wait(2, 1)

        for i in (1, 2, 3):
            ref = all_ref.at[origins[i], :, rows]
            remote(
                ref, ref, a_send.at[r, i - 1], a_recv.at[r, i - 1], (b, origins[i])
            ).wait_recv()
        attn = jnp.zeros((size, model), f32)
        for s in range(4):
            attn = attn + lax.dot_general(
                all_ref[s, :, rows], wo[s], (((0,), (0,)), ((), ())), preferred_element_type=f32
            )
        n1, scale1 = normed(tok_ref[rows, :].astype(f32) + attn + out_bias)
        n1_ref[rows, :] = n1
        scale_ref[rows, :] = jnp.broadcast_to(scale1, (size, scale_ref.shape[1]))
        norm_ref[rows, :] = (n1 * gain1 + shift1).astype(low)
        return 0

    span = 2 * group

    def weights(c, start):
        return jnp.concatenate(
            [
                packs[2 * c + n, :, pl.ds(start, ff), :].reshape(group, model)
                for n in range(2)
            ],
            axis=0,
        )

    def tile_rows(r):
        return pl.ds(pl.multiple_of(r * size, size), size)

    def feed(who):
        c = who // 2
        lanes = pl.ds(pl.multiple_of(c * span, span), span)

        def one(r, _):
            rows = tile_rows(r)
            act = mul_t(norm_ref[rows, :], weights(c, 0)) + bin_ref[1:2, lanes]
            phi, density = cumulative(act)
            hidden = (act * phi).astype(low)
            hidden_ref[rows, lanes] = hidden
            slope[rows, lanes] = phi + act * density
            total[rows, :] += mul(hidden, weights(c, ff))
            return 0

        lax.fori_loop(0, tiles, one, 0)

    lax.fori_loop(0, tiles, first_rows, 0)

    def group_step(k, _):
        def mates(slot, who):
            for n in range(1, count):
                mate_wait(n, slot, who)

        @pl.when(k == 0)
        def _():
            mates(0, b)

        @pl.when(k == 1)
        def _():
            side_wait(3, 0)
            side_wait(3, 1)
            mates(1, bx)

        @pl.when(k == 2)
        def _():
            corner_wait(1)
            mates(2, by)

        @pl.when(k == 3)
        def _():
            corner_wait(2)
            corner_wait(3)
            mates(3, both)

        feed(b + (k % 2) * (bx - b) + (k // 2) * (by - b))
        return 0

    lax.fori_loop(0, 4, group_step, 0)

    def turn_copy(r, i):
        to = lax.rem(z + i, 4)
        src = turned.at[r, pl.ds(pl.multiple_of(to * width, width), width)]
        dst = grad_ref.at[:, pl.ds(pl.multiple_of(z * quarter + r * size, size), size)]
        return remote(src, dst, g_send.at[r, i - 1], g_recv.at[r, i - 1], (b, to))

    def turn_own(r):
        src = turned.at[r, pl.ds(pl.multiple_of(z * width, width), width)]
        dst = grad_ref.at[:, pl.ds(pl.multiple_of(z * quarter + r * size, size), size)]
        return pltpu.make_async_copy(src, dst, own_turn.at[r])

    stores = (
        (out_ref, out_hbm), (first_ref, first_hbm), (attn_ref, attn_hbm), (pre_ref, pre_hbm),
        (ffn_ref, ffn_hbm), (hidden_ref, hidden_hbm), (norm_ref, norm_hbm),
    )

    def store(r, n):
        src, dst = stores[n]
        rows = tile_rows(r)
        return pltpu.make_async_copy(src.at[rows], dst.at[rows], out_sem.at[r, n])

    cot_load.wait()

    def row_tile(r, _):
        rows = tile_rows(r)
        n1 = n1_ref[rows, :]
        norm1 = n1 * gain1 + shift1
        n2, scale2 = normed(norm1 + total[rows, :] + down_bias)
        out_ref[rows, :] = (n2 * gain2 + shift2).astype(low)
        cot = cot_ref[rows, :].astype(f32)
        row_sum(1, cot * n2)
        row_sum(2, cot)
        grad2 = norm_back(cot, gain2, n2, scale2)
        grad_low = grad2.astype(low)
        ffn_ref[rows, :] = grad_low
        row_sum(0, grad_low.astype(f32))
        total[rows, :] = grad2

        def backward(c, _):
            lanes = pl.ds(pl.multiple_of(c * span, span), span)
            grad = (slope[rows, lanes] * mul_t(grad_low, weights(c, ff))).astype(low)
            pre_ref[rows, lanes] = grad
            bin_ref[0:1, lanes] += jnp.sum(grad.astype(f32), axis=0, keepdims=True)
            total[rows, :] += mul(grad, weights(c, 0))
            return 0

        lax.fori_loop(0, 4, backward, 0)
        grad1 = total[rows, :]
        row_sum(3, grad1 * n1)
        row_sum(4, grad1)
        first = norm_back(grad1, gain1, n1, scale_ref[rows, 0:1])
        first_ref[rows, :] = first
        attn_low = first.astype(low)
        attn_ref[rows, :] = attn_low
        row_sum(5, attn_low.astype(f32))
        for s in range(4):
            turned[r, pl.ds(s * width, width), :] = mul_t(wo[s], attn_low).astype(low)
        for i in (1, 2, 3):
            turn_copy(r, i).start()
        turn_own(r).start()
        for n in range(len(stores)):
            store(r, n).start()
        return 0

    lax.fori_loop(0, tiles, row_tile, 0)

    def finish(r, _):
        for i in (1, 2, 3):
            source = origins[i]
            ref = grad_ref.at[:, pl.ds(pl.multiple_of(source * quarter + r * size, size), size)]
            remote(ref, ref, g_send.at[r, i - 1], g_recv.at[r, i - 1], (b, source)).wait_recv()
            turn_copy(r, i).wait_send()
        turn_own(r).wait()
        for n in range(len(stores)):
            store(r, n).wait()
        return 0

    lax.fori_loop(0, tiles, finish, 0)

    @pl.when(is_end)
    def _():
        end_copy.wait_send()

    @pl.when(jnp.logical_not(is_end))
    def _():
        remote(
            end_hbm, end_hbm, w_send.at[0], w_recv.at[0], (b, jnp.where(z < 2, 0, 3))
        ).wait_recv()

    for n in range(count):
        corner(n).wait_send()
        for slot, who in enumerate((b, bx, by, both)):
            mate(n, slot, who).wait_send()
    for copy in issued:
        copy.wait_send()


def ffn_middle(mixed_t, packs, tokens, cot, weight_t, vectors, ff, share):
    width, tok_count = mixed_t.shape
    quarter, model = tok_count // 4, tokens.shape[1]
    size = quarter // 3
    rows = packs[0].shape[0]
    shape = jax.ShapeDtypeStruct
    vmem = pl.BlockSpec(memory_space=pltpu.VMEM)
    hbm = pl.BlockSpec(memory_space=pl.ANY)
    dma = pltpu.SemaphoreType.DMA
    kept = [
        ((quarter, model), low),
        ((quarter, model), f32),
        ((quarter, model), low),
        ((quarter, 32 * ff), low),
        ((quarter, 32 * ff), low),
        ((quarter, model), low),
        ((quarter, model), low),
    ]
    return pl.pallas_call(
        partial(middle_kernel, share),
        out_shape=[shape(*x) for x in kept]
        + [
            shape((4, width, quarter), low),
            shape((width, tok_count), low),
            shape((8, model), f32),
            shape((8, 32 * ff), f32),
            shape(weight_t.shape, low),
        ],
        in_specs=[hbm] * 8 + [vmem],
        out_specs=[hbm] * 7 + [vmem, hbm, vmem, vmem, hbm],
        scratch_shapes=[pltpu.VMEM(*x) for x in kept]
        + [
            pltpu.VMEM((quarter, model), low),
            pltpu.VMEM((quarter, model), low),
            pltpu.VMEM((8, 4, rows, model), low),
            pltpu.VMEM((4 * width, model), f32),
            pltpu.VMEM((4, width, model), low),
            pltpu.VMEM((quarter, 32 * ff), f32),
            pltpu.VMEM((quarter, model), f32),
            pltpu.VMEM((quarter, model), f32),
            pltpu.VMEM((quarter, 128), f32),
            pltpu.VMEM((3, 4 * width, size), low),
            dma((3, 3)), dma((3, 3)), dma((4, 2, 4)), dma((4, 2, 4)), dma((4,)), dma((4,)),
            dma((4, 4)), dma((4, 4)), dma((3, 3)), dma((3, 3)),
            dma((7,)), dma((3,)), dma((3, 7)), dma((1,)), dma((1,)),
        ],
        compiler_params=pltpu.CompilerParams(
            collective_id=1, has_side_effects=True, vmem_limit_bytes=63 * 1024 * 1024
        ),
        name="middle",
    )(mixed_t, *packs, tokens, cot, weight_t, vectors)


def settle_kernel(count, pieces, *refs):
    sources, results = refs[:count], refs[count : 2 * count]
    held, came, went = refs[2 * count : 3 * count], refs[3 * count], refs[3 * count + 1]
    moves = []
    for n in range(count):
        rows = held[n].shape[0] // pieces[n]
        for k in range(pieces[n]):
            at = pl.ds(k * rows, rows)
            moves.append((sources[n].at[at], held[n].at[at], results[n].at[at]))
    coming = [
        pltpu.make_async_copy(src, mid, came.at[n]) for n, (src, mid, _) in enumerate(moves)
    ]
    going = [
        pltpu.make_async_copy(mid, dst, went.at[n]) for n, (_, mid, dst) in enumerate(moves)
    ]
    for copy in coming:
        copy.start()
    for arrival, copy in zip(coming, going):
        arrival.wait()
        copy.start()
    for copy in going:
        copy.wait()


def settle(*arrays):
    count = len(arrays)
    pieces = [4 if x.size > 2**18 else 1 for x in arrays]
    hbm = pl.BlockSpec(memory_space=pl.ANY)
    return pl.pallas_call(
        partial(settle_kernel, count, pieces),
        out_shape=[jax.ShapeDtypeStruct(x.shape, x.dtype) for x in arrays],
        in_specs=[hbm] * count,
        out_specs=[hbm] * count,
        scratch_shapes=[pltpu.VMEM(x.shape, x.dtype) for x in arrays]
        + [pltpu.SemaphoreType.DMA((sum(pieces),))] * 2,
        name="settle",
    )(*arrays)


def slice_body(
    tokens,
    qkv_weight,
    qv_bias,
    conv_weight,
    out_weight,
    out_bias,
    norm1_gain,
    norm1_bias,
    ffn_in_weight,
    ffn_in_bias,
    ffn_out_weight,
    ffn_out_bias,
    norm2_gain,
    norm2_bias,
    cotangent,
    seq_lengths,
    segment_ids,
    landmark_bounds,
):
    model = tokens.shape[1]
    width = qkv_weight.shape[2]
    kernel_taps = conv_weight.shape[1]
    slots, marks = landmark_bounds.shape
    z = lax.axis_index("heads")
    b = lax.axis_index("batch")
    weight_t = jnp.transpose(qkv_weight.reshape(model, 3 * width))
    ff_own = ffn_out_weight.shape[0]
    share = width // 8
    bias_row = lax.dynamic_update_slice_in_dim(
        jnp.zeros((4 * ff_own,), low), ffn_in_bias, z * ff_own, 0
    )
    misc_own = jnp.concatenate(
        [
            lax.dynamic_slice_in_dim(out_weight, b * share, share, 0),
            jnp.zeros((32 - share, model), low).at[0, : 4 * ff_own].set(bias_row),
        ],
        axis=0,
    )
    pack = jnp.concatenate([jnp.transpose(ffn_in_weight), ffn_out_weight, misc_own], axis=0)
    packs = [pack] + [
        lax.ppermute(pack, "heads", [(n, (n + i) % 4) for n in range(4)]) for i in (1, 2, 3)
    ]
    forward = mix_forward(
        seq_lengths, tokens, weight_t, qv_bias, conv_weight, slots, marks
    )
    qkv_t, first, last, mixed_t, mark, value, inner, denom, middle, steps, inverse, bound = forward
    vectors = jnp.stack(
        [out_bias, norm1_gain, norm1_bias, ffn_out_bias, norm2_gain, norm2_bias]
    )
    (
        final_low, grad_first, grad_attn_low, hidden_low, grad_pre, norm1_low, grad_ffn_low,
        mixed_all, grad_mix_t, vector_sums, bias_sums, weight_end,
    ) = ffn_middle(mixed_t, packs, tokens, cotangent, weight_t, vectors, ff_own, share)
    saved = (qkv_t, first, last, mark, value, inner, denom, middle, steps, inverse)
    grad_t, grad_bias, grad_conv = mix_backward(
        seq_lengths, grad_mix_t, saved, conv_weight, slots, marks
    )
    (
        input_grad, down_share, up_share, out_share, qkv_share,
        in_bias_share, vector_share, bias_out, conv_out, condition,
    ) = tail(
        seq_lengths, grad_t, weight_t, weight_end, hidden_low, grad_pre, norm1_low, grad_ffn_low,
        grad_attn_low, mixed_all, tokens, grad_first, vector_sums, bias_sums, grad_bias,
        grad_conv, bound, kernel_taps,
    )
    (
        final_low, input_grad, down_share, up_share, out_share, qkv_share,
        in_bias_share, vector_share, bias_out, conv_out, condition,
    ) = settle(
        final_low, input_grad, down_share, up_share, out_share, qkv_share,
        in_bias_share, vector_share, bias_out, conv_out, condition,
    )
    return (
        final_low,
        input_grad,
        jnp.swapaxes(qkv_share, 0, 1),
        bias_out,
        conv_out,
        out_share,
        jnp.transpose(up_share),
        in_bias_share.reshape(ff_own),
        down_share,
        vector_share,
        condition.reshape(()),
    )


def solution(mesh):
    chosen = slice_body if dict(mesh.shape) == {"batch": 8, "heads": 4} else body
    in_specs = (
        P("batch", None),
        P(None, None, "heads"),
        P(),
        P(),
        P("heads", None),
        P(),
        P(),
        P(),
        P(None, ("batch", "heads")),
        P(("batch", "heads")),
        P(("batch", "heads"), None),
        P(),
        P(),
        P(),
        P(("batch", "heads"), None),
        P("batch"),
        P("batch"),
        P("batch", None),
    )
    out_specs = (
        P(("batch", "heads"), None),
        P(("batch", "heads"), None),
        P("batch", None, "heads"),
        P(None, "heads"),
        P("heads", None),
        P("heads", "batch"),
        P(None, ("batch", "heads")),
        P(("batch", "heads")),
        P(("batch", "heads"), None),
        P(None, ("batch", "heads")),
        P(),
    )
    return jax.shard_map(chosen, mesh=mesh, in_specs=in_specs, out_specs=out_specs, check_vma=False)
```

```python
from functools import partial

import jax
import jax.numpy as jnp
from jax import lax
from jax.experimental import pallas as pl
from jax.experimental.pallas import tpu as pltpu
from jax.sharding import PartitionSpec as P

HEAD_DIM = 64
PINV_ITERS = 6
TILE = 512
SUB = 128

f32 = jnp.float32
low = jnp.bfloat16
mask_fill = -1000000000.0


def split(x):
    high = x.astype(low)
    return high, (x - high.astype(f32)).astype(low)


def mul(a, b):
    return lax.dot_general(a, b, (((1,), (0,)), ((), ())), preferred_element_type=f32)


def mul_t(a, b):
    return lax.dot_general(a, b, (((1,), (1,)), ((), ())), preferred_element_type=f32)


def wide(form, left, right):
    left_high, left_low = split(left)
    right_high, right_low = split(right)
    return form(left_high, right_high) + (
        form(left_high, right_low) + form(left_low, right_high)
    )


def block_grid(rows, cols):
    row_block = lax.broadcasted_iota(jnp.int32, (rows, cols), 0) // HEAD_DIM
    col_block = lax.broadcasted_iota(jnp.int32, (rows, cols), 1) // HEAD_DIM
    return row_block == col_block


def spread(x, blocks):
    count = blocks.shape[0] // x.shape[0]
    return jnp.where(blocks, jnp.concatenate([x] * count, axis=0), jnp.zeros_like(x[:1, :1]))


def fold(x, blocks):
    kept = jnp.where(blocks, x, jnp.zeros_like(x[:1, :1]))
    rows = HEAD_DIM
    out = kept[:rows]
    for n in range(1, x.shape[0] // rows):
        out = out + kept[n * rows : (n + 1) * rows]
    return out


def ready(x, ones):
    count = ones.shape[0] // HEAD_DIM
    high, rest = split(x)
    return [jnp.concatenate([part] * count, axis=0) * ones for part in (high, rest)]


def pack_mul(lefts, right, form=mul):
    halves = [split(x) for x in lefts]
    high = [x[0] for x in halves]
    count = len(lefts)
    both_parts = form(jnp.concatenate(high + [x[1] for x in halves], axis=0), right[0])
    rest = form(jnp.concatenate(high, axis=0), right[1])
    out = []
    for n in range(count):
        at = slice(n * HEAD_DIM, (n + 1) * HEAD_DIM)
        more = slice((count + n) * HEAD_DIM, (count + n + 1) * HEAD_DIM)
        out.append(both_parts[at] + (both_parts[more] + rest[at]))
    return out


def block_ones(size):
    return jnp.where(block_grid(size, size), 1.0, 0.0).astype(low)


def slot_bounds(len_ref, s, slots):
    start = jnp.int32(0)
    for n in range(slots):
        start = start + jnp.where(n < s, len_ref[n], 0)
    return start, start + len_ref[s]


def eye_pack(width):
    row = lax.broadcasted_iota(jnp.int32, (HEAD_DIM, width), 0)
    col = lax.broadcasted_iota(jnp.int32, (HEAD_DIM, width), 1) % HEAD_DIM
    return jnp.where(row == col, 1.0, 0.0).astype(f32)


def lane_mask(start, end, at, width):
    tok = at + lax.broadcasted_iota(jnp.int32, (1, width), 1)
    return (tok >= start) & (tok < end)


def band(taps_row, width):
    row = lax.broadcasted_iota(jnp.int32, (SUB, 3 * SUB), 0)
    col = lax.broadcasted_iota(jnp.int32, (SUB, 3 * SUB), 1)
    off = col - row - (SUB - width // 2)
    out = jnp.zeros((SUB, 3 * SUB), f32)
    for n in range(width):
        out = jnp.where(off == n, taps_row[:, n : n + 1], out)
    return out


def slot_marks(len_ref, at, slots, marks, width):
    rows = slots * marks
    row = lax.broadcasted_iota(jnp.int32, (rows, 1), 0)
    slot = row // marks
    mark = row % marks
    start = jnp.zeros((rows, 1), jnp.int32)
    length = jnp.zeros((rows, 1), jnp.int32)
    for n in range(slots):
        start = start + jnp.where(slot > n, len_ref[n], 0)
        length = jnp.where(slot == n, len_ref[n], length)
    lower = start + (mark * length) // marks
    upper = start + ((mark + 1) * length) // marks
    inv_count = 1.0 / jnp.maximum((upper - lower).astype(f32), 1.0)
    tok = at + lax.broadcasted_iota(jnp.int32, (rows, width), 1)
    member = jnp.where((tok >= lower) & (tok < upper), 1.0, 0.0)
    return member, inv_count


def mix_forward_kernel(
    slots, marks, taps,
    len_ref, tok_ref, weight_ref, bias_ref, conv_ref,
    qkv_hbm, first_hbm, last_hbm, mixed_ref, mark_ref, value_ref, inner_ref,
    denom_ref, middle_ref, steps_hbm, inverse_ref, bound_ref,
    qkv_ref, first_ref, last_ref, steps_ref,
    vpad, scores, vsum, bias_col, conv_own, out_sem,
):
    step = pl.program_id(0)
    width = first_ref.shape[0]
    heads = width // HEAD_DIM
    tok_count = qkv_ref.shape[1]
    tiles = tok_count // TILE
    packed = slots * marks
    at = pl.multiple_of(step * TILE, TILE)

    @pl.when(step == 0)
    def _():
        z = lax.axis_index("heads")
        own_taps(conv_own, conv_ref, z)
        columns = jnp.transpose(jnp.concatenate([bias_ref[...], bias_ref[...]], axis=0))
        bias_col[: bias_ref.shape[1], :] = columns
        mark_ref[...] = jnp.zeros_like(mark_ref)
        vsum[...] = jnp.zeros_like(vsum)
        vpad[:, :SUB] = jnp.zeros((width, SUB), low)
        vpad[:, tok_count + SUB :] = jnp.zeros((width, SUB), low)

    at_head = pl.ds(pl.multiple_of(lax.axis_index("heads") * width, HEAD_DIM), width)
    rows = mul_t(weight_ref[...], tok_ref[...])
    rows = jnp.concatenate(
        [
            rows[:width] + bias_col[at_head, 0:1],
            rows[width : 2 * width],
            rows[2 * width :] + bias_col[at_head, 1:2],
        ],
        axis=0,
    ).astype(low)
    qkv_ref[:, pl.ds(at, TILE)] = rows
    vpad[:, pl.ds(pl.multiple_of(at + SUB, SUB), TILE)] = rows[2 * width :]
    member, inv_count = slot_marks(len_ref, at, slots, marks, TILE)
    mark_ref[...] += mul_t(member.astype(low), rows[: 2 * width])
    vsum[...] += mul_t(jnp.ones((8, TILE), low), rows[2 * width :])
    first_ref[:, pl.ds(at, TILE)] = jnp.zeros((width, TILE), low)
    last_ref[:, pl.ds(at, TILE)] = jnp.zeros((width, TILE), low)
    mixed_ref[:, pl.ds(at, TILE)] = jnp.zeros((width, TILE), low)

    leaving = [
        pltpu.make_async_copy(src, dst, out_sem.at[n])
        for n, (src, dst) in enumerate(
            (
                (qkv_ref, qkv_hbm), (steps_ref, steps_hbm), (first_ref, first_hbm),
                (last_ref, last_hbm),
            )
        )
    ]

    @pl.when(step == tiles - 1)
    def _():
        leaving[0].start()
        mark_ref[...] = mark_ref[...] * inv_count
        head_blocks = block_grid(width, width)
        slot_blocks = block_grid(packed, packed)
        ones = block_ones(packed)
        eye = eye_pack(packed)
        scale = HEAD_DIM ** -0.5

        middles, inverses_t, products = [], [], []
        bound_total = jnp.zeros((1, 1), f32)
        lane_slot = lax.broadcasted_iota(jnp.int32, (1, packed), 1) // marks
        for h in range(heads):
            q_marks = mark_ref[:, h * HEAD_DIM : (h + 1) * HEAD_DIM]
            k_marks = mark_ref[:, width + h * HEAD_DIM : width + (h + 1) * HEAD_DIM]
            sim = wide(mul_t, q_marks, k_marks) * scale
            sim = jnp.where(slot_blocks, sim, -1e30)
            sim = jnp.exp(sim - jnp.max(sim, axis=1, keepdims=True))
            sim = sim / jnp.sum(sim, axis=1, keepdims=True)
            middle = fold(sim, slot_blocks)
            col_sums = jnp.sum(middle, axis=0, keepdims=True)
            bound = jnp.zeros((1, packed), f32)
            for s in range(slots):
                top = jnp.max(jnp.where(lane_slot == s, col_sums, 0.0), axis=1, keepdims=True)
                bound = jnp.where(lane_slot == s, top, bound)
                bound_total += jnp.where(len_ref[s] > 0, top, 0.0)
            middle_ref[h] = middle
            middles.append(middle)
            inverses_t.append(middle / bound)
            products.append(pack_mul([middle], ready(middle, ones), mul_t)[0] / bound)
        bound_ref[...] = jnp.broadcast_to(bound_total, bound_ref.shape)

        def newton(n, carry):
            out = []
            for h in range(heads):
                before_t, weight, product = carry[h]
                (inverse_t,) = pack_mul([0.25 * weight], ready(before_t, ones))
                (square,) = pack_mul([product], ready(product, ones))
                cube, fourth = pack_mul([product, square], ready(square, ones))
                third = 13.0 * eye - 15.0 * product + 7.0 * square - cube
                steps_ref[n, 0, h] = product
                steps_ref[n, 1, h] = square
                steps_ref[n, 2, h] = third
                steps_ref[n, 3, h] = inverse_t
                after = 0.25 * (13.0 * product - 15.0 * square + 7.0 * cube - fourth)
                out.append((inverse_t, third, after))
            return tuple(out)

        start = tuple((x, 4.0 * eye, p) for x, p in zip(inverses_t, products))
        final = lax.fori_loop(0, PINV_ITERS, newton, start)
        for h in range(heads):
            inverse_t, third, _ = final[h]
            inverse_ref[h] = pack_mul([0.25 * third], ready(inverse_t, ones))[0]
        leaving[1].start()

        def one_slot(s, _):
            start, end = slot_bounds(len_ref, s, slots)
            lo, hi = start // TILE, (end + TILE - 1) // TILE
            hi = jnp.where(end > start, hi, lo)
            own = mark_ref[pl.ds(pl.multiple_of(s * marks, marks), marks), :] * scale
            q_block = spread(own[:, :width], head_blocks).astype(low)
            k_block = spread(own[:, width:], head_blocks).astype(low)

            def score_tile(n, top):
                t = pl.multiple_of(n * TILE, TILE)
                mask = lane_mask(start, end, t, TILE)
                sim = mul(k_block, qkv_ref[:width, pl.ds(t, TILE)])
                sim = sim.reshape(heads, marks, TILE)
                sim = jnp.exp(sim - jnp.max(sim, axis=1, keepdims=True))
                sim = sim / jnp.sum(sim, axis=1, keepdims=True)
                sim = sim.reshape(width, TILE)
                old = first_ref[:, pl.ds(t, TILE)].astype(f32)
                first_ref[:, pl.ds(t, TILE)] = jnp.where(mask, sim, old).astype(low)
                sim = mul(q_block, qkv_ref[width : 2 * width, pl.ds(t, TILE)])
                sim = jnp.where(mask, sim, mask_fill)
                scores[:, pl.ds(t, TILE)] = sim
                for c in range(TILE // SUB):
                    top = jnp.maximum(top, sim[:, c * SUB : (c + 1) * SUB])
                return top

            top = lax.fori_loop(lo, hi, score_tile, jnp.full((width, SUB), mask_fill, f32))
            top = jnp.max(top, axis=1, keepdims=True)

            def value_tile(n, carry):
                denom, total = carry
                t = pl.multiple_of(n * TILE, TILE)
                mask = lane_mask(start, end, t, TILE)
                part = jnp.exp(scores[:, pl.ds(t, TILE)] - top)
                old = last_ref[:, pl.ds(t, TILE)].astype(f32)
                last_ref[:, pl.ds(t, TILE)] = jnp.where(mask, part, old).astype(low)
                total = total + mul_t(part.astype(low), qkv_ref[2 * width :, pl.ds(t, TILE)])
                for c in range(TILE // SUB):
                    denom = denom + part[:, c * SUB : (c + 1) * SUB]
                return denom, total

            denom, total = lax.fori_loop(
                lo, hi, value_tile,
                (jnp.zeros((width, SUB), f32), jnp.zeros((width, width), f32)),
            )
            denom = jnp.sum(denom, axis=1, keepdims=True)
            inv = 1.0 / jnp.where(denom > 0.0, denom, 1.0)
            denom_ref[s] = inv
            values = fold(total * inv, head_blocks)
            values = jnp.where(end > start, values, vsum[:1] / tok_count)
            value_ref[pl.ds(pl.multiple_of(s * marks, marks), marks), :] = values
            return 0

        lax.fori_loop(0, slots, one_slot, 0)
        leaving[2].start()
        leaving[3].start()

        lane_head = lax.broadcasted_iota(jnp.int32, (1, width), 1) // HEAD_DIM
        inner = jnp.zeros((packed, width), f32)
        for h in range(heads):
            (inverse,) = pack_mul([eye], ready(inverse_ref[h], ones), mul_t)
            own_values = jnp.where(lane_head == h, value_ref[...], 0.0)
            inner = inner + wide(mul, spread(inverse, slot_blocks), own_values)
        inner_ref[...] = inner

        bands = [band(conv_own[h : h + 1, :], taps).astype(low) for h in range(heads)]

        def out_slot(s, _):
            start, end = slot_bounds(len_ref, s, slots)
            lo, hi = start // TILE, (end + TILE - 1) // TILE
            hi = jnp.where(end > start, hi, lo)
            own = inner_ref[pl.ds(pl.multiple_of(s * marks, marks), marks), :]
            a_block = jnp.transpose(spread(own, head_blocks)).astype(low)

            def out_tile(n, _):
                t = pl.multiple_of(n * TILE, TILE)
                mask = lane_mask(start, end, t, TILE)
                rows = mul(a_block, first_ref[:, pl.ds(t, TILE)])
                rows = rows + convolve(vpad, bands, start, end, t, heads)
                old = mixed_ref[:, pl.ds(t, TILE)].astype(f32)
                mixed_ref[:, pl.ds(t, TILE)] = jnp.where(mask, rows, old).astype(low)
                return 0

            return lax.fori_loop(lo, hi, out_tile, 0)

        lax.fori_loop(0, slots, out_slot, 0)
        for copy in leaving:
            copy.wait()


def own_taps(own_ref, all_ref, z):
    heads = own_ref.shape[0]
    for n in range(all_ref.shape[0] // heads):

        @pl.when(z == n)
        def _():
            own_ref[...] = all_ref[n * heads : (n + 1) * heads, :]


def windows(padded, start, end, t):
    full = padded[:, pl.ds(t, TILE + 2 * SUB)]
    keep = lane_mask(start, end, t - SUB, TILE + 2 * SUB)
    return jnp.where(keep, full.astype(f32), 0.0).astype(low)


def convolve(padded, bands, start, end, t, heads):
    full = windows(padded, start, end, t)
    out = []
    count = TILE // SUB
    for h in range(heads):
        own = full[h * HEAD_DIM : (h + 1) * HEAD_DIM]
        stack = jnp.concatenate(
            [own[:, c * SUB : (c + 3) * SUB] for c in range(count)], axis=0
        )
        res = mul_t(stack, bands[h])
        out.append(
            jnp.concatenate(
                [res[c * HEAD_DIM : (c + 1) * HEAD_DIM] for c in range(count)], axis=1
            )
        )
    return jnp.concatenate(out, axis=0)


def mix_backward_kernel(
    slots, marks, taps,
    len_ref, grad_ref, qkv_ref, first_ref, last_hbm, mark_ref, value_ref, inner_ref,
    denom_ref, middle_ref, steps_hbm, inverse_ref, conv_ref,
    out_hbm, bias_ref, conv_out_ref,
    last_ref, steps_ref, out_ref, move_sem,
    gpad, vpad, ds_first, ds_last, conv_grad, d_inner, d_k, d_q, d_value, conv_own,
):
    width = first_ref.shape[0]
    heads = width // HEAD_DIM
    tok_count = qkv_ref.shape[1]
    packed = slots * marks
    scale = HEAD_DIM ** -0.5
    head_blocks = block_grid(width, width)
    slot_blocks = block_grid(packed, packed)
    ones = block_ones(packed)
    eye = eye_pack(packed)
    count = TILE // SUB
    last_in = pltpu.make_async_copy(last_hbm, last_ref, move_sem.at[0])
    steps_in = pltpu.make_async_copy(steps_hbm, steps_ref, move_sem.at[1])
    steps_in.start()
    last_in.start()

    for padded, source in ((gpad, grad_ref[...]), (vpad, qkv_ref[2 * width :, :])):
        padded[:, :SUB] = jnp.zeros((width, SUB), low)
        padded[:, tok_count + SUB :] = jnp.zeros((width, SUB), low)
        padded[:, SUB : tok_count + SUB] = source
    out_ref[...] = jnp.zeros_like(out_ref)
    ds_first[...] = jnp.zeros_like(ds_first)
    ds_last[...] = jnp.zeros_like(ds_last)
    conv_grad[...] = jnp.zeros_like(conv_grad)

    own_taps(conv_own, conv_ref, lax.axis_index("heads"))

    def reach(s):
        start, end = slot_bounds(len_ref, s, slots)
        lo, hi = start // TILE, (end + TILE - 1) // TILE
        return start, end, lo, jnp.where(end > start, hi, lo)

    def own_rows(s):
        return pl.ds(pl.multiple_of(s * marks, marks), marks)

    def first_slot(s, _):
        start, end, lo, hi = reach(s)
        a_block = spread(inner_ref[own_rows(s), :], head_blocks).astype(low)

        def tile(n, carry):
            inner_total, key_total = carry
            t = pl.multiple_of(n * TILE, TILE)
            mask = lane_mask(start, end, t, TILE)
            own_grad = grad_ref[:, pl.ds(t, TILE)]
            kernel_rows = jnp.where(mask, first_ref[:, pl.ds(t, TILE)].astype(f32), 0.0)
            d_kernel = mul(a_block, own_grad)
            prod = (kernel_rows * d_kernel).reshape(heads, marks, TILE)
            row_sum = jnp.sum(prod, axis=1, keepdims=True)
            d_sim = prod - kernel_rows.reshape(heads, marks, TILE) * row_sum
            d_sim = d_sim.reshape(width, TILE)
            d_sim_low = d_sim.astype(low)
            old = ds_first[:, pl.ds(t, TILE)].astype(f32)
            ds_first[:, pl.ds(t, TILE)] = jnp.where(mask, d_sim, old).astype(low)
            inner_total = inner_total + mul_t(kernel_rows.astype(low), own_grad)
            key_total = key_total + mul_t(d_sim_low, qkv_ref[:width, pl.ds(t, TILE)])
            full = windows(vpad, start, end, t)
            grad_own = jnp.where(mask, own_grad.astype(f32), 0.0).astype(low)
            for h in range(heads):
                sel = slice(h * HEAD_DIM, (h + 1) * HEAD_DIM)
                left = jnp.concatenate(
                    [grad_own[sel, c * SUB : (c + 1) * SUB] for c in range(count)], axis=0
                )
                right = jnp.concatenate(
                    [full[sel, c * SUB : (c + 3) * SUB] for c in range(count)], axis=0
                )
                conv_grad[h] += lax.dot_general(
                    left, right, (((0,), (0,)), ((), ())), preferred_element_type=f32
                )
            return inner_total, key_total

        zero = jnp.zeros((width, width), f32)
        inner_total, key_total = lax.fori_loop(lo, hi, tile, (zero, zero))
        d_inner[own_rows(s), :] = fold(inner_total, head_blocks)
        d_k[own_rows(s), :] = fold(key_total, head_blocks) * scale
        return 0

    lax.fori_loop(0, slots, first_slot, 0)

    row = lax.broadcasted_iota(jnp.int32, (SUB, 3 * SUB), 0)
    col = lax.broadcasted_iota(jnp.int32, (SUB, 3 * SUB), 1)
    off = col - row - (SUB - taps // 2)
    tap_lane = lax.broadcasted_iota(jnp.int32, (1, SUB), 1)
    for h in range(heads):
        found = jnp.zeros((1, SUB), f32)
        square = conv_grad[h]
        for n in range(taps):
            part = jnp.sum(jnp.where(off == n, square, 0.0), axis=0, keepdims=True)
            part = jnp.sum(part, axis=1, keepdims=True)
            found = jnp.where(tap_lane == n, part, found)
        conv_out_ref[h : h + 1, :] = found

    lane_head = lax.broadcasted_iota(jnp.int32, (1, width), 1) // HEAD_DIM
    value_total = jnp.zeros((packed, width), f32)
    d_inverses = []
    for h in range(heads):
        own = jnp.where(lane_head == h, d_inner[...], 0.0)
        value_total = value_total + wide(mul, spread(inverse_ref[h], slot_blocks), own)
        d_inverses.append(fold(wide(mul_t, own, value_ref[...]), slot_blocks))
    d_value[...] = value_total

    def before(n, h, d_inverse):
        third, inverse_t = steps_ref[n, 2, h], steps_ref[n, 3, h]
        (d_third,) = pack_mul([0.25 * inverse_t], ready(d_inverse, ones))
        (earlier,) = pack_mul([0.25 * d_inverse], ready(third, ones))
        return earlier, d_third

    def newton(k, carry):
        n = PINV_ITERS - 1 - k
        out = []
        for h in range(heads):
            d_inverse, d_third, grad = carry[h]
            product, square, third = [steps_ref[n, i, h] for i in range(3)]
            mixed = 7.0 * product - square
            by_third, by_one, by_two = pack_mul([third, product, square], ready(grad, ones))
            left_mixed, left_one = pack_mul([mixed, product], ready(d_third, ones))
            (right,) = pack_mul([grad], ready(third, ones))
            (more,) = pack_mul([0.25 * by_one + d_third], ready(mixed, ones))
            (less,) = pack_mul([0.25 * by_two + left_one], ready(product, ones))
            d_product = (
                0.25 * (right + by_third - 13.0 * grad) - 15.0 * d_third + left_mixed + more - less
            )
            earlier, d_before = before(jnp.maximum(n - 1, 0), h, d_inverse)
            last = n == 0
            out.append((jnp.where(last, d_inverse, earlier), d_before, d_product))
        return tuple(out)

    steps_in.wait()
    zero = jnp.zeros((HEAD_DIM, packed), f32)
    start = []
    for h in range(heads):
        start.append(before(PINV_ITERS - 1, h, d_inverses[h]) + (zero,))
    final = lax.fori_loop(0, PINV_ITERS, newton, tuple(start))
    lane_slot = lax.broadcasted_iota(jnp.int32, (1, packed), 1) // marks
    dq_total = jnp.zeros((packed, width), f32)
    dk_total = jnp.zeros((packed, width), f32)
    for h in range(heads):
        d_inverse, _, d_product = final[h]
        middle = middle_ref[h]
        first_t = steps_ref[0, 3, h]
        (d_inverse_t,) = pack_mul([eye], ready(d_inverse, ones), mul_t)
        (d_product_t,) = pack_mul([eye], ready(d_product, ones), mul_t)
        (d_middle,) = pack_mul([d_product + d_product_t], ready(middle, ones))
        col_sums = jnp.sum(middle, axis=0, keepdims=True)
        share = jnp.sum(
            d_inverse_t * first_t + d_product * steps_ref[0, 0, h], axis=0, keepdims=True
        )
        bound = jnp.zeros((1, packed), f32)
        d_bound = jnp.zeros((1, packed), f32)
        hits = jnp.zeros((1, packed), f32)
        for s in range(slots):
            mine = lane_slot == s
            top = jnp.max(jnp.where(mine, col_sums, 0.0), axis=1, keepdims=True)
            total = jnp.sum(jnp.where(mine, share, 0.0), axis=1, keepdims=True)
            number = jnp.sum(
                jnp.where(mine & (col_sums == top), 1.0, 0.0), axis=1, keepdims=True
            )
            bound = jnp.where(mine, top, bound)
            d_bound = jnp.where(mine, -total / top, d_bound)
            hits = jnp.where(mine, number, hits)
        d_middle = (d_middle + d_inverse_t) / bound
        d_middle = d_middle + jnp.where(col_sums == bound, d_bound / hits, 0.0)
        prod = spread(middle * d_middle, slot_blocks)
        d_sim = prod - spread(middle, slot_blocks) * jnp.sum(prod, axis=1, keepdims=True)
        d_sim = d_sim * scale
        own = lane_head == h
        q_marks = jnp.where(own, mark_ref[:, :width], 0.0)
        k_marks = jnp.where(own, mark_ref[:, width:], 0.0)
        dq_total = dq_total + wide(mul, d_sim, k_marks)
        dk_total = dk_total + wide(mul, jnp.transpose(d_sim), q_marks)
    d_q[...] = dq_total
    d_k[...] += dk_total

    flipped = []
    for h in range(heads):
        flipped.append(
            band(
                jnp.concatenate(
                    [conv_own[h : h + 1, n : n + 1] for n in reversed(range(taps))], axis=1
                ),
                taps,
            ).astype(low)
        )

    def last_slot(s, _):
        start, end, lo, hi = reach(s)
        inv = denom_ref[s]
        own_d = d_value[own_rows(s), :]
        own_v = value_ref[own_rows(s), :]
        d_block = spread(own_d, head_blocks)
        row_sum = jnp.sum(
            d_block * jnp.concatenate([own_v] * heads, axis=0), axis=1, keepdims=True
        )
        row_sum = row_sum * inv
        d_block = d_block * inv
        d_block_t = jnp.transpose(d_block).astype(low)
        d_block = d_block.astype(low)

        def tile(n, query_total):
            t = pl.multiple_of(n * TILE, TILE)
            mask = lane_mask(start, end, t, TILE)
            kernel_rows = jnp.where(mask, last_ref[:, pl.ds(t, TILE)].astype(f32), 0.0)
            v_rows = qkv_ref[2 * width :, pl.ds(t, TILE)]
            d_sim = kernel_rows * (mul(d_block, v_rows) - row_sum)
            d_low = d_sim.astype(low)
            old = ds_last[:, pl.ds(t, TILE)].astype(f32)
            ds_last[:, pl.ds(t, TILE)] = jnp.where(mask, d_sim, old).astype(low)
            dv = mul(d_block_t, kernel_rows.astype(low))
            dv = dv + convolve(gpad, flipped, start, end, t, heads)
            old = out_ref[2 * width :, pl.ds(t, TILE)].astype(f32)
            out_ref[2 * width :, pl.ds(t, TILE)] = jnp.where(mask, dv, old).astype(low)
            return query_total + mul_t(d_low, qkv_ref[width : 2 * width, pl.ds(t, TILE)])

        query_total = lax.fori_loop(lo, hi, tile, jnp.zeros((width, width), f32))
        d_q[own_rows(s), :] += fold(query_total, head_blocks) * scale
        return 0

    last_in.wait()
    lax.fori_loop(0, slots, last_slot, 0)
    values = pl.ds(2 * width, width)
    values_out = pltpu.make_async_copy(out_ref.at[values], out_hbm.at[values], move_sem.at[2])
    values_out.start()

    inv_count = slot_marks(len_ref, 0, slots, marks, SUB)[1]
    d_q[...] = d_q[...] * inv_count
    d_k[...] = d_k[...] * inv_count

    def final_slot(s, _):
        start, end, lo, hi = reach(s)
        length = end - start
        own = mark_ref[own_rows(s), :] * scale

        def left(block, d_mark):
            wide_rows = jnp.concatenate([spread(block, head_blocks), d_mark], axis=0)
            return jnp.transpose(wide_rows).astype(low)

        q_left = left(own[:, width:], d_q[own_rows(s), :])
        k_left = left(own[:, :width], d_k[own_rows(s), :])
        mark = lax.broadcasted_iota(jnp.int32, (marks, 1), 0)
        lower = start + (mark * length) // marks
        upper = start + ((mark + 1) * length) // marks

        def tile(n, _):
            t = pl.multiple_of(n * TILE, TILE)
            mask = lane_mask(start, end, t, TILE)
            tok = t + lax.broadcasted_iota(jnp.int32, (marks, TILE), 1)
            member = jnp.where((tok >= lower) & (tok < upper), 1.0, 0.0).astype(low)
            for at, lhs, source in ((0, q_left, ds_first), (width, k_left, ds_last)):
                rhs = jnp.concatenate([source[:, pl.ds(t, TILE)], member], axis=0)
                rows = mul(lhs, rhs)
                old = out_ref[at : at + width, pl.ds(t, TILE)].astype(f32)
                out_ref[at : at + width, pl.ds(t, TILE)] = jnp.where(mask, rows, old).astype(low)
            return 0

        return lax.fori_loop(lo, hi, tile, 0)

    lax.fori_loop(0, slots, final_slot, 0)
    others = pl.ds(0, 2 * width)
    others_out = pltpu.make_async_copy(out_ref.at[others], out_hbm.at[others], move_sem.at[3])
    others_out.start()

    def bias_tile(n, carry):
        t = pl.multiple_of(n * TILE, TILE)
        q_sum, v_sum = carry
        q_rows = out_ref[:width, pl.ds(t, TILE)].astype(f32)
        v_rows = out_ref[2 * width :, pl.ds(t, TILE)].astype(f32)
        for c in range(count):
            q_sum = q_sum + q_rows[:, c * SUB : (c + 1) * SUB]
            v_sum = v_sum + v_rows[:, c * SUB : (c + 1) * SUB]
        return q_sum, v_sum

    zero = jnp.zeros((width, SUB), f32)
    q_sum, v_sum = lax.fori_loop(0, tok_count // TILE, bias_tile, (zero, zero))
    bias_ref[...] = jnp.zeros_like(bias_ref)
    bias_ref[0:1, :] = jnp.sum(jnp.transpose(q_sum), axis=0, keepdims=True)
    bias_ref[1:2, :] = jnp.sum(jnp.transpose(v_sum), axis=0, keepdims=True)
    values_out.wait()
    others_out.wait()


def mix_forward(seq_lengths, tokens, weight_t, bias, conv, slots, marks):
    tok_count, model = tokens.shape
    width = weight_t.shape[0] // 3
    heads = width // HEAD_DIM
    packed = slots * marks
    taps = conv.shape[1]
    whole = lambda *shape: pl.BlockSpec(shape, lambda i, lens: (0,) * len(shape))
    shapes = [
        ((3 * width, tok_count), low),
        ((width, tok_count), low),
        ((width, tok_count), low),
        ((width, tok_count), low),
        ((packed, 2 * width), f32),
        ((packed, width), f32),
        ((packed, width), f32),
        ((slots, width, 1), f32),
        ((heads, HEAD_DIM, packed), f32),
        ((PINV_ITERS, 4, heads, HEAD_DIM, packed), f32),
        ((heads, HEAD_DIM, packed), f32),
        ((8, 128), f32),
    ]
    apart = (0, 1, 2, 9)
    return pl.pallas_call(
        partial(mix_forward_kernel, slots, marks, taps),
        out_shape=[jax.ShapeDtypeStruct(s, t) for s, t in shapes],
        grid_spec=pltpu.PrefetchScalarGridSpec(
            num_scalar_prefetch=1,
            grid=(tok_count // TILE,),
            in_specs=[
                pl.BlockSpec((TILE, model), lambda i, lens: (i, 0)),
                whole(3 * width, model),
                whole(*bias.shape),
                whole(*conv.shape),
            ],
            out_specs=[
                pl.BlockSpec(memory_space=pl.ANY) if n in apart else whole(*s)
                for n, (s, _) in enumerate(shapes)
            ],
            scratch_shapes=[pltpu.VMEM(*shapes[n]) for n in apart]
            + [
                pltpu.VMEM((width, tok_count + 2 * SUB), low),
                pltpu.VMEM((width, tok_count), f32),
                pltpu.VMEM((8, width), f32),
                pltpu.VMEM((bias.shape[1], 2 * bias.shape[0]), f32),
                pltpu.VMEM((heads, taps), f32),
                pltpu.SemaphoreType.DMA((len(apart),)),
            ],
        ),
        compiler_params=pltpu.CompilerParams(vmem_limit_bytes=56 * 1024 * 1024),
        cost_estimate=pl.CostEstimate(
            flops=20 * 10**9, bytes_accessed=30 * 10**6, transcendentals=10**6
        ),
        name="mix_forward",
    )(seq_lengths, tokens, weight_t, bias, conv)


def mix_backward(seq_lengths, grad_t, saved, conv, slots, marks):
    qkv_t, first, last, mark, value, inner, denom, middle, steps, inverse = saved
    width, tok_count = grad_t.shape
    heads = width // HEAD_DIM
    packed = slots * marks
    taps = conv.shape[1]
    args = (grad_t, qkv_t, first, last, mark, value, inner, denom, middle, steps, inverse, conv)
    whole = lambda shape: pl.BlockSpec(
        shape, lambda i, lens: (0,) * len(shape), pipeline_mode=pl.Buffered(1)
    )
    shapes = [((3 * width, tok_count), low), ((8, width), f32), ((heads, SUB), f32)]
    square = pltpu.VMEM((packed, width), f32)
    hbm = pl.BlockSpec(memory_space=pl.ANY)
    return pl.pallas_call(
        partial(mix_backward_kernel, slots, marks, taps),
        out_shape=[jax.ShapeDtypeStruct(s, t) for s, t in shapes],
        grid_spec=pltpu.PrefetchScalarGridSpec(
            num_scalar_prefetch=1,
            grid=(1,),
            in_specs=[hbm if n in (3, 9) else whole(x.shape) for n, x in enumerate(args)],
            out_specs=[hbm] + [whole(s) for s, _ in shapes[1:]],
            scratch_shapes=[
                pltpu.VMEM(last.shape, low),
                pltpu.VMEM(steps.shape, f32),
                pltpu.VMEM(*shapes[0]),
                pltpu.SemaphoreType.DMA((4,)),
                pltpu.VMEM((width, tok_count + 2 * SUB), low),
                pltpu.VMEM((width, tok_count + 2 * SUB), low),
                pltpu.VMEM((width, tok_count), low),
                pltpu.VMEM((width, tok_count), low),
                pltpu.VMEM((heads, SUB, 3 * SUB), f32),
                square, square, square, square,
                pltpu.VMEM((heads, taps), f32),
            ],
        ),
        compiler_params=pltpu.CompilerParams(vmem_limit_bytes=56 * 1024 * 1024),
        cost_estimate=pl.CostEstimate(
            flops=20 * 10**9, bytes_accessed=30 * 10**6, transcendentals=10**6
        ),
        name="mix_backward",
    )(seq_lengths, *args)


contract_rows = (((0,), (0,)), ((), ()))
contract_cols = (((1,), (1,)), ((), ()))
norm_eps = 1e-05


def split_up(x, dim, peers):
    before, after = (x.shape[:dim], x.shape[dim + 1 :])
    return jnp.moveaxis(x.reshape(*before, peers, -1, *after), dim, 0)


def sum_at_owner(x, axis, dim):
    peers = lax.axis_size(axis)
    tiles = lax.all_to_all(split_up(x, dim, peers), axis, 0, 0, tiled=True)
    return jnp.sum(tiles.astype(f32), axis=0)


def layer_norm(row_data, gain_vec, shift_vec):
    centre = row_data - jnp.mean(row_data, axis=1, keepdims=True)
    spread_row = jnp.mean(centre * centre, axis=1, keepdims=True)
    return centre * lax.rsqrt(spread_row + norm_eps) * gain_vec[None, :] + shift_vec[None, :]


def gelu_exact(values):
    return jax.nn.gelu(values, approximate=False)


def body(
    tokens,
    qkv_weight,
    qv_bias,
    conv_weight,
    out_weight,
    out_bias,
    norm1_gain,
    norm1_bias,
    ffn_in_weight,
    ffn_in_bias,
    ffn_out_weight,
    ffn_out_bias,
    norm2_gain,
    norm2_bias,
    cotangent,
    seq_lengths,
    segment_ids,
    landmark_bounds,
):
    tok_count, model_width = tokens.shape
    head_width = qkv_weight.shape[2]
    heads_here = head_width // HEAD_DIM
    head_total = conv_weight.shape[0]
    kernel_taps = conv_weight.shape[1]
    slots, marks = landmark_bounds.shape
    quarter = tok_count // lax.axis_size("heads")
    head_index = lax.axis_index("heads")
    own_start = head_index * quarter
    both = ("batch", "heads")
    own_rows_low = lax.dynamic_slice_in_dim(tokens, own_start, quarter, 0)
    own_tokens = own_rows_low.astype(f32)
    flat_qkv = qkv_weight.reshape(model_width, 3 * head_width)
    forward = mix_forward(
        seq_lengths, tokens, jnp.transpose(flat_qkv), qv_bias, conv_weight, slots, marks
    )
    qkv_t, first, last, mixed_t, mark, value, inner, denom, middle, steps, inverse, bound = forward
    bound_total = bound[0, 0]
    attn_part = lax.psum_scatter(
        lax.dot_general(mixed_t, out_weight, contract_rows, preferred_element_type=f32).astype(low),
        "heads",
        scatter_dimension=0,
        tiled=True,
    ).astype(f32)
    live_count = jnp.sum((seq_lengths > 0).astype(f32)) * heads_here
    first_res = own_tokens + attn_part + out_bias[None, :]
    norm1_out, norm1_pull = jax.vjp(layer_norm, first_res, norm1_gain, norm1_bias)
    norm1_low = norm1_out.astype(low)
    ff_own = ffn_out_weight.shape[0]
    bias_row = jnp.zeros((16, model_width), low).at[0, :ff_own].set(ffn_in_bias)
    whole_in = lax.all_gather(ffn_in_weight, both, axis=1, tiled=True)
    out_pack = lax.all_gather(jnp.concatenate([ffn_out_weight, bias_row], axis=0), both, axis=0)
    whole_out = out_pack[:, :ff_own].reshape(-1, model_width)
    whole_in_bias = out_pack[:, ff_own, :ff_own].reshape(-1)
    pre_act = (
        jnp.dot(norm1_low, whole_in, preferred_element_type=f32)
        + whole_in_bias.astype(f32)[None, :]
    )
    hidden_act, gelu_pull = jax.vjp(gelu_exact, pre_act)
    hidden_low = hidden_act.astype(low)
    ffn_result = jnp.dot(hidden_low, whole_out, preferred_element_type=f32) + ffn_out_bias[None, :]
    final_out, norm2_pull = jax.vjp(layer_norm, norm1_out + ffn_result, norm2_gain, norm2_bias)
    grad_second, grad_gain_two, grad_shift_two = norm2_pull(cotangent.astype(f32))
    grad_ffn_low = grad_second.astype(low)
    grad_ffn_bias = jnp.sum(grad_ffn_low.astype(f32), axis=0)
    down_term = lax.dot_general(
        hidden_low, grad_ffn_low, contract_rows, preferred_element_type=f32
    ).astype(low)
    grad_hidden = lax.dot_general(
        grad_ffn_low, whole_out, contract_cols, preferred_element_type=f32
    )
    grad_pre = gelu_pull(grad_hidden)[0].astype(low)
    grad_in_bias = jnp.sum(grad_pre.astype(f32), axis=0)
    up_term = lax.dot_general(
        norm1_low, grad_pre, contract_rows, preferred_element_type=f32
    ).astype(low)
    grad_norm1 = grad_second + lax.dot_general(
        grad_pre, whole_in, contract_cols, preferred_element_type=f32
    )
    grad_first, grad_gain_one, grad_shift_one = norm1_pull(grad_norm1)
    grad_attn_low = grad_first.astype(low)
    grad_out_bias = jnp.sum(grad_attn_low.astype(f32), axis=0)
    piece_rows = lax.all_gather(grad_attn_low, "heads", axis=0, tiled=True)
    grad_mix_t = lax.dot_general(
        out_weight, piece_rows, contract_cols, preferred_element_type=f32
    ).astype(low)
    grad_mix_t, down_term, up_term = lax.optimization_barrier((grad_mix_t, down_term, up_term))
    up_share = lax.psum_scatter(up_term, both, scatter_dimension=1, tiled=True).astype(f32)
    down_share = lax.psum_scatter(down_term, both, scatter_dimension=0, tiled=True).astype(f32)
    saved = (qkv_t, first, last, mark, value, inner, denom, middle, steps, inverse)
    grad_t, grad_bias, grad_conv = mix_backward(
        seq_lengths, grad_mix_t, saved, conv_weight, slots, marks
    )
    out_part = lax.dot_general(
        mixed_t, piece_rows, (((1,), (0,)), ((), ())), preferred_element_type=f32
    )
    grad_qv_own = grad_bias[:2]
    qkv_part = lax.dot_general(
        tokens, grad_t, (((0,), (1,)), ((), ())), preferred_element_type=f32
    ).reshape(model_width, 3, head_width)
    input_part = lax.psum_scatter(
        lax.dot_general(
            grad_t, flat_qkv, (((0,), (1,)), ((), ())), preferred_element_type=f32
        ).astype(low),
        "heads",
        scatter_dimension=0,
        tiled=True,
    ).astype(f32)
    input_grad = grad_first + input_part
    conv_full = lax.dynamic_update_slice_in_dim(
        jnp.zeros((head_total, kernel_taps), f32),
        grad_conv[:, :kernel_taps],
        head_index * heads_here,
        0,
    )
    bias_full = lax.dynamic_update_slice_in_dim(
        jnp.zeros((2, head_total * HEAD_DIM), f32), grad_qv_own, head_index * head_width, 1
    )
    qkv_share, out_share = (
        sum_at_owner(qkv_part.astype(low), "batch", 0),
        sum_at_owner(out_part.astype(low), "batch", 1),
    )
    vector_all = jnp.stack(
        [grad_ffn_bias, grad_gain_two, grad_shift_two, grad_gain_one, grad_shift_one, grad_out_bias]
    )
    in_bias_share, vector_share = (
        lax.psum_scatter(grad_in_bias, both, scatter_dimension=0, tiled=True),
        lax.psum_scatter(vector_all, both, scatter_dimension=1, tiled=True),
    )
    conv_sum, bias_sum, bound_all, count_all = lax.psum(
        (conv_full, bias_full, bound_total, live_count), both
    )
    conv_out = lax.dynamic_slice_in_dim(conv_sum, head_index * heads_here, heads_here, 0)
    bias_out = lax.dynamic_slice_in_dim(bias_sum, head_index * head_width, head_width, 1)
    condition = bound_all / count_all
    return (
        final_out.astype(low),
        input_grad,
        qkv_share,
        bias_out,
        conv_out,
        out_share,
        up_share,
        in_bias_share,
        down_share,
        vector_share,
        condition,
    )


def place():
    b, z = lax.axis_index("batch"), lax.axis_index("heads")
    core, x, y = b % 2, (b // 2) % 2, b // 4
    return b, z, b + 1 - 2 * core, b + 2 - 4 * x, b + 4 - 8 * y


def remote(src, dst, send, recv, device):
    return pltpu.make_async_remote_copy(
        src_ref=src,
        dst_ref=dst,
        send_sem=send,
        recv_sem=recv,
        device_id=device,
        device_id_type=pl.DeviceIdType.MESH,
    )


def greet(devices):
    barrier = pltpu.get_barrier_semaphore()
    for device in devices:
        pl.semaphore_signal(
            barrier, inc=1, device_id=device, device_id_type=pl.DeviceIdType.MESH
        )
    pl.semaphore_wait(barrier, len(devices))


def tail_kernel(
    len_ref,
    gt_hbm, wq_hbm, we_hbm, hid_hbm, pre_hbm, n1_hbm, gf_hbm, ga_hbm, mx_hbm, tok_hbm, first_hbm,
    sums_ref, bin_ref, qv_ref, conv_ref, bound_ref,
    input_ref, down_own, up_own, outw_own, qkvw_own, in_bias, vector_own, qv_own, conv_own, ratio,
    small_out,
    gt, wq, we, hid, pre, n1, gf, ga, mx, tok,
    q_in, r_out, r_in, s_in, out_down, out_up, full_outw, full_qkvw, acc_qkvw,
    core_down, core_up, core_outw, core_qkvw,
    one_down, one_up, one_outw, one_qkvw, two_down, two_up, two_outw, two_qkvw,
    e_down, e_up, e_outw, g_down, g_up, g_outw, h_down, h_up, h_outw, small_in,
    load_sem, q_send, q_recv, r_send, r_recv, t_send, t_recv, c_send, c_recv, x_send, x_recv, e_send, e_recv,
    g_send, g_recv, h_send, h_recv, s_send, s_recv,
):
    b, z, bc, bx, by = place()
    both = bx + by - b
    flip = bc - b
    peers = [(b, lax.rem(z + i, 4)) for i in (1, 2, 3)]
    issued = []
    loads = [
        pltpu.make_async_copy(src, dst, load_sem.at[n])
        for n, (src, dst) in enumerate(
            (
                (pre_hbm, pre), (n1_hbm, n1), (hid_hbm, hid), (gf_hbm, gf), (gt_hbm, gt),
                (wq_hbm, wq), (we_hbm, we), (mx_hbm, mx), (ga_hbm, ga), (tok_hbm, tok),
                (first_hbm, input_ref),
            )
        )
    ]
    for copy in loads:
        copy.start()
    greet(peers + [(bc, z), (bx, z), (by, z)])
    chunks, size = r_in.shape[1:3]
    quarter = chunks * size
    ff = down_own.shape[0]
    group = 4 * ff

    zf = z + 1 - 2 * (z % 2)
    zg = z + 2 - 4 * (z // 2)
    partners = ((bc, z), (bx, z), (by, z), (b, zf), (b, zg))

    def small_start(k):
        copy = remote(
            small_out.at[k], small_in.at[k], s_send.at[k], s_recv.at[k], partners[k]
        )
        copy.start()
        issued.append(copy)

    def small_event(k):
        ref = small_in.at[k]
        remote(ref, ref, s_send.at[k], s_recv.at[k], partners[k]).wait_recv()
        small_out[k + 1] = small_out[k] + small_in[k]
        if k < 4:
            small_start(k + 1)

    model = input_ref.shape[1]
    bias_rows = bin_ref.shape[1] // model
    at_vec, at_qv = bias_rows, bias_rows + 6
    heads, taps = conv_own.shape
    at_conv = at_qv + 8
    at_end = at_conv + 4 * heads
    width = qv_own.shape[1]
    small_out[0] = jnp.zeros(small_out.shape[1:], f32)
    for n in range(bias_rows):
        small_out[0, n : n + 1, :] = bin_ref[0:1, n * model : (n + 1) * model]
    small_out[0, at_vec : at_vec + 6, :] = sums_ref[0:6, :]
    live = jnp.int32(0)
    for n in range(len_ref.shape[0]):
        live = live + jnp.where(len_ref[n] > 0, heads, 0)
    lane = lax.broadcasted_iota(jnp.int32, (1, 128), 1)
    small_out[0, at_end : at_end + 1, 0:128] = jnp.where(
        lane == 0, bound_ref[0:1, :], jnp.where(lane == 1, live.astype(f32), 0.0)
    )
    for n in range(4):

        @pl.when(z == n)
        def _():
            for r in range(2):
                row = at_qv + 2 * n + r
                small_out[0, row : row + 1, :width] = qv_ref[r : r + 1, :]
            for r in range(heads):
                row = at_conv + heads * n + r
                small_out[0, row : row + 1, 0:128] = conv_ref[r : r + 1, :]

    small_start(0)

    is_end = (z == 0) | (z == 3)
    low_side = z < 2
    to_inner = jnp.where(low_side, 1, 2)
    across = jnp.where(z == 1, 2, 1)
    to_end = jnp.where(low_side, 0, 3)

    def owner(k):
        return jnp.where(low_side, 3 - k, k)

    def columns(who, c):
        return pl.ds(pl.multiple_of(who * quarter + c * size, size), size)

    def times(x, w):
        return lax.dot_general(x, w, (((0,), (0,)), ((), ())), preferred_element_type=f32)

    def part(who, c):
        return times(gt[:, columns(who, c)], wq[...])

    def q_copy(k, c):
        return remote(
            gt_hbm.at[:, columns(owner(k), c)], q_in.at[k, c], q_send.at[k, c], q_recv.at[k, c],
            (b, to_inner),
        )

    def q_wait(k, c):
        ref = q_in.at[k, c]
        remote(ref, ref, q_send.at[k, c], q_recv.at[k, c], (b, to_end)).wait_recv()

    def r_copy(k, c):
        return remote(
            r_out.at[k, c], r_in.at[k, c], r_send.at[k, c], r_recv.at[k, c], (b, across)
        )

    def t_copy(c):
        return remote(r_in.at[0, c], s_in.at[c], t_send.at[c], t_recv.at[c], (b, to_end))

    def first_hop(k, c):
        @pl.when(jnp.logical_not(is_end))
        def _():
            own = part(owner(k), c)
            q_wait(k, c)
            r_out[k, c] = (own + times(q_in[k, c], we[...])).astype(low)
            r_copy(k, c).start()

    def last_hop(c):
        @pl.when(jnp.logical_not(is_end))
        def _():
            own = part(to_end, c)
            r_copy(0, c).wait_recv()
            r_in[0, c] = (r_in[0, c].astype(f32) + own).astype(low)
            t_copy(c).start()

    cores = (core_down, core_up, core_outw, core_qkvw)
    ones = (one_down, one_up, one_outw, one_qkvw)
    twos = (two_down, two_up, two_outw, two_qkvw)
    outs = (out_down, out_up)
    left = (hid, pre)
    right = (gf, n1)

    def who(slot):
        return b + (slot % 2) * (bx - b) + (slot // 2) * (by - b)

    def term(n, owner):
        at = pl.ds(pl.multiple_of(owner * group, group), group)
        return lax.dot_general(
            left[n][:, at], right[n][...], (((0,), (0,)), ((), ())), preferred_element_type=f32
        )

    def core_copy(n, slot):
        if n < 2:
            src = outs[n].at[slot]
        elif n == 2:
            src = full_outw.at[:, who(slot) + flip]
        else:
            src = full_qkvw.at[who(slot) + flip]
        return remote(src, cores[n].at[slot], c_send.at[n, slot], c_recv.at[n, slot], (bc, z))

    def give(n, slot):
        if n < 2:
            value = term(n, who(slot) + flip).astype(low)
            outs[n][slot] = value.reshape(outs[n].shape[1:])
        core_copy(n, slot).start()

    def keep(n, slot):
        if n < 2:
            own = term(n, who(slot)).reshape(outs[n].shape[1:])
        elif n == 2:
            own = full_outw[:, who(slot)].astype(f32)
        else:
            own = full_qkvw[who(slot)].astype(f32)
        core_copy(n, slot).wait_recv()
        cores[n][slot] = (cores[n][slot].astype(f32) + own).astype(low)

    def side_copy(n, dst, src):
        partner = by if n % 2 == 0 else bx
        return remote(
            cores[n].at[src], ones[n].at[dst], x_send.at[n, dst], x_recv.at[n, dst], (partner, z)
        )

    def small_group(n):
        def one(i, _):
            give(n, 3 - i)
            return 0

        lax.fori_loop(0, 4, one, 0)

    def small_keep(n):
        def one(i, _):
            keep(n, 3 - i)
            return 0

        lax.fori_loop(0, 4, one, 0)
        side_copy(n, 1, 3).start()
        side_copy(n, 0, 2 if n % 2 == 0 else 1).start()

    def half(h, _):
        def one(i, _):
            slot_up, slot_down = 3 - 2 * i - h, 3 - i - 2 * h
            give(1, slot_up)
            give(0, slot_down)
            keep(1, slot_up)

            @pl.when(h == 0)
            def _():
                side_copy(1, 1 - i, slot_up).start()

            keep(0, slot_down)

            @pl.when(h == 0)
            def _():
                side_copy(0, 1 - i, slot_down).start()

            return 0

        lax.fori_loop(0, 2, one, 0)

        @pl.when(h == 0)
        def _():
            for n in (4, 5, 6):
                loads[n].wait()
            first_hop(0, 0)

        return 0

    def one_event(n):
        second = 1 if n % 2 == 0 else 2
        partner, other = (by, bx) if n % 2 == 0 else (bx, by)
        ref = ones[n].at[1]
        remote(ref, ref, x_send.at[n, 1], x_recv.at[n, 1], (partner, z)).wait_recv()
        ones[n][1] = (ones[n][1].astype(f32) + cores[n][second].astype(f32)).astype(low)
        copy = remote(ones[n].at[1], twos[n], x_send.at[n, 2], x_recv.at[n, 2], (other, z))
        copy.start()
        issued.append(copy)

    e_bufs = (e_down, e_up, e_outw)
    g_bufs = (g_down, g_up, g_outw)
    h_bufs = (h_down, h_up, h_outw)

    def e_copy(n, k):
        return remote(
            twos[n].at[owner(k)], e_bufs[n].at[k], e_send.at[n, k], e_recv.at[n, k], (b, to_inner)
        )

    def e_wait(n, k):
        ref = e_bufs[n].at[k]
        remote(ref, ref, e_send.at[n, k], e_recv.at[n, k], (b, to_end)).wait_recv()

    def g_copy(n, k):
        return remote(
            e_bufs[n].at[k], g_bufs[n].at[k], g_send.at[n, k], g_recv.at[n, k], (b, across)
        )

    def h_copy(n):
        return remote(g_bufs[n].at[0], h_bufs[n], h_send.at[n], h_recv.at[n], (b, to_end))

    def two_event(n):
        partner, other = (by, bx) if n % 2 == 0 else (bx, by)
        ref = ones[n].at[0]
        remote(ref, ref, x_send.at[n, 0], x_recv.at[n, 0], (partner, z)).wait_recv()
        ref = twos[n]
        remote(ref, ref, x_send.at[n, 2], x_recv.at[n, 2], (other, z)).wait_recv()
        own = ones[n][0].astype(f32) + cores[n][0].astype(f32)
        if n == 3:
            own = twos[n][...].astype(f32) + own
            for i in range(3):
                qkvw_own[i] = own[:, i * width : (i + 1) * width]
            return
        twos[n][...] = (twos[n][...].astype(f32) + own).astype(low)

    def line_start(n, k):
        @pl.when(is_end)
        def _():
            e_copy(n, k).start()

    def line_across(n, k):
        @pl.when(jnp.logical_not(is_end))
        def _():
            e_wait(n, k)
            e_bufs[n][k] = (
                e_bufs[n][k].astype(f32) + twos[n][owner(k)].astype(f32)
            ).astype(low)
            g_copy(n, k).start()

    def line_back(n):
        @pl.when(jnp.logical_not(is_end))
        def _():
            g_copy(n, 0).wait_recv()
            g_bufs[n][0] = (
                g_bufs[n][0].astype(f32) + twos[n][to_end].astype(f32)
            ).astype(low)
            h_copy(n).start()

    def end_event(n):
        def write(value):
            out = (down_own, up_own, outw_own)[n]
            out[...] = jnp.transpose(value) if n == 2 else value

        @pl.when(is_end)
        def _():
            ref = h_bufs[n]
            remote(ref, ref, h_send.at[n], h_recv.at[n], (b, to_inner)).wait_recv()
            write(twos[n][z].astype(f32) + h_bufs[n][...].astype(f32))
            for k in range(3):
                e_copy(n, k).wait_send()

        @pl.when(jnp.logical_not(is_end))
        def _():
            g_copy(n, 1).wait_recv()
            e_wait(n, 2)
            write(
                twos[n][z].astype(f32)
                + g_bufs[n][1].astype(f32)
                + e_bufs[n][2].astype(f32)
            )
            for k in range(2):
                g_copy(n, k).wait_send()
            h_copy(n).wait_send()

    def projections():
        on, oh = full_outw.shape[2:]
        for s in range(4):
            value = jnp.transpose(mul(mx[s], ga[...]))
            full_outw[s] = value.astype(low).reshape(full_outw.shape[1:])
        acc_qkvw[...] = jnp.zeros_like(acc_qkvw)
        span = quarter

        def one(n, _):
            at = pl.ds(pl.multiple_of(n * span, span), span)
            acc_qkvw[...] += mul(gt[:, at], tok[at, :])
            return 0

        lax.fori_loop(0, 4, one, 0)
        full_qkvw[...] = jnp.transpose(acc_qkvw[...]).astype(low).reshape(full_qkvw.shape)

    @pl.when(is_end)
    def _():
        for k in range(3):
            for c in range(chunks):
                q_copy(k, c).start()

    for n in range(4):
        loads[n].wait()

    lax.fori_loop(0, 2, half, 0)
    first_hop(0, 1)
    one_event(1)
    one_event(0)
    first_hop(0, 2)
    last_hop(0)
    for n in (7, 8, 9):
        loads[n].wait()
    projections()
    first_hop(1, 0)
    last_hop(1)
    small_group(2)
    small_group(3)
    small_event(0)
    first_hop(1, 1)
    last_hop(2)
    small_keep(2)
    small_keep(3)
    small_event(1)
    first_hop(1, 2)
    two_event(1)
    two_event(0)
    small_event(2)
    one_event(2)
    one_event(3)
    small_event(3)
    two_event(2)
    for k in range(3):
        for n in (1, 0, 2):
            line_start(n, k)
    two_event(3)
    small_event(4)
    loads[10].wait()

    def own_rows(c, _):
        rows = pl.ds(pl.multiple_of(c * size, size), size)
        input_ref[rows, :] += part(z, c)

        @pl.when(is_end)
        def _():
            ref = s_in.at[c]
            remote(ref, ref, t_send.at[c], t_recv.at[c], (b, to_inner)).wait_recv()
            input_ref[rows, :] += s_in[c].astype(f32)

        @pl.when(jnp.logical_not(is_end))
        def _():
            r_copy(1, c).wait_recv()
            q_wait(2, c)
            input_ref[rows, :] += r_in[1, c].astype(f32) + times(q_in[2, c], we[...])

        return 0

    lax.fori_loop(0, chunks, own_rows, 0)
    for n, k in ((1, 0), (0, 0), (1, 1), (0, 1), (2, 0), (2, 1)):
        line_across(n, k)
        if k == 1:
            line_back(n)
    for n in (1, 0, 2):
        end_event(n)

    @pl.when(is_end)
    def _():
        for k in range(3):
            for c in range(chunks):
                q_copy(k, c).wait_send()

    @pl.when(jnp.logical_not(is_end))
    def _():
        for c in range(chunks):
            r_copy(0, c).wait_send()
            r_copy(1, c).wait_send()
            t_copy(c).wait_send()

    final = small_out.at[5]
    in_bias[...] = jnp.zeros_like(in_bias)
    index = b * 4 + z
    per_row = model // ff
    for n in range(bias_rows):

        @pl.when(index // per_row == n)
        def _():
            row = pltpu.roll(final[n : n + 1, :], (model - (index % per_row) * ff) % model, 1)
            in_bias[...] = row[:, :ff]

    share = vector_own.shape[1]
    vectors = final[at_vec : at_vec + 6, :]
    vector_own[...] = pltpu.roll(vectors, (model - index * share) % model, 1)[:, :share]
    for n in range(4):

        @pl.when(z == n)
        def _():
            qv_own[...] = final[at_qv + 2 * n : at_qv + 2 * n + 2, :width]
            conv_own[...] = final[at_conv + heads * n : at_conv + heads * (n + 1), :taps]

    ratio[...] = final[at_end : at_end + 1, 0:1] / final[at_end : at_end + 1, 1:2]

    for n in range(4):
        for dst in range(2):
            side_copy(n, dst, dst).wait_send()
        for slot in range(4):
            core_copy(n, slot).wait_send()
    for copy in issued:
        copy.wait_send()


def tail(
    lengths, gt, wq, we, hid, pre, n1, gf, ga, mx, tok, first, sums, bins, qv_grad, conv_grad, bound,
    taps,
):
    quarter, model = first.shape
    chunks = 3
    size = quarter // chunks
    ff = hid.shape[1] // 32
    width = mx.shape[1]
    heads = width // HEAD_DIM
    on, oh = model // 8, width
    qn, qh = model // 8, gt.shape[0]
    blocks = ((4, ff, model), (4, ff, model), (4, on, oh), (qn, qh))
    own = lambda *s: jax.ShapeDtypeStruct(s, f32)
    vm = lambda *s: pltpu.VMEM(s, low)
    dma = pltpu.SemaphoreType.DMA
    sources = (gt, wq, we, hid, pre, n1, gf, ga, mx, tok)
    small = -(-(bins.shape[1] // model + 15 + 4 * heads) // 8) * 8
    vmem = pl.BlockSpec(memory_space=pltpu.VMEM)
    return pl.pallas_call(
        tail_kernel,
        out_shape=[
            own(quarter, model), own(ff, model), own(ff, model), own(oh, on), own(3, qn, width),
            own(1, ff), own(6, model // 32), own(2, width), own(heads, taps), own(1, 1),
        ],
        in_specs=[pl.BlockSpec(memory_space=pltpu.SMEM)]
        + [pl.BlockSpec(memory_space=pl.ANY)] * 11
        + [vmem] * 5,
        out_specs=[vmem] * 10,
        scratch_shapes=[
            pltpu.VMEM((6, small, model), f32),
            *[vm(*x.shape) for x in sources],
            vm(3, chunks, qh, size), vm(2, chunks, size, model), vm(2, chunks, size, model),
            vm(chunks, size, model),
            vm(4, *blocks[0]), vm(4, *blocks[1]),
            vm(4, 8, on, oh), vm(8, qn, qh), pltpu.VMEM((qh, model), f32),
            *[vm(4, *s) for s in blocks],
            *[vm(2, *s) for s in blocks],
            *[vm(*s) for s in blocks],
            *[vm(3, *s[1:]) for s in blocks[:3]],
            *[vm(2, *s[1:]) for s in blocks[:3]],
            *[vm(*s[1:]) for s in blocks[:3]],
            pltpu.VMEM((5, small, model), f32),
            dma((11,)),
            dma((3, chunks)), dma((3, chunks)), dma((2, chunks)), dma((2, chunks)),
            dma((chunks,)), dma((chunks,)), dma((4, 4)), dma((4, 4)),
            dma((4, 3)), dma((4, 3)), dma((3, 3)), dma((3, 3)), dma((3, 2)), dma((3, 2)),
            dma((3,)), dma((3,)), dma((5,)), dma((5,)),
        ],
        compiler_params=pltpu.CompilerParams(
            collective_id=3, has_side_effects=True, vmem_limit_bytes=63 * 1024 * 1024
        ),
        name="tail",
    )(lengths, *sources, first, sums, bins, qv_grad, conv_grad, bound)


def cumulative(x):
    t = 1.0 / (1.0 + 0.23164189 * jnp.abs(x))
    density = jnp.exp(-0.5 * x * x) * 0.3989422804
    poly = t * (
        0.319381530 + t * (-0.356563782 + t * (1.781477937 + t * (-1.821255978 + t * 1.330274429)))
    )
    upper = density * poly
    return jnp.where(x >= 0.0, 1.0 - upper, upper), density


def normed(x):
    centre = x - jnp.mean(x, axis=1, keepdims=True)
    scale = lax.rsqrt(jnp.mean(centre * centre, axis=1, keepdims=True) + norm_eps)
    return centre * scale, scale


def norm_back(grad, gain, rows, scale):
    e = grad * gain
    return scale * (
        e - jnp.mean(e, axis=1, keepdims=True) - rows * jnp.mean(e * rows, axis=1, keepdims=True)
    )


def middle_kernel(
    share,
    mixed_ref, own0, own1, own2, own3, tok_hbm, cot_hbm, weight_hbm,
    vec_ref,
    out_hbm, first_hbm, attn_hbm, hidden_hbm, pre_hbm, norm_hbm, ffn_hbm, all_ref, grad_ref,
    sums_ref, bin_ref, end_hbm,
    out_ref, first_ref, attn_ref, hidden_ref, pre_ref, norm_ref, ffn_ref, tok_ref, cot_ref,
    packs, wof, wo, slope, total, n1_ref, scale_ref, turned,
    a_send, a_recv, f_send, f_recv, s_send, s_recv, p_send, p_recv, g_send, g_recv,
    own_sem, own_turn, out_sem, w_send, w_recv,
):
    b, z, bc, bx, by = place()
    both = bx + by - b
    flip = bc - b
    peers = [(b, lax.rem(z + i, 4)) for i in (1, 2, 3)]
    width, quarter = all_ref.shape[1:]
    model = tok_hbm.shape[1]
    owns = (own0, own1, own2, own3)
    origins = [lax.rem(z + 4 - i, 4) for i in range(4)]
    size = turned.shape[2]
    tiles = quarter // size
    issued = []

    def own_columns(n):
        return pl.ds(pl.multiple_of(n * quarter, quarter), quarter)

    local = [
        pltpu.make_async_copy(own, packs.at[b, origin], own_sem.at[i])
        for i, (own, origin) in enumerate(zip(owns, origins))
    ]
    local.append(
        pltpu.make_async_copy(mixed_ref.at[:, own_columns(z)], all_ref.at[z], own_sem.at[4])
    )
    local.append(
        pltpu.make_async_copy(
            tok_hbm.at[pl.ds(pl.multiple_of(z * quarter, quarter), quarter)], tok_ref, own_sem.at[5]
        )
    )
    cot_load = pltpu.make_async_copy(cot_hbm, cot_ref, own_sem.at[6])
    for copy in local:
        copy.start()
    cot_load.start()
    greet(peers + [(bc, z), (bx, z), (by, z)])

    ff = (packs.shape[2] - 32) // 2
    half = ff // 2
    pieces = ((2 * ff, 32), (0, half), (half, half), (ff, ff))
    through_y = (True, True, True, False)
    count = len(pieces)

    def rows_of(n):
        return pl.ds(*pieces[n])

    def mix_copy(r, i):
        to = lax.rem(z + i, 4)
        src = mixed_ref.at[:, pl.ds(pl.multiple_of(to * quarter + r * size, size), size)]
        return remote(
            src, all_ref.at[z, :, pl.ds(r * size, size)], a_send.at[r, i - 1], a_recv.at[r, i - 1],
            (b, to),
        )

    def side(n, axis):
        out = []
        for i in range(4):
            out.append(
                remote(
                    owns[i].at[rows_of(n)], packs.at[b, origins[i], rows_of(n)],
                    f_send.at[n, axis, i], f_recv.at[n, axis, i], (by if axis else bx, z),
                )
            )
        return out

    def side_start(n):
        for axis in (0, 1):
            for copy in side(n, axis):
                copy.start()
                issued.append(copy)

    def block(n, who):
        return packs.at[who, :, rows_of(n)]

    def corner(n):
        who, device = (bx, by) if through_y[n] else (by, bx)
        return remote(block(n, who), block(n, who), s_send.at[n], s_recv.at[n], (device, z))

    def mate(n, slot, who):
        return remote(
            block(n, who), block(n, who), p_send.at[n, slot], p_recv.at[n, slot], (bc, z)
        )

    def mate_start(n, slot, who):
        mate(n, slot, who).start()

    def side_wait(n, axis):
        who = by if axis else bx
        for i in range(4):
            ref = packs.at[who, origins[i], rows_of(n)]
            remote(
                ref, ref, f_send.at[n, axis, i], f_recv.at[n, axis, i], (who, z)
            ).wait_recv()
        if through_y[n] == (axis == 0):
            corner(n).start()
        mate_start(n, 1 + axis, who)

    def corner_wait(n):
        device = by if through_y[n] else bx
        ref = block(n, both)
        remote(ref, ref, s_send.at[n], s_recv.at[n], (device, z)).wait_recv()
        mate_start(n, 3, both)

    def mate_wait(n, slot, who):
        mate(n, slot, who + flip).wait_recv()

    side_start(0)
    side_start(1)
    for r in range(tiles):
        for i in (1, 2, 3):
            copy = mix_copy(r, i)
            copy.start()
            issued.append(copy)
    is_end = (z == 0) | (z == 3)
    end_copy = remote(
        weight_hbm, end_hbm, w_send.at[0], w_recv.at[0], (b, jnp.where(z < 2, 1, 2))
    )

    @pl.when(is_end)
    def _():
        end_copy.start()

    for copy in local:
        copy.wait()
    for n in range(count):
        mate_start(n, 0, b)
    out_bias, gain1, shift1, down_bias, gain2, shift2 = [
        vec_ref[n : n + 1, :] for n in range(6)
    ]
    sums_ref[...] = jnp.zeros_like(sums_ref)
    bin_ref[...] = jnp.zeros_like(bin_ref)
    total[...] = jnp.zeros_like(total)
    side_wait(0, 0)
    side_wait(0, 1)
    side_start(2)
    side_start(3)
    corner_wait(0)
    for slot, who in enumerate((b, bx, by, both)):
        mate_wait(0, slot, who)
    group = 4 * ff
    for q in range(8):
        for s in range(4):
            wof[pl.ds(s * width + q * share, share), :] = packs[
                q, s, pl.ds(2 * ff, share), :
            ].astype(f32)
    wo[...] = wof[...].astype(low).reshape(wo.shape)
    for q in range(8):
        row = jnp.zeros((1, group), f32)
        for s in range(4):
            row = row + packs[q, s, 2 * ff + share : 2 * ff + share + 1, :group].astype(f32)
        bin_ref[1:2, q * group : (q + 1) * group] = row

    def row_sum(n, x):
        sums_ref[n : n + 1, :] += jnp.sum(x, axis=0, keepdims=True)

    def first_rows(r, _):
        rows = pl.ds(pl.multiple_of(r * size, size), size)

        @pl.when(r == 1)
        def _():
            side_wait(1, 0)
            side_wait(1, 1)

        @pl.when(r == 2)
        def _():
            side_wait(2, 0)
            side_wait(2, 1)

        for i in (1, 2, 3):
            ref = all_ref.at[origins[i], :, rows]
            remote(
                ref, ref, a_send.at[r, i - 1], a_recv.at[r, i - 1], (b, origins[i])
            ).wait_recv()
        attn = jnp.zeros((size, model), f32)
        for s in range(4):
            attn = attn + lax.dot_general(
                all_ref[s, :, rows], wo[s], (((0,), (0,)), ((), ())), preferred_element_type=f32
            )
        n1, scale1 = normed(tok_ref[rows, :].astype(f32) + attn + out_bias)
        n1_ref[rows, :] = n1
        scale_ref[rows, :] = jnp.broadcast_to(scale1, (size, scale_ref.shape[1]))
        norm_ref[rows, :] = (n1 * gain1 + shift1).astype(low)
        return 0

    span = 2 * group

    def weights(c, start):
        return jnp.concatenate(
            [
                packs[2 * c + n, :, pl.ds(start, ff), :].reshape(group, model)
                for n in range(2)
            ],
            axis=0,
        )

    def tile_rows(r):
        return pl.ds(pl.multiple_of(r * size, size), size)

    def feed(who):
        c = who // 2
        lanes = pl.ds(pl.multiple_of(c * span, span), span)

        def one(r, _):
            rows = tile_rows(r)
            act = mul_t(norm_ref[rows, :], weights(c, 0)) + bin_ref[1:2, lanes]
            phi, density = cumulative(act)
            hidden = (act * phi).astype(low)
            hidden_ref[rows, lanes] = hidden
            slope[rows, lanes] = phi + act * density
            total[rows, :] += mul(hidden, weights(c, ff))
            return 0

        lax.fori_loop(0, tiles, one, 0)

    lax.fori_loop(0, tiles, first_rows, 0)

    def group_step(k, _):
        def mates(slot, who):
            for n in range(1, count):
                mate_wait(n, slot, who)

        @pl.when(k == 0)
        def _():
            mates(0, b)

        @pl.when(k == 1)
        def _():
            side_wait(3, 0)
            side_wait(3, 1)
            mates(1, bx)

        @pl.when(k == 2)
        def _():
            corner_wait(1)
            mates(2, by)

        @pl.when(k == 3)
        def _():
            corner_wait(2)
            corner_wait(3)
            mates(3, both)

        feed(b + (k % 2) * (bx - b) + (k // 2) * (by - b))
        return 0

    lax.fori_loop(0, 4, group_step, 0)

    def turn_copy(r, i):
        to = lax.rem(z + i, 4)
        src = turned.at[r, pl.ds(pl.multiple_of(to * width, width), width)]
        dst = grad_ref.at[:, pl.ds(pl.multiple_of(z * quarter + r * size, size), size)]
        return remote(src, dst, g_send.at[r, i - 1], g_recv.at[r, i - 1], (b, to))

    def turn_own(r):
        src = turned.at[r, pl.ds(pl.multiple_of(z * width, width), width)]
        dst = grad_ref.at[:, pl.ds(pl.multiple_of(z * quarter + r * size, size), size)]
        return pltpu.make_async_copy(src, dst, own_turn.at[r])

    stores = (
        (out_ref, out_hbm), (first_ref, first_hbm), (attn_ref, attn_hbm), (pre_ref, pre_hbm),
        (ffn_ref, ffn_hbm), (hidden_ref, hidden_hbm), (norm_ref, norm_hbm),
    )

    def store(r, n):
        src, dst = stores[n]
        rows = tile_rows(r)
        return pltpu.make_async_copy(src.at[rows], dst.at[rows], out_sem.at[r, n])

    cot_load.wait()

    def row_tile(r, _):
        rows = tile_rows(r)
        n1 = n1_ref[rows, :]
        norm1 = n1 * gain1 + shift1
        n2, scale2 = normed(norm1 + total[rows, :] + down_bias)
        out_ref[rows, :] = (n2 * gain2 + shift2).astype(low)
        cot = cot_ref[rows, :].astype(f32)
        row_sum(1, cot * n2)
        row_sum(2, cot)
        grad2 = norm_back(cot, gain2, n2, scale2)
        grad_low = grad2.astype(low)
        ffn_ref[rows, :] = grad_low
        row_sum(0, grad_low.astype(f32))
        total[rows, :] = grad2

        def backward(c, _):
            lanes = pl.ds(pl.multiple_of(c * span, span), span)
            grad = (slope[rows, lanes] * mul_t(grad_low, weights(c, ff))).astype(low)
            pre_ref[rows, lanes] = grad
            bin_ref[0:1, lanes] += jnp.sum(grad.astype(f32), axis=0, keepdims=True)
            total[rows, :] += mul(grad, weights(c, 0))
            return 0

        lax.fori_loop(0, 4, backward, 0)
        grad1 = total[rows, :]
        row_sum(3, grad1 * n1)
        row_sum(4, grad1)
        first = norm_back(grad1, gain1, n1, scale_ref[rows, 0:1])
        first_ref[rows, :] = first
        attn_low = first.astype(low)
        attn_ref[rows, :] = attn_low
        row_sum(5, attn_low.astype(f32))
        for s in range(4):
            turned[r, pl.ds(s * width, width), :] = mul_t(wo[s], attn_low).astype(low)
        for i in (1, 2, 3):
            turn_copy(r, i).start()
        turn_own(r).start()
        for n in range(len(stores)):
            store(r, n).start()
        return 0

    lax.fori_loop(0, tiles, row_tile, 0)

    def finish(r, _):
        for i in (1, 2, 3):
            source = origins[i]
            ref = grad_ref.at[:, pl.ds(pl.multiple_of(source * quarter + r * size, size), size)]
            remote(ref, ref, g_send.at[r, i - 1], g_recv.at[r, i - 1], (b, source)).wait_recv()
            turn_copy(r, i).wait_send()
        turn_own(r).wait()
        for n in range(len(stores)):
            store(r, n).wait()
        return 0

    lax.fori_loop(0, tiles, finish, 0)

    @pl.when(is_end)
    def _():
        end_copy.wait_send()

    @pl.when(jnp.logical_not(is_end))
    def _():
        remote(
            end_hbm, end_hbm, w_send.at[0], w_recv.at[0], (b, jnp.where(z < 2, 0, 3))
        ).wait_recv()

    for n in range(count):
        corner(n).wait_send()
        for slot, who in enumerate((b, bx, by, both)):
            mate(n, slot, who).wait_send()
    for copy in issued:
        copy.wait_send()


def ffn_middle(mixed_t, packs, tokens, cot, weight_t, vectors, ff, share):
    width, tok_count = mixed_t.shape
    quarter, model = tok_count // 4, tokens.shape[1]
    size = quarter // 3
    rows = packs[0].shape[0]
    shape = jax.ShapeDtypeStruct
    vmem = pl.BlockSpec(memory_space=pltpu.VMEM)
    hbm = pl.BlockSpec(memory_space=pl.ANY)
    dma = pltpu.SemaphoreType.DMA
    kept = [
        ((quarter, model), low),
        ((quarter, model), f32),
        ((quarter, model), low),
        ((quarter, 32 * ff), low),
        ((quarter, 32 * ff), low),
        ((quarter, model), low),
        ((quarter, model), low),
    ]
    return pl.pallas_call(
        partial(middle_kernel, share),
        out_shape=[shape(*x) for x in kept]
        + [
            shape((4, width, quarter), low),
            shape((width, tok_count), low),
            shape((8, model), f32),
            shape((8, 32 * ff), f32),
            shape(weight_t.shape, low),
        ],
        in_specs=[hbm] * 8 + [vmem],
        out_specs=[hbm] * 7 + [vmem, hbm, vmem, vmem, hbm],
        scratch_shapes=[pltpu.VMEM(*x) for x in kept]
        + [
            pltpu.VMEM((quarter, model), low),
            pltpu.VMEM((quarter, model), low),
            pltpu.VMEM((8, 4, rows, model), low),
            pltpu.VMEM((4 * width, model), f32),
            pltpu.VMEM((4, width, model), low),
            pltpu.VMEM((quarter, 32 * ff), f32),
            pltpu.VMEM((quarter, model), f32),
            pltpu.VMEM((quarter, model), f32),
            pltpu.VMEM((quarter, 128), f32),
            pltpu.VMEM((3, 4 * width, size), low),
            dma((3, 3)), dma((3, 3)), dma((4, 2, 4)), dma((4, 2, 4)), dma((4,)), dma((4,)),
            dma((4, 4)), dma((4, 4)), dma((3, 3)), dma((3, 3)),
            dma((7,)), dma((3,)), dma((3, 7)), dma((1,)), dma((1,)),
        ],
        compiler_params=pltpu.CompilerParams(
            collective_id=1, has_side_effects=True, vmem_limit_bytes=63 * 1024 * 1024
        ),
        name="middle",
    )(mixed_t, *packs, tokens, cot, weight_t, vectors)


def settle_kernel(count, pieces, *refs):
    sources, results = refs[:count], refs[count : 2 * count]
    held, came, went = refs[2 * count : 3 * count], refs[3 * count], refs[3 * count + 1]
    moves = []
    for n in range(count):
        rows = held[n].shape[0] // pieces[n]
        for k in range(pieces[n]):
            at = pl.ds(k * rows, rows)
            moves.append((sources[n].at[at], held[n].at[at], results[n].at[at]))
    coming = [
        pltpu.make_async_copy(src, mid, came.at[n]) for n, (src, mid, _) in enumerate(moves)
    ]
    going = [
        pltpu.make_async_copy(mid, dst, went.at[n]) for n, (_, mid, dst) in enumerate(moves)
    ]
    for copy in coming:
        copy.start()
    for arrival, copy in zip(coming, going):
        arrival.wait()
        copy.start()
    for copy in going:
        copy.wait()


def settle(*arrays):
    count = len(arrays)
    pieces = [4 if x.size > 2**18 else 1 for x in arrays]
    hbm = pl.BlockSpec(memory_space=pl.ANY)
    return pl.pallas_call(
        partial(settle_kernel, count, pieces),
        out_shape=[jax.ShapeDtypeStruct(x.shape, x.dtype) for x in arrays],
        in_specs=[hbm] * count,
        out_specs=[hbm] * count,
        scratch_shapes=[pltpu.VMEM(x.shape, x.dtype) for x in arrays]
        + [pltpu.SemaphoreType.DMA((sum(pieces),))] * 2,
        name="settle",
    )(*arrays)


def slice_body(
    tokens,
    qkv_weight,
    qv_bias,
    conv_weight,
    out_weight,
    out_bias,
    norm1_gain,
    norm1_bias,
    ffn_in_weight,
    ffn_in_bias,
    ffn_out_weight,
    ffn_out_bias,
    norm2_gain,
    norm2_bias,
    cotangent,
    seq_lengths,
    segment_ids,
    landmark_bounds,
):
    model = tokens.shape[1]
    width = qkv_weight.shape[2]
    kernel_taps = conv_weight.shape[1]
    slots, marks = landmark_bounds.shape
    z = lax.axis_index("heads")
    b = lax.axis_index("batch")
    weight_t = jnp.transpose(qkv_weight.reshape(model, 3 * width))
    ff_own = ffn_out_weight.shape[0]
    share = width // 8
    bias_row = lax.dynamic_update_slice_in_dim(
        jnp.zeros((4 * ff_own,), low), ffn_in_bias, z * ff_own, 0
    )
    misc_own = jnp.concatenate(
        [
            lax.dynamic_slice_in_dim(out_weight, b * share, share, 0),
            jnp.zeros((32 - share, model), low).at[0, : 4 * ff_own].set(bias_row),
        ],
        axis=0,
    )
    pack = jnp.concatenate([jnp.transpose(ffn_in_weight), ffn_out_weight, misc_own], axis=0)
    packs = [pack] + [
        lax.ppermute(pack, "heads", [(n, (n + i) % 4) for n in range(4)]) for i in (1, 2, 3)
    ]
    forward = mix_forward(
        seq_lengths, tokens, weight_t, qv_bias, conv_weight, slots, marks
    )
    qkv_t, first, last, mixed_t, mark, value, inner, denom, middle, steps, inverse, bound = forward
    vectors = jnp.stack(
        [out_bias, norm1_gain, norm1_bias, ffn_out_bias, norm2_gain, norm2_bias]
    )
    (
        final_low, grad_first, grad_attn_low, hidden_low, grad_pre, norm1_low, grad_ffn_low,
        mixed_all, grad_mix_t, vector_sums, bias_sums, weight_end,
    ) = ffn_middle(mixed_t, packs, tokens, cotangent, weight_t, vectors, ff_own, share)
    saved = (qkv_t, first, last, mark, value, inner, denom, middle, steps, inverse)
    grad_t, grad_bias, grad_conv = mix_backward(
        seq_lengths, grad_mix_t, saved, conv_weight, slots, marks
    )
    (
        input_grad, down_share, up_share, out_share, qkv_share,
        in_bias_share, vector_share, bias_out, conv_out, condition,
    ) = tail(
        seq_lengths, grad_t, weight_t, weight_end, hidden_low, grad_pre, norm1_low, grad_ffn_low,
        grad_attn_low, mixed_all, tokens, grad_first, vector_sums, bias_sums, grad_bias,
        grad_conv, bound, kernel_taps,
    )
    (
        final_low, input_grad, down_share, up_share, out_share, qkv_share,
        in_bias_share, vector_share, bias_out, conv_out, condition,
    ) = settle(
        final_low, input_grad, down_share, up_share, out_share, qkv_share,
        in_bias_share, vector_share, bias_out, conv_out, condition,
    )
    return (
        final_low,
        input_grad,
        jnp.swapaxes(qkv_share, 0, 1),
        bias_out,
        conv_out,
        out_share,
        jnp.transpose(up_share),
        in_bias_share.reshape(ff_own),
        down_share,
        vector_share,
        condition.reshape(()),
    )


def solution(mesh):
    chosen = slice_body if dict(mesh.shape) == {"batch": 8, "heads": 4} else body
    in_specs = (
        P("batch", None),
        P(None, None, "heads"),
        P(),
        P(),
        P("heads", None),
        P(),
        P(),
        P(),
        P(None, ("batch", "heads")),
        P(("batch", "heads")),
        P(("batch", "heads"), None),
        P(),
        P(),
        P(),
        P(("batch", "heads"), None),
        P("batch"),
        P("batch"),
        P("batch", None),
    )
    out_specs = (
        P(("batch", "heads"), None),
        P(("batch", "heads"), None),
        P("batch", None, "heads"),
        P(None, "heads"),
        P("heads", None),
        P("heads", "batch"),
        P(None, ("batch", "heads")),
        P(("batch", "heads")),
        P(("batch", "heads"), None),
        P(None, ("batch", "heads")),
        P(),
    )
    return jax.shard_map(chosen, mesh=mesh, in_specs=in_specs, out_specs=out_specs, check_vma=False)
```
